32 devices in a mesh: data: 1 (over z), seq: 32 (over y, x, core).
Axes of the slice: x: 4, y: 4, z: 1, core: 2. Of those that a mesh axis runs over, the one named last changes fastest.
The devices are a block of a 4x4x8 slice.
Arguments:
- hidden: bfloat16 [3, 12288, 768], P('data', 'seq')
- positions: int32 [3, 12288], P('data', 'seq')
- g_attn: float32 [1, 768], replicated
- g_mlp: float32 [1, 768], replicated
- w_query: bfloat16 [1, 768, 12, 64], replicated
- w_key: bfloat16 [1, 768, 12, 64], replicated
- w_value: bfloat16 [1, 768, 12, 64], replicated
- w_out: bfloat16 [1, 768, 768], replicated
- w_gate: bfloat16 [1, 768, 3072], replicated
- w_up: bfloat16 [1, 768, 3072], replicated
- w_down: bfloat16 [1, 3072, 768], replicated
- d_out: bfloat16 [3, 12288, 768], P('data', 'seq')
Outputs:
- output 1: bfloat16 [3, 12288, 768], P('data', 'seq')
- output 2: float32 [1, 768], P(None, ('data', 'seq'))
- output 3: float32 [1, 768], P(None, ('data', 'seq'))
- output 4: float32 [1, 768, 12, 64], P(None, ('data', 'seq'))
- output 5: float32 [1, 768, 12, 64], P(None, ('data', 'seq'))
- output 6: float32 [1, 768, 12, 64], P(None, ('data', 'seq'))
- output 7: float32 [1, 768, 768], P(None, ('data', 'seq'))
- output 8: float32 [1, 768, 3072], P(None, ('data', 'seq'))
- output 9: float32 [1, 768, 3072], P(None, ('data', 'seq'))
- output 10: float32 [1, 3072, 768], P(None, ('data', 'seq'))
All inputs are finite; a program needn't handle non-finite values.
Results may differ from the reference program's by a relative error of at most 0.02.
Values are sent between devices in bfloat16 or wider.
A program may use at most 768 MiB of HBM per device.

```python
import math
import jax
import jax.numpy as jnp
from jax import lax

BATCH_ROWS = 3
TOK_DEV = 384
SEQ_DEVS = 32
D_MODEL = 768
QUERY_HEADS = 12
KV_HEADS = 12
HEAD_DIM = 64
FF_DIM = 3072
LAYERS = 1
WINDOW = 256
SEQ_LEN = TOK_DEV * SEQ_DEVS
Q_GROUP = QUERY_HEADS // KV_HEADS
NORM_EPS = 1e-5


def normal_weights(rng_key, shape, scale):
    return (jax.random.normal(rng_key, shape, jnp.float32) * scale).astype(jnp.bfloat16)


def setup_inputs(seed: int = 0, part: int = 0) -> dict:
    part_key = jax.random.fold_in(jax.random.key(seed), part)
    key_x, key_gap, key_start, key_dy = jax.random.split(part_key, 4)
    weight_keys = jax.random.split(jax.random.key(seed + 1), 9)
    hidden = jax.random.normal(key_x, (BATCH_ROWS, SEQ_LEN, D_MODEL), jnp.float32).astype(jnp.bfloat16)
    pos_gaps = jax.random.randint(key_gap, (BATCH_ROWS, SEQ_LEN), 1, 3, jnp.int32)
    offsets = jax.random.randint(key_start, (BATCH_ROWS, 1), 0, 1024, jnp.int32)
    positions = (offsets + jnp.cumsum(pos_gaps, axis=1) - 1).astype(jnp.int32)
    d_scale = D_MODEL ** -0.5
    g_attn = 1.0 + 0.25 * jax.random.normal(weight_keys[0], (LAYERS, D_MODEL), jnp.float32)
    g_mlp = 1.0 + 0.25 * jax.random.normal(weight_keys[1], (LAYERS, D_MODEL), jnp.float32)
    w_query = normal_weights(weight_keys[2], (LAYERS, D_MODEL, QUERY_HEADS, HEAD_DIM), 3.0 * d_scale)
    w_key = normal_weights(weight_keys[3], (LAYERS, D_MODEL, KV_HEADS, HEAD_DIM), d_scale)
    w_value = normal_weights(weight_keys[4], (LAYERS, D_MODEL, KV_HEADS, HEAD_DIM), d_scale)
    w_out = normal_weights(weight_keys[5], (LAYERS, QUERY_HEADS * HEAD_DIM, D_MODEL), (QUERY_HEADS * HEAD_DIM) ** -0.5)
    w_gate = normal_weights(weight_keys[6], (LAYERS, D_MODEL, FF_DIM), d_scale)
    w_up = normal_weights(weight_keys[7], (LAYERS, D_MODEL, FF_DIM), d_scale)
    w_down = normal_weights(weight_keys[8], (LAYERS, FF_DIM, D_MODEL), FF_DIM ** -0.5)
    d_out = jax.random.normal(key_dy, (BATCH_ROWS, SEQ_LEN, D_MODEL), jnp.float32).astype(jnp.bfloat16)
    return dict(hidden=hidden, positions=positions, g_attn=g_attn, g_mlp=g_mlp, w_query=w_query, w_key=w_key, w_value=w_value, w_out=w_out, w_gate=w_gate, w_up=w_up, w_down=w_down, d_out=d_out)


def rope_tables(positions):
    half_dim = HEAD_DIM // 2
    inv_freq = 1.0 / (10000.0 ** (jnp.arange(half_dim, dtype=jnp.float32) * (2.0 / HEAD_DIM)))
    angles = positions.astype(jnp.float32)[:, :, None] * inv_freq
    return jnp.cos(angles)[:, :, None, :], jnp.sin(angles)[:, :, None, :]


def rotate(values, cos_t, sin_t):
    half_dim = values.shape[-1] // 2
    first = values[..., :half_dim]
    second = values[..., half_dim:]
    return jnp.concatenate([first * cos_t - second * sin_t, second * cos_t + first * sin_t], axis=-1)


def rms_norm(hidden, gain_vec):
    hidden_f = hidden.astype(jnp.float32)
    inv_rms = lax.rsqrt(jnp.mean(hidden_f * hidden_f, axis=-1, keepdims=True) + NORM_EPS)
    return (hidden_f * inv_rms * gain_vec).astype(jnp.bfloat16)


def window_attention(q_rot, k_ext, v_ext):
    batch_rows, seq_len, kv_heads, q_group, head_dim = q_rot.shape
    qblock = math.gcd(seq_len, 128)
    span_len = qblock + WINDOW - 1
    row_ids = jnp.arange(qblock)[:, None]
    col_ids = jnp.arange(span_len)[None, :]
    band_mask = (col_ids >= row_ids) & (col_ids < row_ids + WINDOW)
    attn_scale = head_dim ** -0.5

    def one_block(blk_idx):
        blk_start = blk_idx * qblock
        q_blk = lax.dynamic_slice_in_dim(q_rot, blk_start, qblock, axis=1).astype(jnp.float32)
        k_blk = lax.dynamic_slice_in_dim(k_ext, blk_start, span_len, axis=1).astype(jnp.float32)
        v_blk = lax.dynamic_slice_in_dim(v_ext, blk_start, span_len, axis=1).astype(jnp.float32)
        scores = jnp.einsum('bqkgd,bckd->bkgqc', q_blk, k_blk) * attn_scale
        keep_mask = band_mask & (blk_start + col_ids >= WINDOW - 1)
        attn_probs = jax.nn.softmax(jnp.where(keep_mask, scores, -1e30), axis=-1).astype(jnp.bfloat16)
        out_blk = jnp.einsum('bkgqc,bckd->bqkgd', attn_probs.astype(jnp.float32), v_blk)
        return out_blk.astype(jnp.bfloat16)

    blocks = lax.map(jax.checkpoint(one_block), jnp.arange(seq_len // qblock))
    return jnp.moveaxis(blocks, 0, 1).reshape(batch_rows, seq_len, kv_heads * q_group * head_dim)


def layer_forward(hidden, layer_w, cos_t, sin_t):
    g_attn, g_mlp, w_query, w_key, w_value, w_out, w_gate, w_up, w_down = layer_w
    flat_tokens = BATCH_ROWS * SEQ_LEN
    normed_a = rms_norm(hidden, g_attn).reshape(flat_tokens, D_MODEL)
    q_proj = jnp.dot(normed_a, w_query.reshape(D_MODEL, QUERY_HEADS * HEAD_DIM), preferred_element_type=jnp.float32)
    k_proj = jnp.dot(normed_a, w_key.reshape(D_MODEL, KV_HEADS * HEAD_DIM), preferred_element_type=jnp.float32)
    v_proj = jnp.dot(normed_a, w_value.reshape(D_MODEL, KV_HEADS * HEAD_DIM), preferred_element_type=jnp.float32)
    q_rot = rotate(q_proj.reshape(BATCH_ROWS, SEQ_LEN, QUERY_HEADS, HEAD_DIM), cos_t, sin_t).astype(jnp.bfloat16)
    k_rot = rotate(k_proj.reshape(BATCH_ROWS, SEQ_LEN, KV_HEADS, HEAD_DIM), cos_t, sin_t).astype(jnp.bfloat16)
    v_val = v_proj.reshape(BATCH_ROWS, SEQ_LEN, KV_HEADS, HEAD_DIM).astype(jnp.bfloat16)
    zero_rows = jnp.zeros((BATCH_ROWS, WINDOW - 1, KV_HEADS, HEAD_DIM), jnp.bfloat16)
    attn_out = window_attention(q_rot.reshape(BATCH_ROWS, SEQ_LEN, KV_HEADS, Q_GROUP, HEAD_DIM), jnp.concatenate([zero_rows, k_rot], axis=1), jnp.concatenate([zero_rows, v_val], axis=1))
    attn_proj = jnp.dot(attn_out.reshape(flat_tokens, QUERY_HEADS * HEAD_DIM), w_out, preferred_element_type=jnp.float32)
    hidden_mid = (hidden.astype(jnp.float32) + attn_proj.reshape(BATCH_ROWS, SEQ_LEN, D_MODEL)).astype(jnp.bfloat16)
    normed_m = rms_norm(hidden_mid, g_mlp).reshape(flat_tokens, D_MODEL)
    gate_pre = jnp.dot(normed_m, w_gate, preferred_element_type=jnp.float32)
    up_proj = jnp.dot(normed_m, w_up, preferred_element_type=jnp.float32)
    act_prod = (jax.nn.silu(gate_pre) * up_proj).astype(jnp.bfloat16)
    down_proj = jnp.dot(act_prod, w_down, preferred_element_type=jnp.float32)
    return (hidden_mid.astype(jnp.float32) + down_proj.reshape(BATCH_ROWS, SEQ_LEN, D_MODEL)).astype(jnp.bfloat16)


def reference(hidden, positions, g_attn, g_mlp, w_query, w_key, w_value, w_out, w_gate, w_up, w_down, d_out):
    cos_t, sin_t = rope_tables(positions)
    weights = (g_attn, g_mlp, w_query, w_key, w_value, w_out, w_gate, w_up, w_down)

    def forward(hidden_in, weight_set):
        def layer_step(carry_in, layer_w):
            return layer_forward(carry_in, layer_w, cos_t, sin_t), None
        final_out, unused = lax.scan(layer_step, hidden_in, weight_set)
        return final_out

    unused_y, pullback = jax.vjp(forward, hidden, weights)
    d_hidden, d_weights = pullback(d_out)
    return (d_hidden, d_weights[0].astype(jnp.float32), d_weights[1].astype(jnp.float32), d_weights[2].astype(jnp.float32), d_weights[3].astype(jnp.float32), d_weights[4].astype(jnp.float32), d_weights[5].astype(jnp.float32), d_weights[6].astype(jnp.float32), d_weights[7].astype(jnp.float32), d_weights[8].astype(jnp.float32))
```

```python
import functools, math
import numpy as np
import jax, jax.numpy as jnp
from jax import lax
from jax.experimental import pallas as pl
from jax.experimental.pallas import tpu as pltpu
from jax.sharding import PartitionSpec as P

WINDOW = 256
NORM_EPS = 1e-5
QB = 128
BF, F32 = jnp.bfloat16, jnp.float32
NN, NT, TN = ((1,), (0,)), ((1,), (1,)), ((0,), (0,))
MESH = pl.DeviceIdType.MESH
NEG = -1e30
VMEM_LIMIT = 67043328


def dot(a, b, dims=NN):
    return lax.dot_general(a, b, (dims, ((), ())), preferred_element_type=F32)


def cdiv_loop(n, body):
    lax.fori_loop(0, n, lambda i, c: (body(i), c)[1], 0)


def rope(blk, cos_b, sin_b, sign, head_dim):
    half = head_dim // 2
    parts = []
    for h in range(blk.shape[0] // head_dim):
        first = blk[h * head_dim:h * head_dim + half]
        second = blk[h * head_dim + half:(h + 1) * head_dim]
        if sign > 0:
            parts += [first * cos_b - second * sin_b, second * cos_b + first * sin_b]
        else:
            parts += [first * cos_b + second * sin_b, second * cos_b - first * sin_b]
    return jnp.concatenate(parts, axis=0)


def normed(x, gain):
    xf = x.astype(F32)
    inv = lax.rsqrt(jnp.mean(xf * xf, axis=-1, keepdims=True) + NORM_EPS)
    return (xf * inv * gain).astype(BF)


def stack_pair(pair_t):
    half = pair_t.shape[0] // 2
    zero = jnp.zeros((half, pair_t.shape[1]), pair_t.dtype)
    return jnp.concatenate(
        [jnp.concatenate([pair_t[:half], zero], axis=0), jnp.concatenate([zero, pair_t[half:]], axis=0)], axis=1)


def unstack_pair(both):
    half, cols = both.shape[0] // 2, both.shape[1] // 2
    return jnp.concatenate([both[:half, :cols], both[half:, cols:]], axis=0)


def probs(k_blk, q_stack, upper, bias0, bias1):
    scores = dot(k_blk, q_stack)
    s02 = jnp.where(upper, scores[:QB] + bias0, scores[2 * QB:])
    s1 = scores[QB:2 * QB] + bias1
    top = jnp.max(jnp.maximum(s02, s1), axis=0, keepdims=True)
    e02, e1 = jnp.exp(s02 - top), jnp.exp(s1 - top)
    inv = 1.0 / jnp.sum(e02 + e1, axis=0, keepdims=True)
    return e02 * inv, e1 * inv


def banded(p02, p1, upper):
    return jnp.concatenate(
        [jnp.where(upper, p02, 0.0).astype(BF), p1.astype(BF), jnp.where(upper, 0.0, p02).astype(BF)], axis=0)


def upper_mask():
    key_ids = lax.broadcasted_iota(jnp.int32, (QB, 2 * QB), 0)
    query_ids = lax.broadcasted_iota(jnp.int32, (QB, 2 * QB), 1) % QB
    return key_ids > query_ids


def start_bias(first, blk):
    bias = jnp.where(first, NEG, 0.0).astype(F32)
    return (bias if blk < 2 else 0.0), (bias if blk < 1 else 0.0)


def fwd_kernel(n, head_dim, x_h, pos, invf, ga, gm, wq_h, wk_h, wv_h, wo_h,
               q_h, kt_h, k_h, v_h, hat_h, ot_h, xm_h, hm_h, hmt_h, cos_t, sin_t,
               xv, halo, pos_halo, wq, wk, wv, wo, q, kt, k, v, vt, hat, ot, xm, hm, hmt, hb, acc, cos_h, sin_h,
               ld, st, snd, rcv):
    rows, toks, width = xv.shape
    ext = toks + WINDOW
    total, n_halo = rows * toks, rows * WINDOW
    n_pairs = wq.shape[0] // (2 * head_dim)
    pw = 2 * head_dim
    me = lax.axis_index("seq")
    right, left = lax.rem(me + 1, n), lax.rem(me + n - 1, n)
    loads = [pltpu.make_async_copy(s, d, ld.at[i]) for i, (s, d) in enumerate(((x_h, xv), (wq_h, wq), (wk_h, wk), (wv_h, wv), (wo_h, wo)))]
    for c in loads:
        c.start()
    barrier = pltpu.get_barrier_semaphore()
    for other in (left, right):
        pl.semaphore_signal(barrier, inc=1, device_id={"seq": other}, device_id_type=MESH)
    pl.semaphore_wait(barrier, 2)
    sends = [pltpu.make_async_remote_copy(src_ref=s, dst_ref=d, send_sem=snd.at[i], recv_sem=rcv.at[i], device_id={"seq": right}, device_id_type=MESH)
             for i, (s, d) in enumerate(((x_h.at[:, toks - WINDOW:, :], halo), (pos, pos_halo)))]
    for c in sends:
        c.start()

    def store(i, s, d):
        c = pltpu.make_async_copy(s, d, st.at[i])
        c.start()
        stores.append(c)

    stores = []
    for b in range(rows):
        ang = invf[...] * pos[b:b + 1, :].astype(F32)
        cos_t[:, b * toks:(b + 1) * toks] = jnp.cos(ang)
        sin_t[:, b * toks:(b + 1) * toks] = jnp.sin(ang)
    loads[0].wait()
    tb = toks // QB

    def norm_blk(i):
        r = pl.multiple_of(i * QB, QB)
        h = normed(xv[i // tb, pl.ds(pl.multiple_of((i % tb) * QB, QB), QB), :], ga[...])
        hb[pl.ds(r, QB), :] = h
        hat[:, pl.ds(r, QB)] = h.T

    cdiv_loop(total // QB, norm_blk)
    store(0, hat, hat_h)

    def rope_q(p):
        r = pl.multiple_of(p * pw, pw)
        q[pl.ds(r, pw), :] = (rope(acc[pl.ds(r, pw), :], cos_t[...], sin_t[...], 1, head_dim) * (head_dim ** -0.5)).astype(BF)

    def put_k(p):
        r = pl.multiple_of(p * pw, pw)
        for b in range(rows):
            blk = rope(acc[pl.ds(r, pw), b * toks:(b + 1) * toks], cos_t[:, b * toks:(b + 1) * toks], sin_t[:, b * toks:(b + 1) * toks], 1, head_dim).astype(BF)
            kt[pl.ds(r, pw), b * ext + WINDOW:(b + 1) * ext] = blk
            k[b * ext + WINDOW:(b + 1) * ext, pl.ds(r, pw)] = blk.T

    def put_v(p):
        r = pl.multiple_of(p * pw, pw)
        for b in range(rows):
            blk = acc[pl.ds(r, pw), b * toks:(b + 1) * toks].astype(BF)
            vt[pl.ds(r, pw), b * ext + WINDOW:(b + 1) * ext] = blk
            v[b * ext + WINDOW:(b + 1) * ext, pl.ds(r, pw)] = blk.T

    for i, (w, put) in enumerate(((wq, rope_q), (wk, put_k), (wv, put_v))):
        loads[i + 1].wait()
        acc[...] = dot(w[...], hb[...], NT)
        cdiv_loop(n_pairs, put)
    store(1, q, q_h)

    for c in sends:
        c.wait()
    for b in range(rows):
        ang = invf[...] * pos_halo[b:b + 1, toks - WINDOW:].astype(F32)
        cos_h[:, b * WINDOW:(b + 1) * WINDOW] = jnp.cos(ang)
        sin_h[:, b * WINDOW:(b + 1) * WINDOW] = jnp.sin(ang)
    wb = WINDOW // QB

    def norm_halo(i):
        h = normed(halo[i // wb, pl.ds(pl.multiple_of((i % wb) * QB, QB), QB), :], ga[...])
        hb[pl.ds(pl.multiple_of(i * QB, QB), QB), :] = h

    cdiv_loop(n_halo // QB, norm_halo)

    def halo_put(is_k, p):
        r = pl.multiple_of(p * pw, pw)
        for b in range(rows):
            blk = acc[pl.ds(r, pw), b * WINDOW:(b + 1) * WINDOW]
            if is_k:
                blk = rope(blk, cos_h[:, b * WINDOW:(b + 1) * WINDOW], sin_h[:, b * WINDOW:(b + 1) * WINDOW], 1, head_dim)
            blk = blk.astype(BF)
            dst_t, dst = (kt, k) if is_k else (vt, v)
            dst_t[pl.ds(r, pw), b * ext:b * ext + WINDOW] = blk
            dst[b * ext:b * ext + WINDOW, pl.ds(r, pw)] = blk.T

    for w, is_k in ((wk, True), (wv, False)):
        acc[:, :n_halo] = dot(w[...], hb[:n_halo, :], NT)
        cdiv_loop(n_pairs, functools.partial(halo_put, is_k))
    store(2, kt, kt_h)
    store(3, k, k_h)
    store(4, v, v_h)

    upper = upper_mask()
    first = me == 0

    def attend(it):
        p, b = it // rows, it % rows
        r = pl.multiple_of(p * pw, pw)
        for blk in range(tb):
            cols = pl.ds(pl.multiple_of(b * toks + blk * QB, QB), QB)
            keys = pl.ds(pl.multiple_of(b * ext + blk * QB, QB), 3 * QB)
            bias0, bias1 = start_bias(first, blk)
            p02, p1 = probs(k[keys, pl.ds(r, pw)], stack_pair(q[pl.ds(r, pw), cols]), upper, bias0, bias1)
            out = dot(vt[pl.ds(r, pw), keys], banded(p02, p1, upper))
            ot[pl.ds(r, pw), cols] = unstack_pair(out).astype(BF)

    cdiv_loop(n_pairs * rows, attend)
    store(5, ot, ot_h)
    loads[4].wait()

    def project(b):
        cols = pl.ds(pl.multiple_of(b * toks, QB), toks)
        mid = (xv[b].astype(F32) + dot(ot[:, cols], wo[...], TN)).astype(BF)
        xm[cols, :] = mid
        h = normed(mid, gm[...])
        hm[cols, :] = h
        hmt[:, cols] = h.T

    cdiv_loop(rows, project)
    store(6, xm, xm_h)
    store(7, hm, hm_h)
    store(8, hmt, hmt_h)
    for c in stores:
        c.wait()


def any_spec(k):
    return [pl.BlockSpec(memory_space=pl.ANY)] * k


def vmem_spec(k):
    return [pl.BlockSpec(memory_space=pltpu.VMEM)] * k


def run_fwd(n, x, pos, invf, ga, gm, wq, wk, wv, wo, head_dim):
    rows, toks, width = x.shape
    hd = wq.shape[0]
    ext, total, n_halo = toks + WINDOW, rows * toks, rows * WINDOW
    half = head_dim // 2
    sds = lambda *s: jax.ShapeDtypeStruct(s, BF)
    outs = [sds(hd, total), sds(hd, rows * ext), sds(rows * ext, hd), sds(rows * ext, hd), sds(width, total), sds(hd, total), sds(total, width), sds(total, width), sds(width, total)]
    outs += [jax.ShapeDtypeStruct((half, total), F32)] * 2
    vm = lambda *s: pltpu.VMEM(s, BF)
    vf = lambda *s: pltpu.VMEM(s, F32)
    scratch = [vm(rows, toks, width), vm(rows, WINDOW, width), pltpu.VMEM((rows, toks), jnp.int32), vm(hd, width), vm(hd, width), vm(hd, width), vm(hd, width),
               vm(hd, total), vm(hd, rows * ext), vm(rows * ext, hd), vm(rows * ext, hd), vm(hd, rows * ext), vm(width, total), vm(hd, total), vm(total, width), vm(total, width), vm(width, total), vm(total, width),
               vf(hd, total), vf(half, n_halo), vf(half, n_halo),
               pltpu.SemaphoreType.DMA((5,)), pltpu.SemaphoreType.DMA((9,)), pltpu.SemaphoreType.DMA((2,)), pltpu.SemaphoreType.DMA((2,))]
    return pl.pallas_call(
        functools.partial(fwd_kernel, n, head_dim), out_shape=outs,
        in_specs=any_spec(1) + vmem_spec(4) + any_spec(4), out_specs=any_spec(9) + vmem_spec(2), scratch_shapes=scratch,
        compiler_params=pltpu.CompilerParams(collective_id=0, has_side_effects=True, vmem_limit_bytes=VMEM_LIMIT),
        name="forward")(x, pos, invf, ga, gm, wq, wk, wv, wo)


LAG = 2
SLOTS = 2 * LAG
RING = 5
CB = 256


def at(ref, *idx):
    return ref.at[idx]


class Torus:
    def __init__(self, n, pairs, odd_pair, parts, recv0, recv1, recv2, recv3, recv4, acc, acc2, fin, snd, rcv):
        self.side = math.isqrt(n // 2)
        assert self.side == 4
        me = lax.axis_index("seq")
        self.core = me % 2
        chip = me // 2
        self.x, self.y = chip % 4, chip // 4
        self.pairs, self.odd_pair = pairs, odd_pair
        self.parts, self.recv0, self.recv1, self.recv2, self.recv3, self.recv4 = parts, recv0, recv1, recv2, recv3, recv4
        self.acc, self.acc2, self.fin, self.snd, self.rcv = acc, acc2, fin, snd, rcv

    def device(self, dy, dx, flip=False):
        core = 1 - self.core if flip else self.core
        return (((self.y + dy) % 4) * 4 + (self.x + dx) % 4) * 2 + core

    def peers(self):
        return [self.device(0, 0, True), self.device(0, 1), self.device(0, 3), self.device(1, 0), self.device(3, 0)]

    def hop(self, kind, axis, step):
        return self.device(0, step) if (axis == kind) else self.device(step, 0)

    def copy(self, lane, kind, slot, src, dst, target):
        return pltpu.make_async_remote_copy(
            src_ref=src, dst_ref=dst, send_sem=self.snd.at[lane, kind, slot], recv_sem=self.rcv.at[lane, kind, slot],
            device_id={"seq": target}, device_id_type=MESH)

    def copies(self, stage, kind, pair, slot):
        held = pair % SLOTS
        if stage == 0:
            src = self.parts.at[pair % RING, kind, :, 1 - self.core]
            return [self.copy(0, kind, slot, src, self.recv0.at[kind, slot], self.device(0, 0, True))]
        axis = 0 if stage < 3 else 1
        plus, minus = self.hop(kind, axis, 1), self.hop(kind, axis, 3)
        if stage == 1:
            ends = [(self.acc.at[kind, held, 2, pl.ds(0, 2)], self.recv1), (self.acc.at[kind, held, 2, pl.ds(2, 2)], self.recv1)]
        elif stage == 2:
            ends = [(self.acc.at[kind, held, 1], self.recv2), (self.acc.at[kind, held, 3], self.recv2)]
        elif stage == 3:
            half = CB // 2
            ends = [(self.acc2.at[kind, held, 2, :, pl.ds(0, half)], self.recv3), (self.acc2.at[kind, held, 2, :, pl.ds(half, half)], self.recv3)]
        else:
            ends = [(self.acc2.at[kind, held, 1], self.recv4), (self.acc2.at[kind, held, 3], self.recv4)]
        lane = 2 * stage - 1
        return [self.copy(lane + i, kind, slot, src, buf.at[kind, slot, i], (plus, minus)[i]) for i, (src, buf) in enumerate(ends)]

    def add(self, stage, kind, pair, slot):
        held = pair % SLOTS
        acc, acc2 = self.acc, self.acc2
        if stage == 1:
            def row(r1):
                for r2 in range(4):
                    ry, rx = (r2, r1) if kind == 0 else (r1, r2)
                    chip = ((self.y + ry) % 4) * 4 + (self.x + rx) % 4
                    acc[kind, held, r1, r2] = self.parts[pair % RING, kind, chip, self.core] + self.recv0[kind, slot, chip]
            cdiv_loop(4, row)
        elif stage == 2:
            acc[kind, held, 1, 0:2] += self.recv1[kind, slot, 0]
            acc[kind, held, 3, 2:4] += self.recv1[kind, slot, 1]
        elif stage == 3:
            acc2[kind, held] = acc[kind, held, 0] + (self.recv2[kind, slot, 0] + self.recv2[kind, slot, 1])
        elif stage == 4:
            half = CB // 2
            acc2[kind, held, 1, :, 0:half] += self.recv3[kind, slot, 0]
            acc2[kind, held, 3, :, half:] += self.recv3[kind, slot, 1]
        else:
            self.fin[2 * pair + kind] = acc2[kind, held, 0] + (self.recv4[kind, slot, 0] + self.recv4[kind, slot, 1])

    def count(self, kind):
        return self.pairs - (1 if kind == 1 and self.odd_pair else 0)

    def when(self, pair, kind, fn):
        if isinstance(pair, int):
            if 0 <= pair < self.count(kind):
                fn()
        else:
            pl.when((pair >= 0) & (pair < self.count(kind)))(fn)

    def tick(self, t):
        for stage in range(5, 0, -1):
            pair = t - LAG * stage
            for kind in (0, 1):
                def take(stage=stage, pair=pair, kind=kind):
                    slot = (t - LAG) % SLOTS
                    for c in self.copies(stage - 1, kind, pair, slot):
                        c.wait()
                    self.add(stage, kind, pair, slot)
                self.when(pair, kind, take)
        for stage in range(4, -1, -1):
            pair = t - LAG * stage
            for kind in (0, 1):
                def give(stage=stage, pair=pair, kind=kind):
                    for c in self.copies(stage, kind, pair, t % SLOTS):
                        c.start()
                self.when(pair, kind, give)


def norm_back(x, gain, grad, res):
    xf = x.astype(F32)
    inv = lax.rsqrt(jnp.mean(xf * xf, axis=-1, keepdims=True) + NORM_EPS)
    unit = xf * inv
    gu = grad * gain
    out = inv * (gu - unit * jnp.mean(gu * unit, axis=-1, keepdims=True)) + res.astype(F32)
    gu = grad * unit
    return out.astype(BF), jnp.sum(gu.reshape(gu.shape[0] // 8, 8, gu.shape[1]), axis=0)


def bwd_kernel(n, head_dim, dims, ga, gm, x_h, dout_h, q_h, kt_h, k_h, v_h, hat_h, ot_h, xm_h, hm_h, hmt_h, cos_i, sin_i,
               wq_h, wk_h, wv_h, wo_h, wg_h, wu_h, wd_h,
               dx_h, dga_o, dgm_o, dq_o, dk_o, dv_o, do_o, dg_o, du_o, dd_o,
               parts, recv0, recv1, recv2, recv3, recv4, acc, acc2, fin, snd, rcv,
               hk_recv, hv_recv, hsnd, hrcv, ld, xbuf, mbuf, gnm, gmid, ot, hat, wo, dgain):
    rows, toks, width, hd, ff = dims
    ext, total = toks + WINDOW, rows * toks
    pw = 2 * head_dim
    n_pairs = hd // pw
    nb, nc, sub = ff // CB, width // CB, ff // width
    rpd = width // n
    n_mlp, n_down = nb, nc * sub // 2
    per, half_sub = CB // pw, sub // 2
    n_tail = 4 * nc + 1
    pairs = n_mlp + n_down + (n_tail + 1) // 2
    base = n_mlp + n_down
    comm = Torus(n, pairs, n_tail % 2 == 1, parts, recv0, recv1, recv2, recv3, recv4, acc, acc2, fin, snd, rcv)
    me = lax.axis_index("seq")
    right, left = lax.rem(me + 1, n), lax.rem(me + n - 1, n)

    def load(i, s, d):
        c = pltpu.make_async_copy(s, d, ld.at[i])
        c.start()
        return c

    ld_x, ld_m, ld_ot, ld_hat, ld_wo = load(0, dout_h, xbuf), load(1, xm_h, mbuf), load(2, ot_h, ot), load(3, hat_h, hat), load(4, wo_h, wo)
    barrier = pltpu.get_barrier_semaphore()
    peers = comm.peers() + [left, right]
    for other in peers:
        pl.semaphore_signal(barrier, inc=1, device_id={"seq": other}, device_id_type=MESH)
    pl.semaphore_wait(barrier, len(peers))

    def put(idx, value):
        parts[(base + idx // 2) % RING, idx % 2] = value.reshape(n // 2, 2, rpd, CB)

    def mlp(hm, hmt, actt, wgu, wd, dgu, wld):
        def weights(j, slot):
            c = pl.multiple_of(j * CB, CB)
            return [pltpu.make_async_copy(wg_h.at[:, pl.ds(c, CB)], wgu.at[slot, :, pl.ds(0, CB)], wld.at[slot, 0]),
                    pltpu.make_async_copy(wu_h.at[:, pl.ds(c, CB)], wgu.at[slot, :, pl.ds(CB, CB)], wld.at[slot, 1]),
                    pltpu.make_async_copy(wd_h.at[pl.ds(c, CB), :], wd.at[slot], wld.at[slot, 2])]

        for c in weights(0, 0):
            c.start()
        ld_hm, ld_hmt = load(5, hm_h, hm), load(6, hmt_h, hmt)
        gnm[...] = jnp.zeros_like(gnm)
        ld_hm.wait()
        ld_x.wait()
        ld_hmt.wait()

        def block(j):
            slot = j % 2
            for c in weights(j, slot):
                c.wait()

            @pl.when(j + 1 < nb)
            def _():
                for c in weights(j + 1, 1 - slot):
                    c.start()

            c0 = pl.multiple_of(j * CB, CB)
            for b in range(rows):
                r = slice(b * toks, (b + 1) * toks)
                gu = dot(hm[r, :], wgu[slot])
                gact = dot(xbuf[r, :], wd[slot], NT).astype(BF).astype(F32)
                gate, up = gu[:, :CB], gu[:, CB:]
                sig = 1.0 / (1.0 + jnp.exp(-gate))
                swish = gate * sig
                actt[pl.ds(c0, CB), r] = (swish * up).astype(BF).T
                dgu[r, :CB] = (gact * up * (sig + swish * (1.0 - sig))).astype(BF)
                dgu[r, CB:] = (gact * swish).astype(BF)
            both = dot(hmt[...], dgu[...])
            parts[j % RING, 0] = both[:, :CB].reshape(n // 2, 2, rpd, CB)
            parts[j % RING, 1] = both[:, CB:].reshape(n // 2, 2, rpd, CB)
            for b in range(rows):
                r = slice(b * toks, (b + 1) * toks)
                gnm[r, :] += dot(dgu[r, :], wgu[slot], NT)
            comm.tick(j)

        cdiv_loop(nb, block)

        def down(c):
            share = n // 2 // sub
            c0 = pl.multiple_of(c * CB, CB)
            for m in range(sub):
                res = dot(actt[m * width:(m + 1) * width, :], xbuf[:, pl.ds(c0, CB)]).reshape(share, 2, sub, rpd, CB)
                for i in range(sub):
                    pair = n_mlp + c * half_sub + i // 2
                    parts[pair % RING, i % 2, m * share:(m + 1) * share] = res[:, :, i]

        ld_m.wait()
        dgain[...] = jnp.zeros_like(dgain)

        def mid(i):
            r = pl.ds(pl.multiple_of(i * QB, QB), QB)
            out, dg = norm_back(mbuf[r, :], gm[...], gnm[r, :], xbuf[r, :])
            gmid[r, :] = out
            dgain[8:16, :] += dg

        def column(c):
            down(c)
            comm.tick(n_mlp + c * half_sub)

            @pl.when(c == 0)
            def _():
                cdiv_loop(total // QB, mid)

            @pl.when(c < nc - 1)
            def _():
                for e in range(1, half_sub):
                    comm.tick(n_mlp + c * half_sub + e)

        cdiv_loop(nc, column)

    vm = lambda *s: pltpu.VMEM(s, BF)
    pl.run_scoped(mlp, vm(total, width), vm(width, total), vm(ff, total), vm(2, width, 2 * CB), vm(2, CB, width), vm(total, 2 * CB),
                  pltpu.SemaphoreType.DMA((2, 3)))

    def attention(q, kt, k, v, dot_, dqt, dkt, dk, dv, hk, hv, wq, wk, wv):
        lds = [load(5 + i, s, d) for i, (s, d) in enumerate(((q_h, q), (kt_h, kt), (k_h, k), (v_h, v)))]
        ldw = [load(9 + i, s, d) for i, (s, d) in enumerate(((wq_h, wq), (wk_h, wk), (wv_h, wv)))]
        ld_x2 = load(0, x_h, xbuf)
        ld_ot.wait()
        ld_wo.wait()
        dot_[...] = dot(wo[...], gmid[...], NT).astype(BF)
        for e in range(1, half_sub):
            comm.tick(base - half_sub + e)

        def out_grad(g):
            put(g, dot(ot[...], gmid[:, pl.ds(pl.multiple_of(g * CB, CB), CB)]))

        cdiv_loop(nc, out_grad)
        for c in lds:
            c.wait()
        ld_hat.wait()
        upper = upper_mask()
        first = me == 0
        tb = toks // QB

        def attend(p, b):
            r = pl.multiple_of(p * pw, pw)
            ks, vs = [], []
            for blk in range(tb):
                cols = pl.ds(pl.multiple_of(b * toks + blk * QB, QB), QB)
                keys = pl.ds(pl.multiple_of(b * ext + blk * QB, QB), 3 * QB)
                bias0, bias1 = start_bias(first, blk)
                q_stack = stack_pair(q[pl.ds(r, pw), cols])
                do_stack = stack_pair(dot_[pl.ds(r, pw), cols])
                p02, p1 = probs(k[keys, pl.ds(r, pw)], q_stack, upper, bias0, bias1)
                dp = dot(v[keys, pl.ds(r, pw)], do_stack)
                dp02, dp1 = jnp.where(upper, dp[:QB], dp[2 * QB:]), dp[QB:2 * QB]
                mean = jnp.sum(p02 * dp02 + p1 * dp1, axis=0, keepdims=True)
                ds = banded(p02 * (dp02 - mean), p1 * (dp1 - mean), upper)
                vs.append(dot(banded(p02, p1, upper), do_stack, NT))
                ks.append(dot(ds, q_stack, NT))
                dq = unstack_pair(dot(kt[pl.ds(r, pw), keys], ds)) * (head_dim ** -0.5)
                dqt[pl.ds(r, pw), cols] = rope(dq, cos_i[:, cols], sin_i[:, cols], -1, head_dim).astype(BF)
            for parts_, own, halo in ((ks, dk, hk), (vs, dv, hv)):
                for j in range(tb + 2):
                    val = sum(parts_[i][(j - i) * QB:(j - i + 1) * QB] for i in range(tb) if 0 <= j - i < 3).astype(BF)
                    if j < 2:
                        halo[p, b, j * QB:(j + 1) * QB, :] = val
                    else:
                        own[pl.ds(pl.multiple_of(b * toks + (j - 2) * QB, QB), QB), pl.ds(r, pw)] = val

        def halo_copies(p):
            return [pltpu.make_async_remote_copy(src_ref=s.at[p], dst_ref=d.at[p], send_sem=hsnd.at[i, p], recv_sem=hrcv.at[i, p],
                                                 device_id={"seq": left}, device_id_type=MESH)
                    for i, (s, d) in enumerate(((hk, hk_recv), (hv, hv_recv)))]

        def finish(p):
            r = pl.multiple_of(p * pw, pw)
            for c in halo_copies(p):
                c.wait()
            for b in range(rows):
                for blk in range(tb):
                    cols = slice(b * toks + blk * QB, b * toks + (blk + 1) * QB)
                    gk = dk[cols, pl.ds(r, pw)].astype(F32)
                    off = blk * QB - (toks - WINDOW)
                    if off >= 0:
                        gk = gk + hk_recv[p, b, off:off + QB, :].astype(F32)
                        gv = dv[cols, pl.ds(r, pw)].astype(F32) + hv_recv[p, b, off:off + QB, :].astype(F32)
                        dv[cols, pl.ds(r, pw)] = gv.astype(BF)
                    dkt[pl.ds(r, pw), cols] = rope(gk.T, cos_i[:, cols], sin_i[:, cols], -1, head_dim).astype(BF)

        def step(p):
            @pl.when(p < n_pairs)
            def _():
                cdiv_loop(rows, functools.partial(attend, p))
                for c in halo_copies(p):
                    c.start()

            g = p // per

            @pl.when(p % per == per - 1)
            def _():
                put(nc + 3 * g, dot(hat[...], dqt[pl.ds(pl.multiple_of(g * CB, CB), CB), :], NT))

            @pl.when((p % per == 0) & (p > 0))
            def _():
                cdiv_loop(per, lambda i: finish((g - 1) * per + i))
                cols = pl.ds(pl.multiple_of((g - 1) * CB, CB), CB)
                put(nc + 3 * g - 2, dot(hat[...], dkt[cols, :], NT))
                put(nc + 3 * g - 1, dot(hat[...], dv[:, cols]))

            chunks = nc + 3 * (p // per) + (p % per) // (per - 1)

            @pl.when(chunks // 2 > before(p) // 2)
            def _():
                comm.tick(base + chunks // 2 - 1)

        def before(p):
            return jnp.where(p == 0, nc // 2 * 2 - 2, nc + 3 * ((p - 1) // per) + ((p - 1) % per) // (per - 1))

        cdiv_loop(n_pairs + 1, step)
        for c in ldw:
            c.wait()
        ld_x2.wait()

        def into(b):
            r = pl.ds(pl.multiple_of(b * toks, QB), toks)
            gnm[r, :] = dot(dqt[:, r], wq[...], TN) + dot(dkt[:, r], wk[...], TN) + dot(dv[r, :], wv[...])

        def final(i):
            r = pl.ds(pl.multiple_of(i * QB, QB), QB)
            out, dg = norm_back(xbuf[r, :], ga[...], gnm[r, :], gmid[r, :])
            mbuf[r, :] = out
            dgain[0:8, :] += dg

        cdiv_loop(rows, into)
        cdiv_loop(total // QB, final)

    pl.run_scoped(attention, vm(hd, total), vm(hd, rows * ext), vm(rows * ext, hd), vm(rows * ext, hd), vm(hd, total), vm(hd, total), vm(hd, total),
                  vm(total, hd), vm(total, hd), vm(n_pairs, rows, WINDOW, pw), vm(n_pairs, rows, WINDOW, pw), vm(hd, width), vm(hd, width), vm(hd, width))
    out_copy = load(1, mbuf, dx_h)
    wide = jnp.concatenate([dgain[...], jnp.zeros((CB - dgain.shape[0], width), F32)], axis=0)
    put(n_tail - 1, wide.T)
    lax.fori_loop(pairs - 1, pairs + 5 * LAG, lambda t, c: (comm.tick(t), c)[1], 0)

    for j in range(nb):
        dg_o[:, j * CB:(j + 1) * CB] = fin[2 * j]
        du_o[:, j * CB:(j + 1) * CB] = fin[2 * j + 1]
    for c in range(nc):
        cols = slice(c * CB, (c + 1) * CB)
        for i in range(sub):
            dd_o[i * rpd:(i + 1) * rpd, cols] = fin[2 * n_mlp + c * sub + i]
    for g in range(nc):
        do_o[:, g * CB:(g + 1) * CB] = fin[2 * base + g]
        for i, ref in enumerate((dq_o, dk_o, dv_o)):
            val = fin[2 * base + nc + 3 * g + i]
            for h in range(CB // head_dim):
                ref[g * (CB // head_dim) + h] = val[:, h * head_dim:(h + 1) * head_dim]
    sums = fin[2 * base + n_tail - 1][:, :128].T
    dga_o[...] = jnp.sum(sums[0:8], axis=0, keepdims=True)
    dgm_o[...] = jnp.sum(sums[8:16], axis=0, keepdims=True)
    out_copy.wait()


def run_bwd(n, head_dim, ga, gm, x, dout, q, kt, k, v, hat, ot, xm, hm, hmt, cos_t, sin_t, wq, wk, wv, wo, wg, wu, wd, rows):
    total, width = x.shape
    hd, ff = wq.shape[0], wg.shape[1]
    toks = total // rows
    rpd, heads = width // n, hd // head_dim
    nb, nc, sub = ff // CB, width // CB, ff // width
    pairs = nb + nc * sub // 2 + (4 * nc + 2) // 2
    n_pairs = hd // (2 * head_dim)
    f = lambda *s: jax.ShapeDtypeStruct(s, F32)
    outs = [jax.ShapeDtypeStruct((total, width), BF), f(1, rpd), f(1, rpd)] + [f(heads, rpd, head_dim)] * 3 + [f(rpd, width), f(rpd, ff), f(rpd, ff), f(ff // n, width)]
    vm = lambda *s: pltpu.VMEM(s, BF)
    vf = lambda *s: pltpu.VMEM(s, F32)
    dma = lambda *s: pltpu.SemaphoreType.DMA(s)
    scratch = [vf(RING, 2, n // 2, 2, rpd, CB), vf(2, SLOTS, n // 2, rpd, CB), vf(2, SLOTS, 2, 2, rpd, CB), vf(2, SLOTS, 2, 4, rpd, CB),
               vf(2, SLOTS, 2, rpd, CB // 2), vf(2, SLOTS, 2, rpd, CB), vf(2, SLOTS, 4, 4, rpd, CB), vf(2, SLOTS, 4, rpd, CB), vf(2 * pairs, rpd, CB),
               dma(9, 2, SLOTS), dma(9, 2, SLOTS),
               vm(n_pairs, rows, WINDOW, 2 * head_dim), vm(n_pairs, rows, WINDOW, 2 * head_dim), dma(2, n_pairs), dma(2, n_pairs), dma(12),
               vm(total, width), vm(total, width), vf(total, width), vm(total, width), vm(hd, total), vm(width, total), vm(hd, width), vf(16, width)]
    return pl.pallas_call(
        functools.partial(bwd_kernel, n, head_dim, (rows, toks, width, hd, ff)), out_shape=outs,
        in_specs=vmem_spec(2) + any_spec(11) + vmem_spec(2) + any_spec(7), out_specs=any_spec(1) + vmem_spec(9), scratch_shapes=scratch,
        compiler_params=pltpu.CompilerParams(collective_id=1, has_side_effects=True, vmem_limit_bytes=VMEM_LIMIT),
        name="backward")(ga, gm, x, dout, q, kt, k, v, hat, ot, xm, hm, hmt, cos_t, sin_t, wq, wk, wv, wo, wg, wu, wd)


def solution(mesh):
    n = mesh.shape["seq"]

    def device_step(hidden, positions, g_attn, g_mlp, w_query, w_key, w_value, w_out, w_gate, w_up, w_down, d_out):
        rows, toks, width = hidden.shape
        layers, _, heads, head_dim = w_query.shape
        hd = heads * head_dim
        half = head_dim // 2
        inv_freq = 1.0 / (10000.0 ** (jnp.arange(half, dtype=F32) * (2.0 / head_dim)))
        turn = lambda w: w[0].transpose(1, 2, 0).reshape(hd, width)
        wq, wk, wv = turn(w_query), turn(w_key), turn(w_value)
        fwd = run_fwd(n, hidden, positions, inv_freq[:, None], g_attn, g_mlp, wq, wk, wv, w_out[0], head_dim)
        out = run_bwd(n, head_dim, g_attn, g_mlp, hidden.reshape(rows * toks, width), d_out.reshape(rows * toks, width), *fwd,
                      wq, wk, wv, w_out[0], w_gate[0], w_up[0], w_down[0], rows)
        dx, dga, dgm, dq, dk, dv, do, dg, du, dd = out
        back = lambda w: w.transpose(1, 0, 2)[None]
        return (dx.reshape(rows, toks, width), dga, dgm, back(dq), back(dk), back(dv), do[None], dg[None], du[None], dd[None])

    tok_spec = P("data", "seq", None)
    vec_spec = P(None, ("data", "seq"))
    mat_spec = P(None, ("data", "seq"), None)
    head_spec = P(None, ("data", "seq"), None, None)
    in_specs = (tok_spec, P("data", "seq")) + (P(),) * 9 + (tok_spec,)
    out_specs = (tok_spec, vec_spec, vec_spec, head_spec, head_spec, head_spec, mat_spec, mat_spec, mat_spec, mat_spec)
    return jax.shard_map(device_step, mesh=mesh, in_specs=in_specs, out_specs=out_specs, check_vma=False)
```

```python
import functools, math
import numpy as np
import jax, jax.numpy as jnp
from jax import lax
from jax.experimental import pallas as pl
from jax.experimental.pallas import tpu as pltpu
from jax.sharding import PartitionSpec as P

WINDOW = 256
NORM_EPS = 1e-5
QB = 128
BF, F32 = jnp.bfloat16, jnp.float32
NN, NT, TN = ((1,), (0,)), ((1,), (1,)), ((0,), (0,))
MESH = pl.DeviceIdType.MESH
NEG = -1e30
VMEM_LIMIT = 67043328


def dot(a, b, dims=NN):
    return lax.dot_general(a, b, (dims, ((), ())), preferred_element_type=F32)


def cdiv_loop(n, body):
    lax.fori_loop(0, n, lambda i, c: (body(i), c)[1], 0)


def mod(a, b):
    return a % b if isinstance(a, int) else lax.rem(a, b)


def aligned(a, b):
    return a if isinstance(a, int) else pl.multiple_of(a, b)


def rope(blk, cos_b, sin_b, sign, head_dim):
    half = head_dim // 2
    parts = []
    for h in range(blk.shape[0] // head_dim):
        first = blk[h * head_dim:h * head_dim + half]
        second = blk[h * head_dim + half:(h + 1) * head_dim]
        if sign > 0:
            parts += [first * cos_b - second * sin_b, second * cos_b + first * sin_b]
        else:
            parts += [first * cos_b + second * sin_b, second * cos_b - first * sin_b]
    return jnp.concatenate(parts, axis=0)


def normed(x, gain):
    xf = x.astype(F32)
    inv = lax.rsqrt(jnp.mean(xf * xf, axis=-1, keepdims=True) + NORM_EPS)
    return (xf * inv * gain).astype(BF)


def stack_pair(pair_t):
    half = pair_t.shape[0] // 2
    zero = jnp.zeros((half, pair_t.shape[1]), pair_t.dtype)
    return jnp.concatenate(
        [jnp.concatenate([pair_t[:half], zero], axis=0), jnp.concatenate([zero, pair_t[half:]], axis=0)], axis=1)


def unstack_pair(both):
    half, cols = both.shape[0] // 2, both.shape[1] // 2
    return jnp.concatenate([both[:half, :cols], both[half:, cols:]], axis=0)


def softmax_parts(scores, upper, bias0, bias1):
    s02 = jnp.where(upper, scores[:QB] + bias0, scores[2 * QB:])
    s1 = scores[QB:2 * QB] + bias1
    top = jnp.max(jnp.maximum(s02, s1), axis=0, keepdims=True)
    e02, e1 = jnp.exp(s02 - top), jnp.exp(s1 - top)
    inv = 1.0 / jnp.sum(e02 + e1, axis=0, keepdims=True)
    return e02 * inv, e1 * inv


def banded(p02, p1, upper):
    return jnp.concatenate(
        [jnp.where(upper, p02, 0.0).astype(BF), p1.astype(BF), jnp.where(upper, 0.0, p02).astype(BF)], axis=0)


def upper_mask():
    key_ids = lax.broadcasted_iota(jnp.int32, (QB, 2 * QB), 0)
    query_ids = lax.broadcasted_iota(jnp.int32, (QB, 2 * QB), 1) % QB
    return key_ids > query_ids


def start_bias(first, blk):
    bias = jnp.where(first, NEG, 0.0).astype(F32)
    return (bias if blk < 2 else 0.0), (bias if blk < 1 else 0.0)


def fwd_kernel(n, head_dim, x_h, pos, invf, ga, gm, wq_h, wk_h, wv_h, wo_h,
               q_h, kt_h, k_h, v_h, hat_h, ot_h, xm_h, hm_h, hmt_h, cos_t, sin_t,
               xv, halo, pos_halo, wq, wk, wv, wo, q, kt, k, v, vt, hat, ot, xm, hm, hmt, hb, acc, cos_h, sin_h,
               sc0, sc1, sc2, pb0, pb1, pb2, ld, st, snd, rcv):
    sc, pb = (sc0, sc1, sc2), (pb0, pb1, pb2)
    rows, toks, width = xv.shape
    ext = toks + WINDOW
    total, n_halo = rows * toks, rows * WINDOW
    n_pairs = wq.shape[0] // (2 * head_dim)
    pw = 2 * head_dim
    me = lax.axis_index("seq")
    right, left = lax.rem(me + 1, n), lax.rem(me + n - 1, n)
    loads = [pltpu.make_async_copy(s, d, ld.at[i]) for i, (s, d) in enumerate(((x_h, xv), (wq_h, wq), (wk_h, wk), (wv_h, wv), (wo_h, wo)))]
    for c in loads:
        c.start()
    barrier = pltpu.get_barrier_semaphore()
    for other in (left, right):
        pl.semaphore_signal(barrier, inc=1, device_id={"seq": other}, device_id_type=MESH)
    pl.semaphore_wait(barrier, 2)
    sends = [pltpu.make_async_remote_copy(src_ref=s, dst_ref=d, send_sem=snd.at[i], recv_sem=rcv.at[i], device_id={"seq": right}, device_id_type=MESH)
             for i, (s, d) in enumerate(((x_h.at[:, toks - WINDOW:, :], halo), (pos, pos_halo)))]
    for c in sends:
        c.start()

    def store(i, s, d):
        c = pltpu.make_async_copy(s, d, st.at[i])
        c.start()
        stores.append(c)

    stores = []
    for b in range(rows):
        ang = invf[...] * pos[b:b + 1, :].astype(F32)
        cos_t[:, b * toks:(b + 1) * toks] = jnp.cos(ang)
        sin_t[:, b * toks:(b + 1) * toks] = jnp.sin(ang)
    loads[0].wait()
    tb = toks // QB

    def norm_blk(i):
        r = pl.multiple_of(i * QB, QB)
        h = normed(xv[i // tb, pl.ds(pl.multiple_of((i % tb) * QB, QB), QB), :], ga[...])
        hb[pl.ds(r, QB), :] = h
        hat[:, pl.ds(r, QB)] = h.T

    with jax.named_scope("f_norm"):
        cdiv_loop(total // QB, norm_blk)
    store(0, hat, hat_h)

    def rope_q(p):
        r = pl.multiple_of(p * pw, pw)
        q[pl.ds(r, pw), :] = (rope(acc[pl.ds(r, pw), :], cos_t[...], sin_t[...], 1, head_dim) * (head_dim ** -0.5)).astype(BF)

    def put_k(p):
        r = pl.multiple_of(p * pw, pw)
        for b in range(rows):
            blk = rope(acc[pl.ds(r, pw), b * toks:(b + 1) * toks], cos_t[:, b * toks:(b + 1) * toks], sin_t[:, b * toks:(b + 1) * toks], 1, head_dim).astype(BF)
            kt[pl.ds(r, pw), b * ext + WINDOW:(b + 1) * ext] = blk
            k[b * ext + WINDOW:(b + 1) * ext, pl.ds(r, pw)] = blk.T

    def put_v(p):
        r = pl.multiple_of(p * pw, pw)
        for b in range(rows):
            blk = acc[pl.ds(r, pw), b * toks:(b + 1) * toks].astype(BF)
            vt[pl.ds(r, pw), b * ext + WINDOW:(b + 1) * ext] = blk
            v[b * ext + WINDOW:(b + 1) * ext, pl.ds(r, pw)] = blk.T

    for i, (w, put) in enumerate(((wq, rope_q), (wk, put_k), (wv, put_v))):
        loads[i + 1].wait()
        with jax.named_scope("f_mm"):
            acc[...] = dot(w[...], hb[...], NT)
        with jax.named_scope("f_put"):
            cdiv_loop(n_pairs, put)
    store(1, q, q_h)

    with jax.named_scope("f_halo_wait"):
        for c in sends:
            c.wait()
    for b in range(rows):
        ang = invf[...] * pos_halo[b:b + 1, toks - WINDOW:].astype(F32)
        cos_h[:, b * WINDOW:(b + 1) * WINDOW] = jnp.cos(ang)
        sin_h[:, b * WINDOW:(b + 1) * WINDOW] = jnp.sin(ang)
    wb = WINDOW // QB

    def norm_halo(i):
        h = normed(halo[i // wb, pl.ds(pl.multiple_of((i % wb) * QB, QB), QB), :], ga[...])
        hb[pl.ds(pl.multiple_of(i * QB, QB), QB), :] = h

    cdiv_loop(n_halo // QB, norm_halo)

    def halo_put(is_k, p):
        r = pl.multiple_of(p * pw, pw)
        for b in range(rows):
            blk = acc[pl.ds(r, pw), b * WINDOW:(b + 1) * WINDOW]
            if is_k:
                blk = rope(blk, cos_h[:, b * WINDOW:(b + 1) * WINDOW], sin_h[:, b * WINDOW:(b + 1) * WINDOW], 1, head_dim)
            blk = blk.astype(BF)
            dst_t, dst = (kt, k) if is_k else (vt, v)
            dst_t[pl.ds(r, pw), b * ext:b * ext + WINDOW] = blk
            dst[b * ext:b * ext + WINDOW, pl.ds(r, pw)] = blk.T

    with jax.named_scope("f_halo_mm"):
        for w, is_k in ((wk, True), (wv, False)):
            acc[:, :n_halo] = dot(w[...], hb[:n_halo, :], NT)
            cdiv_loop(n_pairs, functools.partial(halo_put, is_k))
    store(2, kt, kt_h)
    store(3, k, k_h)
    store(4, v, v_h)

    upper = upper_mask()
    first = me == 0
    n_steps = n_pairs * rows

    def spots(it, blk):
        p, b = it // rows, mod(it, rows)
        pr = pl.ds(aligned(p * pw, pw), pw)
        return pr, pl.ds(aligned(b * toks + blk * QB, QB), QB), pl.ds(aligned(b * ext + blk * QB, QB), 3 * QB)

    def score(it):
        for blk in range(tb):
            pr, cols, keys = spots(it, blk)
            sc[blk][...] = dot(k[keys, pr], stack_pair(q[pr, cols]))

    def soften(blk):
        p02, p1 = softmax_parts(sc[blk][...], upper, *start_bias(first, blk))
        pb[blk][...] = banded(p02, p1, upper)

    def mix(it):
        for blk in range(tb):
            pr, cols, keys = spots(it, blk)
            ot[pr, cols] = unstack_pair(dot(vt[pr, keys], pb[blk][...])).astype(BF)

    def attend(it):
        mix(jnp.maximum(it - 1, 0))
        for blk in range(tb):
            soften(blk)
        score(jnp.minimum(it + 1, n_steps - 1))

    for blk in range(tb):
        pb[blk][...] = jnp.zeros(pb[blk].shape, BF)
    score(0)
    with jax.named_scope("f_attn"):
        cdiv_loop(n_steps, attend)
    mix(n_steps - 1)
    loads[4].wait()
    for b in range(rows):
        cols = slice(b * toks, (b + 1) * toks)
        store(5 + 4 * b, ot.at[:, cols], ot_h.at[:, cols])
        mid = (xv[b].astype(F32) + dot(ot[:, cols], wo[...], TN)).astype(BF)
        xm[cols, :] = mid
        h = normed(mid, gm[...])
        hm[cols, :] = h
        hmt[:, cols] = h.T
        store(6 + 4 * b, hm.at[cols, :], hm_h.at[cols, :])
        store(7 + 4 * b, hmt.at[:, cols], hmt_h.at[:, cols])
        store(8 + 4 * b, xm.at[cols, :], xm_h.at[cols, :])
    with jax.named_scope("f_store_wait"):
        for c in stores:
            c.wait()


def any_spec(k):
    return [pl.BlockSpec(memory_space=pl.ANY)] * k


def vmem_spec(k):
    return [pl.BlockSpec(memory_space=pltpu.VMEM)] * k


def run_fwd(n, x, pos, invf, ga, gm, wq, wk, wv, wo, head_dim):
    rows, toks, width = x.shape
    hd = wq.shape[0]
    ext, total, n_halo = toks + WINDOW, rows * toks, rows * WINDOW
    half = head_dim // 2
    sds = lambda *s: jax.ShapeDtypeStruct(s, BF)
    outs = [sds(hd, total), sds(hd, rows * ext), sds(rows * ext, hd), sds(rows * ext, hd), sds(width, total), sds(hd, total), sds(total, width), sds(total, width), sds(width, total)]
    outs += [jax.ShapeDtypeStruct((half, total), F32)] * 2
    vm = lambda *s: pltpu.VMEM(s, BF)
    vf = lambda *s: pltpu.VMEM(s, F32)
    scratch = [vm(rows, toks, width), vm(rows, WINDOW, width), pltpu.VMEM((rows, toks), jnp.int32), vm(hd, width), vm(hd, width), vm(hd, width), vm(hd, width),
               vm(hd, total), vm(hd, rows * ext), vm(rows * ext, hd), vm(rows * ext, hd), vm(hd, rows * ext), vm(width, total), vm(hd, total), vm(total, width), vm(total, width), vm(width, total), vm(total, width),
               vf(hd, total), vf(half, n_halo), vf(half, n_halo),
               *[vf(3 * QB, 2 * QB)] * 3, *[vm(3 * QB, 2 * QB)] * 3,
               pltpu.SemaphoreType.DMA((5,)), pltpu.SemaphoreType.DMA((5 + 4 * rows,)), pltpu.SemaphoreType.DMA((2,)), pltpu.SemaphoreType.DMA((2,))]
    return pl.pallas_call(
        functools.partial(fwd_kernel, n, head_dim), out_shape=outs,
        in_specs=any_spec(1) + vmem_spec(4) + any_spec(4), out_specs=any_spec(9) + vmem_spec(2), scratch_shapes=scratch,
        compiler_params=pltpu.CompilerParams(collective_id=0, has_side_effects=True, vmem_limit_bytes=VMEM_LIMIT),
        name="forward")(x, pos, invf, ga, gm, wq, wk, wv, wo)


LAG = 2
SLOTS = 2 * LAG
RING = 5
SWAPS = 5
CB = 256


def at(ref, *idx):
    return ref.at[idx]


class Torus:
    def __init__(self, n, pairs, holes, turn, parts, recv0, recv1, recv2, recv3, recv4, acc, acc2, fin, snd, rcv):
        self.side = math.isqrt(n // 2)
        assert self.side == 4
        me = lax.axis_index("seq")
        self.core = lax.rem(me, 2)
        chip = me // 2
        self.x, self.y = lax.rem(chip, 4), chip // 4
        self.pairs, self.holes, self.turn = pairs, holes, turn
        self.parts, self.recv0, self.recv1, self.recv2, self.recv3, self.recv4 = parts, recv0, recv1, recv2, recv3, recv4
        self.acc, self.acc2, self.fin, self.snd, self.rcv = acc, acc2, fin, snd, rcv
        self.partner = me + 1 - 2 * self.core
        self.hops = {(axis, step): self.device(*((0, step) if axis == 0 else (step, 0))) for axis in (0, 1) for step in (1, 3)}

    def device(self, dy, dx):
        return (lax.rem(self.y + dy, 4) * 4 + lax.rem(self.x + dx, 4)) * 2 + self.core

    def peers(self):
        return [self.partner, *self.hops.values()]

    def copy(self, lane, kind, slot, src, dst, target):
        return pltpu.make_async_remote_copy(
            src_ref=src, dst_ref=dst, send_sem=self.snd.at[lane, kind, slot], recv_sem=self.rcv.at[lane, kind, slot],
            device_id={"seq": target}, device_id_type=MESH)

    def late(self, pair, yes, no):
        if isinstance(pair, int):
            return yes if pair >= self.turn else no
        return jnp.where(pair >= self.turn, yes, no)

    def swap(self, ring, slot):
        return self.copy(0, 0, slot, self.parts.at[ring, :, :, 1 - self.core], self.recv0.at[slot], self.partner)

    def copies(self, stage, kind, pair, held, slot):
        axis = kind if stage < 3 else 1 - kind
        plus, minus = self.hops[axis, 1], self.hops[axis, 3]
        half = CB // 2
        if stage == 1:
            if axis == 0:
                minus = self.late(pair, plus, minus)
            ends = [(self.acc.at[kind, held, 2, pl.ds(0, 2)], self.recv1), (self.acc.at[kind, held, 2, pl.ds(2, 2)], self.recv1)]
        elif stage == 2:
            ends = [(self.acc.at[kind, held, 1], self.recv2), (self.acc.at[kind, held, 3], self.recv2)]
        elif stage == 3:
            ends = [(self.acc2.at[kind, held, 2, :, pl.ds(0, half)], self.recv3), (self.acc2.at[kind, held, 2, :, pl.ds(half, half)], self.recv3)]
        else:
            ends = [(self.acc2.at[kind, held, 1], self.recv4), (self.acc2.at[kind, held, 3], self.recv4)]
        lane = 2 * stage - 1
        return [self.copy(lane + i, kind, slot, src, buf.at[kind, slot, i], (plus, minus)[i]) for i, (src, buf) in enumerate(ends)]

    def add(self, stage, kind, pair, held, slot, ring):
        acc, acc2 = self.acc, self.acc2
        if stage == 1:
            def row(r1):
                for r2 in range(4):
                    ry, rx = (r2, r1) if kind == 0 else (r1, r2)
                    chip = lax.rem(self.y + ry, 4) * 4 + lax.rem(self.x + rx, 4)
                    acc[kind, held, r1, r2] = self.parts[ring, kind, chip, self.core] + self.recv0[slot, kind, chip]
            cdiv_loop(4, row)
        elif stage == 2:
            back = self.late(pair, 1, 3) if kind == 0 else 3
            acc[kind, held, 1, 0:2] += self.recv1[kind, slot, 0]
            acc[kind, held, back, 2:4] += self.recv1[kind, slot, 1]
        elif stage == 3:
            acc2[kind, held] = acc[kind, held, 0] + (self.recv2[kind, slot, 0] + self.recv2[kind, slot, 1])
        elif stage == 4:
            half = CB // 2
            acc2[kind, held, 1, :, 0:half] += self.recv3[kind, slot, 0]
            acc2[kind, held, 3, :, half:] += self.recv3[kind, slot, 1]
        else:
            self.fin[pair, kind] = acc2[kind, held, 0] + (self.recv4[kind, slot, 0] + self.recv4[kind, slot, 1])

    def when(self, pair, fn):
        if isinstance(pair, int):
            if 0 <= pair < self.pairs and pair not in self.holes:
                fn()
            return
        ok = (pair >= 0) & (pair < self.pairs)
        for h in self.holes:
            ok &= pair != h
        pl.when(ok)(fn)

    def tick(self, t):
        rem = mod
        now, land = rem(t, SLOTS), rem(t + SLOTS - LAG, SLOTS)
        held = [now, land, now, land, now, land]
        swap_now, swap_land = rem(t, SWAPS), rem(t + SWAPS - LAG, SWAPS)
        ring_now, ring_land = rem(t, RING), rem(t + RING - LAG, RING)
        for stage in range(5, 0, -1):
            pair = t - LAG * stage

            def take(stage=stage, pair=pair):
                if stage == 1:
                    with jax.named_scope("t_wait1"):
                        self.swap(ring_land, swap_land).wait()
                    for kind in (0, 1):
                        self.add(1, kind, pair, held[1], swap_land, ring_land)
                    return
                with jax.named_scope(f"t_wait{stage}"):
                    for kind in (0, 1):
                        for c in self.copies(stage - 1, kind, pair, held[stage], land):
                            c.wait()
                for kind in (0, 1):
                    self.add(stage, kind, pair, held[stage], land, 0)
            self.when(pair, take)
        for stage in range(4, -1, -1):
            pair = t - LAG * stage

            def give(stage=stage, pair=pair):
                if stage == 0:
                    self.swap(ring_now, swap_now).start()
                    return
                for kind in (0, 1):
                    for c in self.copies(stage, kind, pair, held[stage], now):
                        c.start()
            self.when(pair, give)


def pick(i, table):
    out = 0
    for key, value in table.items():
        out = jnp.where(i == key, value, out)
    return out


def norm_back(x, gain, grad, res):
    xf = x.astype(F32)
    inv = lax.rsqrt(jnp.mean(xf * xf, axis=-1, keepdims=True) + NORM_EPS)
    unit = xf * inv
    gu = grad * gain
    out = inv * (gu - unit * jnp.mean(gu * unit, axis=-1, keepdims=True)) + res.astype(F32)
    gu = grad * unit
    return out.astype(BF), jnp.sum(gu.reshape(gu.shape[0] // 8, 8, gu.shape[1]), axis=0)


def plan(n_mlp, n_down, nc, per):
    base = n_mlp + n_down
    waiting, place, tick_of, holes = [("o", g) for g in range(nc)], {}, {}, []
    t, last_hole = base, False

    def pair_up():
        nonlocal t
        for kind in (0, 1):
            place[waiting.pop(0)] = (t, kind)
        t += 1

    for p in range(nc * per):
        g = p // per
        if p % per == per - 1:
            waiting.append(("q", g))
            if 1 <= g < nc - 1:
                waiting += [("k", g - 1), ("v", g - 1)]
        tick_of[p] = -1
        if len(waiting) >= 2:
            tick_of[p] = t
            pair_up()
            last_hole = False
        elif not last_hole:
            tick_of[p] = t
            holes.append(t)
            t += 1
            last_hole = True
    rest = list(range(max(nc - 2, 0), nc))
    for g in rest:
        waiting += [("k", g), ("v", g)]
        pair_up()
    assert not waiting
    return base, place, tick_of, tuple(holes), rest, t


def bwd_kernel(n, head_dim, dims, ga, gm, x_h, dout_h, q_h, kt_h, k_h, v_h, hat_h, ot_h, xm_h, hm_h, hmt_h, cos_i, sin_i,
               wq_h, wk_h, wv_h, wo_h, wg_h, wu_h, wd_h,
               dx_h, fin, dga_o, dgm_o,
               parts, recv0, recv1, recv2, recv3, recv4, acc, acc2, snd, rcv,
               hk_recv, hv_recv, hsnd, hrcv, gsend, grecv, gsem, ld, xbuf, mbuf, gnm, gmid, ot, hat, wo, dgain):
    rows, toks, width, hd, ff = dims
    ext, total = toks + WINDOW, rows * toks
    pw = 2 * head_dim
    n_pairs = hd // pw
    nb, nc, sub = ff // CB, width // CB, ff // width
    rpd = width // n
    n_mlp, n_down = nb, nc * sub // 2
    per, half_sub = CB // pw, sub // 2
    base, place, tick_of, holes, rest, pairs = plan(n_mlp, n_down, nc, per)
    comm = Torus(n, pairs, holes, n_mlp, parts, recv0, recv1, recv2, recv3, recv4, acc, acc2, fin, snd, rcv)
    me = lax.axis_index("seq")
    left = lax.rem(me + n - 1, n)
    barrier = pltpu.get_barrier_semaphore()

    def greet(i):
        pl.semaphore_signal(barrier, inc=1, device_id={"seq": lax.rem(me + i + 1, n)}, device_id_type=MESH)

    cdiv_loop(n - 1, greet)

    def load(i, s, d):
        c = pltpu.make_async_copy(s, d, ld.at[i])
        c.start()
        return c

    def put(spot, value):
        pair, kind = spot
        parts[mod(pair, RING), kind] = value.reshape(n // 2, 2, rpd, CB)

    def late(i):
        s, d = ((xm_h, mbuf), (ot_h, ot), (hat_h, hat), (wo_h, wo))[i]
        return pltpu.make_async_copy(s, d, ld.at[1 + i])

    def mlp(hm, hmt, actt, wgu, wd, dgu, wld):
        def weights(j, slot):
            c = aligned(j * CB, CB)
            return [pltpu.make_async_copy(wg_h.at[:, pl.ds(c, CB)], wgu.at[slot, :, pl.ds(0, CB)], wld.at[slot, 0]),
                    pltpu.make_async_copy(wu_h.at[:, pl.ds(c, CB)], wgu.at[slot, :, pl.ds(CB, CB)], wld.at[slot, 1]),
                    pltpu.make_async_copy(wd_h.at[pl.ds(c, CB), :], wd.at[slot], wld.at[slot, 2])]

        for c in weights(0, 0):
            c.start()
        ld_hm, ld_x, ld_hmt = load(5, hm_h, hm), load(0, dout_h, xbuf), load(6, hmt_h, hmt)
        for i in range(4):
            late(i).start()
        gnm[...] = jnp.zeros_like(gnm)
        gsend[...] = jnp.zeros_like(gsend)
        dgain[...] = jnp.zeros_like(dgain)
        ld_hm.wait()
        ld_x.wait()
        ld_hmt.wait()

        def block(j):
            slot = lax.rem(j, 2)
            for c in weights(j, slot):
                c.wait()

            @pl.when(j + 1 < nb)
            def _():
                for c in weights(j + 1, 1 - slot):
                    c.start()

            c0 = pl.multiple_of(j * CB, CB)
            with jax.named_scope("b_mlp"):
                for b in range(rows):
                    r = slice(b * toks, (b + 1) * toks)
                    gu = dot(hm[r, :], wgu[slot])
                    gact = dot(xbuf[r, :], wd[slot], NT).astype(BF).astype(F32)
                    gate, up = gu[:, :CB], gu[:, CB:]
                    sig = 1.0 / (1.0 + jnp.exp(-gate))
                    swish = gate * sig
                    actt[pl.ds(c0, CB), r] = (swish * up).astype(BF).T
                    dgu[r, :CB] = (gact * up * (sig + swish * (1.0 - sig))).astype(BF)
                    dgu[r, CB:] = (gact * swish).astype(BF)
                both = dot(hmt[...], dgu[...])
                ring = lax.rem(j, RING)
                parts[ring, 0] = both[:, :CB].reshape(n // 2, 2, rpd, CB)
                parts[ring, 1] = both[:, CB:].reshape(n // 2, 2, rpd, CB)
                for b in range(rows):
                    r = slice(b * toks, (b + 1) * toks)
                    gnm[r, :] += dot(dgu[r, :], wgu[slot], NT)

            @pl.when(j == 0)
            def _():
                pl.semaphore_wait(barrier, n - 1)

            comm.tick(j)

        cdiv_loop(nb, block)

        def down(c):
            share = n // 2 // sub
            c0 = pl.multiple_of(c * CB, CB)
            for m in range(sub):
                res = dot(actt[m * width:(m + 1) * width, :], xbuf[:, pl.ds(c0, CB)]).reshape(share, 2, sub, rpd, CB)
                for i in range(sub):
                    pair = n_mlp + c * half_sub + i // 2
                    parts[lax.rem(pair, RING), i % 2, m * share:(m + 1) * share] = res[:, :, i]

        late(0).wait()

        def mid(i):
            r = pl.ds(pl.multiple_of(i * QB, QB), QB)
            out, dg = norm_back(mbuf[r, :], gm[...], gnm[r, :], xbuf[r, :])
            gmid[r, :] = out
            dgain[8:16, :] += dg

        def column(c):
            with jax.named_scope("b_down"):
                down(c)
            comm.tick(n_mlp + c * half_sub)

            @pl.when(c == 0)
            def _():
                with jax.named_scope("b_mid"):
                    cdiv_loop(total // QB, mid)

            @pl.when(c < nc - 1)
            def _():
                for e in range(1, half_sub):
                    comm.tick(n_mlp + c * half_sub + e)

        cdiv_loop(nc, column)

    vm = lambda *s: pltpu.VMEM(s, BF)
    vf = lambda *s: pltpu.VMEM(s, F32)
    pl.run_scoped(mlp, vm(total, width), vm(width, total), vm(ff, total), vm(2, width, 2 * CB), vm(2, CB, width), vm(total, 2 * CB),
                  pltpu.SemaphoreType.DMA((2, 3)))

    def attention(q, kt, k, v, dot_, dkt, dk, dv, hk, hv, wq, wk, wv,
                  sc0, sc1, sc2, dp0, dp1, dp2, pb0, pb1, pb2, ds0, ds1, ds2):
        dqt = ot
        sc, dp, pb, ds = (sc0, sc1, sc2), (dp0, dp1, dp2), (pb0, pb1, pb2), (ds0, ds1, ds2)
        lds = [load(5 + i, s, d) for i, (s, d) in enumerate(((q_h, q), (kt_h, kt), (k_h, k), (v_h, v)))]
        ldw = [load(9 + i, s, d) for i, (s, d) in enumerate(((wq_h, wq), (wk_h, wk), (wv_h, wv)))]
        ld_x2 = load(0, x_h, xbuf)
        late(1).wait()
        late(3).wait()
        with jax.named_scope("b_dot"):
            dot_[...] = dot(wo[...], gmid[...], NT).astype(BF)
        for e in range(1, half_sub):
            comm.tick(base - half_sub + e)

        def out_grad(g):
            spot = pick(g, {i: place["o", i][0] for i in range(nc)}), pick(g, {i: place["o", i][1] for i in range(nc)})
            put(spot, dot(ot[...], gmid[:, pl.ds(pl.multiple_of(g * CB, CB), CB)]))

        with jax.named_scope("b_dwo"):
            cdiv_loop(nc, out_grad)
        for c in lds:
            c.wait()
        late(2).wait()
        upper = upper_mask()
        first = me == 0
        tb = toks // QB
        n_steps = n_pairs * rows

        def spots(it, blk):
            p, b = it // rows, mod(it, rows)
            pr = pl.ds(aligned(p * pw, pw), pw)
            return pr, pl.ds(aligned(b * toks + blk * QB, QB), QB), pl.ds(aligned(b * ext + blk * QB, QB), 3 * QB)

        def score(it):
            for blk in range(tb):
                pr, cols, keys = spots(it, blk)
                sc[blk][...] = dot(k[keys, pr], stack_pair(q[pr, cols]))
                dp[blk][...] = dot(v[keys, pr], stack_pair(dot_[pr, cols]))

        def soften(blk):
            p02, p1 = softmax_parts(sc[blk][...], upper, *start_bias(first, blk))
            g02, g1 = jnp.where(upper, dp[blk][:QB], dp[blk][2 * QB:]), dp[blk][QB:2 * QB]
            mean = jnp.sum(p02 * g02 + p1 * g1, axis=0, keepdims=True)
            pb[blk][...] = banded(p02, p1, upper)
            ds[blk][...] = banded(p02 * (g02 - mean), p1 * (g1 - mean), upper)

        def grads(it):
            p, b = it // rows, mod(it, rows)
            ks, vs = [], []
            for blk in range(tb):
                pr, cols, keys = spots(it, blk)
                vs.append(dot(pb[blk][...], stack_pair(dot_[pr, cols]), NT))
                ks.append(dot(ds[blk][...], stack_pair(q[pr, cols]), NT))
                dq = unstack_pair(dot(kt[pr, keys], ds[blk][...])) * (head_dim ** -0.5)
                dqt[pr, cols] = rope(dq, cos_i[:, cols], sin_i[:, cols], -1, head_dim).astype(BF)
            for parts_, own, halo in ((ks, dk, hk), (vs, dv, hv)):
                for j in range(tb + 2):
                    val = sum(parts_[i][(j - i) * QB:(j - i + 1) * QB] for i in range(tb) if 0 <= j - i < 3).astype(BF)
                    if j < 2:
                        halo[p, b, j * QB:(j + 1) * QB, :] = val
                    else:
                        own[pl.ds(aligned(b * toks + (j - 2) * QB, QB), QB), pr] = val

        def halo_copies(p):
            return [pltpu.make_async_remote_copy(src_ref=s.at[p], dst_ref=d.at[p], send_sem=hsnd.at[i, p], recv_sem=hrcv.at[i, p],
                                                 device_id={"seq": left}, device_id_type=MESH)
                    for i, (s, d) in enumerate(((hk, hk_recv), (hv, hv_recv)))]

        def finish(p):
            r = pl.multiple_of(p * pw, pw)
            with jax.named_scope("b_hwait"):
                for c in halo_copies(p):
                    c.wait()
            for b in range(rows):
                for blk in range(tb):
                    cols = slice(b * toks + blk * QB, b * toks + (blk + 1) * QB)
                    gk = dk[cols, pl.ds(r, pw)].astype(F32)
                    off = blk * QB - (toks - WINDOW)
                    if off >= 0:
                        gk = gk + hk_recv[p, b, off:off + QB, :].astype(F32)
                        gv = dv[cols, pl.ds(r, pw)].astype(F32) + hv_recv[p, b, off:off + QB, :].astype(F32)
                        dv[cols, pl.ds(r, pw)] = gv.astype(BF)
                    dkt[pl.ds(r, pw), cols] = rope(gk.T, cos_i[:, cols], sin_i[:, cols], -1, head_dim).astype(BF)

        def spot_of(name, g):
            known = {i: place[name, i] for i in range(nc)}
            return pick(g, {i: s[0] for i, s in known.items()}), pick(g, {i: s[1] for i, s in known.items()})

        def close_group(g):
            with jax.named_scope("b_finish"):
                cdiv_loop(per, lambda i: finish(g * per + i))
            cols = pl.ds(pl.multiple_of(g * CB, CB), CB)
            with jax.named_scope("b_dwkv"):
                put(spot_of("k", g), dot(hat[...], dkt[cols, :], NT))
                put(spot_of("v", g), dot(hat[...], dv[:, cols]))

        def step(p):
            for c in halo_copies(p):
                c.start()
            g = p // per

            @pl.when(lax.rem(p, per) == per - 1)
            def _():
                with jax.named_scope("b_dwq"):
                    put(spot_of("q", g), dot(hat[...], dqt[pl.ds(pl.multiple_of(g * CB, CB), CB), :], NT))

                if rest[0] > 0:
                    @pl.when((g > 0) & (g <= rest[0]))
                    def _():
                        close_group(g - 1)

            t = pick(p, tick_of)

            @pl.when(t >= 0)
            def _():
                comm.tick(t)

        def walk(it):
            @pl.when(it < n_steps)
            def _():
                with jax.named_scope("b_attn"):
                    grads(jnp.maximum(it - 1, 0))
                    for blk in range(tb):
                        soften(blk)
                    score(jnp.minimum(it + 1, n_steps - 1))

            @pl.when(it == n_steps)
            def _():
                grads(n_steps - 1)

            @pl.when((lax.rem(it, rows) == 0) & (it > 0))
            def _():
                step(it // rows - 1)

        for blk in range(tb):
            pb[blk][...] = jnp.zeros(pb[blk].shape, BF)
            ds[blk][...] = jnp.zeros(ds[blk].shape, BF)
        score(0)
        cdiv_loop(n_steps + 1, walk)
        for c in ldw:
            c.wait()
        ld_x2.wait()

        def into_q(b):
            r = pl.ds(pl.multiple_of(b * toks, QB), toks)
            gnm[r, :] = dot(dqt[:, r], wq[...], TN)

        with jax.named_scope("b_intoq"):
            cdiv_loop(rows, into_q)

        def close_rest(i):
            close_group(rest[0] + i)
            comm.tick(pairs - len(rest) + i)

        cdiv_loop(len(rest), close_rest)

        def into(b):
            r = pl.ds(pl.multiple_of(b * toks, QB), toks)
            with jax.named_scope("b_into"):
                gnm[r, :] += dot(dkt[:, r], wk[...], TN) + dot(dv[r, :], wv[...])

            def final(i):
                r = pl.ds(pl.multiple_of((b * tb + i) * QB, QB), QB)
                out, dg = norm_back(xbuf[r, :], ga[...], gnm[r, :], gmid[r, :])
                mbuf[r, :] = out
                dgain[0:8, :] += dg

            with jax.named_scope("b_final"):
                cdiv_loop(tb, final)
            comm.tick(pairs + b)

        cdiv_loop(rows, into)

    score_bufs = [vf(3 * QB, 2 * QB)] * 6 + [vm(3 * QB, 2 * QB)] * 6
    pl.run_scoped(attention, vm(hd, total), vm(hd, rows * ext), vm(rows * ext, hd), vm(rows * ext, hd), vm(hd, total), vm(hd, total),
                  vm(total, hd), vm(total, hd), vm(n_pairs, rows, WINDOW, pw), vm(n_pairs, rows, WINDOW, pw), vm(hd, width), vm(hd, width), vm(hd, width), *score_bufs)
    out_copy = load(1, mbuf, dx_h)
    gains = jnp.concatenate([jnp.sum(dgain[0:8, :], axis=0, keepdims=True), jnp.sum(dgain[8:16, :], axis=0, keepdims=True), jnp.zeros((6, width), F32)], axis=0)
    for p in range(n):
        gsend[p, :, 0:rpd] = gains[:, p * rpd:(p + 1) * rpd]

    def spread(i):
        to = lax.rem(me + i + 1, n)
        pltpu.make_async_remote_copy(src_ref=gsend.at[to], dst_ref=grecv.at[i], send_sem=gsem.at[0], recv_sem=gsem.at[1],
                                     device_id={"seq": to}, device_id_type=MESH).start()

    cdiv_loop(n - 1, spread)
    lax.fori_loop(pairs + rows, pairs + 5 * LAG, lambda t, c: (comm.tick(t), c)[1], 0)
    with jax.named_scope("b_gain"):
        pltpu.make_async_remote_copy(src_ref=gsend.at[pl.ds(0, n - 1)], dst_ref=grecv, send_sem=gsem.at[0], recv_sem=gsem.at[1],
                                     device_id={"seq": left}, device_id_type=MESH).wait()
    sums = gsend[me]
    for i in range(n - 1):
        sums = sums + grecv[i]
    dga_o[...] = sums[0:1, 0:rpd]
    dgm_o[...] = sums[1:2, 0:rpd]
    out_copy.wait()


def spread_kernel(dims, dx_i, fin, dga_i, dgm_i, dx_o, dga_o, dgm_o, dq_o, dk_o, dv_o, do_o, dg_o, du_o, dd_o, buf, sem):
    head_dim, n, width, ff = dims
    nb, nc, sub = ff // CB, width // CB, ff // width
    rpd = width // n
    n_mlp, n_down = nb, nc * sub // 2
    place = plan(n_mlp, n_down, nc, CB // (2 * head_dim))[1]
    get = pltpu.make_async_copy(dx_i, buf, sem)
    get.start()
    dga_o[...] = dga_i[...]
    dgm_o[...] = dgm_i[...]
    for j in range(nb):
        dg_o[:, j * CB:(j + 1) * CB] = fin[j, 0]
        du_o[:, j * CB:(j + 1) * CB] = fin[j, 1]
    for c in range(nc):
        for i in range(sub):
            dd_o[i * rpd:(i + 1) * rpd, c * CB:(c + 1) * CB] = fin[n_mlp + (c * sub + i) // 2, i % 2]
    get.wait()
    out = pltpu.make_async_copy(buf, dx_o, sem)
    out.start()
    for g in range(nc):
        do_o[:, g * CB:(g + 1) * CB] = fin[place["o", g]]
        for name, ref in (("q", dq_o), ("k", dk_o), ("v", dv_o)):
            val = fin[place[name, g]]
            for h in range(CB // head_dim):
                ref[g * (CB // head_dim) + h] = val[:, h * head_dim:(h + 1) * head_dim]
    out.wait()


def run_bwd(n, head_dim, ga, gm, x, dout, q, kt, k, v, hat, ot, xm, hm, hmt, cos_t, sin_t, wq, wk, wv, wo, wg, wu, wd, rows):
    total, width = x.shape
    hd, ff = wq.shape[0], wg.shape[1]
    toks = total // rows
    rpd, heads = width // n, hd // head_dim
    nb, nc, sub = ff // CB, width // CB, ff // width
    pairs = plan(nb, nc * sub // 2, nc, CB // (2 * head_dim))[5]
    n_pairs = hd // (2 * head_dim)
    f = lambda *s: jax.ShapeDtypeStruct(s, F32)
    dx_t = jax.ShapeDtypeStruct((total, width), BF)
    vm = lambda *s: pltpu.VMEM(s, BF)
    vf = lambda *s: pltpu.VMEM(s, F32)
    dma = lambda *s: pltpu.SemaphoreType.DMA(s)
    scratch = [vf(RING, 2, n // 2, 2, rpd, CB), vf(SWAPS, 2, n // 2, rpd, CB), vf(2, SLOTS, 2, 2, rpd, CB), vf(2, SLOTS, 2, 4, rpd, CB),
               vf(2, SLOTS, 2, rpd, CB // 2), vf(2, SLOTS, 2, rpd, CB), vf(2, SLOTS, 4, 4, rpd, CB), vf(2, SLOTS, 4, rpd, CB),
               dma(9, 2, SWAPS), dma(9, 2, SWAPS),
               vm(n_pairs, rows, WINDOW, 2 * head_dim), vm(n_pairs, rows, WINDOW, 2 * head_dim), dma(2, n_pairs), dma(2, n_pairs),
               vf(n, 8, 128), vf(n - 1, 8, 128), dma(2), dma(12),
               vm(total, width), vm(total, width), vf(total, width), vm(total, width), vm(hd, total), vm(width, total), vm(hd, width), vf(16, width)]
    mid = pl.pallas_call(
        functools.partial(bwd_kernel, n, head_dim, (rows, toks, width, hd, ff)), out_shape=[dx_t, f(pairs, 2, rpd, CB), f(1, rpd), f(1, rpd)],
        in_specs=vmem_spec(2) + any_spec(11) + vmem_spec(2) + any_spec(7), out_specs=any_spec(1) + vmem_spec(3), scratch_shapes=scratch,
        compiler_params=pltpu.CompilerParams(collective_id=1, has_side_effects=True, vmem_limit_bytes=VMEM_LIMIT),
        name="backward")(ga, gm, x, dout, q, kt, k, v, hat, ot, xm, hm, hmt, cos_t, sin_t, wq, wk, wv, wo, wg, wu, wd)
    outs = [dx_t, f(1, rpd), f(1, rpd)] + [f(heads, rpd, head_dim)] * 3 + [f(rpd, width), f(rpd, ff), f(rpd, ff), f(ff // n, width)]
    return pl.pallas_call(
        functools.partial(spread_kernel, (head_dim, n, width, ff)), out_shape=outs,
        in_specs=any_spec(1) + vmem_spec(3), out_specs=any_spec(1) + vmem_spec(9), scratch_shapes=[vm(total, width), pltpu.SemaphoreType.DMA],
        name="spread")(*mid)


def solution(mesh):
    n = mesh.shape["seq"]

    def device_step(hidden, positions, g_attn, g_mlp, w_query, w_key, w_value, w_out, w_gate, w_up, w_down, d_out):
        rows, toks, width = hidden.shape
        layers, _, heads, head_dim = w_query.shape
        hd = heads * head_dim
        half = head_dim // 2
        inv_freq = 1.0 / (10000.0 ** (jnp.arange(half, dtype=F32) * (2.0 / head_dim)))
        turn = lambda w: w[0].transpose(1, 2, 0).reshape(hd, width)
        wq, wk, wv = turn(w_query), turn(w_key), turn(w_value)
        fwd = run_fwd(n, hidden, positions, inv_freq[:, None], g_attn, g_mlp, wq, wk, wv, w_out[0], head_dim)
        out = run_bwd(n, head_dim, g_attn, g_mlp, hidden.reshape(rows * toks, width), d_out.reshape(rows * toks, width), *fwd,
                      wq, wk, wv, w_out[0], w_gate[0], w_up[0], w_down[0], rows)
        dx, dga, dgm, dq, dk, dv, do, dg, du, dd = out
        back = lambda w: w.transpose(1, 0, 2)[None]
        return (dx.reshape(rows, toks, width), dga, dgm, back(dq), back(dk), back(dv), do[None], dg[None], du[None], dd[None])

    tok_spec = P("data", "seq", None)
    vec_spec = P(None, ("data", "seq"))
    mat_spec = P(None, ("data", "seq"), None)
    head_spec = P(None, ("data", "seq"), None, None)
    in_specs = (tok_spec, P("data", "seq")) + (P(),) * 9 + (tok_spec,)
    out_specs = (tok_spec, vec_spec, vec_spec, head_spec, head_spec, head_spec, mat_spec, mat_spec, mat_spec, mat_spec)
    return jax.shard_map(device_step, mesh=mesh, in_specs=in_specs, out_specs=out_specs, check_vma=False)
```

```python
import functools, math
import numpy as np
import jax, jax.numpy as jnp
from jax import lax
from jax.experimental import pallas as pl
from jax.experimental.pallas import tpu as pltpu
from jax.sharding import PartitionSpec as P

WINDOW = 256
NORM_EPS = 1e-5
QB = 128
BF, F32 = jnp.bfloat16, jnp.float32
NN, NT, TN = ((1,), (0,)), ((1,), (1,)), ((0,), (0,))
MESH = pl.DeviceIdType.MESH
NEG = -1e30
VMEM_LIMIT = 67043328


def dot(a, b, dims=NN):
    return lax.dot_general(a, b, (dims, ((), ())), preferred_element_type=F32)


def cdiv_loop(n, body):
    lax.fori_loop(0, n, lambda i, c: (body(i), c)[1], 0)


def mod(a, b):
    return a % b if isinstance(a, int) else lax.rem(a, b)


def aligned(a, b):
    return a if isinstance(a, int) else pl.multiple_of(a, b)


def rope(blk, cos_b, sin_b, sign, head_dim):
    half = head_dim // 2
    parts = []
    for h in range(blk.shape[0] // head_dim):
        first = blk[h * head_dim:h * head_dim + half]
        second = blk[h * head_dim + half:(h + 1) * head_dim]
        if sign > 0:
            parts += [first * cos_b - second * sin_b, second * cos_b + first * sin_b]
        else:
            parts += [first * cos_b + second * sin_b, second * cos_b - first * sin_b]
    return jnp.concatenate(parts, axis=0)


def normed(x, gain):
    xf = x.astype(F32)
    inv = lax.rsqrt(jnp.mean(xf * xf, axis=-1, keepdims=True) + NORM_EPS)
    return (xf * inv * gain).astype(BF)


def stack_pair(pair_t):
    half = pair_t.shape[0] // 2
    zero = jnp.zeros((half, pair_t.shape[1]), pair_t.dtype)
    return jnp.concatenate(
        [jnp.concatenate([pair_t[:half], zero], axis=0), jnp.concatenate([zero, pair_t[half:]], axis=0)], axis=1)


def unstack_pair(both):
    half, cols = both.shape[0] // 2, both.shape[1] // 2
    return jnp.concatenate([both[:half, :cols], both[half:, cols:]], axis=0)


def softmax_parts(scores, upper, bias0, bias1):
    s02 = jnp.where(upper, scores[:QB] + bias0, scores[2 * QB:])
    s1 = scores[QB:2 * QB] + bias1
    top = jnp.max(jnp.maximum(s02, s1), axis=0, keepdims=True)
    e02, e1 = jnp.exp(s02 - top), jnp.exp(s1 - top)
    inv = 1.0 / jnp.sum(e02 + e1, axis=0, keepdims=True)
    return e02 * inv, e1 * inv


def banded(p02, p1, upper):
    return jnp.concatenate(
        [jnp.where(upper, p02, 0.0).astype(BF), p1.astype(BF), jnp.where(upper, 0.0, p02).astype(BF)], axis=0)


def upper_mask():
    key_ids = lax.broadcasted_iota(jnp.int32, (QB, 2 * QB), 0)
    query_ids = lax.broadcasted_iota(jnp.int32, (QB, 2 * QB), 1) % QB
    return key_ids > query_ids


def start_bias(first, blk):
    bias = jnp.where(first, NEG, 0.0).astype(F32)
    return (bias if blk < 2 else 0.0), (bias if blk < 1 else 0.0)


def fwd_kernel(n, head_dim, x_h, pos, invf, ga, gm, wq_h, wk_h, wv_h, wo_h,
               q_h, kt_h, k_h, v_h, hat_h, ot_h, xm_h, hm_h, hmt_h, cos_t, sin_t,
               xv, halo, pos_halo, wq, wk, wv, wo, q, kt, k, v, vt, hat, ot, xm, hm, hmt, hb, hh, acc, acc2, ak, av, cos_h, sin_h,
               sc0, sc1, sc2, pb0, pb1, pb2, ldx, ld, st, snd, rcv):
    sc, pb = (sc0, sc1, sc2), (pb0, pb1, pb2)
    rows, toks, width = xv.shape
    ext, total, pw = toks + WINDOW, rows * toks, 2 * head_dim
    n_pairs = wq.shape[0] // pw
    tb, n_steps = toks // QB, n_pairs * rows
    me = lax.axis_index("seq")
    right, left = lax.rem(me + 1, n), lax.rem(me + n - 1, n)
    load_x = [pltpu.make_async_copy(x_h.at[b], xv.at[b], ldx.at[b]) for b in range(rows)]
    load_w = [pltpu.make_async_copy(s, d, ld.at[i]) for i, (s, d) in enumerate(((wq_h, wq), (wk_h, wk), (wv_h, wv), (wo_h, wo)))]
    for c in load_x + load_w:
        c.start()
    barrier = pltpu.get_barrier_semaphore()
    for other in (left, right):
        pl.semaphore_signal(barrier, inc=1, device_id={"seq": other}, device_id_type=MESH)
    pl.semaphore_wait(barrier, 2)

    def push(i, s, d):
        return pltpu.make_async_remote_copy(src_ref=s, dst_ref=d, send_sem=snd.at[i], recv_sem=rcv.at[i], device_id={"seq": right}, device_id_type=MESH)

    def push_rows(b):
        return push(b, x_h.at[b, toks - WINDOW:, :], halo.at[b])

    send_pos = push(rows, pos, pos_halo)
    send_pos.start()
    for b in range(rows):
        push_rows(b).start()

    def angles(cos_ref, sin_ref, positions):
        count = positions.shape[1]
        for b in range(rows):
            ang = invf[:] * positions[b:b + 1, :].astype(F32)
            cos_ref[:, b * count:(b + 1) * count] = jnp.cos(ang)
            sin_ref[:, b * count:(b + 1) * count] = jnp.sin(ang)

    angles(cos_t, sin_t, pos[:])

    def norm_blk(i):
        h = normed(xv[i // tb, pl.ds(pl.multiple_of(lax.rem(i, tb) * QB, QB), QB), :], ga[:])
        r = pl.ds(pl.multiple_of(i * QB, QB), QB)
        hb[r, :] = h
        hat[:, r] = h.T

    with jax.named_scope("f_norm"):
        for c in load_x:
            c.wait()
        cdiv_loop(total // QB, norm_blk)
    keep_hat = pltpu.make_async_copy(hat, hat_h, st.at[0])
    keep_hat.start()
    tables = cos_t[:], sin_t[:]

    def put_q(src):
        for p in range(n_pairs):
            r = slice(p * pw, (p + 1) * pw)
            q[r, :] = (rope(src[r, :], *tables, 1, head_dim) * (head_dim ** -0.5)).astype(BF)

    def put_own(src, dst_t, dst, turn):
        for p in range(n_pairs):
            r = slice(p * pw, (p + 1) * pw)
            both = (rope(src[r, :], *tables, 1, head_dim) if turn else src[r, :]).astype(BF)
            for b in range(rows):
                blk = both[:, b * toks:(b + 1) * toks]
                own = slice(b * ext + WINDOW, (b + 1) * ext)
                dst_t[r, own] = blk
                dst[own, r] = blk.T

    with jax.named_scope("f_mm"):
        load_w[0].wait()
        load_w[1].wait()
        load_w[2].wait()
        acc[:] = dot(wq[:], hb[:], NT)
        acc2[:] = dot(wk[:], hb[:], NT)
        put_q(acc)
        acc[:] = dot(wv[:], hb[:], NT)
        put_own(acc2, kt, k, True)
        put_own(acc, vt, v, False)
    keep_q = pltpu.make_async_copy(q, q_h, st.at[1])
    keep_q.start()
    send_pos.wait()
    angles(cos_h, sin_h, pos_halo[:, toks - WINDOW:])

    def keeps(b):
        wide, cols = pl.ds(pl.multiple_of(b * ext, QB), ext), pl.ds(pl.multiple_of(b * toks, QB), toks)
        ends = ((kt.at[:, wide], kt_h.at[:, wide]), (k.at[wide, :], k_h.at[wide, :]), (v.at[wide, :], v_h.at[wide, :]),
                (ot.at[:, cols], ot_h.at[:, cols]), (hm.at[cols, :], hm_h.at[cols, :]), (hmt.at[:, cols], hmt_h.at[:, cols]),
                (xm.at[cols, :], xm_h.at[cols, :]))
        return [pltpu.make_async_copy(s, d, st.at[2 + b * len(ends) + i]) for i, (s, d) in enumerate(ends)]

    def halo_in(b):
        with jax.named_scope("f_halo_wait"):
            push_rows(b).wait()
        with jax.named_scope("f_halo"):
            for i in range(WINDOW // QB):
                r = slice(i * QB, (i + 1) * QB)
                hh[r, :] = normed(halo[b, r, :], ga[:])
            ak[:] = dot(wk[:], hh[:], NT)
            av[:] = dot(wv[:], hh[:], NT)
            cols = pl.ds(pl.multiple_of(b * WINDOW, QB), WINDOW)
            wide = pl.ds(pl.multiple_of(b * ext, QB), WINDOW)
            near = cos_h[:, cols], sin_h[:, cols]
            for src, dst_t, dst in ((ak, kt, k), (av, vt, v)):
                for p in range(n_pairs):
                    r = slice(p * pw, (p + 1) * pw)
                    blk = (rope(src[r, :], *near, 1, head_dim) if dst is k else src[r, :]).astype(BF)
                    dst_t[r, wide] = blk
                    dst[wide, r] = blk.T
        for c in keeps(b)[:3]:
            c.start()

    upper = upper_mask()
    first = me == 0

    def spots(it, blk):
        b, p = it // n_pairs, mod(it, n_pairs)
        pr = pl.ds(aligned(p * pw, pw), pw)
        return pr, pl.ds(aligned(b * toks + blk * QB, QB), QB), pl.ds(aligned(b * ext + blk * QB, QB), 3 * QB)

    def score(it):
        for blk in range(tb):
            pr, cols, keys = spots(it, blk)
            sc[blk][:] = dot(k[keys, pr], stack_pair(q[pr, cols]))

    def soften(blk):
        p02, p1 = softmax_parts(sc[blk][:], upper, *start_bias(first, blk))
        pb[blk][:] = banded(p02, p1, upper)

    def mix(it):
        for blk in range(tb):
            pr, cols, keys = spots(it, blk)
            ot[pr, cols] = unstack_pair(dot(vt[pr, keys], pb[blk][:])).astype(BF)

    def project(b):
        cols = pl.ds(pl.multiple_of(b * toks, QB), toks)
        with jax.named_scope("f_proj"):
            mid = (xv[b].astype(F32) + dot(ot[:, cols], wo[:], TN)).astype(BF)
            xm[cols, :] = mid
            h = normed(mid, gm[:])
            hm[cols, :] = h
            hmt[:, cols] = h.T
        for c in keeps(b)[3:]:
            c.start()

    load_w[3].wait()
    for blk in range(tb):
        pb[blk][:] = jnp.zeros(pb[blk].shape, BF)

    def walk(i):
        it = i - 1

        @pl.when((lax.rem(i, n_pairs) == 0) & (i < n_steps))
        def _():
            halo_in(i // n_pairs)

        @pl.when(i == 0)
        def _():
            score(0)

        @pl.when((i > 0) & (i <= n_steps))
        def _():
            with jax.named_scope("f_attn"):
                mix(jnp.maximum(it - 1, 0))
                for blk in range(tb):
                    soften(blk)
                score(jnp.minimum(i, n_steps - 1))

        @pl.when(i > n_steps)
        def _():
            mix(n_steps - 1)

        @pl.when((lax.rem(it, n_pairs) == 0) & (it > 0))
        def _():
            project(it // n_pairs - 1)

    cdiv_loop(n_steps + 2, walk)
    with jax.named_scope("f_store_wait"):
        keep_hat.wait()
        keep_q.wait()
        for b in range(rows):
            for c in keeps(b):
                c.wait()


def any_spec(k):
    return [pl.BlockSpec(memory_space=pl.ANY)] * k


def vmem_spec(k):
    return [pl.BlockSpec(memory_space=pltpu.VMEM)] * k


def run_fwd(n, x, pos, invf, ga, gm, wq, wk, wv, wo, head_dim):
    rows, toks, width = x.shape
    hd = wq.shape[0]
    ext, total, n_halo = toks + WINDOW, rows * toks, rows * WINDOW
    half = head_dim // 2
    sds = lambda *s: jax.ShapeDtypeStruct(s, BF)
    dma = lambda *s: pltpu.SemaphoreType.DMA(s)
    outs = [sds(hd, total), sds(hd, rows * ext), sds(rows * ext, hd), sds(rows * ext, hd), sds(width, total), sds(hd, total), sds(total, width), sds(total, width), sds(width, total)]
    outs += [jax.ShapeDtypeStruct((half, total), F32)] * 2
    vm = lambda *s: pltpu.VMEM(s, BF)
    vf = lambda *s: pltpu.VMEM(s, F32)
    scratch = [vm(rows, toks, width), vm(rows, WINDOW, width), pltpu.VMEM((rows, toks), jnp.int32), vm(hd, width), vm(hd, width), vm(hd, width), vm(hd, width),
               vm(hd, total), vm(hd, rows * ext), vm(rows * ext, hd), vm(rows * ext, hd), vm(hd, rows * ext), vm(width, total), vm(hd, total), vm(total, width), vm(total, width), vm(width, total), vm(total, width), vm(WINDOW, width),
               vf(hd, total), vf(hd, total), vf(hd, WINDOW), vf(hd, WINDOW), vf(half, n_halo), vf(half, n_halo),
               *[vf(3 * QB, 2 * QB)] * 3, *[vm(3 * QB, 2 * QB)] * 3,
               dma(rows), dma(4), dma(2 + 7 * rows), dma(rows + 1), dma(rows + 1)]
    return pl.pallas_call(
        functools.partial(fwd_kernel, n, head_dim), out_shape=outs,
        in_specs=any_spec(1) + vmem_spec(4) + any_spec(4), out_specs=any_spec(9) + vmem_spec(2), scratch_shapes=scratch,
        compiler_params=pltpu.CompilerParams(collective_id=0, has_side_effects=True, vmem_limit_bytes=VMEM_LIMIT),
        name="forward")(x, pos, invf, ga, gm, wq, wk, wv, wo)


LAG = 2
SLOTS = 2 * LAG
RING = 8
CB = 256


def at(ref, *idx):
    return ref.at[idx]


class Torus:
    def __init__(self, n, pairs, turn, parts, recv0, recv1, recv2, recv3, recv4, acc, acc2, fin, snd, rcv):
        self.side = math.isqrt(n // 2)
        assert self.side == 4
        me = lax.axis_index("seq")
        self.core = lax.rem(me, 2)
        chip = me // 2
        self.x, self.y = lax.rem(chip, 4), chip // 4
        self.pairs, self.turn = pairs, turn
        self.parts, self.recv0, self.recv1, self.recv2, self.recv3, self.recv4 = parts, recv0, recv1, recv2, recv3, recv4
        self.acc, self.acc2, self.fin, self.snd, self.rcv = acc, acc2, fin, snd, rcv
        self.partner = me + 1 - 2 * self.core
        self.hops = {(axis, step): self.device(*((0, step) if axis == 0 else (step, 0))) for axis in (0, 1) for step in (1, 3)}

    def device(self, dy, dx):
        return (lax.rem(self.y + dy, 4) * 4 + lax.rem(self.x + dx, 4)) * 2 + self.core

    def peers(self):
        return [self.partner, *self.hops.values()]

    def copy(self, lane, kind, slot, src, dst, target):
        return pltpu.make_async_remote_copy(
            src_ref=src, dst_ref=dst, send_sem=self.snd.at[lane, kind, slot], recv_sem=self.rcv.at[lane, kind, slot],
            device_id={"seq": target}, device_id_type=MESH)

    def late(self, pair, yes, no):
        if isinstance(pair, int):
            return yes if pair >= self.turn else no
        return jnp.where(pair >= self.turn, yes, no)

    def swap(self, ring, slot):
        return self.copy(0, 0, slot, self.parts.at[ring, :, :, 1 - self.core], self.recv0.at[slot], self.partner)

    def copies(self, stage, kind, pair, held, slot):
        axis = kind if stage < 3 else 1 - kind
        plus, minus = self.hops[axis, 1], self.hops[axis, 3]
        half = CB // 2
        if stage == 1:
            if axis == 0:
                minus = self.late(pair, plus, minus)
            ends = [(self.acc.at[kind, held, 2, pl.ds(0, 2)], self.recv1), (self.acc.at[kind, held, 2, pl.ds(2, 2)], self.recv1)]
        elif stage == 2:
            ends = [(self.acc.at[kind, held, 1], self.recv2), (self.acc.at[kind, held, 3], self.recv2)]
        elif stage == 3:
            ends = [(self.acc2.at[kind, held, 2, :, pl.ds(0, half)], self.recv3), (self.acc2.at[kind, held, 2, :, pl.ds(half, half)], self.recv3)]
        else:
            ends = [(self.acc2.at[kind, held, 1], self.recv4), (self.acc2.at[kind, held, 3], self.recv4)]
        lane = 2 * stage - 1
        return [self.copy(lane + i, kind, slot, src, buf.at[kind, slot, i], (plus, minus)[i]) for i, (src, buf) in enumerate(ends)]

    def add(self, stage, kind, pair, held, slot, ring):
        acc, acc2 = self.acc, self.acc2
        if stage == 1:
            def row(r1):
                for r2 in range(4):
                    ry, rx = (r2, r1) if kind == 0 else (r1, r2)
                    chip = lax.rem(self.y + ry, 4) * 4 + lax.rem(self.x + rx, 4)
                    acc[kind, held, r1, r2] = self.parts[ring, kind, chip, self.core] + self.recv0[slot, kind, chip]
            cdiv_loop(4, row)
        elif stage == 2:
            back = self.late(pair, 1, 3) if kind == 0 else 3
            acc[kind, held, 1, 0:2] += self.recv1[kind, slot, 0]
            acc[kind, held, back, 2:4] += self.recv1[kind, slot, 1]
        elif stage == 3:
            acc2[kind, held] = acc[kind, held, 0] + (self.recv2[kind, slot, 0] + self.recv2[kind, slot, 1])
        elif stage == 4:
            half = CB // 2
            acc2[kind, held, 1, :, 0:half] += self.recv3[kind, slot, 0]
            acc2[kind, held, 3, :, half:] += self.recv3[kind, slot, 1]
        else:
            self.fin[pair, kind] = acc2[kind, held, 0] + (self.recv4[kind, slot, 0] + self.recv4[kind, slot, 1])

    def when(self, pair, fn):
        if isinstance(pair, int):
            if 0 <= pair < self.pairs:
                fn()
        else:
            pl.when((pair >= 0) & (pair < self.pairs))(fn)

    def tick(self, t):
        now, land = mod(t, SLOTS), mod(t + SLOTS - LAG, SLOTS)
        ring_now, ring_land = mod(t, RING), mod(t + RING - LAG, RING)
        for stage in range(5, -1, -1):
            pair = t - LAG * stage
            held = land if stage % 2 else now

            def move(stage=stage, pair=pair, held=held):
                if stage == 0:
                    self.swap(ring_now, now).start()
                    return
                if stage == 1:
                    with jax.named_scope("t_wait1"):
                        self.swap(ring_land, land).wait()
                for kind in (0, 1):
                    if stage > 1:
                        with jax.named_scope(f"t_wait{stage}"):
                            for c in self.copies(stage - 1, kind, pair, held, land):
                                c.wait()
                    self.add(stage, kind, pair, held, land, ring_land)
                    if stage < 5:
                        for c in self.copies(stage, kind, pair, held, now):
                            c.start()
            self.when(pair, move)


def pick(i, table):
    out = 0
    for key, value in table.items():
        out = jnp.where(i == key, value, out)
    return out


def norm_back(x, gain, grad, res):
    xf = x.astype(F32)
    inv = lax.rsqrt(jnp.mean(xf * xf, axis=-1, keepdims=True) + NORM_EPS)
    unit = xf * inv
    gu = grad * gain
    out = inv * (gu - unit * jnp.mean(gu * unit, axis=-1, keepdims=True)) + res.astype(F32)
    gu = grad * unit
    return out.astype(BF), jnp.sum(gu.reshape(gu.shape[0] // 8, 8, gu.shape[1]), axis=0)


def plan(n_mlp, n_down, nc, per):
    order = [("o", g) for g in range(nc)]
    for g in range(nc):
        order.append(("q", g))
        if 0 < g < nc - 1:
            order += [("k", g - 1), ("v", g - 1)]
    rest = range(max(nc - 2, 0), nc)
    for g in rest:
        order += [("k", g), ("v", g)]
    base = n_mlp + n_down
    place = {name: (base + i // 2, i % 2) for i, name in enumerate(order)}
    return base, place, rest, base + len(order) // 2


def bwd_kernel(n, head_dim, dims, ga, gm, x_h, dout_h, q_h, kt_h, k_h, v_h, hat_h, ot_h, xm_h, hm_h, hmt_h, cos_i, sin_i,
               wq_h, wk_h, wv_h, wo_h, wg_h, wu_h, wd_h,
               dx_h, fin, dga_o, dgm_o,
               parts, recv0, recv1, recv2, recv3, recv4, acc, acc2, snd, rcv,
               hk_recv, hv_recv, hsnd, hrcv, gsend, grecv, gsem, ld, xbuf, mbuf, gnm, gmid, ot, hat, wo, dgain):
    rows, toks, width, hd, ff = dims
    ext, total = toks + WINDOW, rows * toks
    pw = 2 * head_dim
    n_pairs = hd // pw
    nb, nc, sub = ff // CB, width // CB, ff // width
    rpd = width // n
    n_mlp, n_down = nb, nc * sub // 2
    per, half_sub = CB // pw, sub // 2
    base, place, rest, pairs = plan(n_mlp, n_down, nc, per)
    comm = Torus(n, pairs, base - 2, parts, recv0, recv1, recv2, recv3, recv4, acc, acc2, fin, snd, rcv)
    me = lax.axis_index("seq")
    left = lax.rem(me + n - 1, n)
    barrier = pltpu.get_barrier_semaphore()

    def greet(i):
        pl.semaphore_signal(barrier, inc=1, device_id={"seq": lax.rem(me + i + 1, n)}, device_id_type=MESH)

    def load(i, s, d):
        c = pltpu.make_async_copy(s, d, ld.at[i])
        c.start()
        return c

    def put(spot, value):
        pair, kind = spot
        parts[mod(pair, RING), kind] = value.reshape(n // 2, 2, rpd, CB)

    def late(i):
        s, d = ((xm_h, mbuf), (ot_h, ot), (hat_h, hat), (wo_h, wo))[i]
        return pltpu.make_async_copy(s, d, ld.at[1 + i])

    def mlp(hm, hmt, actt, wgu, wd, dgu, wld):
        def weights(j, slot):
            c = aligned(j * CB, CB)
            return [pltpu.make_async_copy(wg_h.at[:, pl.ds(c, CB)], wgu.at[slot, :, pl.ds(0, CB)], wld.at[slot, 0]),
                    pltpu.make_async_copy(wu_h.at[:, pl.ds(c, CB)], wgu.at[slot, :, pl.ds(CB, CB)], wld.at[slot, 1]),
                    pltpu.make_async_copy(wd_h.at[pl.ds(c, CB), :], wd.at[slot], wld.at[slot, 2])]

        for c in weights(0, 0):
            c.start()
        ld_hm, ld_x, ld_hmt = load(5, hm_h, hm), load(0, dout_h, xbuf), load(6, hmt_h, hmt)
        for i in range(4):
            late(i).start()
        cdiv_loop(n - 1, greet)
        gnm[:] = jnp.zeros_like(gnm)
        gsend[:] = jnp.zeros_like(gsend)
        dgain[:] = jnp.zeros_like(dgain)
        ld_hm.wait()
        ld_x.wait()
        ld_hmt.wait()

        def block(j):
            slot = lax.rem(j, 2)
            for c in weights(j, slot):
                c.wait()

            @pl.when(j + 1 < nb)
            def _():
                for c in weights(j + 1, 1 - slot):
                    c.start()

            c0 = pl.multiple_of(j * CB, CB)
            with jax.named_scope("b_mlp"):
                for b in range(rows):
                    r = slice(b * toks, (b + 1) * toks)
                    gu = dot(hm[r, :], wgu[slot])
                    gact = dot(xbuf[r, :], wd[slot], NT).astype(BF).astype(F32)
                    gate, up = gu[:, :CB], gu[:, CB:]
                    sig = 1.0 / (1.0 + jnp.exp(-gate))
                    swish = gate * sig
                    actt[pl.ds(c0, CB), r] = (swish * up).astype(BF).T
                    dgu[r, :CB] = (gact * up * (sig + swish * (1.0 - sig))).astype(BF)
                    dgu[r, CB:] = (gact * swish).astype(BF)
                both = dot(hmt[:], dgu[:])
                ring = lax.rem(j, RING)
                parts[ring, 0] = both[:, :CB].reshape(n // 2, 2, rpd, CB)
                parts[ring, 1] = both[:, CB:].reshape(n // 2, 2, rpd, CB)
                for b in range(rows):
                    r = slice(b * toks, (b + 1) * toks)
                    gnm[r, :] += dot(dgu[r, :], wgu[slot], NT)

            @pl.when(j == 0)
            def _():
                pl.semaphore_wait(barrier, n - 1)

            comm.tick(j)

        cdiv_loop(nb, block)

        def down(c):
            share = n // 2 // sub
            c0 = pl.multiple_of(c * CB, CB)
            for m in range(sub):
                res = dot(actt[m * width:(m + 1) * width, :], xbuf[:, pl.ds(c0, CB)]).reshape(share, 2, sub, rpd, CB)
                for i in range(sub):
                    pair = n_mlp + c * half_sub + i // 2
                    parts[lax.rem(pair, RING), i % 2, m * share:(m + 1) * share] = res[:, :, i]

        late(0).wait()

        def mid(i):
            r = pl.ds(pl.multiple_of(i * QB, QB), QB)
            out, dg = norm_back(mbuf[r, :], gm[:], gnm[r, :], xbuf[r, :])
            gmid[r, :] = out
            dgain[8:16, :] += dg

        def column(c):
            with jax.named_scope("b_down"):
                down(c)

            @pl.when(c == 0)
            def _():
                with jax.named_scope("b_mid"):
                    cdiv_loop(total // QB, mid)

            @pl.when(lax.rem(c, 2) == 0)
            def _():
                comm.tick(nb + c // 2)

        cdiv_loop(nc, column)

    vm = lambda *s: pltpu.VMEM(s, BF)
    vf = lambda *s: pltpu.VMEM(s, F32)
    pl.run_scoped(mlp, vm(total, width), vm(width, total), vm(ff, total), vm(2, width, 2 * CB), vm(2, CB, width), vm(total, 2 * CB),
                  pltpu.SemaphoreType.DMA((2, 3)))

    def attention(q, kt, k, v, dot_, dk, dv, hk, hv,
                  sc0, sc1, sc2, dp0, dp1, dp2, pb0, pb1, pb2, ds0, ds1, ds2):
        dqt, dkt = ot, q
        wq, wk, wv = k.at[:hd], kt.at[:, :width], v.at[:hd]
        sc, dp, pb, ds = (sc0, sc1, sc2), (dp0, dp1, dp2), (pb0, pb1, pb2), (ds0, ds1, ds2)
        lds = [load(5 + i, s, d) for i, (s, d) in enumerate(((q_h, q), (kt_h, kt), (k_h, k), (v_h, v)))]
        ld_x2 = load(0, x_h, xbuf)
        late(1).wait()
        late(3).wait()
        with jax.named_scope("b_dot"):
            dot_[:] = dot(wo[:], gmid[:], NT).astype(BF)
        def out_grad(g):
            spot = pick(g, {i: place["o", i][0] for i in range(nc)}), pick(g, {i: place["o", i][1] for i in range(nc)})
            put(spot, dot(ot[:], gmid[:, pl.ds(pl.multiple_of(g * CB, CB), CB)]))

        with jax.named_scope("b_dwo"):
            cdiv_loop(nc, out_grad)
        head = nb + (nc + 1) // 2
        comm.tick(head)
        for c in lds:
            c.wait()
        late(2).wait()
        upper = upper_mask()
        first = me == 0
        tb = toks // QB
        n_steps = n_pairs * rows

        def spots(it, blk):
            p, b = it // rows, mod(it, rows)
            pr = pl.ds(aligned(p * pw, pw), pw)
            return pr, pl.ds(aligned(b * toks + blk * QB, QB), QB), pl.ds(aligned(b * ext + blk * QB, QB), 3 * QB)

        def score(it):
            for blk in range(tb):
                pr, cols, keys = spots(it, blk)
                sc[blk][:] = dot(k[keys, pr], stack_pair(q[pr, cols]))
                dp[blk][:] = dot(v[keys, pr], stack_pair(dot_[pr, cols]))

        def soften(blk):
            p02, p1 = softmax_parts(sc[blk][:], upper, *start_bias(first, blk))
            g02, g1 = jnp.where(upper, dp[blk][:QB], dp[blk][2 * QB:]), dp[blk][QB:2 * QB]
            mean = jnp.sum(p02 * g02 + p1 * g1, axis=0, keepdims=True)
            pb[blk][:] = banded(p02, p1, upper)
            ds[blk][:] = banded(p02 * (g02 - mean), p1 * (g1 - mean), upper)

        def grads(it):
            p, b = it // rows, mod(it, rows)
            ks, vs = [], []
            for blk in range(tb):
                pr, cols, keys = spots(it, blk)
                vs.append(dot(pb[blk][:], stack_pair(dot_[pr, cols]), NT))
                ks.append(dot(ds[blk][:], stack_pair(q[pr, cols]), NT))
                dq = unstack_pair(dot(kt[pr, keys], ds[blk][:])) * (head_dim ** -0.5)
                dqt[pr, cols] = rope(dq, cos_i[:, cols], sin_i[:, cols], -1, head_dim).astype(BF)
            for parts_, own, halo in ((ks, dk, hk), (vs, dv, hv)):
                for j in range(tb + 2):
                    val = sum(parts_[i][(j - i) * QB:(j - i + 1) * QB] for i in range(tb) if 0 <= j - i < 3).astype(BF)
                    if j < 2:
                        halo[p, b, j * QB:(j + 1) * QB, :] = val
                    else:
                        own[pl.ds(aligned(b * toks + (j - 2) * QB, QB), QB), pr] = val

        def halo_copies(p):
            return [pltpu.make_async_remote_copy(src_ref=s.at[p], dst_ref=d.at[p], send_sem=hsnd.at[i, p], recv_sem=hrcv.at[i, p],
                                                 device_id={"seq": left}, device_id_type=MESH)
                    for i, (s, d) in enumerate(((hk, hk_recv), (hv, hv_recv)))]

        def finish(p):
            r = pl.multiple_of(p * pw, pw)
            with jax.named_scope("b_hwait"):
                for c in halo_copies(p):
                    c.wait()
            for b in range(rows):
                for blk in range(tb):
                    cols = slice(b * toks + blk * QB, b * toks + (blk + 1) * QB)
                    gk = dk[cols, pl.ds(r, pw)].astype(F32)
                    off = blk * QB - (toks - WINDOW)
                    if off >= 0:
                        gk = gk + hk_recv[p, b, off:off + QB, :].astype(F32)
                        gv = dv[cols, pl.ds(r, pw)].astype(F32) + hv_recv[p, b, off:off + QB, :].astype(F32)
                        dv[cols, pl.ds(r, pw)] = gv.astype(BF)
                    dkt[pl.ds(r, pw), cols] = rope(gk.T, cos_i[:, cols], sin_i[:, cols], -1, head_dim).astype(BF)

        def spot_of(name, g):
            known = {i: place[name, i] for i in range(nc)}
            return pick(g, {i: s[0] for i, s in known.items()}), pick(g, {i: s[1] for i, s in known.items()})

        def close_group(g):
            with jax.named_scope("b_finish"):
                cdiv_loop(per, lambda i: finish(g * per + i))
            cols = pl.ds(pl.multiple_of(g * CB, CB), CB)
            with jax.named_scope("b_dwkv"):
                put(spot_of("k", g), dot(hat[:], dkt[cols, :], NT))
                put(spot_of("v", g), dot(hat[:], dv[:, cols]))

        def step(p):
            for c in halo_copies(p):
                c.start()
            g = p // per

            @pl.when(lax.rem(p, per) == per - 1)
            def _():
                with jax.named_scope("b_dwq"):
                    put(spot_of("q", g), dot(hat[:], dqt[pl.ds(pl.multiple_of(g * CB, CB), CB), :], NT))

                if rest[0] > 0:
                    @pl.when((g > 0) & (g <= rest[0]))
                    def _():
                        close_group(g - 1)

            comm.tick(head + 1 + p)

        def weights():
            return [pltpu.make_async_copy(s, d, ld.at[9 + i]) for i, (s, d) in enumerate(((wq_h, wq), (wk_h, wk), (wv_h, wv)))]

        def walk(it):
            @pl.when(it < n_steps)
            def _():
                with jax.named_scope("b_attn"):
                    grads(jnp.maximum(it - 1, 0))
                    for blk in range(tb):
                        soften(blk)
                    score(jnp.minimum(it + 1, n_steps - 1))

            @pl.when(it == n_steps)
            def _():
                grads(n_steps - 1)
                for c in weights():
                    c.start()

            @pl.when((lax.rem(it, rows) == 0) & (it > 0))
            def _():
                step(it // rows - 1)

        for blk in range(tb):
            pb[blk][:] = jnp.zeros(pb[blk].shape, BF)
            ds[blk][:] = jnp.zeros(ds[blk].shape, BF)
        score(0)
        cdiv_loop(n_steps + 1, walk)
        for c in weights():
            c.wait()
        ld_x2.wait()

        def into_q(b):
            r = pl.ds(pl.multiple_of(b * toks, QB), toks)
            gnm[r, :] = dot(dqt[:, r], wq[:], TN)

        with jax.named_scope("b_intoq"):
            cdiv_loop(rows, into_q)

        after = head + 1 + n_pairs
        if after < place["k", rest[0]][0]:
            comm.tick(after)
            after += 1
        assert after + len(rest) == pairs

        def close_rest(i):
            close_group(rest[0] + i)
            comm.tick(after + i)

        cdiv_loop(len(rest), close_rest)

        def into(b):
            r = pl.ds(pl.multiple_of(b * toks, QB), toks)
            with jax.named_scope("b_into"):
                gnm[r, :] += dot(dkt[:, r], wk[:], TN) + dot(dv[r, :], wv[:])

            def final(i):
                r = pl.ds(pl.multiple_of((b * tb + i) * QB, QB), QB)
                out, dg = norm_back(xbuf[r, :], ga[:], gnm[r, :], gmid[r, :])
                mbuf[r, :] = out
                dgain[0:8, :] += dg

            with jax.named_scope("b_final"):
                cdiv_loop(tb, final)
            comm.tick(pairs + b)

        cdiv_loop(rows, into)

    score_bufs = [vf(3 * QB, 2 * QB)] * 6 + [vm(3 * QB, 2 * QB)] * 6
    pl.run_scoped(attention, vm(hd, total), vm(hd, rows * ext), vm(rows * ext, hd), vm(rows * ext, hd), vm(hd, total),
                  vm(total, hd), vm(total, hd), vm(n_pairs, rows, WINDOW, pw), vm(n_pairs, rows, WINDOW, pw), *score_bufs)
    out_copy = load(1, mbuf, dx_h)
    gains = jnp.concatenate([jnp.sum(dgain[0:8, :], axis=0, keepdims=True), jnp.sum(dgain[8:16, :], axis=0, keepdims=True), jnp.zeros((6, width), F32)], axis=0)
    for p in range(n):
        gsend[p, :, 0:rpd] = gains[:, p * rpd:(p + 1) * rpd]

    def spread(i):
        to = lax.rem(me + i + 1, n)
        pltpu.make_async_remote_copy(src_ref=gsend.at[to], dst_ref=grecv.at[i], send_sem=gsem.at[0], recv_sem=gsem.at[1],
                                     device_id={"seq": to}, device_id_type=MESH).start()

    cdiv_loop(n - 1, spread)
    lax.fori_loop(pairs + rows, pairs + 5 * LAG, lambda t, c: (comm.tick(t), c)[1], 0)
    with jax.named_scope("b_gain"):
        pltpu.make_async_remote_copy(src_ref=gsend.at[pl.ds(0, n - 1)], dst_ref=grecv, send_sem=gsem.at[0], recv_sem=gsem.at[1],
                                     device_id={"seq": left}, device_id_type=MESH).wait()
    sums = gsend[me]
    for i in range(n - 1):
        sums = sums + grecv[i]
    dga_o[:] = sums[0:1, 0:rpd]
    dgm_o[:] = sums[1:2, 0:rpd]
    out_copy.wait()


def spread_kernel(dims, dx_i, fin_i, dga_i, dgm_i, dx_o, dga_o, dgm_o, dq_o, dk_o, dv_o, do_o, dg_o, du_o, dd_o, buf, fin, sem):
    head_dim, n, width, ff = dims
    nb, nc, sub = ff // CB, width // CB, ff // width
    rpd = width // n
    n_mlp, n_down = nb, nc * sub // 2
    place = plan(n_mlp, n_down, nc, CB // (2 * head_dim))[1]
    get, get_fin, out = (pltpu.make_async_copy(*ends, sem.at[i]) for i, ends in enumerate(((dx_i, buf), (fin_i, fin), (buf, dx_o))))
    get_fin.start()
    get.start()
    dga_o[:] = dga_i[:]
    dgm_o[:] = dgm_i[:]
    get.wait()
    out.start()
    get_fin.wait()
    for j in range(nb):
        dg_o[:, j * CB:(j + 1) * CB] = fin[j, 0]
        du_o[:, j * CB:(j + 1) * CB] = fin[j, 1]
    for c in range(nc):
        for i in range(sub):
            dd_o[i * rpd:(i + 1) * rpd, c * CB:(c + 1) * CB] = fin[n_mlp + (c * sub + i) // 2, i % 2]
    for g in range(nc):
        do_o[:, g * CB:(g + 1) * CB] = fin[place["o", g]]
        for name, ref in (("q", dq_o), ("k", dk_o), ("v", dv_o)):
            val = fin[place[name, g]]
            for h in range(CB // head_dim):
                ref[g * (CB // head_dim) + h] = val[:, h * head_dim:(h + 1) * head_dim]
    out.wait()


def run_bwd(n, head_dim, ga, gm, x, dout, q, kt, k, v, hat, ot, xm, hm, hmt, cos_t, sin_t, wq, wk, wv, wo, wg, wu, wd, rows):
    total, width = x.shape
    hd, ff = wq.shape[0], wg.shape[1]
    toks = total // rows
    rpd, heads = width // n, hd // head_dim
    nb, nc, sub = ff // CB, width // CB, ff // width
    pairs = plan(nb, nc * sub // 2, nc, CB // (2 * head_dim))[3]
    n_pairs = hd // (2 * head_dim)
    f = lambda *s: jax.ShapeDtypeStruct(s, F32)
    dx_t = jax.ShapeDtypeStruct((total, width), BF)
    vm = lambda *s: pltpu.VMEM(s, BF)
    vf = lambda *s: pltpu.VMEM(s, F32)
    dma = lambda *s: pltpu.SemaphoreType.DMA(s)
    scratch = [vf(RING, 2, n // 2, 2, rpd, CB), vf(SLOTS, 2, n // 2, rpd, CB), vf(2, SLOTS, 2, 2, rpd, CB), vf(2, SLOTS, 2, 4, rpd, CB),
               vf(2, SLOTS, 2, rpd, CB // 2), vf(2, SLOTS, 2, rpd, CB), vf(2, SLOTS, 4, 4, rpd, CB), vf(2, SLOTS, 4, rpd, CB),
               dma(9, 2, SLOTS), dma(9, 2, SLOTS),
               vm(n_pairs, rows, WINDOW, 2 * head_dim), vm(n_pairs, rows, WINDOW, 2 * head_dim), dma(2, n_pairs), dma(2, n_pairs),
               vf(n, 8, 128), vf(n - 1, 8, 128), dma(2), dma(12),
               vm(total, width), vm(total, width), vf(total, width), vm(total, width), vm(hd, total), vm(width, total), vm(hd, width), vf(16, width)]
    mid = pl.pallas_call(
        functools.partial(bwd_kernel, n, head_dim, (rows, toks, width, hd, ff)), out_shape=[dx_t, f(pairs, 2, rpd, CB), f(1, rpd), f(1, rpd)],
        in_specs=vmem_spec(2) + any_spec(11) + vmem_spec(2) + any_spec(7), out_specs=any_spec(1) + vmem_spec(3), scratch_shapes=scratch,
        compiler_params=pltpu.CompilerParams(collective_id=1, has_side_effects=True, vmem_limit_bytes=VMEM_LIMIT),
        name="backward")(ga, gm, x, dout, q, kt, k, v, hat, ot, xm, hm, hmt, cos_t, sin_t, wq, wk, wv, wo, wg, wu, wd)
    outs = [dx_t, f(1, rpd), f(1, rpd)] + [f(heads, rpd, head_dim)] * 3 + [f(rpd, width), f(rpd, ff), f(rpd, ff), f(ff // n, width)]
    return pl.pallas_call(
        functools.partial(spread_kernel, (head_dim, n, width, ff)), out_shape=outs,
        in_specs=any_spec(2) + vmem_spec(2), out_specs=any_spec(1) + vmem_spec(9), scratch_shapes=[vm(total, width), vf(pairs, 2, rpd, CB), dma(3)],
        name="spread")(*mid)


def solution(mesh):
    n = mesh.shape["seq"]

    def device_step(hidden, positions, g_attn, g_mlp, w_query, w_key, w_value, w_out, w_gate, w_up, w_down, d_out):
        rows, toks, width = hidden.shape
        layers, _, heads, head_dim = w_query.shape
        hd = heads * head_dim
        half = head_dim // 2
        inv_freq = 1.0 / (10000.0 ** (jnp.arange(half, dtype=F32) * (2.0 / head_dim)))
        turn = lambda w: w[0].transpose(1, 2, 0).reshape(hd, width)
        wq, wk, wv = turn(w_query), turn(w_key), turn(w_value)
        fwd = run_fwd(n, hidden, positions, inv_freq[:, None], g_attn, g_mlp, wq, wk, wv, w_out[0], head_dim)
        out = run_bwd(n, head_dim, g_attn, g_mlp, hidden.reshape(rows * toks, width), d_out.reshape(rows * toks, width), *fwd,
                      wq, wk, wv, w_out[0], w_gate[0], w_up[0], w_down[0], rows)
        dx, dga, dgm, dq, dk, dv, do, dg, du, dd = out
        back = lambda w: w.transpose(1, 0, 2)[None]
        return (dx.reshape(rows, toks, width), dga, dgm, back(dq), back(dk), back(dv), do[None], dg[None], du[None], dd[None])

    tok_spec = P("data", "seq", None)
    vec_spec = P(None, ("data", "seq"))
    mat_spec = P(None, ("data", "seq"), None)
    head_spec = P(None, ("data", "seq"), None, None)
    in_specs = (tok_spec, P("data", "seq")) + (P(),) * 9 + (tok_spec,)
    out_specs = (tok_spec, vec_spec, vec_spec, head_spec, head_spec, head_spec, mat_spec, mat_spec, mat_spec, mat_spec)
    return jax.shard_map(device_step, mesh=mesh, in_specs=in_specs, out_specs=out_specs, check_vma=False)
```

```python
import functools, math
import numpy as np
import jax, jax.numpy as jnp
from jax import lax
from jax.experimental import pallas as pl
from jax.experimental.pallas import tpu as pltpu
from jax.sharding import PartitionSpec as P

WINDOW = 256
NORM_EPS = 1e-5
QB = 128
BF, F32 = jnp.bfloat16, jnp.float32
NN, NT, TN = ((1,), (0,)), ((1,), (1,)), ((0,), (0,))
MESH = pl.DeviceIdType.MESH
NEG = -1e30
VMEM_LIMIT = 67043328


def dot(a, b, dims=NN):
    return lax.dot_general(a, b, (dims, ((), ())), preferred_element_type=F32)


def cdiv_loop(n, body):
    lax.fori_loop(0, n, lambda i, c: (body(i), c)[1], 0)


def mod(a, b):
    return a % b if isinstance(a, int) else lax.rem(a, b)


def aligned(a, b):
    return a if isinstance(a, int) else pl.multiple_of(a, b)


def rope(blk, cos_b, sin_b, sign, head_dim):
    half = head_dim // 2
    parts = []
    for h in range(blk.shape[0] // head_dim):
        first = blk[h * head_dim:h * head_dim + half]
        second = blk[h * head_dim + half:(h + 1) * head_dim]
        if sign > 0:
            parts += [first * cos_b - second * sin_b, second * cos_b + first * sin_b]
        else:
            parts += [first * cos_b + second * sin_b, second * cos_b - first * sin_b]
    return jnp.concatenate(parts, axis=0)


def normed(x, gain):
    xf = x.astype(F32)
    inv = lax.rsqrt(jnp.mean(xf * xf, axis=-1, keepdims=True) + NORM_EPS)
    return (xf * inv * gain).astype(BF)


def stack_pair(pair_t):
    half = pair_t.shape[0] // 2
    zero = jnp.zeros((half, pair_t.shape[1]), pair_t.dtype)
    return jnp.concatenate(
        [jnp.concatenate([pair_t[:half], zero], axis=0), jnp.concatenate([zero, pair_t[half:]], axis=0)], axis=1)


def unstack_pair(both):
    half, cols = both.shape[0] // 2, both.shape[1] // 2
    return jnp.concatenate([both[:half, :cols], both[half:, cols:]], axis=0)


def col_sum(x):
    return jnp.sum(x, axis=0, keepdims=True)


def merged(scores, upper, bias0, bias1):
    return jnp.where(upper, scores[:QB] + bias0, scores[2 * QB:]), scores[QB:2 * QB] + bias1


def banded(p02, p1, upper):
    return jnp.concatenate(
        [jnp.where(upper, p02, 0.0).astype(BF), p1.astype(BF), jnp.where(upper, 0.0, p02).astype(BF)], axis=0)


def upper_mask():
    key_ids = lax.broadcasted_iota(jnp.int32, (QB, 2 * QB), 0)
    query_ids = lax.broadcasted_iota(jnp.int32, (QB, 2 * QB), 1) % QB
    return key_ids > query_ids


def start_bias(first, blk):
    bias = jnp.where(first, NEG, 0.0).astype(F32)
    return (bias if blk < 2 else 0.0), (bias if blk < 1 else 0.0)


def fwd_kernel(n, head_dim, x_h, pos, invf, ga, gm, wq_h, wk_h, wv_h, wo_h,
               q_h, kt_h, k_h, v_h, hat_h, ot_h, xm_h, hm_h, hmt_h, qr_h, lse_h, cos_t, sin_t,
               xv, halo, qr, lse, pos_halo, wq, wk, wv, wo, q, kt, k, v, vt, hat, ot, xm, hm, hmt, hb, hh, acc, acc2, ak, av, cos_h, sin_h,
               sc0, sc1, sc2, pb0, pb1, pb2, ldx, ld, st, snd, rcv, qsnd, qrcv):
    sc, pb = (sc0, sc1, sc2), (pb0, pb1, pb2)
    rows, toks, width = xv.shape
    ext, total, pw = toks + WINDOW, rows * toks, 2 * head_dim
    n_pairs = wq.shape[0] // pw
    tb, n_steps = toks // QB, n_pairs * rows
    me = lax.axis_index("seq")
    right, left = lax.rem(me + 1, n), lax.rem(me + n - 1, n)
    load_x = [pltpu.make_async_copy(x_h.at[b], xv.at[b], ldx.at[b]) for b in range(rows)]
    load_w = [pltpu.make_async_copy(s, d, ld.at[i]) for i, (s, d) in enumerate(((wq_h, wq), (wk_h, wk), (wv_h, wv), (wo_h, wo)))]
    for c in load_x:
        c.start()
    barrier = pltpu.get_barrier_semaphore()
    for other in (left, right):
        pl.semaphore_signal(barrier, inc=1, device_id={"seq": other}, device_id_type=MESH)
    pl.semaphore_wait(barrier, 2)

    def push(i, s, d):
        return pltpu.make_async_remote_copy(src_ref=s, dst_ref=d, send_sem=snd.at[i], recv_sem=rcv.at[i], device_id={"seq": right}, device_id_type=MESH)

    def push_rows(b):
        return push(b, x_h.at[b, toks - WINDOW:, :], halo.at[b])

    send_pos = push(rows, pos, pos_halo)
    send_pos.start()
    for b in range(rows):
        push_rows(b).start()

    def angles(cos_ref, sin_ref, positions):
        count = positions.shape[1]
        for b in range(rows):
            ang = invf[:] * positions[b:b + 1, :].astype(F32)
            cos_ref[:, b * count:(b + 1) * count] = jnp.cos(ang)
            sin_ref[:, b * count:(b + 1) * count] = jnp.sin(ang)

    angles(cos_t, sin_t, pos[:])

    def norm_blk(i):
        h = normed(xv[i // tb, pl.ds(pl.multiple_of(lax.rem(i, tb) * QB, QB), QB), :], ga[:])
        r = pl.ds(pl.multiple_of(i * QB, QB), QB)
        hb[r, :] = h
        hat[:, r] = h.T

    with jax.named_scope("f_norm"):
        for c in load_x:
            c.wait()
        for c in load_w:
            c.start()
        cdiv_loop(total // QB, norm_blk)
    keep_hat = pltpu.make_async_copy(hat, hat_h, st.at[0])
    keep_hat.start()
    tables = cos_t[:], sin_t[:]

    def put_q(src):
        for p in range(n_pairs):
            r = slice(p * pw, (p + 1) * pw)
            q[r, :] = (rope(src[r, :], *tables, 1, head_dim) * (head_dim ** -0.5)).astype(BF)

    def put_own(src, dst_t, dst, turn):
        for p in range(n_pairs):
            r = slice(p * pw, (p + 1) * pw)
            both = (rope(src[r, :], *tables, 1, head_dim) if turn else src[r, :]).astype(BF)
            for b in range(rows):
                blk = both[:, b * toks:(b + 1) * toks]
                own = slice(b * ext + WINDOW, (b + 1) * ext)
                dst_t[r, own] = blk
                dst[own, r] = blk.T

    with jax.named_scope("f_mm"):
        load_w[0].wait()
        load_w[1].wait()
        load_w[2].wait()
        acc[:] = dot(wq[:], hb[:], NT)
        acc2[:] = dot(wk[:], hb[:], NT)
        put_q(acc)
        acc[:] = dot(wv[:], hb[:], NT)
        put_own(acc2, kt, k, True)
        put_own(acc, vt, v, False)
    keep_q = pltpu.make_async_copy(q, q_h, st.at[1])
    keep_q.start()

    def push_q(b):
        return pltpu.make_async_remote_copy(src_ref=q.at[:, b * toks:b * toks + WINDOW], dst_ref=qr.at[:, b * WINDOW:(b + 1) * WINDOW],
                                            send_sem=qsnd.at[b], recv_sem=qrcv.at[b], device_id={"seq": left}, device_id_type=MESH)

    for b in range(rows):
        push_q(b).start()
    send_pos.wait()
    angles(cos_h, sin_h, pos_halo[:, toks - WINDOW:])

    def keeps(b):
        wide, cols = pl.ds(pl.multiple_of(b * ext, QB), ext), pl.ds(pl.multiple_of(b * toks, QB), toks)
        ends = ((kt.at[:, wide], kt_h.at[:, wide]), (k.at[wide, :], k_h.at[wide, :]), (v.at[wide, :], v_h.at[wide, :]),
                (ot.at[:, cols], ot_h.at[:, cols]), (hm.at[cols, :], hm_h.at[cols, :]), (hmt.at[:, cols], hmt_h.at[:, cols]),
                (xm.at[cols, :], xm_h.at[cols, :]))
        return [pltpu.make_async_copy(s, d, st.at[2 + b * len(ends) + i]) for i, (s, d) in enumerate(ends)]

    def halo_in(b):
        with jax.named_scope("f_halo_wait"):
            push_rows(b).wait()
        with jax.named_scope("f_halo"):
            for i in range(WINDOW // QB):
                r = slice(i * QB, (i + 1) * QB)
                hh[r, :] = normed(halo[b, r, :], ga[:])
            ak[:] = dot(wk[:], hh[:], NT)
            av[:] = dot(wv[:], hh[:], NT)
            cols = pl.ds(pl.multiple_of(b * WINDOW, QB), WINDOW)
            wide = pl.ds(pl.multiple_of(b * ext, QB), WINDOW)
            near = cos_h[:, cols], sin_h[:, cols]
            for src, dst_t, dst in ((ak, kt, k), (av, vt, v)):
                for p in range(n_pairs):
                    r = slice(p * pw, (p + 1) * pw)
                    blk = (rope(src[r, :], *near, 1, head_dim) if dst is k else src[r, :]).astype(BF)
                    dst_t[r, wide] = blk
                    dst[wide, r] = blk.T
        for c in keeps(b)[:3]:
            c.start()

    upper = upper_mask()
    first = me == 0

    def spots(it, blk):
        b, p = it // n_pairs, mod(it, n_pairs)
        pr = pl.ds(aligned(p * pw, pw), pw)
        return pr, pl.ds(aligned(b * toks + blk * QB, QB), QB), pl.ds(aligned(b * ext + blk * QB, QB), 3 * QB)

    def score(it):
        for blk in range(tb):
            pr, cols, keys = spots(it, blk)
            sc[blk][:] = dot(k[keys, pr], stack_pair(q[pr, cols]))

    def soften(it, blk):
        s02, s1 = merged(sc[blk][:], upper, *start_bias(first, blk))
        top = jnp.max(jnp.maximum(s02, s1), axis=0, keepdims=True)
        e02, e1 = jnp.exp(s02 - top), jnp.exp(s1 - top)
        mass = col_sum(e02 + e1)
        inv = 1.0 / mass
        lse[it, blk:blk + 1, :] = top + jnp.log(mass)
        pb[blk][:] = banded(e02 * inv, e1 * inv, upper)

    def mix(it):
        for blk in range(tb):
            pr, cols, keys = spots(it, blk)
            ot[pr, cols] = unstack_pair(dot(vt[pr, keys], pb[blk][:])).astype(BF)

    def project(b):
        cols = pl.ds(pl.multiple_of(b * toks, QB), toks)
        with jax.named_scope("f_proj"):
            mid = (xv[b].astype(F32) + dot(ot[:, cols], wo[:], TN)).astype(BF)
            xm[cols, :] = mid
            h = normed(mid, gm[:])
            hm[cols, :] = h
            hmt[:, cols] = h.T
        for c in keeps(b)[3:]:
            c.start()

    load_w[3].wait()
    for blk in range(tb):
        pb[blk][:] = jnp.zeros(pb[blk].shape, BF)

    def walk(i):
        it = i - 1

        @pl.when((lax.rem(i, n_pairs) == 0) & (i < n_steps))
        def _():
            halo_in(i // n_pairs)

        @pl.when(i == 0)
        def _():
            score(0)

        @pl.when((i > 0) & (i <= n_steps))
        def _():
            with jax.named_scope("f_attn"):
                mix(jnp.maximum(it - 1, 0))
                for blk in range(tb):
                    soften(it, blk)
                score(jnp.minimum(i, n_steps - 1))

        @pl.when(i > n_steps)
        def _():
            mix(n_steps - 1)

        @pl.when((lax.rem(it, n_pairs) == 0) & (it > 0))
        def _():
            project(it // n_pairs - 1)

    cdiv_loop(n_steps + 2, walk)
    with jax.named_scope("f_store_wait"):
        for b in range(rows):
            push_q(b).wait()
        keep_qr, keep_lse = (pltpu.make_async_copy(*ends, ld.at[i]) for i, ends in enumerate(((qr, qr_h), (lse, lse_h))))
        keep_qr.start()
        keep_lse.start()
        keep_hat.wait()
        keep_q.wait()
        keep_qr.wait()
        keep_lse.wait()
        for b in range(rows):
            for c in keeps(b):
                c.wait()


def any_spec(k):
    return [pl.BlockSpec(memory_space=pl.ANY)] * k


def vmem_spec(k):
    return [pl.BlockSpec(memory_space=pltpu.VMEM)] * k


def run_fwd(n, x, pos, invf, ga, gm, wq, wk, wv, wo, head_dim):
    rows, toks, width = x.shape
    hd = wq.shape[0]
    ext, total, n_halo = toks + WINDOW, rows * toks, rows * WINDOW
    half = head_dim // 2
    sds = lambda *s: jax.ShapeDtypeStruct(s, BF)
    dma = lambda *s: pltpu.SemaphoreType.DMA(s)
    outs = [sds(hd, total), sds(hd, rows * ext), sds(rows * ext, hd), sds(rows * ext, hd), sds(width, total), sds(hd, total), sds(total, width), sds(total, width), sds(width, total)]
    outs += [sds(hd, n_halo), jax.ShapeDtypeStruct((rows * hd // (2 * head_dim), 8, 2 * QB), F32)] + [jax.ShapeDtypeStruct((half, total), F32)] * 2
    vm = lambda *s: pltpu.VMEM(s, BF)
    vf = lambda *s: pltpu.VMEM(s, F32)
    scratch = [vm(rows, toks, width), vm(rows, WINDOW, width), vm(hd, n_halo), vf(rows * hd // (2 * head_dim), 8, 2 * QB), pltpu.VMEM((rows, toks), jnp.int32), vm(hd, width), vm(hd, width), vm(hd, width), vm(hd, width),
               vm(hd, total), vm(hd, rows * ext), vm(rows * ext, hd), vm(rows * ext, hd), vm(hd, rows * ext), vm(width, total), vm(hd, total), vm(total, width), vm(total, width), vm(width, total), vm(total, width), vm(WINDOW, width),
               vf(hd, total), vf(hd, total), vf(hd, WINDOW), vf(hd, WINDOW), vf(half, n_halo), vf(half, n_halo),
               *[vf(3 * QB, 2 * QB)] * 3, *[vm(3 * QB, 2 * QB)] * 3,
               dma(rows), dma(4), dma(2 + 7 * rows), dma(rows + 1), dma(rows + 1), dma(rows), dma(rows)]
    return pl.pallas_call(
        functools.partial(fwd_kernel, n, head_dim), out_shape=outs,
        in_specs=any_spec(1) + vmem_spec(4) + any_spec(4), out_specs=any_spec(11) + vmem_spec(2), scratch_shapes=scratch,
        compiler_params=pltpu.CompilerParams(collective_id=0, has_side_effects=True, vmem_limit_bytes=VMEM_LIMIT),
        name="forward")(x, pos, invf, ga, gm, wq, wk, wv, wo)


LAG = 2
SLOTS = 2 * LAG
RING = 8
CB = 256


def at(ref, *idx):
    return ref.at[idx]


class Torus:
    def __init__(self, n, pairs, turn, parts, recv0, recv1, recv2, recv3, recv4, acc, acc2, fin, snd, rcv):
        self.side = math.isqrt(n // 2)
        assert self.side == 4
        me = lax.axis_index("seq")
        self.core = lax.rem(me, 2)
        chip = me // 2
        self.x, self.y = lax.rem(chip, 4), chip // 4
        self.pairs, self.turn = pairs, turn
        self.parts, self.recv0, self.recv1, self.recv2, self.recv3, self.recv4 = parts, recv0, recv1, recv2, recv3, recv4
        self.acc, self.acc2, self.fin, self.snd, self.rcv = acc, acc2, fin, snd, rcv
        self.partner = me + 1 - 2 * self.core
        self.hops = {(axis, step): self.device(*((0, step) if axis == 0 else (step, 0))) for axis in (0, 1) for step in (1, 3)}

    def device(self, dy, dx):
        return (lax.rem(self.y + dy, 4) * 4 + lax.rem(self.x + dx, 4)) * 2 + self.core

    def peers(self):
        return [self.partner, *self.hops.values()]

    def copy(self, lane, kind, slot, src, dst, target):
        return pltpu.make_async_remote_copy(
            src_ref=src, dst_ref=dst, send_sem=self.snd.at[lane, kind, slot], recv_sem=self.rcv.at[lane, kind, slot],
            device_id={"seq": target}, device_id_type=MESH)

    def late(self, pair, yes, no):
        if isinstance(pair, int):
            return yes if pair >= self.turn else no
        return jnp.where(pair >= self.turn, yes, no)

    def swap(self, ring, slot):
        return self.copy(0, 0, slot, self.parts.at[ring, :, :, 1 - self.core], self.recv0.at[slot], self.partner)

    def copies(self, stage, kind, pair, held, slot):
        axis = kind if stage < 3 else 1 - kind
        plus, minus = self.hops[axis, 1], self.hops[axis, 3]
        half = CB // 2
        if stage == 1:
            if axis == 0:
                minus = self.late(pair, plus, minus)
            ends = [(self.acc.at[kind, held, 2, pl.ds(0, 2)], self.recv1), (self.acc.at[kind, held, 2, pl.ds(2, 2)], self.recv1)]
        elif stage == 2:
            ends = [(self.acc.at[kind, held, 1], self.recv2), (self.acc.at[kind, held, 3], self.recv2)]
        elif stage == 3:
            ends = [(self.acc2.at[kind, held, 2, :, pl.ds(0, half)], self.recv3), (self.acc2.at[kind, held, 2, :, pl.ds(half, half)], self.recv3)]
        else:
            ends = [(self.acc2.at[kind, held, 1], self.recv4), (self.acc2.at[kind, held, 3], self.recv4)]
        lane = 2 * stage - 1
        return [self.copy(lane + i, kind, slot, src, buf.at[kind, slot, i], (plus, minus)[i]) for i, (src, buf) in enumerate(ends)]

    def add(self, stage, kind, pair, held, slot, ring):
        acc, acc2 = self.acc, self.acc2
        if stage == 1:
            def row(r1):
                for r2 in range(4):
                    ry, rx = (r2, r1) if kind == 0 else (r1, r2)
                    chip = lax.rem(self.y + ry, 4) * 4 + lax.rem(self.x + rx, 4)
                    acc[kind, held, r1, r2] = self.parts[ring, kind, chip, self.core] + self.recv0[slot, kind, chip]
            cdiv_loop(4, row)
        elif stage == 2:
            back = self.late(pair, 1, 3) if kind == 0 else 3
            acc[kind, held, 1, 0:2] += self.recv1[kind, slot, 0]
            acc[kind, held, back, 2:4] += self.recv1[kind, slot, 1]
        elif stage == 3:
            acc2[kind, held] = acc[kind, held, 0] + (self.recv2[kind, slot, 0] + self.recv2[kind, slot, 1])
        elif stage == 4:
            half = CB // 2
            acc2[kind, held, 1, :, 0:half] += self.recv3[kind, slot, 0]
            acc2[kind, held, 3, :, half:] += self.recv3[kind, slot, 1]
        else:
            self.fin[pair, kind] = acc2[kind, held, 0] + (self.recv4[kind, slot, 0] + self.recv4[kind, slot, 1])

    def when(self, pair, fn):
        if isinstance(pair, int):
            if 0 <= pair < self.pairs:
                fn()
        else:
            pl.when((pair >= 0) & (pair < self.pairs))(fn)

    def tick(self, t):
        now, land = mod(t, SLOTS), mod(t + SLOTS - LAG, SLOTS)
        ring_now, ring_land = mod(t, RING), mod(t + RING - LAG, RING)
        for stage in range(5, -1, -1):
            pair = t - LAG * stage
            held = land if stage % 2 else now

            def move(stage=stage, pair=pair, held=held):
                if stage == 0:
                    self.swap(ring_now, now).start()
                    return
                if stage == 1:
                    with jax.named_scope("t_wait1"):
                        self.swap(ring_land, land).wait()
                for kind in (0, 1):
                    if stage > 1:
                        with jax.named_scope(f"t_wait{stage}"):
                            for c in self.copies(stage - 1, kind, pair, held, land):
                                c.wait()
                    self.add(stage, kind, pair, held, land, ring_land)
                    if stage < 5:
                        for c in self.copies(stage, kind, pair, held, now):
                            c.start()
            self.when(pair, move)


def pick(i, table):
    out = 0
    for key, value in table.items():
        out = jnp.where(i == key, value, out)
    return out


def norm_back(x, gain, grad, res):
    xf = x.astype(F32)
    inv = lax.rsqrt(jnp.mean(xf * xf, axis=-1, keepdims=True) + NORM_EPS)
    unit = xf * inv
    gu = grad * gain
    out = inv * (gu - unit * jnp.mean(gu * unit, axis=-1, keepdims=True)) + res.astype(F32)
    gu = grad * unit
    return out.astype(BF), jnp.sum(gu.reshape(gu.shape[0] // 8, 8, gu.shape[1]), axis=0)


def plan(n_mlp, n_down, nc):
    order = [("o", g) for g in range(nc)] + [(name, g) for g in range(nc) for name in "qkv"]
    base = n_mlp + n_down
    return base, {name: (base + i // 2, i % 2) for i, name in enumerate(order)}, base + len(order) // 2


def bwd_kernel(n, head_dim, dims, ga, gm, x_h, dout_h, q_h, kt_h, k_h, v_h, hat_h, ot_h, xm_h, hm_h, hmt_h, qr_h, lse_h, cos_i, sin_i,
               wq_h, wk_h, wv_h, wo_h, wg_h, wu_h, wd_h,
               dx_h, fin_h, dga_o, dgm_o,
               parts, recv0, recv1, recv2, recv3, recv4, acc, acc2, fin, snd, rcv,
               dor, lser, deltar, hsnd, hrcv, osnd, orcv, gsend, grecv, gsem, ld,
               xbuf, mbuf, gnm, gmid, ot, hat, wo, dot_, lse, delta, dgain):
    rows, toks, width, hd, ff = dims
    ext, total = toks + WINDOW, rows * toks
    pw = 2 * head_dim
    n_pairs = hd // pw
    tb, n_steps = toks // QB, n_pairs * rows
    nb, nc, sub = ff // CB, width // CB, ff // width
    rpd = width // n
    per, half_sub = CB // pw, sub // 2
    base, place, pairs = plan(nb, nc * half_sub, nc)
    comm = Torus(n, pairs, base - 2, parts, recv0, recv1, recv2, recv3, recv4, acc, acc2, fin, snd, rcv)
    me = lax.axis_index("seq")
    left = lax.rem(me + n - 1, n)
    barrier = pltpu.get_barrier_semaphore()

    def greet(i):
        pl.semaphore_signal(barrier, inc=1, device_id={"seq": lax.rem(me + i + 1, n)}, device_id_type=MESH)

    def load(i, s, d):
        c = pltpu.make_async_copy(s, d, ld.at[i])
        c.start()
        return c

    def late(i):
        s, d = ((xm_h, mbuf), (ot_h, ot), (hat_h, hat), (wo_h, wo), (lse_h, lse))[i]
        return pltpu.make_async_copy(s, d, ld.at[1 + i])

    def to_left(src, dst, send_sem, recv_sem):
        return pltpu.make_async_remote_copy(src_ref=src, dst_ref=dst, send_sem=send_sem, recv_sem=recv_sem,
                                            device_id={"seq": left}, device_id_type=MESH)

    def push_rows(i):
        return to_left(*((lse_h, lser), (delta, deltar))[i], hsnd.at[i], hrcv.at[i])

    def push_out(p):
        pr = pl.ds(aligned(p * pw, pw), pw)
        return [to_left(dot_.at[pr, pl.ds(b * toks, WINDOW)], dor.at[pr, pl.ds(b * WINDOW, WINDOW)], osnd.at[p, b], orcv.at[p, b])
                for b in range(rows)]

    def put(spot, value):
        pair, kind = spot
        parts[mod(pair, RING), kind] = value.reshape(n // 2, 2, rpd, CB)

    def spot_of(name, g):
        known = {i: place[name, i] for i in range(nc)}
        return pick(g, {i: s[0] for i, s in known.items()}), pick(g, {i: s[1] for i, s in known.items()})

    def spots(it, blk):
        p, b = it // rows, mod(it, rows)
        pr = pl.ds(aligned(p * pw, pw), pw)
        return pr, pl.ds(aligned(b * toks + blk * QB, QB), QB), pl.ds(aligned(b * ext + blk * QB, QB), 3 * QB)

    def row_of(it):
        return mod(it, rows) * n_pairs + it // rows

    def mlp(hm, hmt, actt, wgu, wd, dgu, wld):
        def weights(j, slot):
            c = aligned(j * CB, CB)
            return [pltpu.make_async_copy(wg_h.at[:, pl.ds(c, CB)], wgu.at[slot, :, pl.ds(0, CB)], wld.at[slot, 0]),
                    pltpu.make_async_copy(wu_h.at[:, pl.ds(c, CB)], wgu.at[slot, :, pl.ds(CB, CB)], wld.at[slot, 1]),
                    pltpu.make_async_copy(wd_h.at[pl.ds(c, CB), :], wd.at[slot], wld.at[slot, 2])]

        for c in weights(0, 0):
            c.start()
        ld_hm, ld_x, ld_hmt = load(6, hm_h, hm), load(0, dout_h, xbuf), load(7, hmt_h, hmt)
        cdiv_loop(n - 1, greet)
        gnm[:] = jnp.zeros_like(gnm)
        gsend[:] = jnp.zeros_like(gsend)
        dgain[:] = jnp.zeros_like(dgain)
        ld_hm.wait()
        ld_x.wait()
        ld_hmt.wait()
        for i in range(5):
            late(i).start()

        def block(j):
            slot = lax.rem(j, 2)
            for c in weights(j, slot):
                c.wait()

            @pl.when(j + 1 < nb)
            def _():
                for c in weights(j + 1, 1 - slot):
                    c.start()

            c0 = pl.multiple_of(j * CB, CB)
            with jax.named_scope("b_mlp"):
                for b in range(rows):
                    r = slice(b * toks, (b + 1) * toks)
                    gu = dot(hm[r, :], wgu[slot])
                    gact = dot(xbuf[r, :], wd[slot], NT).astype(BF).astype(F32)
                    gate, up = gu[:, :CB], gu[:, CB:]
                    sig = 1.0 / (1.0 + jnp.exp(-gate))
                    swish = gate * sig
                    actt[pl.ds(c0, CB), r] = (swish * up).astype(BF).T
                    dgu[r, :CB] = (gact * up * (sig + swish * (1.0 - sig))).astype(BF)
                    dgu[r, CB:] = (gact * swish).astype(BF)
                both = dot(hmt[:], dgu[:])
                ring = lax.rem(j, RING)
                parts[ring, 0] = both[:, :CB].reshape(n // 2, 2, rpd, CB)
                parts[ring, 1] = both[:, CB:].reshape(n // 2, 2, rpd, CB)
                for b in range(rows):
                    r = slice(b * toks, (b + 1) * toks)
                    gnm[r, :] += dot(dgu[r, :], wgu[slot], NT)

            @pl.when(j == 0)
            def _():
                pl.semaphore_wait(barrier, n - 1)
                push_rows(0).start()

            comm.tick(j)

        cdiv_loop(nb, block)

        def down(c):
            share = n // 2 // sub
            c0 = pl.multiple_of(c * CB, CB)
            for m in range(sub):
                res = dot(actt[m * width:(m + 1) * width, :], xbuf[:, pl.ds(c0, CB)]).reshape(share, 2, sub, rpd, CB)
                for i in range(sub):
                    pair = nb + c * half_sub + i // 2
                    parts[lax.rem(pair, RING), i % 2, m * share:(m + 1) * share] = res[:, :, i]

        for i in range(5):
            late(i).wait()

        def mid(i):
            r = pl.ds(pl.multiple_of(i * QB, QB), QB)
            out, dg = norm_back(mbuf[r, :], gm[:], gnm[r, :], xbuf[r, :])
            gmid[r, :] = out
            dgain[8:, :] += dg

        def deltas(it):
            for blk in range(tb):
                pr, cols, _ = spots(it, blk)
                both = dot_[pr, cols].astype(F32) * ot[pr, cols].astype(F32)
                delta[row_of(it), blk:blk + 1, :] = jnp.concatenate(
                    [col_sum(both[:head_dim]), col_sum(both[head_dim:])], axis=1)

        def column(c):
            with jax.named_scope("b_down"):
                down(c)
            comm.tick(nb + c + jnp.minimum(c, 1))

            @pl.when(c == 0)
            def _():
                with jax.named_scope("b_mid"):
                    cdiv_loop(total // QB, mid)
                with jax.named_scope("b_dot"):
                    dot_[:] = dot(wo[:], gmid[:], NT).astype(BF)
                    cdiv_loop(n_steps, deltas)
                push_rows(1).start()
                for p in range(n_pairs):
                    for c_ in push_out(p):
                        c_.start()
                comm.tick(nb + 1)

        cdiv_loop(nc, column)

    vm = lambda *s: pltpu.VMEM(s, BF)
    vf = lambda *s: pltpu.VMEM(s, F32)
    pl.run_scoped(mlp, vm(total, width), vm(width, total), vm(ff, total), vm(2, width, 2 * CB), vm(2, CB, width), vm(total, 2 * CB),
                  pltpu.SemaphoreType.DMA((2, 3)))
    head = nb + nc + 1

    def attention(q, kt, k, v, qr, dv, sc0, sc1, sc2, sr, dp0, dp1, dp2, dr, pb0, pb1, pb2, pr_, ds0, ds1, ds2, dsr):
        dqt, dkt = ot, q
        wq, wk, wv = k.at[:hd], kt.at[:, :width], v.at[:hd]
        sc, dp, pb, ds = (sc0, sc1, sc2), (dp0, dp1, dp2), (pb0, pb1, pb2), (ds0, ds1, ds2)
        lds = [load(6 + i, s, d) for i, (s, d) in enumerate(((q_h, q), (k_h, k), (v_h, v), (qr_h, qr), (kt_h, kt)))]
        ld_x2 = load(0, x_h, xbuf)

        def out_grad(g):
            put(spot_of("o", g), dot(ot[:], gmid[:, pl.ds(pl.multiple_of(g * CB, CB), CB)]))

        with jax.named_scope("b_dwo"):
            cdiv_loop(nc, out_grad)
        for c in lds:
            c.wait()
        upper = upper_mask()
        first, last = me == 0, me == n - 1

        def right(it, i):
            p, b = it // rows, mod(it, rows)
            return pl.ds(aligned(p * pw, pw), pw), pl.ds(aligned(b * WINDOW + i * QB, QB), QB), pl.ds(aligned(b * ext + toks + i * QB, QB), WINDOW - i * QB)

        def score(it):
            for blk in range(tb):
                pr, cols, keys = spots(it, blk)
                sc[blk][:] = dot(k[keys, pr], stack_pair(q[pr, cols]))
                dp[blk][:] = dot(v[keys, pr], stack_pair(dot_[pr, cols]))
            for i, rs in enumerate((slice(0, WINDOW), slice(WINDOW, 3 * QB))):
                pr, cols, keys = right(it, i)
                sr[rs, :] = dot(k[keys, pr], stack_pair(qr[pr, cols]))
                dr[rs, :] = dot(v[keys, pr], stack_pair(dor[pr, cols]))

        def soften(it):
            row = row_of(it)
            for blk in range(tb):
                s02, s1 = merged(sc[blk][:], upper, *start_bias(first, blk))
                norm, mean = lse[row, blk:blk + 1, :], delta[row, blk:blk + 1, :]
                p02, p1 = jnp.exp(s02 - norm), jnp.exp(s1 - norm)
                g02, g1 = jnp.where(upper, dp[blk][:QB], dp[blk][2 * QB:]), dp[blk][QB:2 * QB]
                pb[blk][:] = banded(p02, p1, upper)
                ds[blk][:] = banded(p02 * (g02 - mean), p1 * (g1 - mean), upper)
            for i, blk in ((0, 0), (0, 1), (1, 2)):
                rs = slice(blk * QB, (blk + 1) * QB)
                p = jnp.exp(sr[rs, :] - jnp.where(last, -NEG, lser[row, i:i + 1, :]))
                g = p * (dr[rs, :] - deltar[row, i:i + 1, :])
                pr_[rs, :] = (p if blk == 1 else jnp.where(upper, p, 0.0)).astype(BF)
                dsr[rs, :] = (g if blk == 1 else jnp.where(upper, g, 0.0)).astype(BF)

        def grads(it):
            ks, vs = [], []
            for blk in range(tb):
                pr, cols, keys = spots(it, blk)
                own = slice(max(0, 2 - blk) * QB, 3 * QB)
                vs.append(dot(pb[blk][own, :], stack_pair(dot_[pr, cols]), NT))
                ks.append(dot(ds[blk][own, :], stack_pair(q[pr, cols]), NT))
                dq = unstack_pair(dot(kt[pr, keys], ds[blk][:])) * (head_dim ** -0.5)
                dqt[pr, cols] = rope(dq, cos_i[:, cols], sin_i[:, cols], -1, head_dim).astype(BF)
            for i, rs in enumerate((slice(0, WINDOW), slice(WINDOW, 3 * QB))):
                pr, cols, _ = right(it, i)
                vs.append(dot(pr_[rs, :], stack_pair(dor[pr, cols]), NT))
                ks.append(dot(dsr[rs, :], stack_pair(qr[pr, cols]), NT))
            for j in range(tb):
                pr, cols, _ = spots(it, j)
                gv, gk = (sum(x[i][(j - max(0, i - 2)) * QB:(j - max(0, i - 2) + 1) * QB] for i in range(j, j + 3)) for x in (vs, ks))
                dv[cols, pr] = gv.astype(BF)
                dkt[pr, cols] = rope(gk.T, cos_i[:, cols], sin_i[:, cols], -1, head_dim).astype(BF)

        def close_group(g):
            cols = pl.ds(pl.multiple_of(g * CB, CB), CB)
            with jax.named_scope("b_dwqkv"):
                put(spot_of("q", g), dot(hat[:], dqt[cols, :], NT))
                put(spot_of("k", g), dot(hat[:], dkt[cols, :], NT))
                put(spot_of("v", g), dot(hat[:], dv[:, cols]))

        def weights():
            return [pltpu.make_async_copy(s, d, ld.at[6 + i]) for i, (s, d) in enumerate(((wq_h, wq), (wk_h, wk), (wv_h, wv)))]

        def arrived(p):
            with jax.named_scope("b_hwait"):
                for c in push_out(p):
                    c.wait()

        def walk(it):
            @pl.when((lax.rem(it + 1, rows) == 0) & (it + 1 < n_steps))
            def _():
                arrived((it + 1) // rows)

            @pl.when(it < n_steps)
            def _():
                with jax.named_scope("b_attn"):
                    grads(it - 1)
                    soften(it)
                    score(jnp.minimum(it + 1, n_steps - 1))

            @pl.when(it == n_steps)
            def _():
                grads(n_steps - 1)
                for c in weights():
                    c.start()

            @pl.when(lax.rem(it, rows) == 0)
            def _():
                p = it // rows - 1

                @pl.when(lax.rem(p, per) == per - 1)
                def _():
                    close_group(p // per)

                comm.tick(head + 1 + p)

        comm.tick(head)
        for i in range(2):
            push_rows(i).wait()
        arrived(0)
        if rows == 1:
            arrived(1)
        score(0)
        soften(0)
        score(1)
        cdiv_loop(n_steps, lambda i: walk(i + 1))
        for c in weights():
            c.wait()
        ld_x2.wait()

        def into(b):
            r = pl.ds(pl.multiple_of(b * toks, QB), toks)
            with jax.named_scope("b_into"):
                gnm[r, :] = dot(dqt[:, r], wq[:], TN) + dot(dkt[:, r], wk[:], TN) + dot(dv[r, :], wv[:])

            def final(i):
                r = pl.ds(pl.multiple_of((b * tb + i) * QB, QB), QB)
                out, dg = norm_back(xbuf[r, :], ga[:], gnm[r, :], gmid[r, :])
                mbuf[r, :] = out
                dgain[:8, :] += dg

            with jax.named_scope("b_final"):
                cdiv_loop(tb, final)
            comm.tick(head + 1 + n_pairs + b)

        cdiv_loop(rows, into)

    score_bufs = [vf(3 * QB, 2 * QB)] * 8 + [vm(3 * QB, 2 * QB)] * 8
    pl.run_scoped(attention, vm(hd, total), vm(hd, rows * ext), vm(rows * ext, hd), vm(rows * ext, hd), vm(hd, rows * WINDOW), vm(total, hd), *score_bufs)
    out_copy = load(1, mbuf, dx_h)
    gains = jnp.concatenate([col_sum(dgain[:8, :]), col_sum(dgain[8:, :]), jnp.zeros((6, width), F32)], axis=0)
    for p in range(n):
        gsend[p, :, 0:rpd] = gains[:, p * rpd:(p + 1) * rpd]

    def spread(i):
        to = lax.rem(me + i + 1, n)
        pltpu.make_async_remote_copy(src_ref=gsend.at[to], dst_ref=grecv.at[i], send_sem=gsem.at[0], recv_sem=gsem.at[1],
                                     device_id={"seq": to}, device_id_type=MESH).start()

    cdiv_loop(n - 1, spread)
    lax.fori_loop(head + 1 + n_pairs + rows, pairs + 5 * LAG, lambda t, c: (comm.tick(t), c)[1], 0)
    keep_fin = load(0, fin, fin_h)
    with jax.named_scope("b_gain"):
        to_left(gsend.at[pl.ds(0, n - 1)], grecv, gsem.at[0], gsem.at[1]).wait()
    sums = gsend[me]
    for i in range(n - 1):
        sums = sums + grecv[i]
    dga_o[:] = sums[0:1, 0:rpd]
    dgm_o[:] = sums[1:2, 0:rpd]
    out_copy.wait()
    keep_fin.wait()


def spread_kernel(dims, dx_i, fin_i, dga_i, dgm_i, dx_o, dga_o, dgm_o, *refs):
    head_dim, n, width, ff = dims
    outs, (buf, fin), stage, sem = refs[:7], refs[7:9], refs[9:16], refs[16]
    dq, dk, dv, do, dg, du, dd = stage
    nb, nc, sub = ff // CB, width // CB, ff // width
    rpd = width // n
    place = plan(nb, nc * sub // 2, nc)[1]
    get, get_fin, out = (pltpu.make_async_copy(*ends, sem.at[len(outs) + i]) for i, ends in enumerate(((dx_i, buf), (fin_i, fin), (buf, dx_o))))
    get_fin.start()
    get.start()
    dga_o[:] = dga_i[:]
    dgm_o[:] = dgm_i[:]
    get_fin.wait()
    for j in range(nb):
        dg[:, j * CB:(j + 1) * CB] = fin[j, 0]
        du[:, j * CB:(j + 1) * CB] = fin[j, 1]
    for c in range(nc):
        for i in range(sub):
            dd[i * rpd:(i + 1) * rpd, c * CB:(c + 1) * CB] = fin[nb + (c * sub + i) // 2, i % 2]
    for g in range(nc):
        do[:, g * CB:(g + 1) * CB] = fin[place["o", g]]
        for name, ref in (("q", dq), ("k", dk), ("v", dv)):
            val = fin[place[name, g]]
            for h in range(CB // head_dim):
                ref[g * (CB // head_dim) + h] = val[:, h * head_dim:(h + 1) * head_dim]
    keeps = [pltpu.make_async_copy(s, d, sem.at[i]) for i, (s, d) in enumerate(zip(stage, outs))]
    for c in keeps:
        c.start()
    get.wait()
    out.start()
    for c in keeps:
        c.wait()
    out.wait()


def run_bwd(n, head_dim, ga, gm, x, dout, q, kt, k, v, hat, ot, xm, hm, hmt, qr, lse, cos_t, sin_t, wq, wk, wv, wo, wg, wu, wd, rows):
    total, width = x.shape
    hd, ff = wq.shape[0], wg.shape[1]
    toks = total // rows
    rpd, heads = width // n, hd // head_dim
    nb, nc, sub = ff // CB, width // CB, ff // width
    pairs = plan(nb, nc * sub // 2, nc)[2]
    n_pairs = hd // (2 * head_dim)
    f = lambda *s: jax.ShapeDtypeStruct(s, F32)
    dx_t = jax.ShapeDtypeStruct((total, width), BF)
    vm = lambda *s: pltpu.VMEM(s, BF)
    vf = lambda *s: pltpu.VMEM(s, F32)
    dma = lambda *s: pltpu.SemaphoreType.DMA(s)
    line = vf(rows * n_pairs, 8, 2 * QB)
    scratch = [vf(RING, 2, n // 2, 2, rpd, CB), vf(SLOTS, 2, n // 2, rpd, CB), vf(2, SLOTS, 2, 2, rpd, CB), vf(2, SLOTS, 2, 4, rpd, CB),
               vf(2, SLOTS, 2, rpd, CB // 2), vf(2, SLOTS, 2, rpd, CB), vf(2, SLOTS, 4, 4, rpd, CB), vf(2, SLOTS, 4, rpd, CB), vf(pairs, 2, rpd, CB),
               dma(9, 2, SLOTS), dma(9, 2, SLOTS),
               vm(hd, rows * WINDOW), line, line, dma(2), dma(2), dma(n_pairs, rows), dma(n_pairs, rows),
               vf(n, 8, 128), vf(n - 1, 8, 128), dma(2), dma(12),
               vm(total, width), vm(total, width), vf(total, width), vm(total, width), vm(hd, total), vm(width, total), vm(hd, width), vm(hd, total), line, line, vf(16, width)]
    mid = pl.pallas_call(
        functools.partial(bwd_kernel, n, head_dim, (rows, toks, width, hd, ff)), out_shape=[dx_t, f(pairs, 2, rpd, CB), f(1, rpd), f(1, rpd)],
        in_specs=vmem_spec(2) + any_spec(13) + vmem_spec(2) + any_spec(7), out_specs=any_spec(2) + vmem_spec(2), scratch_shapes=scratch,
        compiler_params=pltpu.CompilerParams(collective_id=1, has_side_effects=True, vmem_limit_bytes=VMEM_LIMIT),
        name="backward")(ga, gm, x, dout, q, kt, k, v, hat, ot, xm, hm, hmt, qr, lse, cos_t, sin_t, wq, wk, wv, wo, wg, wu, wd)
    outs = [f(heads, rpd, head_dim)] * 3 + [f(rpd, width), f(rpd, ff), f(rpd, ff), f(ff // n, width)]
    return pl.pallas_call(
        functools.partial(spread_kernel, (head_dim, n, width, ff)), out_shape=[dx_t, f(1, rpd), f(1, rpd)] + outs,
        in_specs=any_spec(2) + vmem_spec(2), out_specs=any_spec(1) + vmem_spec(2) + any_spec(7),
        scratch_shapes=[vm(total, width), vf(pairs, 2, rpd, CB), *[vf(*o.shape) for o in outs], dma(10)],
        name="spread")(*mid)


def solution(mesh):
    n = mesh.shape["seq"]

    def device_step(hidden, positions, g_attn, g_mlp, w_query, w_key, w_value, w_out, w_gate, w_up, w_down, d_out):
        rows, toks, width = hidden.shape
        layers, _, heads, head_dim = w_query.shape
        hd = heads * head_dim
        half = head_dim // 2
        inv_freq = 1.0 / (10000.0 ** (jnp.arange(half, dtype=F32) * (2.0 / head_dim)))
        turn = lambda w: w[0].transpose(1, 2, 0).reshape(hd, width)
        wq, wk, wv = turn(w_query), turn(w_key), turn(w_value)
        fwd = run_fwd(n, hidden, positions, inv_freq[:, None], g_attn, g_mlp, wq, wk, wv, w_out[0], head_dim)
        out = run_bwd(n, head_dim, g_attn, g_mlp, hidden.reshape(rows * toks, width), d_out.reshape(rows * toks, width), *fwd,
                      wq, wk, wv, w_out[0], w_gate[0], w_up[0], w_down[0], rows)
        dx, dga, dgm, dq, dk, dv, do, dg, du, dd = out
        back = lambda w: w.transpose(1, 0, 2)[None]
        return (dx.reshape(rows, toks, width), dga, dgm, back(dq), back(dk), back(dv), do[None], dg[None], du[None], dd[None])

    tok_spec = P("data", "seq", None)
    vec_spec = P(None, ("data", "seq"))
    mat_spec = P(None, ("data", "seq"), None)
    head_spec = P(None, ("data", "seq"), None, None)
    in_specs = (tok_spec, P("data", "seq")) + (P(),) * 9 + (tok_spec,)
    out_specs = (tok_spec, vec_spec, vec_spec, head_spec, head_spec, head_spec, mat_spec, mat_spec, mat_spec, mat_spec)
    return jax.shard_map(device_step, mesh=mesh, in_specs=in_specs, out_specs=out_specs, check_vma=False)
```

```python
import functools, math
import numpy as np
import jax, jax.numpy as jnp
from jax import lax
from jax.experimental import pallas as pl
from jax.experimental.pallas import tpu as pltpu
from jax.sharding import PartitionSpec as P

WINDOW = 256
NORM_EPS = 1e-5
QB = 128
BF, F32 = jnp.bfloat16, jnp.float32
NN, NT, TN = ((1,), (0,)), ((1,), (1,)), ((0,), (0,))
MESH = pl.DeviceIdType.MESH
NEG = -1e30
VMEM_LIMIT = 67043328


def dot(a, b, dims=NN):
    return lax.dot_general(a, b, (dims, ((), ())), preferred_element_type=F32)


def cdiv_loop(n, body):
    lax.fori_loop(0, n, lambda i, c: (body(i), c)[1], 0)


def mod(a, b):
    return a % b if isinstance(a, int) else lax.rem(a, b)


def aligned(a, b):
    return a if isinstance(a, int) else pl.multiple_of(a, b)


def rope(blk, cos_b, sin_b, sign, head_dim):
    half = head_dim // 2
    parts = []
    for h in range(blk.shape[0] // head_dim):
        first = blk[h * head_dim:h * head_dim + half]
        second = blk[h * head_dim + half:(h + 1) * head_dim]
        if sign > 0:
            parts += [first * cos_b - second * sin_b, second * cos_b + first * sin_b]
        else:
            parts += [first * cos_b + second * sin_b, second * cos_b - first * sin_b]
    return jnp.concatenate(parts, axis=0)


def normed(x, gain):
    xf = x.astype(F32)
    inv = lax.rsqrt(jnp.mean(xf * xf, axis=-1, keepdims=True) + NORM_EPS)
    return (xf * inv * gain).astype(BF)


def stack_pair(pair_t):
    half = pair_t.shape[0] // 2
    zero = jnp.zeros((half, pair_t.shape[1]), pair_t.dtype)
    return jnp.concatenate(
        [jnp.concatenate([pair_t[:half], zero], axis=0), jnp.concatenate([zero, pair_t[half:]], axis=0)], axis=1)


def unstack_pair(both):
    half, cols = both.shape[0] // 2, both.shape[1] // 2
    return jnp.concatenate([both[:half, :cols], both[half:, cols:]], axis=0)


def col_sum(x):
    return jnp.sum(x, axis=0, keepdims=True)


def merged(scores, upper, bias0, bias1):
    return jnp.where(upper, scores[:QB] + bias0, scores[2 * QB:]), scores[QB:2 * QB] + bias1


def banded(p02, p1, upper):
    return jnp.concatenate(
        [jnp.where(upper, p02, 0.0).astype(BF), p1.astype(BF), jnp.where(upper, 0.0, p02).astype(BF)], axis=0)


def upper_mask():
    key_ids = lax.broadcasted_iota(jnp.int32, (QB, 2 * QB), 0)
    query_ids = lax.broadcasted_iota(jnp.int32, (QB, 2 * QB), 1) % QB
    return key_ids > query_ids


def start_bias(first, blk):
    bias = jnp.where(first, NEG, 0.0).astype(F32)
    return (bias if blk < 2 else 0.0), (bias if blk < 1 else 0.0)


def fwd_kernel(n, head_dim, x_h, pos, invf, ga, gm, wq_h, wk_h, wv_h, wo_h,
               q_h, kt_h, k_h, v_h, hat_h, ot_h, xm_h, hm_h, hmt_h, qr_h, lse_h, cos_t, sin_t,
               xv, halo, qr, lse, pos_halo, wq, wk, wv, wo, q, kt, k, v, vt, hat, ot, xm, hm, hmt, hb, hh, acc, acc2, ak, av, cos_h, sin_h,
               sc0, sc1, sc2, pb0, pb1, pb2, ldx, ld, st, snd, rcv, qsnd, qrcv):
    sc, pb = (sc0, sc1, sc2), (pb0, pb1, pb2)
    rows, toks, width = xv.shape
    ext, total, pw = toks + WINDOW, rows * toks, 2 * head_dim
    n_pairs = wq.shape[0] // pw
    tb, n_steps = toks // QB, n_pairs * rows
    me = lax.axis_index("seq")
    right, left = lax.rem(me + 1, n), lax.rem(me + n - 1, n)
    load_x = [pltpu.make_async_copy(x_h.at[b], xv.at[b], ldx.at[b]) for b in range(rows)]
    load_w = [pltpu.make_async_copy(s, d, ld.at[i]) for i, (s, d) in enumerate(((wq_h, wq), (wk_h, wk), (wv_h, wv), (wo_h, wo)))]
    for c in load_x:
        c.start()
    barrier = pltpu.get_barrier_semaphore()
    for other in (left, right):
        pl.semaphore_signal(barrier, inc=1, device_id={"seq": other}, device_id_type=MESH)
    pl.semaphore_wait(barrier, 2)

    def push(i, s, d):
        return pltpu.make_async_remote_copy(src_ref=s, dst_ref=d, send_sem=snd.at[i], recv_sem=rcv.at[i], device_id={"seq": right}, device_id_type=MESH)

    def push_rows(b):
        return push(b, x_h.at[b, toks - WINDOW:, :], halo.at[b])

    send_pos = push(rows, pos, pos_halo)
    send_pos.start()
    for b in range(rows):
        push_rows(b).start()

    def angles(cos_ref, sin_ref, positions):
        count = positions.shape[1]
        for b in range(rows):
            ang = invf[:] * positions[b:b + 1, :].astype(F32)
            cos_ref[:, b * count:(b + 1) * count] = jnp.cos(ang)
            sin_ref[:, b * count:(b + 1) * count] = jnp.sin(ang)

    angles(cos_t, sin_t, pos[:])

    def norm_blk(i):
        h = normed(xv[i // tb, pl.ds(pl.multiple_of(lax.rem(i, tb) * QB, QB), QB), :], ga[:])
        r = pl.ds(pl.multiple_of(i * QB, QB), QB)
        hb[r, :] = h
        hat[:, r] = h.T

    with jax.named_scope("f_norm"):
        for c in load_x:
            c.wait()
        for c in load_w:
            c.start()
        cdiv_loop(total // QB, norm_blk)
    keep_hat = pltpu.make_async_copy(hat, hat_h, st.at[0])
    keep_hat.start()
    tables = cos_t[:], sin_t[:]

    def put_q(src):
        for p in range(n_pairs):
            r = slice(p * pw, (p + 1) * pw)
            q[r, :] = (rope(src[r, :], *tables, 1, head_dim) * (head_dim ** -0.5)).astype(BF)

    def put_own(src, dst_t, dst, turn):
        for p in range(n_pairs):
            r = slice(p * pw, (p + 1) * pw)
            both = (rope(src[r, :], *tables, 1, head_dim) if turn else src[r, :]).astype(BF)
            for b in range(rows):
                blk = both[:, b * toks:(b + 1) * toks]
                own = slice(b * ext + WINDOW, (b + 1) * ext)
                dst_t[r, own] = blk
                dst[own, r] = blk.T

    with jax.named_scope("f_mm"):
        load_w[0].wait()
        load_w[1].wait()
        load_w[2].wait()
        acc[:] = dot(wq[:], hb[:], NT)
        acc2[:] = dot(wk[:], hb[:], NT)
        put_q(acc)
        acc[:] = dot(wv[:], hb[:], NT)
        put_own(acc2, kt, k, True)
        put_own(acc, vt, v, False)
    keep_q = pltpu.make_async_copy(q, q_h, st.at[1])
    keep_q.start()

    def push_q(b):
        return pltpu.make_async_remote_copy(src_ref=q.at[:, b * toks:b * toks + WINDOW], dst_ref=qr.at[:, b * WINDOW:(b + 1) * WINDOW],
                                            send_sem=qsnd.at[b], recv_sem=qrcv.at[b], device_id={"seq": left}, device_id_type=MESH)

    for b in range(rows):
        push_q(b).start()
    send_pos.wait()
    angles(cos_h, sin_h, pos_halo[:, toks - WINDOW:])

    def keeps(b):
        wide, cols = pl.ds(pl.multiple_of(b * ext, QB), ext), pl.ds(pl.multiple_of(b * toks, QB), toks)
        ends = ((kt.at[:, wide], kt_h.at[:, wide]), (k.at[wide, :], k_h.at[wide, :]), (v.at[wide, :], v_h.at[wide, :]),
                (ot.at[:, cols], ot_h.at[:, cols]), (hm.at[cols, :], hm_h.at[cols, :]), (hmt.at[:, cols], hmt_h.at[:, cols]),
                (xm.at[cols, :], xm_h.at[cols, :]))
        return [pltpu.make_async_copy(s, d, st.at[2 + b * len(ends) + i]) for i, (s, d) in enumerate(ends)]

    def halo_in(b):
        with jax.named_scope("f_halo_wait"):
            push_rows(b).wait()
        with jax.named_scope("f_halo"):
            for i in range(WINDOW // QB):
                r = slice(i * QB, (i + 1) * QB)
                hh[r, :] = normed(halo[b, r, :], ga[:])
            ak[:] = dot(wk[:], hh[:], NT)
            av[:] = dot(wv[:], hh[:], NT)
            cols = pl.ds(pl.multiple_of(b * WINDOW, QB), WINDOW)
            wide = pl.ds(pl.multiple_of(b * ext, QB), WINDOW)
            near = cos_h[:, cols], sin_h[:, cols]
            for src, dst_t, dst in ((ak, kt, k), (av, vt, v)):
                for p in range(n_pairs):
                    r = slice(p * pw, (p + 1) * pw)
                    blk = (rope(src[r, :], *near, 1, head_dim) if dst is k else src[r, :]).astype(BF)
                    dst_t[r, wide] = blk
                    dst[wide, r] = blk.T
        for c in keeps(b)[:3]:
            c.start()

    upper = upper_mask()
    first = me == 0

    def spots(it, blk):
        b, p = it // n_pairs, mod(it, n_pairs)
        pr = pl.ds(aligned(p * pw, pw), pw)
        return pr, pl.ds(aligned(b * toks + blk * QB, QB), QB), pl.ds(aligned(b * ext + blk * QB, QB), 3 * QB)

    def score(it):
        for blk in range(tb):
            pr, cols, keys = spots(it, blk)
            sc[blk][:] = dot(k[keys, pr], stack_pair(q[pr, cols]))

    def soften(it, blk):
        s02, s1 = merged(sc[blk][:], upper, *start_bias(first, blk))
        top = jnp.max(jnp.maximum(s02, s1), axis=0, keepdims=True)
        e02, e1 = jnp.exp(s02 - top), jnp.exp(s1 - top)
        mass = col_sum(e02 + e1)
        inv = 1.0 / mass
        lse[it, blk:blk + 1, :] = top + jnp.log(mass)
        pb[blk][:] = banded(e02 * inv, e1 * inv, upper)

    def mix(it):
        for blk in range(tb):
            pr, cols, keys = spots(it, blk)
            ot[pr, cols] = unstack_pair(dot(vt[pr, keys], pb[blk][:])).astype(BF)

    def project(b):
        cols = pl.ds(pl.multiple_of(b * toks, QB), toks)
        with jax.named_scope("f_proj"):
            mid = (xv[b].astype(F32) + dot(ot[:, cols], wo[:], TN)).astype(BF)
            xm[cols, :] = mid
            h = normed(mid, gm[:])
            hm[cols, :] = h
            hmt[:, cols] = h.T
        for c in keeps(b)[3:]:
            c.start()

    keep_qr, keep_lse = (pltpu.make_async_copy(*ends, ld.at[i]) for i, ends in enumerate(((qr, qr_h), (lse, lse_h))))
    load_w[3].wait()
    for blk in range(tb):
        pb[blk][:] = jnp.zeros(pb[blk].shape, BF)

    def walk(i):
        it = i - 1

        @pl.when((lax.rem(i, n_pairs) == 0) & (i < n_steps))
        def _():
            halo_in(i // n_pairs)

        @pl.when(i == 0)
        def _():
            score(0)

        @pl.when((i > 0) & (i <= n_steps))
        def _():
            with jax.named_scope("f_attn"):
                mix(jnp.maximum(it - 1, 0))
                for blk in range(tb):
                    soften(it, blk)
                score(jnp.minimum(i, n_steps - 1))

        @pl.when(i == n_steps)
        def _():
            for b in range(rows):
                push_q(b).wait()
            keep_qr.start()

        @pl.when(i > n_steps)
        def _():
            mix(n_steps - 1)

        @pl.when((lax.rem(it, n_pairs) == 0) & (it > 0))
        def _():
            project(it // n_pairs - 1)

    cdiv_loop(n_steps + 2, walk)
    with jax.named_scope("f_store_wait"):
        keep_lse.start()
        keep_hat.wait()
        keep_q.wait()
        keep_qr.wait()
        keep_lse.wait()
        for b in range(rows):
            for c in keeps(b):
                c.wait()


def any_spec(k):
    return [pl.BlockSpec(memory_space=pl.ANY)] * k


def vmem_spec(k):
    return [pl.BlockSpec(memory_space=pltpu.VMEM)] * k


def run_fwd(n, x, pos, invf, ga, gm, wq, wk, wv, wo, head_dim):
    rows, toks, width = x.shape
    hd = wq.shape[0]
    ext, total, n_halo = toks + WINDOW, rows * toks, rows * WINDOW
    half = head_dim // 2
    sds = lambda *s: jax.ShapeDtypeStruct(s, BF)
    dma = lambda *s: pltpu.SemaphoreType.DMA(s)
    outs = [sds(hd, total), sds(hd, rows * ext), sds(rows * ext, hd), sds(rows * ext, hd), sds(width, total), sds(hd, total), sds(total, width), sds(total, width), sds(width, total)]
    outs += [sds(hd, n_halo), jax.ShapeDtypeStruct((rows * hd // (2 * head_dim), 8, 2 * QB), F32)] + [jax.ShapeDtypeStruct((half, total), F32)] * 2
    vm = lambda *s: pltpu.VMEM(s, BF)
    vf = lambda *s: pltpu.VMEM(s, F32)
    scratch = [vm(rows, toks, width), vm(rows, WINDOW, width), vm(hd, n_halo), vf(rows * hd // (2 * head_dim), 8, 2 * QB), pltpu.VMEM((rows, toks), jnp.int32), vm(hd, width), vm(hd, width), vm(hd, width), vm(hd, width),
               vm(hd, total), vm(hd, rows * ext), vm(rows * ext, hd), vm(rows * ext, hd), vm(hd, rows * ext), vm(width, total), vm(hd, total), vm(total, width), vm(total, width), vm(width, total), vm(total, width), vm(WINDOW, width),
               vf(hd, total), vf(hd, total), vf(hd, WINDOW), vf(hd, WINDOW), vf(half, n_halo), vf(half, n_halo),
               *[vf(3 * QB, 2 * QB)] * 3, *[vm(3 * QB, 2 * QB)] * 3,
               dma(rows), dma(4), dma(2 + 7 * rows), dma(rows + 1), dma(rows + 1), dma(rows), dma(rows)]
    return pl.pallas_call(
        functools.partial(fwd_kernel, n, head_dim), out_shape=outs,
        in_specs=any_spec(1) + vmem_spec(4) + any_spec(4), out_specs=any_spec(11) + vmem_spec(2), scratch_shapes=scratch,
        compiler_params=pltpu.CompilerParams(collective_id=0, has_side_effects=True, vmem_limit_bytes=VMEM_LIMIT),
        name="forward")(x, pos, invf, ga, gm, wq, wk, wv, wo)


LAG = 2
SLOTS = 2 * LAG
RING = 8
CB = 256


def at(ref, *idx):
    return ref.at[idx]


class Torus:
    def __init__(self, n, pairs, turn, parts, recv0, recv1, recv2, recv3, recv4, acc, acc2, fin, snd, rcv):
        self.side = math.isqrt(n // 2)
        assert self.side == 4
        me = lax.axis_index("seq")
        self.core = lax.rem(me, 2)
        chip = me // 2
        self.x, self.y = lax.rem(chip, 4), chip // 4
        self.pairs, self.turn = pairs, turn
        self.parts, self.recv0, self.recv1, self.recv2, self.recv3, self.recv4 = parts, recv0, recv1, recv2, recv3, recv4
        self.acc, self.acc2, self.fin, self.snd, self.rcv = acc, acc2, fin, snd, rcv
        self.partner = me + 1 - 2 * self.core
        self.hops = {(axis, step): self.device(*((0, step) if axis == 0 else (step, 0))) for axis in (0, 1) for step in (1, 3)}

    def device(self, dy, dx):
        return (lax.rem(self.y + dy, 4) * 4 + lax.rem(self.x + dx, 4)) * 2 + self.core

    def peers(self):
        return [self.partner, *self.hops.values()]

    def copy(self, lane, kind, slot, src, dst, target):
        return pltpu.make_async_remote_copy(
            src_ref=src, dst_ref=dst, send_sem=self.snd.at[lane, kind, slot], recv_sem=self.rcv.at[lane, kind, slot],
            device_id={"seq": target}, device_id_type=MESH)

    def late(self, pair, yes, no):
        first, end = self.turn
        return jnp.where((pair >= first) & (pair < end), yes, no)

    def swap(self, ring, slot):
        return self.copy(0, 0, slot, self.parts.at[ring, :, :, 1 - self.core], self.recv0.at[slot], self.partner)

    def copies(self, stage, kind, pair, held, slot):
        axis = kind if stage < 3 else 1 - kind
        plus, minus = self.hops[axis, 1], self.hops[axis, 3]
        half = CB // 2
        if stage == 1:
            if axis == 0:
                minus = self.late(pair, plus, minus)
            ends = [(self.acc.at[kind, held, 2, pl.ds(0, 2)], self.recv1), (self.acc.at[kind, held, 2, pl.ds(2, 2)], self.recv1)]
        elif stage == 2:
            ends = [(self.acc.at[kind, held, 1], self.recv2), (self.acc.at[kind, held, 3], self.recv2)]
        elif stage == 3:
            ends = [(self.acc2.at[kind, held, 2, :, pl.ds(0, half)], self.recv3), (self.acc2.at[kind, held, 2, :, pl.ds(half, half)], self.recv3)]
        else:
            ends = [(self.acc2.at[kind, held, 1], self.recv4), (self.acc2.at[kind, held, 3], self.recv4)]
        lane = 2 * stage - 1
        return [self.copy(lane + i, kind, slot, src, buf.at[kind, slot, i], (plus, minus)[i]) for i, (src, buf) in enumerate(ends)]

    def add(self, stage, kind, pair, held, slot, ring):
        acc, acc2 = self.acc, self.acc2
        if stage == 1:
            def row(r1):
                for r2 in range(4):
                    ry, rx = (r2, r1) if kind == 0 else (r1, r2)
                    chip = lax.rem(self.y + ry, 4) * 4 + lax.rem(self.x + rx, 4)
                    acc[kind, held, r1, r2] = self.parts[ring, kind, chip, self.core] + self.recv0[slot, kind, chip]
            cdiv_loop(4, row)
        elif stage == 2:
            back = self.late(pair, 1, 3) if kind == 0 else 3
            acc[kind, held, 1, 0:2] += self.recv1[kind, slot, 0]
            acc[kind, held, back, 2:4] += self.recv1[kind, slot, 1]
        elif stage == 3:
            acc2[kind, held] = acc[kind, held, 0] + (self.recv2[kind, slot, 0] + self.recv2[kind, slot, 1])
        elif stage == 4:
            half = CB // 2
            acc2[kind, held, 1, :, 0:half] += self.recv3[kind, slot, 0]
            acc2[kind, held, 3, :, half:] += self.recv3[kind, slot, 1]
        else:
            self.fin[pair, kind] = acc2[kind, held, 0] + (self.recv4[kind, slot, 0] + self.recv4[kind, slot, 1])

    def when(self, pair, fn):
        if isinstance(pair, int):
            if 0 <= pair < self.pairs:
                fn()
        else:
            pl.when((pair >= 0) & (pair < self.pairs))(fn)

    def tick(self, t):
        now, land = mod(t, SLOTS), mod(t + SLOTS - LAG, SLOTS)
        ring_now, ring_land = mod(t, RING), mod(t + RING - LAG, RING)
        for stage in range(5, -1, -1):
            pair = t - LAG * stage
            held = land if stage % 2 else now

            def move(stage=stage, pair=pair, held=held):
                if stage == 0:
                    self.swap(ring_now, now).start()
                    return
                if stage == 1:
                    with jax.named_scope("t_wait1"):
                        self.swap(ring_land, land).wait()
                for kind in (0, 1):
                    if stage > 1:
                        with jax.named_scope(f"t_wait{stage}"):
                            for c in self.copies(stage - 1, kind, pair, held, land):
                                c.wait()
                    self.add(stage, kind, pair, held, land, ring_land)
                    if stage < 5:
                        for c in self.copies(stage, kind, pair, held, now):
                            c.start()
            self.when(pair, move)


def pick(i, table):
    out = 0
    for key, value in table.items():
        out = jnp.where(i == key, value, out)
    return out


def norm_back(x, gain, grad, res):
    xf = x.astype(F32)
    inv = lax.rsqrt(jnp.mean(xf * xf, axis=-1, keepdims=True) + NORM_EPS)
    unit = xf * inv
    gu = grad * gain
    out = inv * (gu - unit * jnp.mean(gu * unit, axis=-1, keepdims=True)) + res.astype(F32)
    gu = grad * unit
    return out.astype(BF), jnp.sum(gu.reshape(gu.shape[0] // 8, 8, gu.shape[1]), axis=0)


def plan(n_mlp, n_down, nc):
    order = [("o", g) for g in range(nc)] + [(name, g) for g in range(nc) for name in "qkv"]
    base = n_mlp + n_down
    return base, {name: (base + i // 2, i % 2) for i, name in enumerate(order)}, base + len(order) // 2


def bwd_kernel(n, head_dim, dims, ga, gm, x_h, dout_h, q_h, kt_h, k_h, v_h, hat_h, ot_h, xm_h, hm_h, hmt_h, qr_h, lse_h, cos_h, sin_h,
               wq_h, wk_h, wv_h, wo_h, wg_h, wu_h, wd_h,
               dx_h, fin_h, dga_o, dgm_o,
               parts, recv0, recv1, recv2, recv3, recv4, acc, acc2, fin, snd, rcv,
               dor, lser, deltar, hsnd, hrcv, osnd, orcv, gsend, grecv, gsem, ld,
               xbuf, mbuf, gnm, gmid, ot, hat, wo, dot_, lse, delta, cos_i, sin_i, dgain):
    rows, toks, width, hd, ff = dims
    ext, total = toks + WINDOW, rows * toks
    pw = 2 * head_dim
    n_pairs = hd // pw
    tb, n_steps = toks // QB, n_pairs * rows
    nb, nc, sub = ff // CB, width // CB, ff // width
    rpd = width // n
    per, half_sub = CB // pw, sub // 2
    base, place, pairs = plan(nb, nc * half_sub, nc)
    comm = Torus(n, pairs, (nb - 1, nb - 1 + n_pairs), parts, recv0, recv1, recv2, recv3, recv4, acc, acc2, fin, snd, rcv)
    me = lax.axis_index("seq")
    left = lax.rem(me + n - 1, n)
    barrier = pltpu.get_barrier_semaphore()

    def greet(i):
        pl.semaphore_signal(barrier, inc=1, device_id={"seq": lax.rem(me + i + 1, n)}, device_id_type=MESH)

    def load(i, s, d):
        c = pltpu.make_async_copy(s, d, ld.at[i])
        c.start()
        return c

    def late(i):
        s, d = ((xm_h, mbuf), (ot_h, ot), (hat_h, hat), (wo_h, wo), (lse_h, lse), (cos_h, cos_i), (sin_h, sin_i))[i]
        return pltpu.make_async_copy(s, d, ld.at[1 + i])

    def to_left(src, dst, send_sem, recv_sem):
        return pltpu.make_async_remote_copy(src_ref=src, dst_ref=dst, send_sem=send_sem, recv_sem=recv_sem,
                                            device_id={"seq": left}, device_id_type=MESH)

    n_late = 7

    def push_rows(i):
        return to_left(*((lse_h, lser), (delta, deltar))[i], hsnd.at[i], hrcv.at[i])

    def push_out(p):
        pr = pl.ds(aligned(p * pw, pw), pw)
        return [to_left(dot_.at[pr, pl.ds(b * toks, WINDOW)], dor.at[pr, pl.ds(b * WINDOW, WINDOW)], osnd.at[p, b], orcv.at[p, b])
                for b in range(rows)]

    def give_out(p):
        for c in push_out(p):
            c.start()

    def put(spot, value):
        pair, kind = spot
        parts[mod(pair, RING), kind] = value.reshape(n // 2, 2, rpd, CB)

    def spot_of(name, g):
        known = {i: place[name, i] for i in range(nc)}
        return pick(g, {i: s[0] for i, s in known.items()}), pick(g, {i: s[1] for i, s in known.items()})

    def spots(it, blk):
        p, b = it // rows, mod(it, rows)
        pr = pl.ds(aligned(p * pw, pw), pw)
        return pr, pl.ds(aligned(b * toks + blk * QB, QB), QB), pl.ds(aligned(b * ext + blk * QB, QB), 3 * QB)

    def row_of(it):
        return mod(it, rows) * n_pairs + it // rows

    def mlp(hm, hmt, actt, wgu, wd, dgu, wld):
        def weights(j, slot):
            c = aligned(j * CB, CB)
            return [pltpu.make_async_copy(wg_h.at[:, pl.ds(c, CB)], wgu.at[slot, :, pl.ds(0, CB)], wld.at[slot, 0]),
                    pltpu.make_async_copy(wu_h.at[:, pl.ds(c, CB)], wgu.at[slot, :, pl.ds(CB, CB)], wld.at[slot, 1]),
                    pltpu.make_async_copy(wd_h.at[pl.ds(c, CB), :], wd.at[slot], wld.at[slot, 2])]

        for c in weights(0, 0):
            c.start()
        ld_hm, ld_x, ld_hmt = load(8, hm_h, hm), load(0, dout_h, xbuf), load(9, hmt_h, hmt)
        cdiv_loop(n - 1, greet)
        gnm[:] = jnp.zeros_like(gnm)
        gsend[:] = jnp.zeros_like(gsend)
        dgain[:] = jnp.zeros_like(dgain)
        ld_hm.wait()
        ld_x.wait()
        ld_hmt.wait()
        for i in range(n_late):
            late(i).start()

        def block(j):
            slot = lax.rem(j, 2)
            for c in weights(j, slot):
                c.wait()

            @pl.when(j + 1 < nb)
            def _():
                for c in weights(j + 1, 1 - slot):
                    c.start()

            c0 = pl.multiple_of(j * CB, CB)
            with jax.named_scope("b_mlp"):
                for b in range(rows):
                    r = slice(b * toks, (b + 1) * toks)
                    gu = dot(hm[r, :], wgu[slot])
                    gact = dot(xbuf[r, :], wd[slot], NT).astype(BF).astype(F32)
                    gate, up = gu[:, :CB], gu[:, CB:]
                    sig = 1.0 / (1.0 + jnp.exp(-gate))
                    swish = gate * sig
                    actt[pl.ds(c0, CB), r] = (swish * up).astype(BF).T
                    dgu[r, :CB] = (gact * up * (sig + swish * (1.0 - sig))).astype(BF)
                    dgu[r, CB:] = (gact * swish).astype(BF)
                both = dot(hmt[:], dgu[:])
                ring = lax.rem(j, RING)
                parts[ring, 0] = both[:, :CB].reshape(n // 2, 2, rpd, CB)
                parts[ring, 1] = both[:, CB:].reshape(n // 2, 2, rpd, CB)
                for b in range(rows):
                    r = slice(b * toks, (b + 1) * toks)
                    gnm[r, :] += dot(dgu[r, :], wgu[slot], NT)

            @pl.when(j == 0)
            def _():
                pl.semaphore_wait(barrier, n - 1)
                push_rows(0).start()

            comm.tick(j)

        cdiv_loop(nb, block)

        def down(c):
            share = n // 2 // sub
            c0 = pl.multiple_of(c * CB, CB)
            for m in range(sub):
                res = dot(actt[m * width:(m + 1) * width, :], xbuf[:, pl.ds(c0, CB)]).reshape(share, 2, sub, rpd, CB)
                for i in range(sub):
                    pair = nb + c * half_sub + i // 2
                    parts[lax.rem(pair, RING), i % 2, m * share:(m + 1) * share] = res[:, :, i]

        for i in range(n_late):
            late(i).wait()

        def mid(i):
            r = pl.ds(pl.multiple_of(i * QB, QB), QB)
            out, dg = norm_back(mbuf[r, :], gm[:], gnm[r, :], xbuf[r, :])
            gmid[r, :] = out
            dgain[8:, :] += dg

        def deltas(it):
            for blk in range(tb):
                pr, cols, _ = spots(it, blk)
                both = dot_[pr, cols].astype(F32) * ot[pr, cols].astype(F32)
                delta[row_of(it), blk:blk + 1, :] = jnp.concatenate(
                    [col_sum(both[:head_dim]), col_sum(both[head_dim:])], axis=1)

        def column(c):
            with jax.named_scope("b_down"):
                down(c)
            comm.tick(nb + c + jnp.minimum(c, 1))

            @pl.when(c > 0)
            def _():
                give_out(c)

            @pl.when(c == 0)
            def _():
                with jax.named_scope("b_mid"):
                    cdiv_loop(total // QB, mid)
                with jax.named_scope("b_dot"):
                    dot_[:] = dot(wo[:], gmid[:], NT).astype(BF)
                    cdiv_loop(n_steps, deltas)
                comm.tick(nb + 1)
                push_rows(1).start()
                give_out(0)

        cdiv_loop(nc, column)

    vm = lambda *s: pltpu.VMEM(s, BF)
    vf = lambda *s: pltpu.VMEM(s, F32)
    pl.run_scoped(mlp, vm(total, width), vm(width, total), vm(ff, total), vm(2, width, 2 * CB), vm(2, CB, width), vm(total, 2 * CB),
                  pltpu.SemaphoreType.DMA((2, 3)))
    head = nb + nc + 1

    def attention(q, kt, k, v, qr, dv, sc0, sc1, sc2, sr, dp0, dp1, dp2, dr, pb0, pb1, pb2, pr_, ds0, ds1, ds2, dsr):
        dqt, dkt = ot, q
        wq, wk, wv = k.at[:hd], kt.at[:, :width], v.at[:hd]
        sc, dp, pb, ds = (sc0, sc1, sc2), (dp0, dp1, dp2), (pb0, pb1, pb2), (ds0, ds1, ds2)
        lds = [load(8 + i, s, d) for i, (s, d) in enumerate(((q_h, q), (k_h, k), (v_h, v), (qr_h, qr), (kt_h, kt)))]
        ld_x2 = load(0, x_h, xbuf)

        def out_grad(g):
            put(spot_of("o", g), dot(ot[:], gmid[:, pl.ds(pl.multiple_of(g * CB, CB), CB)]))

        with jax.named_scope("b_dwo"):
            cdiv_loop(nc, out_grad)
        for c in lds:
            c.wait()
        upper = upper_mask()
        first, last = me == 0, me == n - 1

        def right(it, i):
            p, b = it // rows, mod(it, rows)
            return pl.ds(aligned(p * pw, pw), pw), pl.ds(aligned(b * WINDOW + i * QB, QB), QB), pl.ds(aligned(b * ext + toks + i * QB, QB), WINDOW - i * QB)

        def score(it):
            for blk in range(tb):
                pr, cols, keys = spots(it, blk)
                sc[blk][:] = dot(k[keys, pr], stack_pair(q[pr, cols]))
                dp[blk][:] = dot(v[keys, pr], stack_pair(dot_[pr, cols]))
            for i, rs in enumerate((slice(0, WINDOW), slice(WINDOW, 3 * QB))):
                pr, cols, keys = right(it, i)
                sr[rs, :] = dot(k[keys, pr], stack_pair(qr[pr, cols]))
                dr[rs, :] = dot(v[keys, pr], stack_pair(dor[pr, cols]))

        def soften(it):
            row = row_of(it)
            for blk in range(tb):
                s02, s1 = merged(sc[blk][:], upper, *start_bias(first, blk))
                norm, mean = lse[row, blk:blk + 1, :], delta[row, blk:blk + 1, :]
                p02, p1 = jnp.exp(s02 - norm), jnp.exp(s1 - norm)
                g02, g1 = jnp.where(upper, dp[blk][:QB], dp[blk][2 * QB:]), dp[blk][QB:2 * QB]
                pb[blk][:] = banded(p02, p1, upper)
                ds[blk][:] = banded(p02 * (g02 - mean), p1 * (g1 - mean), upper)
            for i, blk in ((0, 0), (0, 1), (1, 2)):
                rs = slice(blk * QB, (blk + 1) * QB)
                p = jnp.exp(sr[rs, :] - jnp.where(last, -NEG, lser[row, i:i + 1, :]))
                g = p * (dr[rs, :] - deltar[row, i:i + 1, :])
                pr_[rs, :] = (p if blk == 1 else jnp.where(upper, p, 0.0)).astype(BF)
                dsr[rs, :] = (g if blk == 1 else jnp.where(upper, g, 0.0)).astype(BF)

        def grads(it):
            ks, vs = [], []
            for blk in range(tb):
                pr, cols, keys = spots(it, blk)
                own = slice(max(0, 2 - blk) * QB, 3 * QB)
                vs.append(dot(pb[blk][own, :], stack_pair(dot_[pr, cols]), NT))
                ks.append(dot(ds[blk][own, :], stack_pair(q[pr, cols]), NT))
                dq = unstack_pair(dot(kt[pr, keys], ds[blk][:])) * (head_dim ** -0.5)
                dqt[pr, cols] = rope(dq, cos_i[:, cols], sin_i[:, cols], -1, head_dim).astype(BF)
            for i, rs in enumerate((slice(0, WINDOW), slice(WINDOW, 3 * QB))):
                pr, cols, _ = right(it, i)
                vs.append(dot(pr_[rs, :], stack_pair(dor[pr, cols]), NT))
                ks.append(dot(dsr[rs, :], stack_pair(qr[pr, cols]), NT))
            for j in range(tb):
                pr, cols, _ = spots(it, j)
                gv, gk = (sum(x[i][(j - max(0, i - 2)) * QB:(j - max(0, i - 2) + 1) * QB] for i in range(j, j + 3)) for x in (vs, ks))
                dv[cols, pr] = gv.astype(BF)
                dkt[pr, cols] = rope(gk.T, cos_i[:, cols], sin_i[:, cols], -1, head_dim).astype(BF)

        def close_group(g):
            cols = pl.ds(pl.multiple_of(g * CB, CB), CB)
            with jax.named_scope("b_dwqkv"):
                put(spot_of("q", g), dot(hat[:], dqt[cols, :], NT))
                put(spot_of("k", g), dot(hat[:], dkt[cols, :], NT))
                put(spot_of("v", g), dot(hat[:], dv[:, cols]))

        def weights():
            return [pltpu.make_async_copy(s, d, ld.at[8 + i]) for i, (s, d) in enumerate(((wq_h, wq), (wk_h, wk), (wv_h, wv)))]

        def arrived(p):
            with jax.named_scope("b_hwait"):
                for c in push_out(p):
                    c.wait()

        def walk(it):
            @pl.when((lax.rem(it + 1, rows) == 0) & (it + 1 < n_steps))
            def _():
                arrived((it + 1) // rows)

            @pl.when(it < n_steps)
            def _():
                with jax.named_scope("b_attn"):
                    grads(it - 1)
                    soften(it)
                    score(jnp.minimum(it + 1, n_steps - 1))

            @pl.when(it == n_steps)
            def _():
                grads(n_steps - 1)
                for c in weights():
                    c.start()

            @pl.when(lax.rem(it, rows) == 0)
            def _():
                p = it // rows - 1

                @pl.when(lax.rem(p, per) == per - 1)
                def _():
                    close_group(p // per)

                comm.tick(head + 1 + p)

                @pl.when(p + nc + 1 < n_pairs)
                def _():
                    give_out(p + nc + 1)

        comm.tick(head)
        give_out(nc)
        for i in range(2):
            push_rows(i).wait()
        arrived(0)
        if rows == 1:
            arrived(1)
        score(0)
        soften(0)
        score(1)
        cdiv_loop(n_steps, lambda i: walk(i + 1))
        for c in weights():
            c.wait()
        ld_x2.wait()

        def into(b):
            r = pl.ds(pl.multiple_of(b * toks, QB), toks)
            with jax.named_scope("b_into"):
                gnm[r, :] = dot(dqt[:, r], wq[:], TN) + dot(dkt[:, r], wk[:], TN) + dot(dv[r, :], wv[:])

            def final(i):
                r = pl.ds(pl.multiple_of((b * tb + i) * QB, QB), QB)
                out, dg = norm_back(xbuf[r, :], ga[:], gnm[r, :], gmid[r, :])
                mbuf[r, :] = out
                dgain[:8, :] += dg

            with jax.named_scope("b_final"):
                cdiv_loop(tb, final)
            comm.tick(head + 1 + n_pairs + b)

        cdiv_loop(rows, into)

    score_bufs = [vf(3 * QB, 2 * QB)] * 8 + [vm(3 * QB, 2 * QB)] * 8
    pl.run_scoped(attention, vm(hd, total), vm(hd, rows * ext), vm(rows * ext, hd), vm(rows * ext, hd), vm(hd, rows * WINDOW), vm(total, hd), *score_bufs)
    out_copy = load(1, mbuf, dx_h)
    gains = jnp.concatenate([col_sum(dgain[:8, :]), col_sum(dgain[8:, :]), jnp.zeros((6, width), F32)], axis=0)
    for p in range(n):
        gsend[p, :, 0:rpd] = gains[:, p * rpd:(p + 1) * rpd]

    def spread(i):
        to = lax.rem(me + i + 1, n)
        pltpu.make_async_remote_copy(src_ref=gsend.at[to], dst_ref=grecv.at[i], send_sem=gsem.at[0], recv_sem=gsem.at[1],
                                     device_id={"seq": to}, device_id_type=MESH).start()

    cdiv_loop(n - 1, spread)
    end = pairs + 5 * LAG
    run = lambda lo, hi: lax.fori_loop(lo, hi, lambda t, c: (comm.tick(t), c)[1], 0)
    run(head + 1 + n_pairs + rows, end - LAG)
    keep_most = load(0, fin.at[pl.ds(0, pairs - LAG)], fin_h.at[pl.ds(0, pairs - LAG)])
    to_left(gsend.at[pl.ds(0, n - 1)], grecv, gsem.at[0], gsem.at[1]).wait()
    sums = gsend[me]
    for i in range(n - 1):
        sums = sums + grecv[i]
    dga_o[:] = sums[0:1, 0:rpd]
    dgm_o[:] = sums[1:2, 0:rpd]
    out_copy.wait()
    run(end - LAG, end)
    with jax.named_scope("b_end"):
        keep_rest = load(1, fin.at[pl.ds(pairs - LAG, LAG)], fin_h.at[pl.ds(pairs - LAG, LAG)])
        keep_most.wait()
        keep_rest.wait()


def spread_kernel(dims, dx_i, fin_i, dga_i, dgm_i, dx_o, dga_o, dgm_o, *refs):
    head_dim, n, width, ff = dims
    outs, (buf, fin), stage, sem = refs[:7], refs[7:9], refs[9:16], refs[16]
    dq, dk, dv, do, dg, du, dd = stage
    nb, nc, sub = ff // CB, width // CB, ff // width
    rpd = width // n
    place = plan(nb, nc * sub // 2, nc)[1]
    get, get_fin, out = (pltpu.make_async_copy(*ends, sem.at[len(outs) + i]) for i, ends in enumerate(((dx_i, buf), (fin_i, fin), (buf, dx_o))))
    get_fin.start()
    get.start()
    dga_o[:] = dga_i[:]
    dgm_o[:] = dgm_i[:]
    get_fin.wait()
    for j in range(nb):
        dg[:, j * CB:(j + 1) * CB] = fin[j, 0]
        du[:, j * CB:(j + 1) * CB] = fin[j, 1]
    for c in range(nc):
        for i in range(sub):
            dd[i * rpd:(i + 1) * rpd, c * CB:(c + 1) * CB] = fin[nb + (c * sub + i) // 2, i % 2]
    for g in range(nc):
        do[:, g * CB:(g + 1) * CB] = fin[place["o", g]]
        for name, ref in (("q", dq), ("k", dk), ("v", dv)):
            val = fin[place[name, g]]
            for h in range(CB // head_dim):
                ref[g * (CB // head_dim) + h] = val[:, h * head_dim:(h + 1) * head_dim]
    keeps = [pltpu.make_async_copy(s, d, sem.at[i]) for i, (s, d) in enumerate(zip(stage, outs))]
    for c in keeps:
        c.start()
    get.wait()
    out.start()
    for c in keeps:
        c.wait()
    out.wait()


def run_bwd(n, head_dim, ga, gm, x, dout, q, kt, k, v, hat, ot, xm, hm, hmt, qr, lse, cos_t, sin_t, wq, wk, wv, wo, wg, wu, wd, rows):
    total, width = x.shape
    hd, ff = wq.shape[0], wg.shape[1]
    toks = total // rows
    rpd, heads = width // n, hd // head_dim
    nb, nc, sub = ff // CB, width // CB, ff // width
    pairs = plan(nb, nc * sub // 2, nc)[2]
    n_pairs = hd // (2 * head_dim)
    f = lambda *s: jax.ShapeDtypeStruct(s, F32)
    dx_t = jax.ShapeDtypeStruct((total, width), BF)
    vm = lambda *s: pltpu.VMEM(s, BF)
    vf = lambda *s: pltpu.VMEM(s, F32)
    dma = lambda *s: pltpu.SemaphoreType.DMA(s)
    line = vf(rows * n_pairs, 8, 2 * QB)
    scratch = [vf(RING, 2, n // 2, 2, rpd, CB), vf(SLOTS, 2, n // 2, rpd, CB), vf(2, SLOTS, 2, 2, rpd, CB), vf(2, SLOTS, 2, 4, rpd, CB),
               vf(2, SLOTS, 2, rpd, CB // 2), vf(2, SLOTS, 2, rpd, CB), vf(2, SLOTS, 4, 4, rpd, CB), vf(2, SLOTS, 4, rpd, CB), vf(pairs, 2, rpd, CB),
               dma(9, 2, SLOTS), dma(9, 2, SLOTS),
               vm(hd, rows * WINDOW), line, line, dma(2), dma(2), dma(n_pairs, rows), dma(n_pairs, rows),
               vf(n, 8, 128), vf(n - 1, 8, 128), dma(2), dma(13),
               vm(total, width), vm(total, width), vf(total, width), vm(total, width), vm(hd, total), vm(width, total), vm(hd, width), vm(hd, total), line, line, vf(*cos_t.shape), vf(*cos_t.shape), vf(16, width)]
    mid = pl.pallas_call(
        functools.partial(bwd_kernel, n, head_dim, (rows, toks, width, hd, ff)), out_shape=[dx_t, f(pairs, 2, rpd, CB), f(1, rpd), f(1, rpd)],
        in_specs=vmem_spec(2) + any_spec(22), out_specs=any_spec(2) + vmem_spec(2), scratch_shapes=scratch,
        compiler_params=pltpu.CompilerParams(collective_id=1, has_side_effects=True, vmem_limit_bytes=VMEM_LIMIT),
        name="backward")(ga, gm, x, dout, q, kt, k, v, hat, ot, xm, hm, hmt, qr, lse, cos_t, sin_t, wq, wk, wv, wo, wg, wu, wd)
    outs = [f(heads, rpd, head_dim)] * 3 + [f(rpd, width), f(rpd, ff), f(rpd, ff), f(ff // n, width)]
    return pl.pallas_call(
        functools.partial(spread_kernel, (head_dim, n, width, ff)), out_shape=[dx_t, f(1, rpd), f(1, rpd)] + outs,
        in_specs=any_spec(2) + vmem_spec(2), out_specs=any_spec(1) + vmem_spec(2) + any_spec(7),
        scratch_shapes=[vm(total, width), vf(pairs, 2, rpd, CB), *[vf(*o.shape) for o in outs], dma(10)],
        name="spread")(*mid)


def solution(mesh):
    n = mesh.shape["seq"]

    def device_step(hidden, positions, g_attn, g_mlp, w_query, w_key, w_value, w_out, w_gate, w_up, w_down, d_out):
        rows, toks, width = hidden.shape
        layers, _, heads, head_dim = w_query.shape
        hd = heads * head_dim
        half = head_dim // 2
        inv_freq = 1.0 / (10000.0 ** (jnp.arange(half, dtype=F32) * (2.0 / head_dim)))
        turn = lambda w: w[0].transpose(1, 2, 0).reshape(hd, width)
        wq, wk, wv = turn(w_query), turn(w_key), turn(w_value)
        fwd = run_fwd(n, hidden, positions, inv_freq[:, None], g_attn, g_mlp, wq, wk, wv, w_out[0], head_dim)
        out = run_bwd(n, head_dim, g_attn, g_mlp, hidden.reshape(rows * toks, width), d_out.reshape(rows * toks, width), *fwd,
                      wq, wk, wv, w_out[0], w_gate[0], w_up[0], w_down[0], rows)
        dx, dga, dgm, dq, dk, dv, do, dg, du, dd = out
        back = lambda w: w.transpose(1, 0, 2)[None]
        return (dx.reshape(rows, toks, width), dga, dgm, back(dq), back(dk), back(dv), do[None], dg[None], du[None], dd[None])

    tok_spec = P("data", "seq", None)
    vec_spec = P(None, ("data", "seq"))
    mat_spec = P(None, ("data", "seq"), None)
    head_spec = P(None, ("data", "seq"), None, None)
    in_specs = (tok_spec, P("data", "seq")) + (P(),) * 9 + (tok_spec,)
    out_specs = (tok_spec, vec_spec, vec_spec, head_spec, head_spec, head_spec, mat_spec, mat_spec, mat_spec, mat_spec)
    return jax.shard_map(device_step, mesh=mesh, in_specs=in_specs, out_specs=out_specs, check_vma=False)
```

```python
import functools, math
import numpy as np
import jax, jax.numpy as jnp
from jax import lax
from jax.experimental import pallas as pl
from jax.experimental.pallas import tpu as pltpu
from jax.sharding import PartitionSpec as P

WINDOW = 256
NORM_EPS = 1e-5
QB = 128
BF, F32 = jnp.bfloat16, jnp.float32
NN, NT, TN = ((1,), (0,)), ((1,), (1,)), ((0,), (0,))
MESH = pl.DeviceIdType.MESH
NEG = -1e30
VMEM_LIMIT = 67043328


def dot(a, b, dims=NN):
    return lax.dot_general(a, b, (dims, ((), ())), preferred_element_type=F32)


def cdiv_loop(n, body):
    lax.fori_loop(0, n, lambda i, c: (body(i), c)[1], 0)


def mod(a, b):
    return a % b if isinstance(a, int) else lax.rem(a, b)


def aligned(a, b):
    return a if isinstance(a, int) else pl.multiple_of(a, b)


def rope(blk, cos_b, sin_b, sign, head_dim):
    half = head_dim // 2
    parts = []
    for h in range(blk.shape[0] // head_dim):
        first = blk[h * head_dim:h * head_dim + half]
        second = blk[h * head_dim + half:(h + 1) * head_dim]
        if sign > 0:
            parts += [first * cos_b - second * sin_b, second * cos_b + first * sin_b]
        else:
            parts += [first * cos_b + second * sin_b, second * cos_b - first * sin_b]
    return jnp.concatenate(parts, axis=0)


def normed(x, gain):
    xf = x.astype(F32)
    inv = lax.rsqrt(jnp.mean(xf * xf, axis=-1, keepdims=True) + NORM_EPS)
    return (xf * inv * gain).astype(BF)


def stack_pair(pair_t):
    half = pair_t.shape[0] // 2
    zero = jnp.zeros((half, pair_t.shape[1]), pair_t.dtype)
    return jnp.concatenate(
        [jnp.concatenate([pair_t[:half], zero], axis=0), jnp.concatenate([zero, pair_t[half:]], axis=0)], axis=1)


def unstack_pair(both):
    half, cols = both.shape[0] // 2, both.shape[1] // 2
    return jnp.concatenate([both[:half, :cols], both[half:, cols:]], axis=0)


def col_sum(x):
    return jnp.sum(x, axis=0, keepdims=True)


def merged(scores, upper, bias0, bias1):
    return jnp.where(upper, scores[:QB] + bias0, scores[2 * QB:]), scores[QB:2 * QB] + bias1


def banded(p02, p1, upper):
    return jnp.concatenate(
        [jnp.where(upper, p02, 0.0).astype(BF), p1.astype(BF), jnp.where(upper, 0.0, p02).astype(BF)], axis=0)


def upper_mask():
    key_ids = lax.broadcasted_iota(jnp.int32, (QB, 2 * QB), 0)
    query_ids = lax.broadcasted_iota(jnp.int32, (QB, 2 * QB), 1) % QB
    return key_ids > query_ids


def start_bias(first, blk):
    bias = jnp.where(first, NEG, 0.0).astype(F32)
    return (bias if blk < 2 else 0.0), (bias if blk < 1 else 0.0)


def fwd_kernel(n, head_dim, x_h, pos, invf, ga, gm, wq_h, wk_h, wv_h, wo_h,
               q_h, kt_h, k_h, v_h, hat_h, ot_h, xm_h, hm_h, hmt_h, qr_h, lse_h, cos_t, sin_t,
               xv, halo, qr, lse, pos_halo, wq, wk, wv, wo, q, kt, k, v, vt, hat, ot, xm, hm, hmt, hb, hh, acc, acc2, ak, av, cos_h, sin_h,
               sc0, sc1, sc2, pb0, pb1, pb2, ldx, ld, st, snd, rcv, qsnd, qrcv):
    sc, pb = (sc0, sc1, sc2), (pb0, pb1, pb2)
    rows, toks, width = xv.shape
    ext, total, pw = toks + WINDOW, rows * toks, 2 * head_dim
    n_pairs = wq.shape[0] // pw
    tb, n_steps = toks // QB, n_pairs * rows
    me = lax.axis_index("seq")
    right, left = lax.rem(me + 1, n), lax.rem(me + n - 1, n)
    load_x = [pltpu.make_async_copy(x_h.at[b], xv.at[b], ldx.at[b]) for b in range(rows)]
    load_w = [pltpu.make_async_copy(s, d, ld.at[i]) for i, (s, d) in enumerate(((wq_h, wq), (wk_h, wk), (wv_h, wv), (wo_h, wo)))]
    for c in load_x:
        c.start()
    barrier = pltpu.get_barrier_semaphore()
    for other in (left, right):
        pl.semaphore_signal(barrier, inc=1, device_id={"seq": other}, device_id_type=MESH)
    pl.semaphore_wait(barrier, 2)

    def push(i, s, d):
        return pltpu.make_async_remote_copy(src_ref=s, dst_ref=d, send_sem=snd.at[i], recv_sem=rcv.at[i], device_id={"seq": right}, device_id_type=MESH)

    def push_rows(b):
        return push(b, x_h.at[b, toks - WINDOW:, :], halo.at[b])

    send_pos = push(rows, pos, pos_halo)
    send_pos.start()
    for b in range(rows):
        push_rows(b).start()

    def angles(cos_ref, sin_ref, positions):
        count = positions.shape[1]
        for b in range(rows):
            ang = invf[:] * positions[b:b + 1, :].astype(F32)
            cos_ref[:, b * count:(b + 1) * count] = jnp.cos(ang)
            sin_ref[:, b * count:(b + 1) * count] = jnp.sin(ang)

    angles(cos_t, sin_t, pos[:])

    def norm_rows(b):
        for i in range(tb):
            h = normed(xv[b, i * QB:(i + 1) * QB, :], ga[:])
            hb[pl.ds(pl.multiple_of((b * tb + i) * QB, QB), QB), :] = h

    with jax.named_scope("f_norm"):
        for c in load_x:
            c.wait()
        for c in load_w:
            c.start()
        cdiv_loop(rows, norm_rows)
    keep_hat = pltpu.make_async_copy(hat, hat_h, st.at[0])
    tables = cos_t[:], sin_t[:]

    def put_q(src):
        for p in range(n_pairs):
            r = slice(p * pw, (p + 1) * pw)
            q[r, :] = (rope(src[r, :], *tables, 1, head_dim) * (head_dim ** -0.5)).astype(BF)

    def put_own(src, dst_t, dst, turn):
        for p in range(n_pairs):
            r = slice(p * pw, (p + 1) * pw)
            both = (rope(src[r, :], *tables, 1, head_dim) if turn else src[r, :]).astype(BF)
            for b in range(rows):
                blk = both[:, b * toks:(b + 1) * toks]
                own = slice(b * ext + WINDOW, (b + 1) * ext)
                dst_t[r, own] = blk
                dst[own, r] = blk.T

    with jax.named_scope("f_mm"):
        load_w[0].wait()
        load_w[1].wait()
        load_w[2].wait()
        acc[:] = dot(wq[:], hb[:], NT)
        acc2[:] = dot(wk[:], hb[:], NT)
        put_q(acc)
        acc[:] = dot(wv[:], hb[:], NT)
        put_own(acc2, kt, k, True)
        for i in range(total // QB):
            r = slice(i * QB, (i + 1) * QB)
            hat[:, r] = hb[r, :].T
        put_own(acc, vt, v, False)
    keep_hat.start()
    keep_q = pltpu.make_async_copy(q, q_h, st.at[1])
    keep_q.start()

    def push_q(b):
        return pltpu.make_async_remote_copy(src_ref=q.at[:, b * toks:b * toks + WINDOW], dst_ref=qr.at[:, b * WINDOW:(b + 1) * WINDOW],
                                            send_sem=qsnd.at[b], recv_sem=qrcv.at[b], device_id={"seq": left}, device_id_type=MESH)

    for b in range(rows):
        push_q(b).start()
    send_pos.wait()
    angles(cos_h, sin_h, pos_halo[:, toks - WINDOW:])

    def keeps(b):
        wide, cols = pl.ds(pl.multiple_of(b * ext, QB), ext), pl.ds(pl.multiple_of(b * toks, QB), toks)
        ends = ((kt.at[:, wide], kt_h.at[:, wide]), (k.at[wide, :], k_h.at[wide, :]), (v.at[wide, :], v_h.at[wide, :]),
                (ot.at[:, cols], ot_h.at[:, cols]), (hm.at[cols, :], hm_h.at[cols, :]), (hmt.at[:, cols], hmt_h.at[:, cols]),
                (xm.at[cols, :], xm_h.at[cols, :]))
        return [pltpu.make_async_copy(s, d, st.at[2 + b * len(ends) + i]) for i, (s, d) in enumerate(ends)]

    def halo_in(b):
        with jax.named_scope("f_halo_wait"):
            push_rows(b).wait()
        with jax.named_scope("f_halo"):
            for i in range(WINDOW // QB):
                r = slice(i * QB, (i + 1) * QB)
                hh[r, :] = normed(halo[b, r, :], ga[:])
            ak[:] = dot(wk[:], hh[:], NT)
            av[:] = dot(wv[:], hh[:], NT)
            cols = pl.ds(pl.multiple_of(b * WINDOW, QB), WINDOW)
            wide = pl.ds(pl.multiple_of(b * ext, QB), WINDOW)
            near = cos_h[:, cols], sin_h[:, cols]
            for src, dst_t, dst in ((ak, kt, k), (av, vt, v)):
                for p in range(n_pairs):
                    r = slice(p * pw, (p + 1) * pw)
                    blk = (rope(src[r, :], *near, 1, head_dim) if dst is k else src[r, :]).astype(BF)
                    dst_t[r, wide] = blk
                    dst[wide, r] = blk.T
        for c in keeps(b)[:3]:
            c.start()

    upper = upper_mask()
    first = me == 0

    def spots(it, blk):
        b, p = it // n_pairs, mod(it, n_pairs)
        pr = pl.ds(aligned(p * pw, pw), pw)
        return pr, pl.ds(aligned(b * toks + blk * QB, QB), QB), pl.ds(aligned(b * ext + blk * QB, QB), 3 * QB)

    def score(it):
        for blk in range(tb):
            pr, cols, keys = spots(it, blk)
            sc[blk][:] = dot(k[keys, pr], stack_pair(q[pr, cols]))

    def soften(it, blk):
        s02, s1 = merged(sc[blk][:], upper, *start_bias(first, blk))
        top = jnp.max(jnp.maximum(s02, s1), axis=0, keepdims=True)
        e02, e1 = jnp.exp(s02 - top), jnp.exp(s1 - top)
        mass = col_sum(e02 + e1)
        inv = 1.0 / mass
        lse[it, blk:blk + 1, :] = top + jnp.log(mass)
        pb[blk][:] = banded(e02 * inv, e1 * inv, upper)

    def mix(it):
        for blk in range(tb):
            pr, cols, keys = spots(it, blk)
            ot[pr, cols] = unstack_pair(dot(vt[pr, keys], pb[blk][:])).astype(BF)

    def project(b):
        cols = pl.ds(pl.multiple_of(b * toks, QB), toks)
        with jax.named_scope("f_proj"):
            mid = (xv[b].astype(F32) + dot(ot[:, cols], wo[:], TN)).astype(BF)
            xm[cols, :] = mid
            h = normed(mid, gm[:])
            hm[cols, :] = h
            hmt[:, cols] = h.T
        for c in keeps(b)[3:]:
            c.start()

    keep_qr, keep_lse = (pltpu.make_async_copy(*ends, ld.at[i]) for i, ends in enumerate(((qr, qr_h), (lse, lse_h))))
    load_w[3].wait()
    for blk in range(tb):
        pb[blk][:] = jnp.zeros(pb[blk].shape, BF)

    def walk(i):
        it = i - 1

        @pl.when((lax.rem(i, n_pairs) == 0) & (i < n_steps))
        def _():
            halo_in(i // n_pairs)

        @pl.when(i == 0)
        def _():
            score(0)

        @pl.when((i > 0) & (i <= n_steps))
        def _():
            with jax.named_scope("f_attn"):
                mix(jnp.maximum(it - 1, 0))
                for blk in range(tb):
                    soften(it, blk)
                score(jnp.minimum(i, n_steps - 1))

        @pl.when(i == n_steps)
        def _():
            for b in range(rows):
                push_q(b).wait()
            keep_qr.start()

        @pl.when(i > n_steps)
        def _():
            mix(n_steps - 1)

        @pl.when((lax.rem(it, n_pairs) == 0) & (it > 0))
        def _():
            project(it // n_pairs - 1)

    cdiv_loop(n_steps + 2, walk)
    with jax.named_scope("f_store_wait"):
        keep_lse.start()
        keep_hat.wait()
        keep_q.wait()
        keep_qr.wait()
        keep_lse.wait()
        for b in range(rows):
            for c in keeps(b):
                c.wait()


def any_spec(k):
    return [pl.BlockSpec(memory_space=pl.ANY)] * k


def vmem_spec(k):
    return [pl.BlockSpec(memory_space=pltpu.VMEM)] * k


def run_fwd(n, x, pos, invf, ga, gm, wq, wk, wv, wo, head_dim):
    rows, toks, width = x.shape
    hd = wq.shape[0]
    ext, total, n_halo = toks + WINDOW, rows * toks, rows * WINDOW
    half = head_dim // 2
    sds = lambda *s: jax.ShapeDtypeStruct(s, BF)
    dma = lambda *s: pltpu.SemaphoreType.DMA(s)
    outs = [sds(hd, total), sds(hd, rows * ext), sds(rows * ext, hd), sds(rows * ext, hd), sds(width, total), sds(hd, total), sds(total, width), sds(total, width), sds(width, total)]
    outs += [sds(hd, n_halo), jax.ShapeDtypeStruct((rows * hd // (2 * head_dim), 8, 2 * QB), F32)] + [jax.ShapeDtypeStruct((half, total), F32)] * 2
    vm = lambda *s: pltpu.VMEM(s, BF)
    vf = lambda *s: pltpu.VMEM(s, F32)
    scratch = [vm(rows, toks, width), vm(rows, WINDOW, width), vm(hd, n_halo), vf(rows * hd // (2 * head_dim), 8, 2 * QB), pltpu.VMEM((rows, toks), jnp.int32), vm(hd, width), vm(hd, width), vm(hd, width), vm(hd, width),
               vm(hd, total), vm(hd, rows * ext), vm(rows * ext, hd), vm(rows * ext, hd), vm(hd, rows * ext), vm(width, total), vm(hd, total), vm(total, width), vm(total, width), vm(width, total), vm(total, width), vm(WINDOW, width),
               vf(hd, total), vf(hd, total), vf(hd, WINDOW), vf(hd, WINDOW), vf(half, n_halo), vf(half, n_halo),
               *[vf(3 * QB, 2 * QB)] * 3, *[vm(3 * QB, 2 * QB)] * 3,
               dma(rows), dma(4), dma(2 + 7 * rows), dma(rows + 1), dma(rows + 1), dma(rows), dma(rows)]
    return pl.pallas_call(
        functools.partial(fwd_kernel, n, head_dim), out_shape=outs,
        in_specs=any_spec(1) + vmem_spec(4) + any_spec(4), out_specs=any_spec(11) + vmem_spec(2), scratch_shapes=scratch,
        compiler_params=pltpu.CompilerParams(collective_id=0, has_side_effects=True, vmem_limit_bytes=VMEM_LIMIT),
        name="forward")(x, pos, invf, ga, gm, wq, wk, wv, wo)


LAG = 2
SLOTS = 2 * LAG
RING = 8
CB = 256


def at(ref, *idx):
    return ref.at[idx]


class Torus:
    def __init__(self, n, pairs, turn, parts, recv0, recv1, recv2, recv3, recv4, acc, acc2, fin, snd, rcv):
        self.side = math.isqrt(n // 2)
        assert self.side == 4
        me = lax.axis_index("seq")
        self.core = lax.rem(me, 2)
        chip = me // 2
        self.x, self.y = lax.rem(chip, 4), chip // 4
        self.pairs, self.turn = pairs, turn
        self.parts, self.recv0, self.recv1, self.recv2, self.recv3, self.recv4 = parts, recv0, recv1, recv2, recv3, recv4
        self.acc, self.acc2, self.fin, self.snd, self.rcv = acc, acc2, fin, snd, rcv
        self.partner = me + 1 - 2 * self.core
        self.hops = {(axis, step): self.device(*((0, step) if axis == 0 else (step, 0))) for axis in (0, 1) for step in (1, 3)}

    def device(self, dy, dx):
        return (lax.rem(self.y + dy, 4) * 4 + lax.rem(self.x + dx, 4)) * 2 + self.core

    def peers(self):
        return [self.partner, *self.hops.values()]

    def copy(self, lane, kind, slot, src, dst, target):
        return pltpu.make_async_remote_copy(
            src_ref=src, dst_ref=dst, send_sem=self.snd.at[lane, kind, slot], recv_sem=self.rcv.at[lane, kind, slot],
            device_id={"seq": target}, device_id_type=MESH)

    def late(self, pair, yes, no):
        first, end = self.turn
        return jnp.where((pair >= first) & (pair < end), yes, no)

    def swap(self, ring, slot):
        return self.copy(0, 0, slot, self.parts.at[ring, :, :, 1 - self.core], self.recv0.at[slot], self.partner)

    def copies(self, stage, kind, pair, held, slot):
        axis = kind if stage < 3 else 1 - kind
        plus, minus = self.hops[axis, 1], self.hops[axis, 3]
        half = CB // 2
        if stage == 1:
            if axis == 0:
                minus = self.late(pair, plus, minus)
            ends = [(self.acc.at[kind, held, 2, pl.ds(0, 2)], self.recv1), (self.acc.at[kind, held, 2, pl.ds(2, 2)], self.recv1)]
        elif stage == 2:
            ends = [(self.acc.at[kind, held, 1], self.recv2), (self.acc.at[kind, held, 3], self.recv2)]
        elif stage == 3:
            ends = [(self.acc2.at[kind, held, 2, :, pl.ds(0, half)], self.recv3), (self.acc2.at[kind, held, 2, :, pl.ds(half, half)], self.recv3)]
        else:
            ends = [(self.acc2.at[kind, held, 1], self.recv4), (self.acc2.at[kind, held, 3], self.recv4)]
        lane = 2 * stage - 1
        return [self.copy(lane + i, kind, slot, src, buf.at[kind, slot, i], (plus, minus)[i]) for i, (src, buf) in enumerate(ends)]

    def add(self, stage, kind, pair, held, slot, ring):
        acc, acc2 = self.acc, self.acc2
        if stage == 1:
            def row(r1):
                for r2 in range(4):
                    ry, rx = (r2, r1) if kind == 0 else (r1, r2)
                    chip = lax.rem(self.y + ry, 4) * 4 + lax.rem(self.x + rx, 4)
                    acc[kind, held, r1, r2] = self.parts[ring, kind, chip, self.core] + self.recv0[slot, kind, chip]
            cdiv_loop(4, row)
        elif stage == 2:
            back = self.late(pair, 1, 3) if kind == 0 else 3
            acc[kind, held, 1, :2] += self.recv1[kind, slot, 0]
            acc[kind, held, back, 2:] += self.recv1[kind, slot, 1]
        elif stage == 3:
            acc2[kind, held] = acc[kind, held, 0] + (self.recv2[kind, slot, 0] + self.recv2[kind, slot, 1])
        elif stage == 4:
            half = CB // 2
            acc2[kind, held, 1, :, :half] += self.recv3[kind, slot, 0]
            acc2[kind, held, 3, :, half:] += self.recv3[kind, slot, 1]
        else:
            self.fin[pair, kind] = acc2[kind, held, 0] + (self.recv4[kind, slot, 0] + self.recv4[kind, slot, 1])

    def when(self, pair, fn):
        if isinstance(pair, int):
            if 0 <= pair < self.pairs:
                fn()
        else:
            pl.when((pair >= 0) & (pair < self.pairs))(fn)

    def tick(self, t):
        now, land = mod(t, SLOTS), mod(t + SLOTS - LAG, SLOTS)
        ring_now, ring_land = mod(t, RING), mod(t + RING - LAG, RING)
        for stage in range(5, -1, -1):
            pair = t - LAG * stage
            held = land if stage % 2 else now

            def move(stage=stage, pair=pair, held=held):
                if stage == 0:
                    self.swap(ring_now, now).start()
                    return
                if stage == 1:
                    with jax.named_scope("t_wait1"):
                        self.swap(ring_land, land).wait()
                for kind in range(2):
                    if stage > 1:
                        with jax.named_scope(f"t_wait{stage}"):
                            for c in self.copies(stage - 1, kind, pair, held, land):
                                c.wait()
                    self.add(stage, kind, pair, held, land, ring_land)
                    if stage < 5:
                        for c in self.copies(stage, kind, pair, held, now):
                            c.start()
            self.when(pair, move)


def pick(i, table):
    out = 0
    for key, value in table.items():
        out = jnp.where(i == key, value, out)
    return out


def norm_back(x, gain, grad, res):
    xf = x.astype(F32)
    inv = lax.rsqrt(jnp.mean(xf * xf, axis=-1, keepdims=True) + NORM_EPS)
    unit = xf * inv
    gu = grad * gain
    out = inv * (gu - unit * jnp.mean(gu * unit, axis=-1, keepdims=True)) + res.astype(F32)
    gu = grad * unit
    return out.astype(BF), jnp.sum(gu.reshape(-1, 8, gu.shape[-1]), axis=0)


def plan(n_mlp, n_down, nc):
    order = [("o", g) for g in range(nc)] + [(name, g) for g in range(nc) for name in "qkv"]
    base = n_mlp + n_down
    return base, {name: (base + i // 2, i % 2) for i, name in enumerate(order)}, base + len(order) // 2


def bwd_kernel(n, head_dim, dims, ga, gm, x_h, dout_h, q_h, kt_h, k_h, v_h, hat_h, ot_h, xm_h, hm_h, hmt_h, qr_h, lse_h, cos_h, sin_h,
               wq_h, wk_h, wv_h, wo_h, wg_h, wu_h, wd_h,
               dx_h, fin_h,
               parts, recv0, recv1, recv2, recv3, recv4, acc, acc2, fin, snd, rcv,
               dor, lser, deltar, hsnd, hrcv, osnd, orcv, gsend, grecv, gsem, ld,
               xbuf, mbuf, gnm, gmid, ot, hat, wo, dot_, lse, delta, cos_i, sin_i, dgain):
    rows, toks, width, hd, ff = dims
    ext, total = toks + WINDOW, rows * toks
    pw = 2 * head_dim
    n_pairs = hd // pw
    tb, n_steps = toks // QB, n_pairs * rows
    nb, nc, sub = ff // CB, width // CB, ff // width
    rpd = width // n
    per, half_sub = CB // pw, sub // 2
    base, place, pairs = plan(nb, nc * half_sub, nc)
    comm = Torus(n, pairs, (nb - 1, nb + n_pairs), parts, recv0, recv1, recv2, recv3, recv4, acc, acc2, fin, snd, rcv)
    me = lax.axis_index("seq")
    left = lax.rem(me + n - 1, n)
    barrier = pltpu.get_barrier_semaphore()

    def greet(i):
        pl.semaphore_signal(barrier, inc=1, device_id={"seq": lax.rem(me + i + 1, n)}, device_id_type=MESH)

    def load(i, s, d):
        c = pltpu.make_async_copy(s, d, ld.at[i])
        c.start()
        return c

    def late(i):
        s, d = ((xm_h, mbuf), (ot_h, ot), (hat_h, hat), (wo_h, wo), (lse_h, lse), (cos_h, cos_i), (sin_h, sin_i))[i]
        return pltpu.make_async_copy(s, d, ld.at[1 + i])

    def to_left(src, dst, send_sem, recv_sem):
        return pltpu.make_async_remote_copy(src_ref=src, dst_ref=dst, send_sem=send_sem, recv_sem=recv_sem,
                                            device_id={"seq": left}, device_id_type=MESH)

    n_late = 7

    def push_rows(i):
        return to_left(*((lse_h, lser), (delta, deltar))[i], hsnd.at[i], hrcv.at[i])

    def push_out(p):
        pr = pl.ds(aligned(p * pw, pw), pw)
        return [to_left(dot_.at[pr, pl.ds(b * toks, WINDOW)], dor.at[pr, pl.ds(b * WINDOW, WINDOW)], osnd.at[p, b], orcv.at[p, b])
                for b in range(rows)]

    def give_out(p):
        for c in push_out(p):
            c.start()

    def put(spot, value):
        pair, kind = spot
        parts[mod(pair, RING), kind] = value.reshape(n // 2, 2, rpd, CB)

    def spot_of(name, g):
        known = {i: place[name, i] for i in range(nc)}
        return pick(g, {i: s[0] for i, s in known.items()}), pick(g, {i: s[1] for i, s in known.items()})

    def spots(it, blk):
        p, b = it // rows, mod(it, rows)
        pr = pl.ds(aligned(p * pw, pw), pw)
        return pr, pl.ds(aligned(b * toks + blk * QB, QB), QB), pl.ds(aligned(b * ext + blk * QB, QB), 3 * QB)

    def row_of(it):
        return mod(it, rows) * n_pairs + it // rows

    def mlp(hm, hmt, actt, wgu, wd, dgu, wld):
        def weights(j, slot):
            c = aligned(j * CB, CB)
            return [pltpu.make_async_copy(wg_h.at[:, pl.ds(c, CB)], wgu.at[slot, :, :CB], wld.at[slot, 0]),
                    pltpu.make_async_copy(wu_h.at[:, pl.ds(c, CB)], wgu.at[slot, :, CB:], wld.at[slot, 1]),
                    pltpu.make_async_copy(wd_h.at[pl.ds(c, CB), :], wd.at[slot], wld.at[slot, 2])]

        for c in weights(0, 0):
            c.start()
        ld_hm, ld_x, ld_hmt = load(8, hm_h, hm), load(0, dout_h, xbuf), load(9, hmt_h, hmt)
        cdiv_loop(n - 1, greet)
        gnm[:] = jnp.zeros_like(gnm)
        gsend[:] = jnp.zeros_like(gsend)
        dgain[:] = jnp.zeros_like(dgain)
        ld_hm.wait()
        ld_x.wait()
        ld_hmt.wait()
        for i in range(n_late):
            late(i).start()

        def block(j):
            slot = lax.rem(j, 2)
            for c in weights(j, slot):
                c.wait()

            @pl.when(j + 1 < nb)
            def _():
                for c in weights(j + 1, 1 - slot):
                    c.start()

            c0 = pl.multiple_of(j * CB, CB)
            with jax.named_scope("b_mlp"):
                for b in range(rows):
                    r = slice(b * toks, (b + 1) * toks)
                    gu = dot(hm[r, :], wgu[slot])
                    gact = dot(xbuf[r, :], wd[slot], NT).astype(BF).astype(F32)
                    gate, up = gu[:, :CB], gu[:, CB:]
                    sig = jax.nn.sigmoid(gate)
                    swish = gate * sig
                    actt[pl.ds(c0, CB), r] = (swish * up).astype(BF).T
                    dgu[r, :CB] = (gact * up * (sig + swish * (1.0 - sig))).astype(BF)
                    dgu[r, CB:] = (gact * swish).astype(BF)
                both = dot(hmt[:], dgu[:])
                ring = lax.rem(j, RING)
                parts[ring, 0] = both[:, :CB].reshape(n // 2, 2, rpd, CB)
                parts[ring, 1] = both[:, CB:].reshape(n // 2, 2, rpd, CB)
                for b in range(rows):
                    r = slice(b * toks, (b + 1) * toks)
                    gnm[r, :] += dot(dgu[r, :], wgu[slot], NT)

            @pl.when(j == 0)
            def _():
                pl.semaphore_wait(barrier, n - 1)
                push_rows(0).start()

            comm.tick(j)

        cdiv_loop(nb, block)

        def down(c):
            share = n // 2 // sub
            c0 = pl.multiple_of(c * CB, CB)
            for m in range(sub):
                res = dot(actt[m * width:(m + 1) * width, :], xbuf[:, pl.ds(c0, CB)]).reshape(share, 2, sub, rpd, CB)
                for i in range(sub):
                    pair = nb + c * half_sub + i // 2
                    parts[lax.rem(pair, RING), i % 2, m * share:(m + 1) * share] = res[:, :, i]

        for i in range(n_late):
            late(i).wait()

        def mid(b):
            for i in range(tb):
                r = pl.ds(pl.multiple_of((b * tb + i) * QB, QB), QB)
                out, dg = norm_back(mbuf[r, :], gm[:], gnm[r, :], xbuf[r, :])
                gmid[r, :] = out
                dgain[8:, :] += dg

        def deltas(p):
            for it in range(rows):
                for blk in range(tb):
                    pr, cols, _ = spots(p * rows + it, blk)
                    both = dot_[pr, cols].astype(F32) * ot[pr, cols].astype(F32)
                    delta[row_of(p * rows + it), blk:blk + 1, :] = jnp.concatenate(
                        [col_sum(both[:head_dim]), col_sum(both[head_dim:])], axis=1)

        def column(c):
            with jax.named_scope("b_down"):
                down(c)
            comm.tick(nb + c + jnp.minimum(c, 1))

            @pl.when(c == 1)
            def _():
                give_out(c)

            @pl.when(c == 0)
            def _():
                with jax.named_scope("b_mid"):
                    cdiv_loop(rows, mid)
                with jax.named_scope("b_dot"):
                    dot_[:] = dot(wo[:], gmid[:], NT).astype(BF)
                    cdiv_loop(n_pairs, deltas)
                comm.tick(nb + 1)
                push_rows(1).start()
                give_out(0)

        cdiv_loop(nc, column)

    vm = lambda *s: pltpu.VMEM(s, BF)
    vf = lambda *s: pltpu.VMEM(s, F32)
    pl.run_scoped(mlp, vm(total, width), vm(width, total), vm(ff, total), vm(2, width, 2 * CB), vm(2, CB, width), vm(total, 2 * CB),
                  pltpu.SemaphoreType.DMA((2, 3)))
    head = nb + nc + 1

    def attention(q, kt, k, v, qr, dv, sc0, sc1, sc2, sr, dp0, dp1, dp2, dr, pb0, pb1, pb2, pr_, ds0, ds1, ds2, dsr):
        dqt, dkt = ot, q
        wq, wk, wv = k.at[:hd], kt.at[:, :width], v.at[:hd]
        sc, dp, pb, ds = (sc0, sc1, sc2), (dp0, dp1, dp2), (pb0, pb1, pb2), (ds0, ds1, ds2)
        lds = [load(8 + i, s, d) for i, (s, d) in enumerate(((q_h, q), (k_h, k), (v_h, v), (qr_h, qr), (kt_h, kt)))]

        def out_grad(g):
            put(spot_of("o", g), dot(ot[:], gmid[:, pl.ds(pl.multiple_of(g * CB, CB), CB)]))

        with jax.named_scope("b_dwo"):
            cdiv_loop(nc, out_grad)
        comm.tick(head)
        give_out(2)
        upper = upper_mask()
        first, last = me == 0, me == n - 1

        def right(it, i):
            p, b = it // rows, mod(it, rows)
            return pl.ds(aligned(p * pw, pw), pw), pl.ds(aligned(b * WINDOW + i * QB, QB), QB), pl.ds(aligned(b * ext + toks + i * QB, QB), WINDOW - i * QB)

        def score(it):
            for blk in range(tb):
                pr, cols, keys = spots(it, blk)
                sc[blk][:] = dot(k[keys, pr], stack_pair(q[pr, cols]))
                dp[blk][:] = dot(v[keys, pr], stack_pair(dot_[pr, cols]))
            for i, rs in enumerate((slice(0, WINDOW), slice(WINDOW, 3 * QB))):
                pr, cols, keys = right(it, i)
                sr[rs, :] = dot(k[keys, pr], stack_pair(qr[pr, cols]))
                dr[rs, :] = dot(v[keys, pr], stack_pair(dor[pr, cols]))

        def soften(it):
            row = row_of(it)
            for blk in range(tb):
                s02, s1 = merged(sc[blk][:], upper, *start_bias(first, blk))
                norm, mean = lse[row, blk:blk + 1, :], delta[row, blk:blk + 1, :]
                p02, p1 = jnp.exp(s02 - norm), jnp.exp(s1 - norm)
                g02, g1 = jnp.where(upper, dp[blk][:QB], dp[blk][2 * QB:]), dp[blk][QB:2 * QB]
                pb[blk][:] = banded(p02, p1, upper)
                ds[blk][:] = banded(p02 * (g02 - mean), p1 * (g1 - mean), upper)
            for i, blk in ((0, 0), (0, 1), (1, 2)):
                rs = slice(blk * QB, (blk + 1) * QB)
                p = jnp.exp(sr[rs, :] - jnp.where(last, -NEG, lser[row, i:i + 1, :]))
                g = p * (dr[rs, :] - deltar[row, i:i + 1, :])
                pr_[rs, :] = (p if blk == 1 else jnp.where(upper, p, 0.0)).astype(BF)
                dsr[rs, :] = (g if blk == 1 else jnp.where(upper, g, 0.0)).astype(BF)

        def grads(it):
            ks, vs = [], []
            for blk in range(tb):
                pr, cols, keys = spots(it, blk)
                own = slice(max(0, 2 - blk) * QB, 3 * QB)
                vs.append(dot(pb[blk][own, :], stack_pair(dot_[pr, cols]), NT))
                ks.append(dot(ds[blk][own, :], stack_pair(q[pr, cols]), NT))
                dq = unstack_pair(dot(kt[pr, keys], ds[blk][:])) * (head_dim ** -0.5)
                dqt[pr, cols] = rope(dq, cos_i[:, cols], sin_i[:, cols], -1, head_dim).astype(BF)
            for i, rs in enumerate((slice(0, WINDOW), slice(WINDOW, 3 * QB))):
                pr, cols, _ = right(it, i)
                vs.append(dot(pr_[rs, :], stack_pair(dor[pr, cols]), NT))
                ks.append(dot(dsr[rs, :], stack_pair(qr[pr, cols]), NT))
            for j in range(tb):
                pr, cols, _ = spots(it, j)
                gv, gk = (sum(x[i][(j - max(0, i - 2)) * QB:(j - max(0, i - 2) + 1) * QB] for i in range(j, j + 3)) for x in (vs, ks))
                dv[cols, pr] = gv.astype(BF)
                dkt[pr, cols] = rope(gk.T, cos_i[:, cols], sin_i[:, cols], -1, head_dim).astype(BF)

        def close_group(g):
            cols = pl.ds(pl.multiple_of(g * CB, CB), CB)
            with jax.named_scope("b_dwqkv"):
                put(spot_of("q", g), dot(hat[:], dqt[cols, :], NT))
                put(spot_of("k", g), dot(hat[:], dkt[cols, :], NT))
                put(spot_of("v", g), dot(hat[:], dv[:, cols]))

        def weights():
            return [pltpu.make_async_copy(s, d, ld.at[8 + i]) for i, (s, d) in enumerate(((wq_h, wq), (wk_h, wk), (wv_h, wv), (x_h, xbuf)))]

        def arrived(p):
            with jax.named_scope("b_hwait"):
                for c in push_out(p):
                    c.wait()

        def walk(it):
            @pl.when((lax.rem(it + 1, rows) == 0) & (it + 1 < n_steps))
            def _():
                arrived((it + 1) // rows)

            @pl.when(it < n_steps)
            def _():
                with jax.named_scope("b_attn"):
                    grads(it - 1)
                    soften(it)
                    score(jnp.minimum(it + 1, n_steps - 1))

            @pl.when(it == n_steps)
            def _():
                grads(n_steps - 1)
                for c in weights():
                    c.start()

            @pl.when(lax.rem(it, rows) == 0)
            def _():
                p = it // rows - 1

                @pl.when(lax.rem(p, per) == per - 1)
                def _():
                    close_group(p // per)

                comm.tick(head + 1 + p)

                @pl.when(p + 3 < n_pairs)
                def _():
                    give_out(p + 3)

        for c in lds[:-1]:
            c.wait()
        for i in range(2):
            push_rows(i).wait()
        arrived(0)
        if rows == 1:
            arrived(1)
        score(0)
        soften(0)
        score(1)
        lds[-1].wait()
        cdiv_loop(n_steps, lambda i: walk(i + 1))
        comm.tick(head + 1 + n_pairs)
        for c in weights():
            c.wait()

        def into(b):
            r = pl.ds(pl.multiple_of(b * toks, QB), toks)
            with jax.named_scope("b_into"):
                gnm[r, :] = dot(dqt[:, r], wq[:], TN) + dot(dkt[:, r], wk[:], TN) + dot(dv[r, :], wv[:])

            with jax.named_scope("b_final"):
                for i in range(tb):
                    r = pl.ds(pl.multiple_of((b * tb + i) * QB, QB), QB)
                    out, dg = norm_back(xbuf[r, :], ga[:], gnm[r, :], gmid[r, :])
                    mbuf[r, :] = out
                    dgain[:8, :] += dg
            comm.tick(head + 2 + n_pairs + b)

        cdiv_loop(rows, into)

    score_bufs = [vf(3 * QB, 2 * QB)] * 8 + [vm(3 * QB, 2 * QB)] * 8
    pl.run_scoped(attention, vm(hd, total), vm(hd, rows * ext), vm(rows * ext, hd), vm(rows * ext, hd), vm(hd, rows * WINDOW), vm(total, hd), *score_bufs)
    out_copy = load(1, mbuf, dx_h)
    gains = jnp.concatenate([col_sum(dgain[:8, :]), col_sum(dgain[8:, :]), jnp.zeros((6, width), F32)], axis=0)
    for p in range(n):
        gsend[p, :, :rpd] = gains[:, p * rpd:(p + 1) * rpd]

    def spread(i):
        to = lax.rem(me + i + 1, n)
        pltpu.make_async_remote_copy(src_ref=gsend.at[to], dst_ref=grecv.at[i], send_sem=gsem.at[0], recv_sem=gsem.at[1],
                                     device_id={"seq": to}, device_id_type=MESH).start()

    cdiv_loop(n - 1, spread)
    end = pairs + 5 * LAG
    run = lambda lo, hi: lax.fori_loop(lo, hi, lambda t, c: (comm.tick(t), c)[1], 0)
    run(head + 2 + n_pairs + rows, end - LAG)
    keep_most = load(0, fin.at[pl.ds(0, pairs - LAG)], fin_h.at[pl.ds(0, pairs - LAG)])
    to_left(gsend.at[pl.ds(0, n - 1)], grecv, gsem.at[0], gsem.at[1]).wait()
    sums = gsend[me]
    for i in range(n - 1):
        sums = sums + grecv[i]
    fin[pairs, 0, :8, :128] = sums
    out_copy.wait()
    run(end - LAG, end)
    with jax.named_scope("b_end"):
        keep_rest = load(1, fin.at[pl.ds(pairs - LAG, LAG + 1)], fin_h.at[pl.ds(pairs - LAG, LAG + 1)])
        keep_most.wait()
        keep_rest.wait()


def spread_kernel(dims, dx_i, fin_i, dx_o, dga_o, dgm_o, *refs):
    head_dim, n, width, ff = dims
    outs, (buf, fin), stage, sem = refs[:7], refs[7:9], refs[9:16], refs[16]
    dq, dk, dv, do, dg, du, dd = stage
    nb, nc, sub = ff // CB, width // CB, ff // width
    rpd = width // n
    _, place, pairs = plan(nb, nc * sub // 2, nc)
    get, get_fin, out = (pltpu.make_async_copy(*ends, sem.at[len(outs) + i]) for i, ends in enumerate(((dx_i, buf), (fin_i, fin), (buf, dx_o))))
    get_fin.start()
    get.start()
    get_fin.wait()
    gains = fin[pairs, 0]
    dga_o[:] = gains[:1, :rpd]
    dgm_o[:] = gains[1:2, :rpd]
    for j in range(nb):
        dg[:, j * CB:(j + 1) * CB] = fin[j, 0]
        du[:, j * CB:(j + 1) * CB] = fin[j, 1]
    for c in range(nc):
        for i in range(sub):
            dd[i * rpd:(i + 1) * rpd, c * CB:(c + 1) * CB] = fin[nb + (c * sub + i) // 2, i % 2]
    for g in range(nc):
        do[:, g * CB:(g + 1) * CB] = fin[place["o", g]]
        for name, ref in (("q", dq), ("k", dk), ("v", dv)):
            val = fin[place[name, g]]
            for h in range(CB // head_dim):
                ref[g * (CB // head_dim) + h] = val[:, h * head_dim:(h + 1) * head_dim]
    keeps = [pltpu.make_async_copy(s, d, sem.at[i]) for i, (s, d) in enumerate(zip(stage, outs))]
    for c in keeps:
        c.start()
    get.wait()
    out.start()
    for c in keeps:
        c.wait()
    out.wait()


def run_bwd(n, head_dim, ga, gm, x, dout, q, kt, k, v, hat, ot, xm, hm, hmt, qr, lse, cos_t, sin_t, wq, wk, wv, wo, wg, wu, wd, rows):
    total, width = x.shape
    hd, ff = wq.shape[0], wg.shape[1]
    toks = total // rows
    rpd, heads = width // n, hd // head_dim
    nb, nc, sub = ff // CB, width // CB, ff // width
    pairs = plan(nb, nc * sub // 2, nc)[2]
    n_pairs = hd // (2 * head_dim)
    f = lambda *s: jax.ShapeDtypeStruct(s, F32)
    dx_t = jax.ShapeDtypeStruct((total, width), BF)
    vm = lambda *s: pltpu.VMEM(s, BF)
    vf = lambda *s: pltpu.VMEM(s, F32)
    dma = lambda *s: pltpu.SemaphoreType.DMA(s)
    line = vf(rows * n_pairs, 8, 2 * QB)
    scratch = [vf(RING, 2, n // 2, 2, rpd, CB), vf(SLOTS, 2, n // 2, rpd, CB), vf(2, SLOTS, 2, 2, rpd, CB), vf(2, SLOTS, 2, 4, rpd, CB),
               vf(2, SLOTS, 2, rpd, CB // 2), vf(2, SLOTS, 2, rpd, CB), vf(2, SLOTS, 4, 4, rpd, CB), vf(2, SLOTS, 4, rpd, CB), vf(pairs + 1, 2, rpd, CB),
               dma(9, 2, SLOTS), dma(9, 2, SLOTS),
               vm(hd, rows * WINDOW), line, line, dma(2), dma(2), dma(n_pairs, rows), dma(n_pairs, rows),
               vf(n, 8, 128), vf(n - 1, 8, 128), dma(2), dma(13),
               vm(total, width), vm(total, width), vf(total, width), vm(total, width), vm(hd, total), vm(width, total), vm(hd, width), vm(hd, total), line, line, vf(*cos_t.shape), vf(*cos_t.shape), vf(16, width)]
    mid = pl.pallas_call(
        functools.partial(bwd_kernel, n, head_dim, (rows, toks, width, hd, ff)), out_shape=[dx_t, f(pairs + 1, 2, rpd, CB)],
        in_specs=vmem_spec(2) + any_spec(22), out_specs=any_spec(2), scratch_shapes=scratch,
        compiler_params=pltpu.CompilerParams(collective_id=1, has_side_effects=True, vmem_limit_bytes=VMEM_LIMIT),
        name="backward")(ga, gm, x, dout, q, kt, k, v, hat, ot, xm, hm, hmt, qr, lse, cos_t, sin_t, wq, wk, wv, wo, wg, wu, wd)
    outs = [f(heads, rpd, head_dim)] * 3 + [f(rpd, width), f(rpd, ff), f(rpd, ff), f(ff // n, width)]
    return pl.pallas_call(
        functools.partial(spread_kernel, (head_dim, n, width, ff)), out_shape=[dx_t, f(1, rpd), f(1, rpd)] + outs,
        in_specs=any_spec(2), out_specs=any_spec(1) + vmem_spec(2) + any_spec(7),
        scratch_shapes=[vm(total, width), vf(pairs + 1, 2, rpd, CB), *[vf(*o.shape) for o in outs], dma(10)],
        name="spread")(*mid)


def solution(mesh):
    n = mesh.shape["seq"]

    def device_step(hidden, positions, g_attn, g_mlp, w_query, w_key, w_value, w_out, w_gate, w_up, w_down, d_out):
        rows, toks, width = hidden.shape
        layers, _, heads, head_dim = w_query.shape
        hd = heads * head_dim
        half = head_dim // 2
        inv_freq = 1.0 / (10000.0 ** (jnp.arange(half, dtype=F32) * (2.0 / head_dim)))
        turn = lambda w: w[0].transpose(1, 2, 0).reshape(hd, width)
        wq, wk, wv = turn(w_query), turn(w_key), turn(w_value)
        fwd = run_fwd(n, hidden, positions, inv_freq[:, None], g_attn, g_mlp, wq, wk, wv, w_out[0], head_dim)
        out = run_bwd(n, head_dim, g_attn, g_mlp, hidden.reshape(rows * toks, width), d_out.reshape(rows * toks, width), *fwd,
                      wq, wk, wv, w_out[0], w_gate[0], w_up[0], w_down[0], rows)
        dx, dga, dgm, dq, dk, dv, do, dg, du, dd = out
        back = lambda w: w.transpose(1, 0, 2)[None]
        return (dx.reshape(rows, toks, width), dga, dgm, back(dq), back(dk), back(dv), do[None], dg[None], du[None], dd[None])

    tok_spec = P("data", "seq", None)
    vec_spec = P(None, ("data", "seq"))
    mat_spec = P(None, ("data", "seq"), None)
    head_spec = P(None, ("data", "seq"), None, None)
    in_specs = (tok_spec, P("data", "seq")) + (P(),) * 9 + (tok_spec,)
    out_specs = (tok_spec, vec_spec, vec_spec, head_spec, head_spec, head_spec, mat_spec, mat_spec, mat_spec, mat_spec)
    return jax.shard_map(device_step, mesh=mesh, in_specs=in_specs, out_specs=out_specs, check_vma=False)
```

```python
import functools, math
import numpy as np
import jax, jax.numpy as jnp
from jax import lax
from jax.experimental import pallas as pl
from jax.experimental.pallas import tpu as pltpu
from jax.sharding import PartitionSpec as P

WINDOW = 256
NORM_EPS = 1e-5
QB = 128
BF, F32 = jnp.bfloat16, jnp.float32
NN, NT, TN = ((1,), (0,)), ((1,), (1,)), ((0,), (0,))
MESH = pl.DeviceIdType.MESH
NEG = -1e30
VMEM_LIMIT = 67043328


def dot(a, b, dims=NN):
    return lax.dot_general(a, b, (dims, ((), ())), preferred_element_type=F32)


def cdiv_loop(n, body):
    lax.fori_loop(0, n, lambda i, c: body(i) or c, 0)


def mod(a, b):
    return a % b if isinstance(a, int) else lax.rem(a, b)


def aligned(a, b):
    return a if isinstance(a, int) else pl.multiple_of(a, b)


def rope(blk, cos_b, sin_b, sign, head_dim):
    half = head_dim // 2
    parts = []
    for h in range(blk.shape[0] // head_dim):
        first = blk[h * head_dim:h * head_dim + half]
        second = blk[h * head_dim + half:(h + 1) * head_dim]
        if sign > 0:
            parts += [first * cos_b - second * sin_b, second * cos_b + first * sin_b]
        else:
            parts += [first * cos_b + second * sin_b, second * cos_b - first * sin_b]
    return jnp.concatenate(parts, axis=0)


def normed(x, gain):
    xf = x.astype(F32)
    inv = lax.rsqrt(jnp.mean(xf * xf, axis=-1, keepdims=True) + NORM_EPS)
    return (xf * inv * gain).astype(BF)


def stack_pair(pair_t):
    half = pair_t.shape[0] // 2
    zero = jnp.zeros((half, pair_t.shape[1]), pair_t.dtype)
    return jnp.concatenate(
        [jnp.concatenate([pair_t[:half], zero], axis=0), jnp.concatenate([zero, pair_t[half:]], axis=0)], axis=1)


def unstack_pair(both):
    half, cols = both.shape[0] // 2, both.shape[1] // 2
    return jnp.concatenate([both[:half, :cols], both[half:, cols:]], axis=0)


def col_sum(x):
    return jnp.sum(x, axis=0, keepdims=True)


def merged(scores, upper, bias0, bias1):
    return jnp.where(upper, scores[:QB] + bias0, scores[2 * QB:]), scores[QB:2 * QB] + bias1


def banded(p02, p1, upper):
    return jnp.concatenate(
        [jnp.where(upper, p02, 0.0).astype(BF), p1.astype(BF), jnp.where(upper, 0.0, p02).astype(BF)], axis=0)


def upper_mask():
    key_ids = lax.broadcasted_iota(jnp.int32, (QB, 2 * QB), 0)
    query_ids = lax.broadcasted_iota(jnp.int32, (QB, 2 * QB), 1) % QB
    return key_ids > query_ids


def start_bias(first, blk):
    bias = jnp.where(first, NEG, 0.0).astype(F32)
    return (bias if blk < 2 else 0.0), (bias if blk < 1 else 0.0)


def fwd_kernel(n, head_dim, x_h, pos, invf, ga, gm, wq_h, wk_h, wv_h, wo_h,
               q_h, kt_h, k_h, v_h, hat_h, ot_h, xm_h, hm_h, hmt_h, qr_h, lse_h, cos_t, sin_t,
               xv, halo, qr, lse, pos_halo, wq, wk, wv, wo, q, kt, k, v, vt, hat, ot, xm, hm, hmt, hb, hh, acc, acc2, ak, av, cos_h, sin_h,
               sc0, sc1, sc2, pb0, pb1, pb2, ldx, ld, st, snd, rcv, qsnd, qrcv):
    sc, pb = (sc0, sc1, sc2), (pb0, pb1, pb2)
    rows, toks, width = xv.shape
    ext, total, pw = toks + WINDOW, rows * toks, 2 * head_dim
    n_pairs = wq.shape[0] // pw
    tb, n_steps = toks // QB, n_pairs * rows
    me = lax.axis_index("seq")
    right, left = lax.rem(me + 1, n), lax.rem(me + n - 1, n)
    load_x = [pltpu.make_async_copy(x_h.at[b], xv.at[b], ldx.at[b]) for b in range(rows)]
    load_w = [pltpu.make_async_copy(s, d, ld.at[i]) for i, (s, d) in enumerate(((wq_h, wq), (wk_h, wk), (wv_h, wv), (wo_h, wo)))]
    for c in load_x:
        c.start()
    barrier = pltpu.get_barrier_semaphore()
    for other in (left, right):
        pl.semaphore_signal(barrier, inc=1, device_id={"seq": other}, device_id_type=MESH)
    pl.semaphore_wait(barrier, 2)

    def push(i, s, d):
        return pltpu.make_async_remote_copy(src_ref=s, dst_ref=d, send_sem=snd.at[i], recv_sem=rcv.at[i], device_id={"seq": right}, device_id_type=MESH)

    def push_rows(b):
        return push(b, x_h.at[b, toks - WINDOW:, :], halo.at[b])

    send_pos = push(rows, pos, pos_halo)
    send_pos.start()
    for b in range(rows):
        push_rows(b).start()

    def angles(cos_ref, sin_ref, positions):
        count = positions.shape[1]
        for b in range(rows):
            ang = invf[:] * positions[b:b + 1, :].astype(F32)
            cos_ref[:, b * count:(b + 1) * count] = jnp.cos(ang)
            sin_ref[:, b * count:(b + 1) * count] = jnp.sin(ang)

    angles(cos_t, sin_t, pos[:])

    def norm_rows(b):
        for i in range(tb):
            h = normed(xv[b, i * QB:(i + 1) * QB, :], ga[:])
            hb[pl.ds(pl.multiple_of((b * tb + i) * QB, QB), QB), :] = h

    with jax.named_scope("f_norm"):
        for c in load_x:
            c.wait()
        for c in load_w:
            c.start()
        cdiv_loop(rows, norm_rows)
    keep_hat = pltpu.make_async_copy(hat, hat_h, st.at[0])
    tables = cos_t[:], sin_t[:]

    def put_q(src):
        for p in range(n_pairs):
            r = slice(p * pw, (p + 1) * pw)
            q[r, :] = (rope(src[r, :], *tables, 1, head_dim) * (head_dim ** -0.5)).astype(BF)

    def put_own(src, dst_t, dst, turn):
        for p in range(n_pairs):
            r = slice(p * pw, (p + 1) * pw)
            both = (rope(src[r, :], *tables, 1, head_dim) if turn else src[r, :]).astype(BF)
            for b in range(rows):
                blk = both[:, b * toks:(b + 1) * toks]
                own = slice(b * ext + WINDOW, (b + 1) * ext)
                dst_t[r, own] = blk
                dst[own, r] = blk.T

    with jax.named_scope("f_mm"):
        load_w[0].wait()
        load_w[1].wait()
        load_w[2].wait()
        acc[:] = dot(wq[:], hb[:], NT)
        acc2[:] = dot(wk[:], hb[:], NT)
        put_q(acc)
        acc[:] = dot(wv[:], hb[:], NT)
        put_own(acc2, kt, k, True)
        for i in range(total // QB):
            r = slice(i * QB, (i + 1) * QB)
            hat[:, r] = hb[r, :].T
        put_own(acc, vt, v, False)
    keep_hat.start()
    keep_q = pltpu.make_async_copy(q, q_h, st.at[1])
    keep_q.start()

    def push_q(b):
        return pltpu.make_async_remote_copy(src_ref=q.at[:, b * toks:b * toks + WINDOW], dst_ref=qr.at[:, b * WINDOW:(b + 1) * WINDOW],
                                            send_sem=qsnd.at[b], recv_sem=qrcv.at[b], device_id={"seq": left}, device_id_type=MESH)

    for b in range(rows):
        push_q(b).start()
    send_pos.wait()
    angles(cos_h, sin_h, pos_halo[:, toks - WINDOW:])

    def keeps(b):
        wide, cols = pl.ds(pl.multiple_of(b * ext, QB), ext), pl.ds(pl.multiple_of(b * toks, QB), toks)
        ends = ((kt.at[:, wide], kt_h.at[:, wide]), (k.at[wide, :], k_h.at[wide, :]), (v.at[wide, :], v_h.at[wide, :]),
                (ot.at[:, cols], ot_h.at[:, cols]), (hm.at[cols, :], hm_h.at[cols, :]), (hmt.at[:, cols], hmt_h.at[:, cols]),
                (xm.at[cols, :], xm_h.at[cols, :]))
        return [pltpu.make_async_copy(s, d, st.at[2 + b * len(ends) + i]) for i, (s, d) in enumerate(ends)]

    def halo_in(b):
        with jax.named_scope("f_halo_wait"):
            push_rows(b).wait()
        with jax.named_scope("f_halo"):
            for i in range(WINDOW // QB):
                r = slice(i * QB, (i + 1) * QB)
                hh[r, :] = normed(halo[b, r, :], ga[:])
            ak[:] = dot(wk[:], hh[:], NT)
            av[:] = dot(wv[:], hh[:], NT)
            cols = pl.ds(pl.multiple_of(b * WINDOW, QB), WINDOW)
            wide = pl.ds(pl.multiple_of(b * ext, QB), WINDOW)
            near = cos_h[:, cols], sin_h[:, cols]
            for src, dst_t, dst in ((ak, kt, k), (av, vt, v)):
                for p in range(n_pairs):
                    r = slice(p * pw, (p + 1) * pw)
                    blk = (rope(src[r, :], *near, 1, head_dim) if dst is k else src[r, :]).astype(BF)
                    dst_t[r, wide] = blk
                    dst[wide, r] = blk.T
        for c in keeps(b)[:3]:
            c.start()

    upper = upper_mask()
    first = me == 0

    def spots(it, blk):
        b, p = it // n_pairs, mod(it, n_pairs)
        pr = pl.ds(aligned(p * pw, pw), pw)
        return pr, pl.ds(aligned(b * toks + blk * QB, QB), QB), pl.ds(aligned(b * ext + blk * QB, QB), 3 * QB)

    def score(it):
        for blk in range(tb):
            pr, cols, keys = spots(it, blk)
            sc[blk][:] = dot(k[keys, pr], stack_pair(q[pr, cols]))

    def soften(it, blk):
        s02, s1 = merged(sc[blk][:], upper, *start_bias(first, blk))
        top = jnp.max(jnp.maximum(s02, s1), axis=0, keepdims=True)
        e02, e1 = jnp.exp(s02 - top), jnp.exp(s1 - top)
        mass = col_sum(e02 + e1)
        inv = 1.0 / mass
        lse[it, blk:blk + 1, :] = top + jnp.log(mass)
        pb[blk][:] = banded(e02 * inv, e1 * inv, upper)

    def mix(it):
        for blk in range(tb):
            pr, cols, keys = spots(it, blk)
            ot[pr, cols] = unstack_pair(dot(vt[pr, keys], pb[blk][:])).astype(BF)

    def project(b):
        cols = pl.ds(pl.multiple_of(b * toks, QB), toks)
        with jax.named_scope("f_proj"):
            mid = (xv[b].astype(F32) + dot(ot[:, cols], wo[:], TN)).astype(BF)
            xm[cols, :] = mid
            h = normed(mid, gm[:])
            hm[cols, :] = h
            hmt[:, cols] = h.T
        for c in keeps(b)[3:]:
            c.start()

    keep_qr, keep_lse = (pltpu.make_async_copy(*ends, ld.at[i]) for i, ends in enumerate(((qr, qr_h), (lse, lse_h))))
    load_w[3].wait()
    for blk in range(tb):
        pb[blk][:] = jnp.zeros(pb[blk].shape, BF)

    def walk(i):
        it = i - 1

        @pl.when((lax.rem(i, n_pairs) == 0) & (i < n_steps))
        def _():
            halo_in(i // n_pairs)

        @pl.when(i == 0)
        def _():
            score(0)

        @pl.when((i > 0) & (i <= n_steps))
        def _():
            with jax.named_scope("f_attn"):
                mix(jnp.maximum(it - 1, 0))
                for blk in range(tb):
                    soften(it, blk)
                score(jnp.minimum(i, n_steps - 1))

        @pl.when(i == n_steps)
        def _():
            for b in range(rows):
                push_q(b).wait()
            keep_qr.start()

        @pl.when(i > n_steps)
        def _():
            mix(n_steps - 1)

        @pl.when((lax.rem(it, n_pairs) == 0) & (it > 0))
        def _():
            project(it // n_pairs - 1)

    cdiv_loop(n_steps + 2, walk)
    with jax.named_scope("f_store_wait"):
        keep_lse.start()
        keep_hat.wait()
        keep_q.wait()
        keep_qr.wait()
        keep_lse.wait()
        for b in range(rows):
            for c in keeps(b):
                c.wait()


def any_spec(k):
    return [pl.BlockSpec(memory_space=pl.ANY)] * k


def vmem_spec(k):
    return [pl.BlockSpec(memory_space=pltpu.VMEM)] * k


def run_fwd(n, x, pos, invf, ga, gm, wq, wk, wv, wo, head_dim):
    rows, toks, width = x.shape
    hd = wq.shape[0]
    ext, total, n_halo = toks + WINDOW, rows * toks, rows * WINDOW
    half = head_dim // 2
    sds = lambda *s: jax.ShapeDtypeStruct(s, BF)
    dma = lambda *s: pltpu.SemaphoreType.DMA(s)
    outs = [sds(hd, total), sds(hd, rows * ext), sds(rows * ext, hd), sds(rows * ext, hd), sds(width, total), sds(hd, total), sds(total, width), sds(total, width), sds(width, total)]
    outs += [sds(hd, n_halo), jax.ShapeDtypeStruct((rows * hd // (2 * head_dim), 8, 2 * QB), F32)] + [jax.ShapeDtypeStruct((half, total), F32)] * 2
    vm = lambda *s: pltpu.VMEM(s, BF)
    vf = lambda *s: pltpu.VMEM(s, F32)
    scratch = [vm(rows, toks, width), vm(rows, WINDOW, width), vm(hd, n_halo), vf(rows * hd // (2 * head_dim), 8, 2 * QB), pltpu.VMEM((rows, toks), jnp.int32), vm(hd, width), vm(hd, width), vm(hd, width), vm(hd, width),
               vm(hd, total), vm(hd, rows * ext), vm(rows * ext, hd), vm(rows * ext, hd), vm(hd, rows * ext), vm(width, total), vm(hd, total), vm(total, width), vm(total, width), vm(width, total), vm(total, width), vm(WINDOW, width),
               vf(hd, total), vf(hd, total), vf(hd, WINDOW), vf(hd, WINDOW), vf(half, n_halo), vf(half, n_halo),
               *[vf(3 * QB, 2 * QB)] * 3, *[vm(3 * QB, 2 * QB)] * 3,
               dma(rows), dma(4), dma(2 + 7 * rows), dma(rows + 1), dma(rows + 1), dma(rows), dma(rows)]
    return pl.pallas_call(
        functools.partial(fwd_kernel, n, head_dim), out_shape=outs,
        in_specs=any_spec(1) + vmem_spec(4) + any_spec(4), out_specs=any_spec(11) + vmem_spec(2), scratch_shapes=scratch,
        compiler_params=pltpu.CompilerParams(collective_id=0, has_side_effects=True, vmem_limit_bytes=VMEM_LIMIT),
        name="forward")(x, pos, invf, ga, gm, wq, wk, wv, wo)


LAG = 2
SLOTS = 2 * LAG
RING = 8
CB = 256


def at(ref, *idx):
    return ref.at[idx]


class Torus:
    def __init__(self, n, head, last, turn, parts, recv0, recv1, recv2, recv3, recv4, acc, acc2, fin, snd, rcv):
        self.side = math.isqrt(n // 2)
        assert self.side == 4
        me = lax.axis_index("seq")
        self.core = lax.rem(me, 2)
        chip = me // 2
        self.x, self.y = lax.rem(chip, 4), chip // 4
        self.head, self.last, self.turn = head, last, turn
        self.parts, self.recv0, self.recv1, self.recv2, self.recv3, self.recv4 = parts, recv0, recv1, recv2, recv3, recv4
        self.acc, self.acc2, self.fin, self.snd, self.rcv = acc, acc2, fin, snd, rcv
        self.partner = me + 1 - 2 * self.core
        self.hops = {(axis, step): self.device(*((0, step) if axis == 0 else (step, 0))) for axis in (0, 1) for step in (1, 3)}

    def device(self, dy, dx):
        return (lax.rem(self.y + dy, 4) * 4 + lax.rem(self.x + dx, 4)) * 2 + self.core

    def peers(self):
        return [self.partner, *self.hops.values()]

    def copy(self, lane, kind, slot, src, dst, target):
        return pltpu.make_async_remote_copy(
            src_ref=src, dst_ref=dst, send_sem=self.snd.at[lane, kind, slot], recv_sem=self.rcv.at[lane, kind, slot],
            device_id={"seq": target}, device_id_type=MESH)

    def late(self, pair, yes, no):
        first, end = self.turn
        return jnp.where((pair >= first) & (pair < end), yes, no)

    def swap(self, ring, slot):
        return self.copy(0, 0, slot, self.parts.at[ring, :, :, 1 - self.core], self.recv0.at[slot], self.partner)

    def copies(self, stage, kind, pair, held, slot):
        axis = kind if stage < 3 else 1 - kind
        plus, minus = self.hops[axis, 1], self.hops[axis, 3]
        half = CB // 2
        if stage == 1:
            if axis == 0:
                minus = self.late(pair, plus, minus)
            ends = [(self.acc.at[kind, held, 2, pl.ds(0, 2)], self.recv1), (self.acc.at[kind, held, 2, pl.ds(2, 2)], self.recv1)]
        elif stage == 2:
            ends = [(self.acc.at[kind, held, 1], self.recv2), (self.acc.at[kind, held, 3], self.recv2)]
        elif stage == 3:
            ends = [(self.acc2.at[kind, held, 2, :, pl.ds(0, half)], self.recv3), (self.acc2.at[kind, held, 2, :, pl.ds(half, half)], self.recv3)]
        else:
            ends = [(self.acc2.at[kind, held, 1], self.recv4), (self.acc2.at[kind, held, 3], self.recv4)]
        lane = 2 * stage - 1
        return [self.copy(lane + i, kind, slot, src, buf.at[kind, slot, i], (plus, minus)[i]) for i, (src, buf) in enumerate(ends)]

    def add(self, stage, kind, pair, held, slot, ring):
        acc, acc2 = self.acc, self.acc2
        if stage == 1:
            def row(r1):
                for r2 in range(4):
                    ry, rx = (r2, r1) if kind == 0 else (r1, r2)
                    chip = lax.rem(self.y + ry, 4) * 4 + lax.rem(self.x + rx, 4)
                    acc[kind, held, r1, r2] = self.parts[ring, kind, chip, self.core] + self.recv0[slot, kind, chip]
            cdiv_loop(4, row)
        elif stage == 2:
            back = self.late(pair, 1, 3) if kind == 0 else 3
            acc[kind, held, 1, :2] += self.recv1[kind, slot, 0]
            acc[kind, held, back, 2:] += self.recv1[kind, slot, 1]
        elif stage == 3:
            acc2[kind, held] = acc[kind, held, 0] + (self.recv2[kind, slot, 0] + self.recv2[kind, slot, 1])
        elif stage == 4:
            half = CB // 2
            acc2[kind, held, 1, :, :half] += self.recv3[kind, slot, 0]
            acc2[kind, held, 3, :, half:] += self.recv3[kind, slot, 1]
        else:
            self.fin[pair, kind] = acc2[kind, held, 0] + (self.recv4[kind, slot, 0] + self.recv4[kind, slot, 1])

    def when(self, pair, fn):
        if isinstance(pair, int):
            if 0 <= pair <= self.last and (pair <= self.head or pair == self.last or (pair - self.head) % 2 == 0):
                fn()
        else:
            pl.when((pair >= 0) & ((pair <= self.head) | (pair == self.last) | ((pair < self.last) & (lax.rem(pair - self.head, 2) == 0))))(fn)

    def tick(self, t):
        now, land = mod(t, SLOTS), mod(t + SLOTS - LAG, SLOTS)
        ring_now, ring_land = mod(t, RING), mod(t + RING - LAG, RING)
        for stage in range(5, -1, -1):
            pair = t - LAG * stage
            held = land if stage % 2 else now

            def move(stage=stage, pair=pair, held=held):
                if stage == 0:
                    self.swap(ring_now, now).start()
                    return
                if stage == 1:
                    with jax.named_scope("t_wait1"):
                        self.swap(ring_land, land).wait()
                for kind in range(2):
                    if stage > 1:
                        with jax.named_scope(f"t_wait{stage}"):
                            for c in self.copies(stage - 1, kind, pair, held, land):
                                c.wait()
                    self.add(stage, kind, pair, held, land, ring_land)
                    if stage < 5:
                        for c in self.copies(stage, kind, pair, held, now):
                            c.start()
            self.when(pair, move)


def pick(i, table):
    out = 0
    for key, value in table.items():
        out = jnp.where(i == key, value, out)
    return out


def norm_back(x, gain, grad, res):
    xf = x.astype(F32)
    inv = lax.rsqrt(jnp.mean(xf * xf, axis=-1, keepdims=True) + NORM_EPS)
    unit = xf * inv
    gu = grad * gain
    out = inv * (gu - unit * jnp.mean(gu * unit, axis=-1, keepdims=True)) + res.astype(F32)
    gu = grad * unit
    return out.astype(BF), jnp.sum(gu.reshape(-1, 8, gu.shape[-1]), axis=0)


def plan(n_mlp, n_down, nc):
    order = [("o", g) for g in range(nc)] + [(name, g) for g in range(nc) for name in "qkv"]
    head = n_mlp + n_down - 2
    last = head + len(order) + 1
    return head, {name: (min(head + 4 + i // 2 * 2, last), i % 2) for i, name in enumerate(order)}, last


def bwd_kernel(n, head_dim, dims, ga, gm, x_h, dout_h, q_h, kt_h, k_h, v_h, hat_h, ot_h, xm_h, hm_h, hmt_h, qr_h, lse_h, cos_h, sin_h,
               wq_h, wk_h, wv_h, wo_h, wg_h, wu_h, wd_h,
               dx_h, fin_h,
               parts, recv0, recv1, recv2, recv3, recv4, acc, acc2, fin, snd, rcv,
               dor, lser, deltar, hsnd, hrcv, osnd, orcv, gsend, grecv, gsem, ld,
               xbuf, mbuf, gnm, gmid, ot, hat, wo, dot_, lse, delta, cos_i, sin_i, dgain):
    rows, toks, width, hd, ff = dims
    ext, total = toks + WINDOW, rows * toks
    pw = 2 * head_dim
    n_pairs = hd // pw
    tb, n_steps = toks // QB, n_pairs * rows
    nb, nc, sub = ff // CB, width // CB, ff // width
    rpd = width // n
    per, half_sub = CB // pw, sub // 2
    head, place, end = plan(nb, nc * half_sub, nc)
    comm = Torus(n, head, end, (nb - 1, nb + n_pairs), parts, recv0, recv1, recv2, recv3, recv4, acc, acc2, fin, snd, rcv)
    me = lax.axis_index("seq")
    left = lax.rem(me + n - 1, n)
    barrier = pltpu.get_barrier_semaphore()

    def greet(i):
        pl.semaphore_signal(barrier, inc=1, device_id={"seq": lax.rem(me + i + 1, n)}, device_id_type=MESH)

    def load(i, s, d):
        c = pltpu.make_async_copy(s, d, ld.at[i])
        c.start()
        return c

    def late(i):
        s, d = ((xm_h, mbuf), (ot_h, ot), (hat_h, hat), (wo_h, wo), (lse_h, lse), (cos_h, cos_i), (sin_h, sin_i))[i]
        return pltpu.make_async_copy(s, d, ld.at[1 + i])

    def to_left(src, dst, send_sem, recv_sem):
        return pltpu.make_async_remote_copy(src_ref=src, dst_ref=dst, send_sem=send_sem, recv_sem=recv_sem,
                                            device_id={"seq": left}, device_id_type=MESH)

    n_late = 7

    def push_rows(i):
        return to_left(*((lse_h, lser), (delta, deltar))[i], hsnd.at[i], hrcv.at[i])

    def push_out(p):
        pr = pl.ds(aligned(p * pw, pw), pw)
        return [to_left(dot_.at[pr, pl.ds(b * toks, WINDOW)], dor.at[pr, pl.ds(b * WINDOW, WINDOW)], osnd.at[p, b], orcv.at[p, b])
                for b in range(rows)]

    def give_out(p):
        for c in push_out(p):
            c.start()

    def put(spot, value):
        pair, kind = spot
        parts[mod(pair, RING), kind] = value.reshape(n // 2, 2, rpd, CB)

    def spot_of(name, g):
        known = {i: place[name, i] for i in range(nc)}
        return pick(g, {i: s[0] for i, s in known.items()}), pick(g, {i: s[1] for i, s in known.items()})

    def spots(it, blk):
        p, b = it // rows, mod(it, rows)
        pr = pl.ds(aligned(p * pw, pw), pw)
        return pr, pl.ds(aligned(b * toks + blk * QB, QB), QB), pl.ds(aligned(b * ext + blk * QB, QB), 3 * QB)

    def row_of(it):
        return mod(it, rows) * n_pairs + it // rows

    def mlp(hm, hmt, actt, wgu, wd, dgu, wld):
        def weights(j, slot):
            c = aligned(j * CB, CB)
            return [pltpu.make_async_copy(wg_h.at[:, pl.ds(c, CB)], wgu.at[slot, :, :CB], wld.at[slot, 0]),
                    pltpu.make_async_copy(wu_h.at[:, pl.ds(c, CB)], wgu.at[slot, :, CB:], wld.at[slot, 1]),
                    pltpu.make_async_copy(wd_h.at[pl.ds(c, CB), :], wd.at[slot], wld.at[slot, 2])]

        for c in weights(0, 0):
            c.start()
        ld_hm, ld_x, ld_hmt = load(8, hm_h, hm), load(0, dout_h, xbuf), load(9, hmt_h, hmt)
        cdiv_loop(n - 1, greet)
        gnm[:] = jnp.zeros_like(gnm)
        gsend[:] = jnp.zeros_like(gsend)
        dgain[:] = jnp.zeros_like(dgain)
        ld_hm.wait()
        ld_x.wait()
        ld_hmt.wait()
        for i in range(n_late):
            late(i).start()

        def block(j):
            slot = lax.rem(j, 2)
            for c in weights(j, slot):
                c.wait()

            @pl.when(j + 1 < nb)
            def _():
                for c in weights(j + 1, 1 - slot):
                    c.start()

            c0 = pl.multiple_of(j * CB, CB)
            with jax.named_scope("b_mlp"):
                for b in range(rows):
                    r = slice(b * toks, (b + 1) * toks)
                    gu = dot(hm[r, :], wgu[slot])
                    gact = dot(xbuf[r, :], wd[slot], NT).astype(BF).astype(F32)
                    gate, up = gu[:, :CB], gu[:, CB:]
                    sig = 1.0 / (1.0 + jnp.exp(-gate))
                    swish = gate * sig
                    actt[pl.ds(c0, CB), r] = (swish * up).astype(BF).T
                    dgu[r, :CB] = (gact * up * (sig + swish * (1.0 - sig))).astype(BF)
                    dgu[r, CB:] = (gact * swish).astype(BF)
                both = dot(hmt[:], dgu[:])
                ring = lax.rem(j, RING)
                parts[ring, 0] = both[:, :CB].reshape(n // 2, 2, rpd, CB)
                parts[ring, 1] = both[:, CB:].reshape(n // 2, 2, rpd, CB)
                for b in range(rows):
                    r = slice(b * toks, (b + 1) * toks)
                    gnm[r, :] += dot(dgu[r, :], wgu[slot], NT)

            @pl.when(j == 0)
            def _():
                pl.semaphore_wait(barrier, n - 1)
                push_rows(0).start()

            comm.tick(j)

        cdiv_loop(nb, block)

        def down(c):
            share = n // 2 // sub
            c0 = pl.multiple_of(c * CB, CB)
            for m in range(sub):
                res = dot(actt[m * width:(m + 1) * width, :], xbuf[:, pl.ds(c0, CB)]).reshape(share, 2, sub, rpd, CB)
                for i in range(sub):
                    pair = nb + c * half_sub + i // 2
                    parts[lax.rem(pair + pair // (head + 1), RING), i % 2, m * share:(m + 1) * share] = res[:, :, i]

        for i in range(n_late):
            late(i).wait()

        def mid(b):
            for i in range(tb):
                r = pl.ds(pl.multiple_of((b * tb + i) * QB, QB), QB)
                out, dg = norm_back(mbuf[r, :], gm[:], gnm[r, :], xbuf[r, :])
                gmid[r, :] = out
                dgain[8:, :] += dg

        def deltas(p):
            for it in range(rows):
                for blk in range(tb):
                    pr, cols, _ = spots(p * rows + it, blk)
                    both = dot_[pr, cols].astype(F32) * ot[pr, cols].astype(F32)
                    delta[row_of(p * rows + it), blk:blk + 1, :] = jnp.concatenate(
                        [col_sum(both[:head_dim]), col_sum(both[head_dim:])], axis=1)

        def column(c):
            with jax.named_scope("b_down"):
                down(c)
            comm.tick(nb + c + jnp.minimum(c, 1))

            @pl.when(c == 1)
            def _():
                give_out(c)

            @pl.when(c == 0)
            def _():
                with jax.named_scope("b_mid"):
                    cdiv_loop(rows, mid)
                with jax.named_scope("b_dot"):
                    dot_[:] = dot(wo[:], gmid[:], NT).astype(BF)
                    cdiv_loop(n_pairs, deltas)
                comm.tick(nb + 1)
                push_rows(1).start()
                give_out(0)

        cdiv_loop(nc, column)

    vm = lambda *s: pltpu.VMEM(s, BF)
    vf = lambda *s: pltpu.VMEM(s, F32)
    pl.run_scoped(mlp, vm(total, width), vm(width, total), vm(ff, total), vm(2, width, 2 * CB), vm(2, CB, width), vm(total, 2 * CB),
                  pltpu.SemaphoreType.DMA((2, 3)))
    def attention(q, kt, k, v, qr, dv, sc0, sc1, sc2, sr, dp0, dp1, dp2, dr, pb0, pb1, pb2, pr_, ds0, ds1, ds2, dsr):
        dqt, dkt = ot, q
        wq, wk, wv = k.at[:hd], kt.at[:, :width], v.at[:hd]
        sc, dp, pb, ds = (sc0, sc1, sc2), (dp0, dp1, dp2), (pb0, pb1, pb2), (ds0, ds1, ds2)
        lds = [load(8 + i, s, d) for i, (s, d) in enumerate(((q_h, q), (k_h, k), (v_h, v), (qr_h, qr), (kt_h, kt)))]

        def out_grad(g):
            put(spot_of("o", g), dot(ot[:], gmid[:, pl.ds(pl.multiple_of(g * CB, CB), CB)]))

        comm.tick(head)
        with jax.named_scope("b_dwo"):
            cdiv_loop(nc, out_grad)
        give_out(2)
        upper = upper_mask()
        first, last = me == 0, me == n - 1
        halves = slice(0, WINDOW), slice(WINDOW, 3 * QB)

        def right(it, i):
            p, b = it // rows, mod(it, rows)
            return pl.ds(aligned(p * pw, pw), pw), pl.ds(aligned(b * WINDOW + i * QB, QB), QB), pl.ds(aligned(b * ext + toks + i * QB, QB), WINDOW - i * QB)

        def score(it):
            for blk in range(tb):
                pr, cols, keys = spots(it, blk)
                sc[blk][:] = dot(k[keys, pr], stack_pair(q[pr, cols]))
                dp[blk][:] = dot(v[keys, pr], stack_pair(dot_[pr, cols]))
            for i, rs in enumerate(halves):
                pr, cols, keys = right(it, i)
                sr[rs, :] = dot(k[keys, pr], stack_pair(qr[pr, cols]))
                dr[rs, :] = dot(v[keys, pr], stack_pair(dor[pr, cols]))

        def soften(it):
            row = row_of(it)
            for blk in range(tb):
                s02, s1 = merged(sc[blk][:], upper, *start_bias(first, blk))
                norm, mean = lse[row, blk:blk + 1, :], delta[row, blk:blk + 1, :]
                p02, p1 = jnp.exp(s02 - norm), jnp.exp(s1 - norm)
                g02, g1 = jnp.where(upper, dp[blk][:QB], dp[blk][2 * QB:]), dp[blk][QB:2 * QB]
                pb[blk][:] = banded(p02, p1, upper)
                ds[blk][:] = banded(p02 * (g02 - mean), p1 * (g1 - mean), upper)
            for blk in range(tb):
                i = blk // 2
                rs = slice(blk * QB, (blk + 1) * QB)
                p = jnp.exp(sr[rs, :] - jnp.where(last, -NEG, lser[row, i:i + 1, :]))
                g = p * (dr[rs, :] - deltar[row, i:i + 1, :])
                pr_[rs, :] = (p if blk == 1 else jnp.where(upper, p, 0.0)).astype(BF)
                dsr[rs, :] = (g if blk == 1 else jnp.where(upper, g, 0.0)).astype(BF)

        def grads(it):
            ks, vs = [], []
            for blk in range(tb):
                pr, cols, keys = spots(it, blk)
                own = slice(max(0, 2 - blk) * QB, 3 * QB)
                vs.append(dot(pb[blk][own, :], stack_pair(dot_[pr, cols]), NT))
                ks.append(dot(ds[blk][own, :], stack_pair(q[pr, cols]), NT))
                dq = unstack_pair(dot(kt[pr, keys], ds[blk][:])) * (head_dim ** -0.5)
                dqt[pr, cols] = rope(dq, cos_i[:, cols], sin_i[:, cols], -1, head_dim).astype(BF)
            for i, rs in enumerate(halves):
                pr, cols, _ = right(it, i)
                vs.append(dot(pr_[rs, :], stack_pair(dor[pr, cols]), NT))
                ks.append(dot(dsr[rs, :], stack_pair(qr[pr, cols]), NT))
            for j in range(tb):
                pr, cols, _ = spots(it, j)
                gv, gk = (sum(x[i][(j - max(0, i - 2)) * QB:(j - max(0, i - 2) + 1) * QB] for i in range(j, j + 3)) for x in (vs, ks))
                dv[cols, pr] = gv.astype(BF)
                dkt[pr, cols] = rope(gk.T, cos_i[:, cols], sin_i[:, cols], -1, head_dim).astype(BF)

        def close_group(g):
            cols = pl.ds(pl.multiple_of(g * CB, CB), CB)
            with jax.named_scope("b_dwqkv"):
                put(spot_of("q", g), dot(hat[:], dqt[cols, :], NT))
                put(spot_of("k", g), dot(hat[:], dkt[cols, :], NT))
                put(spot_of("v", g), dot(hat[:], dv[:, cols]))

        def weights():
            return [pltpu.make_async_copy(s, d, ld.at[8 + i]) for i, (s, d) in enumerate(((wq_h, wq), (wk_h, wk), (wv_h, wv), (x_h, xbuf)))]

        def arrived(p):
            with jax.named_scope("b_hwait"):
                for c in push_out(p):
                    c.wait()

        def walk(it):
            @pl.when((lax.rem(it + 1, rows) == 0) & (it + 1 < n_steps))
            def _():
                arrived((it + 1) // rows)

            @pl.when(it < n_steps)
            def _():
                with jax.named_scope("b_attn"):
                    grads(it - 1)
                    soften(it)
                    score(jnp.minimum(it + 1, n_steps - 1))

            @pl.when(it == n_steps)
            def _():
                grads(n_steps - 1)
                for c in weights():
                    c.start()

            p, step = it // rows - 1, lax.rem(it, rows)

            @pl.when((step == 0) & (lax.rem(p, per) == per - 1))
            def _():
                close_group(p // per)

            @pl.when((step == 0) | (step == rows - 1))
            def _():
                comm.tick(head + 2 * (p + 1) + step // (rows - 1))

            @pl.when((step == 0) & (p + 3 < n_pairs))
            def _():
                give_out(p + 3)

        for c in lds[:-1]:
            c.wait()
        for i in range(2):
            push_rows(i).wait()
        arrived(0)
        if rows == 1:
            arrived(1)
        score(0)
        soften(0)
        score(1)
        lds[-1].wait()
        cdiv_loop(n_steps, lambda i: walk(i + 1))
        comm.tick(end)
        for c in weights():
            c.wait()

        def into(b):
            r = pl.ds(pl.multiple_of(b * toks, QB), toks)
            with jax.named_scope("b_into"):
                gnm[r, :] = dot(dqt[:, r], wq[:], TN) + dot(dkt[:, r], wk[:], TN) + dot(dv[r, :], wv[:])

            with jax.named_scope("b_final"):
                for i in range(tb):
                    r = pl.ds(pl.multiple_of((b * tb + i) * QB, QB), QB)
                    out, dg = norm_back(xbuf[r, :], ga[:], gnm[r, :], gmid[r, :])
                    mbuf[r, :] = out
                    dgain[:8, :] += dg
            comm.tick(end + 1 + b)

        cdiv_loop(rows, into)

    score_bufs = [vf(3 * QB, 2 * QB)] * 8 + [vm(3 * QB, 2 * QB)] * 8
    pl.run_scoped(attention, vm(hd, total), vm(hd, rows * ext), vm(rows * ext, hd), vm(rows * ext, hd), vm(hd, rows * WINDOW), vm(total, hd), *score_bufs)
    out_copy = load(1, mbuf, dx_h)
    gains = jnp.concatenate([col_sum(dgain[:8, :]), col_sum(dgain[8:, :]), jnp.zeros((6, width), F32)], axis=0)
    for p in range(n):
        gsend[p, :, :rpd] = gains[:, p * rpd:(p + 1) * rpd]

    def spread(i):
        to = lax.rem(me + i + 1, n)
        pltpu.make_async_remote_copy(src_ref=gsend.at[to], dst_ref=grecv.at[i], send_sem=gsem.at[0], recv_sem=gsem.at[1],
                                     device_id={"seq": to}, device_id_type=MESH).start()

    cdiv_loop(n - 1, spread)
    stop = end + 1 + 5 * LAG
    run = lambda lo, hi: lax.fori_loop(lo, hi, lambda t, c: comm.tick(t) or c, 0)
    run(end + 1 + rows, stop - LAG)
    most, rest = pl.ds(0, end - 1), pl.ds(end - 1, LAG + 1)
    keep_most = load(0, fin.at[most], fin_h.at[most])
    to_left(gsend.at[pl.ds(0, n - 1)], grecv, gsem.at[0], gsem.at[1]).wait()
    sums = gsend[me]
    for i in range(n - 1):
        sums = sums + grecv[i]
    fin[end + 1, 0, :8, :128] = sums
    out_copy.wait()
    run(stop - LAG, stop)
    with jax.named_scope("b_end"):
        keep_rest = load(1, fin.at[rest], fin_h.at[rest])
        keep_most.wait()
        keep_rest.wait()


def spread_kernel(dims, dx_i, fin_i, dx_o, dga_o, dgm_o, *refs):
    head_dim, n, width, ff = dims
    outs, (buf, fin), stage, sem = refs[:7], refs[7:9], refs[9:16], refs[16]
    dq, dk, dv, do, dg, du, dd = stage
    nb, nc, sub = ff // CB, width // CB, ff // width
    rpd = width // n
    head, place, end = plan(nb, nc * sub // 2, nc)
    get, get_fin, out = (pltpu.make_async_copy(*ends, sem.at[len(outs) + i]) for i, ends in enumerate(((dx_i, buf), (fin_i, fin), (buf, dx_o))))
    get_fin.start()
    get.start()
    get_fin.wait()
    gains = fin[end + 1, 0]
    dga_o[:] = gains[:1, :rpd]
    dgm_o[:] = gains[1:2, :rpd]
    for j in range(nb):
        dg[:, j * CB:(j + 1) * CB] = fin[j, 0]
        du[:, j * CB:(j + 1) * CB] = fin[j, 1]
    for c in range(nc):
        for i in range(sub):
            pair = nb + (c * sub + i) // 2
            dd[i * rpd:(i + 1) * rpd, c * CB:(c + 1) * CB] = fin[pair + pair // (head + 1), i % 2]
    for g in range(nc):
        do[:, g * CB:(g + 1) * CB] = fin[place["o", g]]
        for name, ref in (("q", dq), ("k", dk), ("v", dv)):
            val = fin[place[name, g]]
            for h in range(CB // head_dim):
                ref[g * (CB // head_dim) + h] = val[:, h * head_dim:(h + 1) * head_dim]
    keeps = [pltpu.make_async_copy(s, d, sem.at[i]) for i, (s, d) in enumerate(zip(stage, outs))]
    for c in keeps:
        c.start()
    get.wait()
    out.start()
    for c in keeps:
        c.wait()
    out.wait()


def run_bwd(n, head_dim, ga, gm, x, dout, q, kt, k, v, hat, ot, xm, hm, hmt, qr, lse, cos_t, sin_t, wq, wk, wv, wo, wg, wu, wd, rows):
    total, width = x.shape
    hd, ff = wq.shape[0], wg.shape[1]
    toks = total // rows
    rpd, heads = width // n, hd // head_dim
    nb, nc, sub = ff // CB, width // CB, ff // width
    slots = plan(nb, nc * sub // 2, nc)[2] + 2
    n_pairs = hd // (2 * head_dim)
    f = lambda *s: jax.ShapeDtypeStruct(s, F32)
    dx_t = jax.ShapeDtypeStruct((total, width), BF)
    vm = lambda *s: pltpu.VMEM(s, BF)
    vf = lambda *s: pltpu.VMEM(s, F32)
    dma = lambda *s: pltpu.SemaphoreType.DMA(s)
    line = vf(rows * n_pairs, 8, 2 * QB)
    scratch = [vf(RING, 2, n // 2, 2, rpd, CB), vf(SLOTS, 2, n // 2, rpd, CB), vf(2, SLOTS, 2, 2, rpd, CB), vf(2, SLOTS, 2, 4, rpd, CB),
               vf(2, SLOTS, 2, rpd, CB // 2), vf(2, SLOTS, 2, rpd, CB), vf(2, SLOTS, 4, 4, rpd, CB), vf(2, SLOTS, 4, rpd, CB), vf(slots, 2, rpd, CB),
               dma(9, 2, SLOTS), dma(9, 2, SLOTS),
               vm(hd, rows * WINDOW), line, line, dma(2), dma(2), dma(n_pairs, rows), dma(n_pairs, rows),
               vf(n, 8, 128), vf(n - 1, 8, 128), dma(2), dma(13),
               vm(total, width), vm(total, width), vf(total, width), vm(total, width), vm(hd, total), vm(width, total), vm(hd, width), vm(hd, total), line, line, vf(*cos_t.shape), vf(*cos_t.shape), vf(16, width)]
    mid = pl.pallas_call(
        functools.partial(bwd_kernel, n, head_dim, (rows, toks, width, hd, ff)), out_shape=[dx_t, f(slots, 2, rpd, CB)],
        in_specs=vmem_spec(2) + any_spec(22), out_specs=any_spec(2), scratch_shapes=scratch,
        compiler_params=pltpu.CompilerParams(collective_id=1, has_side_effects=True, vmem_limit_bytes=VMEM_LIMIT),
        name="backward")(ga, gm, x, dout, q, kt, k, v, hat, ot, xm, hm, hmt, qr, lse, cos_t, sin_t, wq, wk, wv, wo, wg, wu, wd)
    outs = [f(heads, rpd, head_dim)] * 3 + [f(rpd, width), f(rpd, ff), f(rpd, ff), f(ff // n, width)]
    return pl.pallas_call(
        functools.partial(spread_kernel, (head_dim, n, width, ff)), out_shape=[dx_t, f(1, rpd), f(1, rpd)] + outs,
        in_specs=any_spec(2), out_specs=any_spec(1) + vmem_spec(2) + any_spec(7),
        scratch_shapes=[vm(total, width), vf(slots, 2, rpd, CB), *[vf(*o.shape) for o in outs], dma(10)],
        name="spread")(*mid)


def solution(mesh):
    n = mesh.shape["seq"]

    def device_step(hidden, positions, g_attn, g_mlp, w_query, w_key, w_value, w_out, w_gate, w_up, w_down, d_out):
        rows, toks, width = hidden.shape
        layers, _, heads, head_dim = w_query.shape
        hd = heads * head_dim
        half = head_dim // 2
        inv_freq = 1.0 / (10000.0 ** (jnp.arange(half, dtype=F32) * (2.0 / head_dim)))
        turn = lambda w: w[0].transpose(1, 2, 0).reshape(hd, width)
        wq, wk, wv = turn(w_query), turn(w_key), turn(w_value)
        fwd = run_fwd(n, hidden, positions, inv_freq[:, None], g_attn, g_mlp, wq, wk, wv, w_out[0], head_dim)
        out = run_bwd(n, head_dim, g_attn, g_mlp, hidden.reshape(rows * toks, width), d_out.reshape(rows * toks, width), *fwd,
                      wq, wk, wv, w_out[0], w_gate[0], w_up[0], w_down[0], rows)
        dx, dga, dgm, dq, dk, dv, do, dg, du, dd = out
        back = lambda w: w.transpose(1, 0, 2)[None]
        return (dx.reshape(rows, toks, width), dga, dgm, back(dq), back(dk), back(dv), do[None], dg[None], du[None], dd[None])

    tok_spec = P("data", "seq", None)
    vec_spec = P(None, ("data", "seq"))
    mat_spec = P(None, ("data", "seq"), None)
    head_spec = P(None, ("data", "seq"), None, None)
    in_specs = (tok_spec, P("data", "seq")) + (P(),) * 9 + (tok_spec,)
    out_specs = (tok_spec, vec_spec, vec_spec, head_spec, head_spec, head_spec, mat_spec, mat_spec, mat_spec, mat_spec)
    return jax.shard_map(device_step, mesh=mesh, in_specs=in_specs, out_specs=out_specs, check_vma=False)
```

```python
import functools, math
import numpy as np
import jax, jax.numpy as jnp
from jax import lax
from jax.experimental import pallas as pl
from jax.experimental.pallas import tpu as pltpu
from jax.sharding import PartitionSpec as P

WINDOW = 256
NORM_EPS = 1e-5
QB = 128
BF, F32 = jnp.bfloat16, jnp.float32
NN, NT, TN = ((1,), (0,)), ((1,), (1,)), ((0,), (0,))
MESH = pl.DeviceIdType.MESH
NEG = -1e30
VMEM_LIMIT = 67043328


def dot(a, b, dims=NN):
    return lax.dot_general(a, b, (dims, ((), ())), preferred_element_type=F32)


def cdiv_loop(n, body):
    lax.fori_loop(0, n, lambda i, c: body(i) or c, 0)


def mod(a, b):
    return a % b if isinstance(a, int) else lax.rem(a, b)


def aligned(a, b):
    return a if isinstance(a, int) else pl.multiple_of(a, b)


def rope(blk, cos_b, sin_b, sign, head_dim):
    half = head_dim // 2
    parts = []
    for h in range(blk.shape[0] // head_dim):
        first = blk[h * head_dim:h * head_dim + half]
        second = blk[h * head_dim + half:(h + 1) * head_dim]
        if sign > 0:
            parts += [first * cos_b - second * sin_b, second * cos_b + first * sin_b]
        else:
            parts += [first * cos_b + second * sin_b, second * cos_b - first * sin_b]
    return jnp.concatenate(parts, axis=0)


def normed(x, gain):
    xf = x.astype(F32)
    inv = lax.rsqrt(jnp.mean(xf * xf, axis=-1, keepdims=True) + NORM_EPS)
    return (xf * inv * gain).astype(BF)


def stack_pair(pair_t):
    half = pair_t.shape[0] // 2
    zero = jnp.zeros((half, pair_t.shape[1]), pair_t.dtype)
    return jnp.concatenate(
        [jnp.concatenate([pair_t[:half], zero], axis=0), jnp.concatenate([zero, pair_t[half:]], axis=0)], axis=1)


def unstack_pair(both):
    half, cols = both.shape[0] // 2, both.shape[1] // 2
    return jnp.concatenate([both[:half, :cols], both[half:, cols:]], axis=0)


def col_sum(x):
    return jnp.sum(x, axis=0, keepdims=True)


def merged(scores, upper, bias0, bias1):
    return jnp.where(upper, scores[:QB] + bias0, scores[2 * QB:]), scores[QB:2 * QB] + bias1


def banded(p02, p1, upper):
    return jnp.concatenate(
        [jnp.where(upper, p02, 0.0).astype(BF), p1.astype(BF), jnp.where(upper, 0.0, p02).astype(BF)], axis=0)


def upper_mask():
    key_ids = lax.broadcasted_iota(jnp.int32, (QB, 2 * QB), 0)
    query_ids = lax.broadcasted_iota(jnp.int32, (QB, 2 * QB), 1) % QB
    return key_ids > query_ids


def start_bias(first, blk):
    bias = jnp.where(first, NEG, 0.0).astype(F32)
    return (bias if blk < 2 else 0.0), (bias if blk < 1 else 0.0)


def fwd_kernel(n, head_dim, x_h, pos, invf, ga, gm, wq_h, wk_h, wv_h, wo_h,
               q_h, kt_h, k_h, v_h, hat_h, ot_h, xm_h, hm_h, hmt_h, qr_h, lse_h, cos_t, sin_t,
               xv, halo, qr, lse, pos_halo, wq, wk, wv, wo, q, kt, k, v, vt, hat, ot, xm, hm, hmt, hb, hh, acc, acc2, ak, av, cos_h, sin_h,
               sc0, sc1, sc2, pb0, pb1, pb2, ldx, ld, st, snd, rcv, qsnd, qrcv):
    sc, pb = (sc0, sc1, sc2), (pb0, pb1, pb2)
    rows, toks, width = xv.shape
    ext, total, pw = toks + WINDOW, rows * toks, 2 * head_dim
    n_pairs = wq.shape[0] // pw
    tb, n_steps = toks // QB, n_pairs * rows
    me = lax.axis_index("seq")
    right, left = lax.rem(me + 1, n), lax.rem(me + n - 1, n)
    load_x = [pltpu.make_async_copy(x_h.at[b], xv.at[b], ldx.at[b]) for b in range(rows)]
    load_w = [pltpu.make_async_copy(s, d, ld.at[i]) for i, (s, d) in enumerate(((wq_h, wq), (wk_h, wk), (wv_h, wv), (wo_h, wo)))]
    for c in load_x:
        c.start()
    barrier = pltpu.get_barrier_semaphore()
    for other in (left, right):
        pl.semaphore_signal(barrier, inc=1, device_id={"seq": other}, device_id_type=MESH)
    pl.semaphore_wait(barrier, 2)

    def push(i, s, d):
        return pltpu.make_async_remote_copy(src_ref=s, dst_ref=d, send_sem=snd.at[i], recv_sem=rcv.at[i], device_id={"seq": right}, device_id_type=MESH)

    def push_rows(b):
        return push(b, x_h.at[b, toks - WINDOW:, :], halo.at[b])

    send_pos = push(rows, pos, pos_halo)
    send_pos.start()
    for b in range(rows):
        push_rows(b).start()

    def angles(cos_ref, sin_ref, positions):
        count = positions.shape[1]
        for b in range(rows):
            ang = invf[:] * positions[b:b + 1, :].astype(F32)
            cos_ref[:, b * count:(b + 1) * count] = jnp.cos(ang)
            sin_ref[:, b * count:(b + 1) * count] = jnp.sin(ang)

    angles(cos_t, sin_t, pos[:])

    def norm_rows(b):
        for i in range(tb):
            h = normed(xv[b, i * QB:(i + 1) * QB, :], ga[:])
            hb[pl.ds(pl.multiple_of((b * tb + i) * QB, QB), QB), :] = h

    with jax.named_scope("f_norm"):
        for c in load_x:
            c.wait()
        for c in load_w:
            c.start()
        cdiv_loop(rows, norm_rows)
    keep_hat = pltpu.make_async_copy(hat, hat_h, st.at[0])
    tables = cos_t[:], sin_t[:]

    def put_q(src):
        for p in range(n_pairs):
            r = slice(p * pw, (p + 1) * pw)
            q[r, :] = (rope(src[r, :], *tables, 1, head_dim) * (head_dim ** -0.5)).astype(BF)

    def put_own(src, dst_t, dst, turn):
        for p in range(n_pairs):
            r = slice(p * pw, (p + 1) * pw)
            both = (rope(src[r, :], *tables, 1, head_dim) if turn else src[r, :]).astype(BF)
            for b in range(rows):
                blk = both[:, b * toks:(b + 1) * toks]
                own = slice(b * ext + WINDOW, (b + 1) * ext)
                dst_t[r, own] = blk
                dst[own, r] = blk.T

    with jax.named_scope("f_mm"):
        load_w[0].wait()
        load_w[1].wait()
        load_w[2].wait()
        acc[:] = dot(wq[:], hb[:], NT)
        acc2[:] = dot(wk[:], hb[:], NT)
        put_q(acc)
        acc[:] = dot(wv[:], hb[:], NT)
        put_own(acc2, kt, k, True)
        for i in range(total // QB):
            r = slice(i * QB, (i + 1) * QB)
            hat[:, r] = hb[r, :].T
        put_own(acc, vt, v, False)
    keep_hat.start()
    keep_q = pltpu.make_async_copy(q, q_h, st.at[1])
    keep_q.start()

    def push_q(b):
        return pltpu.make_async_remote_copy(src_ref=q.at[:, b * toks:b * toks + WINDOW], dst_ref=qr.at[:, b * WINDOW:(b + 1) * WINDOW],
                                            send_sem=qsnd.at[b], recv_sem=qrcv.at[b], device_id={"seq": left}, device_id_type=MESH)

    for b in range(rows):
        push_q(b).start()
    send_pos.wait()
    angles(cos_h, sin_h, pos_halo[:, toks - WINDOW:])

    def keeps(b):
        wide, cols = pl.ds(pl.multiple_of(b * ext, QB), ext), pl.ds(pl.multiple_of(b * toks, QB), toks)
        ends = ((kt.at[:, wide], kt_h.at[:, wide]), (k.at[wide, :], k_h.at[wide, :]), (v.at[wide, :], v_h.at[wide, :]),
                (ot.at[:, cols], ot_h.at[:, cols]), (hm.at[cols, :], hm_h.at[cols, :]), (hmt.at[:, cols], hmt_h.at[:, cols]),
                (xm.at[cols, :], xm_h.at[cols, :]))
        return [pltpu.make_async_copy(s, d, st.at[2 + b * len(ends) + i]) for i, (s, d) in enumerate(ends)]

    def halo_in(b):
        with jax.named_scope("f_halo_wait"):
            push_rows(b).wait()
        with jax.named_scope("f_halo"):
            for i in range(WINDOW // QB):
                r = slice(i * QB, (i + 1) * QB)
                hh[r, :] = normed(halo[b, r, :], ga[:])
            ak[:] = dot(wk[:], hh[:], NT)
            av[:] = dot(wv[:], hh[:], NT)
            cols = pl.ds(pl.multiple_of(b * WINDOW, QB), WINDOW)
            wide = pl.ds(pl.multiple_of(b * ext, QB), WINDOW)
            near = cos_h[:, cols], sin_h[:, cols]
            for src, dst_t, dst in ((ak, kt, k), (av, vt, v)):
                for p in range(n_pairs):
                    r = slice(p * pw, (p + 1) * pw)
                    blk = (rope(src[r, :], *near, 1, head_dim) if dst is k else src[r, :]).astype(BF)
                    dst_t[r, wide] = blk
                    dst[wide, r] = blk.T
        for c in keeps(b)[:3]:
            c.start()

    upper = upper_mask()
    first = me == 0

    def spots(it, blk):
        b, p = it // n_pairs, mod(it, n_pairs)
        pr = pl.ds(aligned(p * pw, pw), pw)
        return pr, pl.ds(aligned(b * toks + blk * QB, QB), QB), pl.ds(aligned(b * ext + blk * QB, QB), 3 * QB)

    def score(it):
        for blk in range(tb):
            pr, cols, keys = spots(it, blk)
            sc[blk][:] = dot(k[keys, pr], stack_pair(q[pr, cols]))

    def soften(it, blk):
        s02, s1 = merged(sc[blk][:], upper, *start_bias(first, blk))
        top = jnp.max(jnp.maximum(s02, s1), axis=0, keepdims=True)
        e02, e1 = jnp.exp(s02 - top), jnp.exp(s1 - top)
        mass = col_sum(e02 + e1)
        inv = 1.0 / mass
        lse[it, blk:blk + 1, :] = top + jnp.log(mass)
        pb[blk][:] = banded(e02 * inv, e1 * inv, upper)

    def mix(it):
        for blk in range(tb):
            pr, cols, keys = spots(it, blk)
            ot[pr, cols] = unstack_pair(dot(vt[pr, keys], pb[blk][:])).astype(BF)

    def project(b):
        cols = pl.ds(pl.multiple_of(b * toks, QB), toks)
        with jax.named_scope("f_proj"):
            mid = (xv[b].astype(F32) + dot(ot[:, cols], wo[:], TN)).astype(BF)
            xm[cols, :] = mid
            h = normed(mid, gm[:])
            hm[cols, :] = h
            hmt[:, cols] = h.T
        for c in keeps(b)[3:]:
            c.start()

    keep_qr, keep_lse = (pltpu.make_async_copy(*ends, ld.at[i]) for i, ends in enumerate(((qr, qr_h), (lse, lse_h))))
    load_w[3].wait()
    for blk in range(tb):
        pb[blk][:] = jnp.zeros(pb[blk].shape, BF)

    def walk(i):
        it = i - 1

        @pl.when((lax.rem(i, n_pairs) == 0) & (i < n_steps))
        def _():
            halo_in(i // n_pairs)

        @pl.when(i == 0)
        def _():
            score(0)

        @pl.when((i > 0) & (i <= n_steps))
        def _():
            with jax.named_scope("f_attn"):
                mix(jnp.maximum(it - 1, 0))
                for blk in range(tb):
                    soften(it, blk)
                score(jnp.minimum(i, n_steps - 1))

        @pl.when(i == n_steps)
        def _():
            for b in range(rows):
                push_q(b).wait()
            keep_qr.start()

        @pl.when(i > n_steps)
        def _():
            mix(n_steps - 1)

        @pl.when((lax.rem(it, n_pairs) == 0) & (it > 0))
        def _():
            project(it // n_pairs - 1)

    cdiv_loop(n_steps + 2, walk)
    with jax.named_scope("f_store_wait"):
        keep_lse.start()
        keep_hat.wait()
        keep_q.wait()
        keep_qr.wait()
        keep_lse.wait()
        for b in range(rows):
            for c in keeps(b):
                c.wait()


def any_spec(k):
    return [pl.BlockSpec(memory_space=pl.ANY)] * k


def vmem_spec(k):
    return [pl.BlockSpec(memory_space=pltpu.VMEM)] * k


def run_fwd(n, x, pos, invf, ga, gm, wq, wk, wv, wo, head_dim):
    rows, toks, width = x.shape
    hd = wq.shape[0]
    ext, total, n_halo = toks + WINDOW, rows * toks, rows * WINDOW
    half = head_dim // 2
    sds = lambda *s: jax.ShapeDtypeStruct(s, BF)
    dma = lambda *s: pltpu.SemaphoreType.DMA(s)
    outs = [sds(hd, total), sds(hd, rows * ext), sds(rows * ext, hd), sds(rows * ext, hd), sds(width, total), sds(hd, total), sds(total, width), sds(total, width), sds(width, total)]
    outs += [sds(hd, n_halo), jax.ShapeDtypeStruct((rows * hd // (2 * head_dim), 8, 2 * QB), F32)] + [jax.ShapeDtypeStruct((half, total), F32)] * 2
    vm = lambda *s: pltpu.VMEM(s, BF)
    vf = lambda *s: pltpu.VMEM(s, F32)
    scratch = [vm(rows, toks, width), vm(rows, WINDOW, width), vm(hd, n_halo), vf(rows * hd // (2 * head_dim), 8, 2 * QB), pltpu.VMEM((rows, toks), jnp.int32), vm(hd, width), vm(hd, width), vm(hd, width), vm(hd, width),
               vm(hd, total), vm(hd, rows * ext), vm(rows * ext, hd), vm(rows * ext, hd), vm(hd, rows * ext), vm(width, total), vm(hd, total), vm(total, width), vm(total, width), vm(width, total), vm(total, width), vm(WINDOW, width),
               vf(hd, total), vf(hd, total), vf(hd, WINDOW), vf(hd, WINDOW), vf(half, n_halo), vf(half, n_halo),
               *[vf(3 * QB, 2 * QB)] * 3, *[vm(3 * QB, 2 * QB)] * 3,
               dma(rows), dma(4), dma(2 + 7 * rows), dma(rows + 1), dma(rows + 1), dma(rows), dma(rows)]
    return pl.pallas_call(
        functools.partial(fwd_kernel, n, head_dim), out_shape=outs,
        in_specs=any_spec(1) + vmem_spec(4) + any_spec(4), out_specs=any_spec(11) + vmem_spec(2), scratch_shapes=scratch,
        compiler_params=pltpu.CompilerParams(collective_id=0, has_side_effects=True, vmem_limit_bytes=VMEM_LIMIT),
        name="forward")(x, pos, invf, ga, gm, wq, wk, wv, wo)


LAG = 2
SLOTS = 2 * LAG
RING = 8
CB = 256


def at(ref, *idx):
    return ref.at[idx]


class Torus:
    def __init__(self, n, head, last, turn, parts, recv0, recv1, recv2, recv3, recv4, acc, acc2, fin, snd, rcv):
        self.side = math.isqrt(n // 2)
        assert self.side == 4
        me = lax.axis_index("seq")
        self.core = lax.rem(me, 2)
        chip = me // 2
        self.x, self.y = lax.rem(chip, 4), chip // 4
        self.head, self.last, self.turn = head, last, turn
        self.parts, self.recv0, self.recv1, self.recv2, self.recv3, self.recv4 = parts, recv0, recv1, recv2, recv3, recv4
        self.acc, self.acc2, self.fin, self.snd, self.rcv = acc, acc2, fin, snd, rcv
        self.partner = me + 1 - 2 * self.core
        self.rows, self.columns = [lax.rem(self.y + d, 4) * 4 for d in range(4)], [lax.rem(self.x + d, 4) for d in range(4)]
        self.hops = [[self.device(0, d) for d in range(4)], [self.device(d, 0) for d in range(4)]]

    def device(self, dy, dx):
        return (self.rows[dy] + self.columns[dx]) * 2 + self.core

    def copy(self, lane, kind, slot, src, dst, target):
        return pltpu.make_async_remote_copy(
            src_ref=src, dst_ref=dst, send_sem=self.snd.at[lane, kind, slot], recv_sem=self.rcv.at[lane, kind, slot],
            device_id={"seq": target}, device_id_type=MESH)

    def late(self, pair, yes, no):
        first, end = self.turn
        return jnp.where((pair >= first) & (pair < end), yes, no)

    def swap(self, ring, slot):
        return self.copy(0, 0, slot, self.parts.at[ring, :, :, 1 - self.core], self.recv0.at[slot], self.partner)

    def copies(self, stage, kind, pair, held, slot):
        axis = kind if stage < 3 else 1 - kind
        plus, minus = self.hops[axis][1], self.hops[axis][-1]
        half = CB // 2
        if stage == 1:
            if axis == 0:
                minus = self.late(pair, plus, minus)
            ends = [(self.acc.at[kind, held, 2, pl.ds(0, 2)], self.recv1), (self.acc.at[kind, held, 2, pl.ds(2, 2)], self.recv1)]
        elif stage == 2:
            ends = [(self.acc.at[kind, held, 1], self.recv2), (self.acc.at[kind, held, 3], self.recv2)]
        elif stage == 3:
            ends = [(self.acc2.at[kind, held, 2, :, pl.ds(0, half)], self.recv3), (self.acc2.at[kind, held, 2, :, pl.ds(half, half)], self.recv3)]
        else:
            ends = [(self.acc2.at[kind, held, 1], self.recv4), (self.acc2.at[kind, held, 3], self.recv4)]
        lane = 2 * stage - 1
        return [self.copy(lane + i, kind, slot, src, buf.at[kind, slot, i], (plus, minus)[i]) for i, (src, buf) in enumerate(ends)]

    def add(self, stage, kind, pair, held, slot, ring):
        acc, acc2 = self.acc, self.acc2
        if stage == 1:
            for r1 in range(4):
                for r2 in range(4):
                    ry, rx = (r2, r1) if kind == 0 else (r1, r2)
                    chip = self.rows[ry] + self.columns[rx]
                    acc[kind, held, r1, r2] = self.parts[ring, kind, chip, self.core] + self.recv0[slot, kind, chip]
        elif stage == 2:
            back = self.late(pair, 1, 3) if kind == 0 else 3
            acc[kind, held, 1, :2] += self.recv1[kind, slot, 0]
            acc[kind, held, back, 2:] += self.recv1[kind, slot, 1]
        elif stage == 3:
            acc2[kind, held] = acc[kind, held, 0] + (self.recv2[kind, slot, 0] + self.recv2[kind, slot, 1])
        elif stage == 4:
            half = CB // 2
            acc2[kind, held, 1, :, :half] += self.recv3[kind, slot, 0]
            acc2[kind, held, 3, :, half:] += self.recv3[kind, slot, 1]
        else:
            self.fin[pair, kind] = acc2[kind, held, 0] + (self.recv4[kind, slot, 0] + self.recv4[kind, slot, 1])

    def when(self, pair, fn):
        if isinstance(pair, int):
            if 0 <= pair <= self.last and (pair <= self.head or pair == self.last or (pair - self.head) % 2 == 0):
                fn()
        else:
            pl.when((pair >= 0) & ((pair <= self.head) | (pair == self.last) | ((pair < self.last) & (lax.rem(pair - self.head, 2) == 0))))(fn)

    def tick(self, t):
        now, land = mod(t, SLOTS), mod(t + SLOTS - LAG, SLOTS)
        ring_now, ring_land = mod(t, RING), mod(t + RING - LAG, RING)
        for stage in range(5, -1, -1):
            pair = t - LAG * stage
            held = land if stage % 2 else now

            def move(stage=stage, pair=pair, held=held):
                if stage == 0:
                    self.swap(ring_now, now).start()
                    return
                if stage == 1:
                    with jax.named_scope("t_wait1"):
                        self.swap(ring_land, land).wait()
                for kind in range(2):
                    if stage > 1:
                        with jax.named_scope(f"t_wait{stage}"):
                            for c in self.copies(stage - 1, kind, pair, held, land):
                                c.wait()
                    self.add(stage, kind, pair, held, land, ring_land)
                    if stage < 5:
                        for c in self.copies(stage, kind, pair, held, now):
                            c.start()
            self.when(pair, move)


def pick(i, table):
    out = 0
    for key, value in table.items():
        out = jnp.where(i == key, value, out)
    return out


def norm_back(x, gain, grad, res):
    xf = x.astype(F32)
    inv = lax.rsqrt(jnp.mean(xf * xf, axis=-1, keepdims=True) + NORM_EPS)
    unit = xf * inv
    gu = grad * gain
    out = inv * (gu - unit * jnp.mean(gu * unit, axis=-1, keepdims=True)) + res.astype(F32)
    gu = grad * unit
    return out.astype(BF), jnp.sum(gu.reshape(-1, 8, gu.shape[-1]), axis=0)


def plan(n_mlp, n_down, nc):
    order = [("o", g) for g in range(nc)] + [(name, g) for g in range(nc) for name in "qkv"]
    base, head = n_mlp + n_down, n_mlp + n_down + nc - 1
    last = 2 * (base - 1 - head + len(order) // 2) + head - 1
    spot = lambda pair: min(max(pair, 2 * pair - head), last)
    return head, {name: (spot(base + i // 2), i % 2) for i, name in enumerate(order)}, last


def bwd_kernel(n, head_dim, dims, ga, gm, x_h, dout_h, q_h, kt_h, k_h, v_h, hat_h, ot_h, xm_h, hm_h, hmt_h, qr_h, lse_h, cos_h, sin_h,
               wq_h, wk_h, wv_h, wo_h, wg_h, wu_h, wd_h,
               dx_h, fin_h,
               parts, recv0, recv1, recv2, recv3, recv4, acc, acc2, fin, snd, rcv,
               dor, lser, deltar, hsnd, hrcv, osnd, orcv, gsend, grecv, gsem, ld,
               xbuf, mbuf, gnm, gmid, ot, hat, wo, dot_, lse, delta, cos_i, sin_i, dgain):
    rows, toks, width, hd, ff = dims
    ext, total = toks + WINDOW, rows * toks
    pw = 2 * head_dim
    n_pairs = hd // pw
    tb, n_steps = toks // QB, n_pairs * rows
    nb, nc, sub = ff // CB, width // CB, ff // width
    rpd = width // n
    per, half_sub = CB // pw, sub // 2
    head, place, end = plan(nb, nc * half_sub, nc)
    comm = Torus(n, head, end, (nb - 1, nb + n_pairs), parts, recv0, recv1, recv2, recv3, recv4, acc, acc2, fin, snd, rcv)
    me = lax.axis_index("seq")
    left = lax.rem(me + n - 1, n)
    barrier = pltpu.get_barrier_semaphore()

    def greet(i):
        pl.semaphore_signal(barrier, inc=1, device_id={"seq": lax.rem(me + i + 1, n)}, device_id_type=MESH)

    def load(i, s, d):
        c = pltpu.make_async_copy(s, d, ld.at[i])
        c.start()
        return c

    def late(i):
        s, d = ((xm_h, mbuf), (ot_h, ot), (hat_h, hat), (wo_h, wo), (lse_h, lse), (cos_h, cos_i), (sin_h, sin_i))[i]
        return pltpu.make_async_copy(s, d, ld.at[1 + i])

    def to_left(src, dst, send_sem, recv_sem):
        return pltpu.make_async_remote_copy(src_ref=src, dst_ref=dst, send_sem=send_sem, recv_sem=recv_sem,
                                            device_id={"seq": left}, device_id_type=MESH)

    n_late = 7

    def push_rows(i):
        return to_left(*((lse_h, lser), (delta, deltar))[i], hsnd.at[i], hrcv.at[i])

    def push_out(p):
        pr = pl.ds(aligned(p * pw, pw), pw)
        return [to_left(dot_.at[pr, pl.ds(b * toks, WINDOW)], dor.at[pr, pl.ds(b * WINDOW, WINDOW)], osnd.at[p, b], orcv.at[p, b])
                for b in range(rows)]

    def give_out(p):
        for c in push_out(p):
            c.start()

    def put(spot, value):
        pair, kind = spot
        parts[mod(pair, RING), kind] = value.reshape(n // 2, 2, rpd, CB)

    def spot_of(name, g):
        known = {i: place[name, i] for i in range(nc)}
        return pick(g, {i: s[0] for i, s in known.items()}), pick(g, {i: s[1] for i, s in known.items()})

    def spots(it, blk):
        p, b = it // rows, mod(it, rows)
        pr = pl.ds(aligned(p * pw, pw), pw)
        return pr, pl.ds(aligned(b * toks + blk * QB, QB), QB), pl.ds(aligned(b * ext + blk * QB, QB), 3 * QB)

    def row_of(it):
        return mod(it, rows) * n_pairs + it // rows

    def mlp(hm, hmt, actt, wgu, wd, dgu, wld):
        def weights(j, slot):
            c = aligned(j * CB, CB)
            return [pltpu.make_async_copy(wg_h.at[:, pl.ds(c, CB)], wgu.at[slot, :, :CB], wld.at[slot, 0]),
                    pltpu.make_async_copy(wu_h.at[:, pl.ds(c, CB)], wgu.at[slot, :, CB:], wld.at[slot, 1]),
                    pltpu.make_async_copy(wd_h.at[pl.ds(c, CB), :], wd.at[slot], wld.at[slot, 2])]

        for c in weights(0, 0):
            c.start()
        ld_hm, ld_x, ld_hmt = load(8, hm_h, hm), load(0, dout_h, xbuf), load(9, hmt_h, hmt)
        cdiv_loop(n - 1, greet)
        gnm[:] = jnp.zeros_like(gnm)
        gsend[:] = jnp.zeros_like(gsend)
        dgain[:] = jnp.zeros_like(dgain)
        ld_hm.wait()
        ld_x.wait()
        ld_hmt.wait()
        for i in range(n_late):
            late(i).start()

        def block(j):
            slot = lax.rem(j, 2)
            for c in weights(j, slot):
                c.wait()

            @pl.when(j + 1 < nb)
            def _():
                for c in weights(j + 1, 1 - slot):
                    c.start()

            c0 = pl.multiple_of(j * CB, CB)
            with jax.named_scope("b_mlp"):
                for b in range(rows):
                    r = slice(b * toks, (b + 1) * toks)
                    gu = dot(hm[r, :], wgu[slot])
                    gact = dot(xbuf[r, :], wd[slot], NT).astype(BF).astype(F32)
                    gate, up = gu[:, :CB], gu[:, CB:]
                    sig = 1.0 / (1.0 + jnp.exp(-gate))
                    swish = gate * sig
                    actt[pl.ds(c0, CB), r] = (swish * up).astype(BF).T
                    dgu[r, :CB] = (gact * up * (sig + swish * (1.0 - sig))).astype(BF)
                    dgu[r, CB:] = (gact * swish).astype(BF)
                both = dot(hmt[:], dgu[:])
                ring = lax.rem(j, RING)
                parts[ring, 0] = both[:, :CB].reshape(n // 2, 2, rpd, CB)
                parts[ring, 1] = both[:, CB:].reshape(n // 2, 2, rpd, CB)
                for b in range(rows):
                    r = slice(b * toks, (b + 1) * toks)
                    gnm[r, :] += dot(dgu[r, :], wgu[slot], NT)

            @pl.when(j == 0)
            def _():
                pl.semaphore_wait(barrier, n - 1)
                push_rows(0).start()

            comm.tick(j)

        cdiv_loop(nb, block)

        def down(c):
            share = n // 2 // sub
            c0 = pl.multiple_of(c * CB, CB)
            for m in range(sub):
                res = dot(actt[m * width:(m + 1) * width, :], xbuf[:, pl.ds(c0, CB)]).reshape(share, 2, sub, rpd, CB)
                for i in range(sub):
                    pair = nb + c * half_sub + i // 2
                    parts[lax.rem(pair, RING), i % 2, m * share:(m + 1) * share] = res[:, :, i]

        for i in range(n_late):
            late(i).wait()

        def mid(b):
            for i in range(tb):
                r = pl.ds(pl.multiple_of((b * tb + i) * QB, QB), QB)
                out, dg = norm_back(mbuf[r, :], gm[:], gnm[r, :], xbuf[r, :])
                gmid[r, :] = out
                dgain[8:, :] += dg

        def deltas(p):
            for it in range(rows):
                for blk in range(tb):
                    pr, cols, _ = spots(p * rows + it, blk)
                    both = dot_[pr, cols].astype(F32) * ot[pr, cols].astype(F32)
                    delta[row_of(p * rows + it), blk:blk + 1, :] = jnp.concatenate(
                        [col_sum(both[:head_dim]), col_sum(both[head_dim:])], axis=1)

        def column(c):
            with jax.named_scope("b_down"):
                down(c)
            comm.tick(nb + c + jnp.minimum(c, 1))

            @pl.when(c == 1)
            def _():
                give_out(c)

            @pl.when(c == 0)
            def _():
                with jax.named_scope("b_mid"):
                    cdiv_loop(rows, mid)
                with jax.named_scope("b_dot"):
                    dot_[:] = dot(wo[:], gmid[:], NT).astype(BF)
                    cdiv_loop(n_pairs, deltas)
                comm.tick(nb + 1)
                push_rows(1).start()
                give_out(0)

        cdiv_loop(nc, column)

    vm = lambda *s: pltpu.VMEM(s, BF)
    vf = lambda *s: pltpu.VMEM(s, F32)
    pl.run_scoped(mlp, vm(total, width), vm(width, total), vm(ff, total), vm(2, width, 2 * CB), vm(2, CB, width), vm(total, 2 * CB),
                  pltpu.SemaphoreType.DMA((2, 3)))
    def attention(q, kt, k, v, qr, dv, sc0, sc1, sc2, sr, dp0, dp1, dp2, dr, pb0, pb1, pb2, pr_, ds0, ds1, ds2, dsr):
        dqt, dkt = ot, q
        wq, wk, wv = k.at[:hd], kt.at[:, :width], v.at[:hd]
        sc, dp, pb, ds = (sc0, sc1, sc2), (dp0, dp1, dp2), (pb0, pb1, pb2), (ds0, ds1, ds2)
        lds = [load(8 + i, s, d) for i, (s, d) in enumerate(((q_h, q), (k_h, k), (v_h, v), (qr_h, qr), (kt_h, kt)))]

        def out_grad(g):
            put(spot_of("o", g), dot(ot[:], gmid[:, pl.ds(pl.multiple_of(g * CB, CB), CB)]))

        with jax.named_scope("b_dwo"):
            cdiv_loop(nc, out_grad)
        first_tick = nb + nc + 1
        comm.tick(first_tick)
        give_out(2)
        upper = upper_mask()
        first, last = me == 0, me == n - 1
        halves = slice(0, WINDOW), slice(WINDOW, 3 * QB)

        def right(it, i):
            p, b = it // rows, mod(it, rows)
            return pl.ds(aligned(p * pw, pw), pw), pl.ds(aligned(b * WINDOW + i * QB, QB), QB), pl.ds(aligned(b * ext + toks + i * QB, QB), WINDOW - i * QB)

        def score(it):
            for blk in range(tb):
                pr, cols, keys = spots(it, blk)
                sc[blk][:] = dot(k[keys, pr], stack_pair(q[pr, cols]))
                dp[blk][:] = dot(v[keys, pr], stack_pair(dot_[pr, cols]))
            for i, rs in enumerate(halves):
                pr, cols, keys = right(it, i)
                sr[rs, :] = dot(k[keys, pr], stack_pair(qr[pr, cols]))
                dr[rs, :] = dot(v[keys, pr], stack_pair(dor[pr, cols]))

        def soften(it):
            row = row_of(it)
            for blk in range(tb):
                s02, s1 = merged(sc[blk][:], upper, *start_bias(first, blk))
                norm, mean = lse[row, blk:blk + 1, :], delta[row, blk:blk + 1, :]
                p02, p1 = jnp.exp(s02 - norm), jnp.exp(s1 - norm)
                g02, g1 = jnp.where(upper, dp[blk][:QB], dp[blk][2 * QB:]), dp[blk][QB:2 * QB]
                pb[blk][:] = banded(p02, p1, upper)
                ds[blk][:] = banded(p02 * (g02 - mean), p1 * (g1 - mean), upper)
            for blk in range(tb):
                i = blk // 2
                rs = slice(blk * QB, (blk + 1) * QB)
                p = jnp.exp(sr[rs, :] - jnp.where(last, -NEG, lser[row, i:i + 1, :]))
                g = p * (dr[rs, :] - deltar[row, i:i + 1, :])
                pr_[rs, :] = (p if blk == 1 else jnp.where(upper, p, 0.0)).astype(BF)
                dsr[rs, :] = (g if blk == 1 else jnp.where(upper, g, 0.0)).astype(BF)

        def grads(it):
            ks, vs = [], []
            for blk in range(tb):
                pr, cols, keys = spots(it, blk)
                own = slice(max(0, 2 - blk) * QB, 3 * QB)
                vs.append(dot(pb[blk][own, :], stack_pair(dot_[pr, cols]), NT))
                ks.append(dot(ds[blk][own, :], stack_pair(q[pr, cols]), NT))
                dq = unstack_pair(dot(kt[pr, keys], ds[blk][:])) * (head_dim ** -0.5)
                dqt[pr, cols] = rope(dq, cos_i[:, cols], sin_i[:, cols], -1, head_dim).astype(BF)
            for i, rs in enumerate(halves):
                pr, cols, _ = right(it, i)
                vs.append(dot(pr_[rs, :], stack_pair(dor[pr, cols]), NT))
                ks.append(dot(dsr[rs, :], stack_pair(qr[pr, cols]), NT))
            for j in range(tb):
                pr, cols, _ = spots(it, j)
                gv, gk = (sum(x[i][(j - max(0, i - 2)) * QB:(j - max(0, i - 2) + 1) * QB] for i in range(j, j + 3)) for x in (vs, ks))
                dv[cols, pr] = gv.astype(BF)
                dkt[pr, cols] = rope(gk.T, cos_i[:, cols], sin_i[:, cols], -1, head_dim).astype(BF)

        def close_group(g):
            cols = pl.ds(pl.multiple_of(g * CB, CB), CB)
            with jax.named_scope("b_dwqkv"):
                put(spot_of("q", g), dot(hat[:], dqt[cols, :], NT))
                put(spot_of("k", g), dot(hat[:], dkt[cols, :], NT))
                put(spot_of("v", g), dot(hat[:], dv[:, cols]))

        def weights():
            return [pltpu.make_async_copy(s, d, ld.at[8 + i]) for i, (s, d) in enumerate(((wq_h, wq), (wk_h, wk), (wv_h, wv), (x_h, xbuf)))]

        def arrived(p):
            with jax.named_scope("b_hwait"):
                for c in push_out(p):
                    c.wait()

        def walk(it):
            ahead = it + 1

            @pl.when((lax.rem(ahead, rows) == 0) & (ahead < n_steps))
            def _():
                arrived(ahead // rows)

            @pl.when(it < n_steps)
            def _():
                with jax.named_scope("b_attn"):
                    grads(it - 1)
                    soften(it)
                    score(jnp.minimum(ahead, n_steps - 1))

            @pl.when(it == n_steps)
            def _():
                grads(n_steps - 1)
                for c in weights():
                    c.start()

            p, step = it // rows - 1, lax.rem(it, rows)

            @pl.when((step == 0) & (lax.rem(p, per) == per - 1))
            def _():
                close_group(p // per)

            now = first_tick + 1 + p + step // (rows - 1)
            twice = now - head

            @pl.when((step == 0) | ((step == rows - 1) & (twice > 0)))
            def _():
                comm.tick(now + jnp.maximum(twice - step // (rows - 1), 0))

            @pl.when((step == 0) & (p + 3 < n_pairs))
            def _():
                give_out(p + 3)

        for c in lds[:-1]:
            c.wait()
        for i in range(2):
            push_rows(i).wait()
        arrived(0)
        score(0)
        soften(0)
        score(1)
        lds[-1].wait()
        cdiv_loop(n_steps, lambda i: walk(i + 1))
        comm.tick(end)
        for c in weights():
            c.wait()

        def into(b):
            r = pl.ds(pl.multiple_of(b * toks, QB), toks)
            with jax.named_scope("b_into"):
                gnm[r, :] = dot(dqt[:, r], wq[:], TN) + dot(dkt[:, r], wk[:], TN) + dot(dv[r, :], wv[:])

            with jax.named_scope("b_final"):
                for i in range(tb):
                    r = pl.ds(pl.multiple_of((b * tb + i) * QB, QB), QB)
                    out, dg = norm_back(xbuf[r, :], ga[:], gnm[r, :], gmid[r, :])
                    mbuf[r, :] = out
                    dgain[:8, :] += dg
            comm.tick(end + 1 + b)

        cdiv_loop(rows, into)

    score_bufs = [vf(3 * QB, 2 * QB)] * 8 + [vm(3 * QB, 2 * QB)] * 8
    pl.run_scoped(attention, vm(hd, total), vm(hd, rows * ext), vm(rows * ext, hd), vm(rows * ext, hd), vm(hd, rows * WINDOW), vm(total, hd), *score_bufs)
    out_copy = load(1, mbuf, dx_h)
    gains = jnp.concatenate([col_sum(dgain[:8, :]), col_sum(dgain[8:, :]), jnp.zeros((6, width), F32)], axis=0)
    for p in range(n):
        gsend[p, :, :rpd] = gains[:, p * rpd:(p + 1) * rpd]

    def spread(i):
        to = lax.rem(me + i + 1, n)
        pltpu.make_async_remote_copy(src_ref=gsend.at[to], dst_ref=grecv.at[i], send_sem=gsem.at[0], recv_sem=gsem.at[1],
                                     device_id={"seq": to}, device_id_type=MESH).start()

    cdiv_loop(n - 1, spread)
    stop = end + 1 + 5 * LAG
    run = lambda lo, hi: lax.fori_loop(lo, hi, lambda t, c: comm.tick(t) or c, 0)
    run(end + 1 + rows, stop - LAG)
    most, rest = pl.ds(0, end - 1), pl.ds(end - 1, LAG + 1)
    keep_most = load(0, fin.at[most], fin_h.at[most])
    to_left(gsend.at[pl.ds(0, n - 1)], grecv, gsem.at[0], gsem.at[1]).wait()
    sums = gsend[me]
    for i in range(n - 1):
        sums = sums + grecv[i]
    fin[end + 1, 0, :8, :128] = sums
    out_copy.wait()
    run(stop - LAG, stop)
    with jax.named_scope("b_end"):
        keep_rest = load(1, fin.at[rest], fin_h.at[rest])
        keep_most.wait()
        keep_rest.wait()


def spread_kernel(dims, dx_i, fin_i, dx_o, dga_o, dgm_o, *refs):
    head_dim, n, width, ff = dims
    outs, (buf, fin), stage, sem = refs[:7], refs[7:9], refs[9:16], refs[16]
    dq, dk, dv, do, dg, du, dd = stage
    nb, nc, sub = ff // CB, width // CB, ff // width
    rpd = width // n
    head, place, end = plan(nb, nc * sub // 2, nc)
    get, get_fin, out = (pltpu.make_async_copy(*ends, sem.at[len(outs) + i]) for i, ends in enumerate(((dx_i, buf), (fin_i, fin), (buf, dx_o))))
    get_fin.start()
    get.start()
    get_fin.wait()
    gains = fin[end + 1, 0]
    dga_o[:] = gains[:1, :rpd]
    dgm_o[:] = gains[1:2, :rpd]
    for j in range(nb):
        dg[:, j * CB:(j + 1) * CB] = fin[j, 0]
        du[:, j * CB:(j + 1) * CB] = fin[j, 1]
    for c in range(nc):
        for i in range(sub):
            pair = nb + (c * sub + i) // 2
            dd[i * rpd:(i + 1) * rpd, c * CB:(c + 1) * CB] = fin[pair, i % 2]
    for g in range(nc):
        do[:, g * CB:(g + 1) * CB] = fin[place["o", g]]
        for name, ref in (("q", dq), ("k", dk), ("v", dv)):
            val = fin[place[name, g]]
            for h in range(CB // head_dim):
                ref[g * (CB // head_dim) + h] = val[:, h * head_dim:(h + 1) * head_dim]
    keeps = [pltpu.make_async_copy(s, d, sem.at[i]) for i, (s, d) in enumerate(zip(stage, outs))]
    for c in keeps:
        c.start()
    get.wait()
    out.start()
    for c in keeps:
        c.wait()
    out.wait()


def run_bwd(n, head_dim, ga, gm, x, dout, q, kt, k, v, hat, ot, xm, hm, hmt, qr, lse, cos_t, sin_t, wq, wk, wv, wo, wg, wu, wd, rows):
    total, width = x.shape
    hd, ff = wq.shape[0], wg.shape[1]
    toks = total // rows
    rpd, heads = width // n, hd // head_dim
    nb, nc, sub = ff // CB, width // CB, ff // width
    slots = plan(nb, nc * sub // 2, nc)[2] + 2
    n_pairs = hd // (2 * head_dim)
    f = lambda *s: jax.ShapeDtypeStruct(s, F32)
    dx_t = jax.ShapeDtypeStruct((total, width), BF)
    vm = lambda *s: pltpu.VMEM(s, BF)
    vf = lambda *s: pltpu.VMEM(s, F32)
    dma = lambda *s: pltpu.SemaphoreType.DMA(s)
    line = vf(rows * n_pairs, 8, 2 * QB)
    scratch = [vf(RING, 2, n // 2, 2, rpd, CB), vf(SLOTS, 2, n // 2, rpd, CB), vf(2, SLOTS, 2, 2, rpd, CB), vf(2, SLOTS, 2, 4, rpd, CB),
               vf(2, SLOTS, 2, rpd, CB // 2), vf(2, SLOTS, 2, rpd, CB), vf(2, SLOTS, 4, 4, rpd, CB), vf(2, SLOTS, 4, rpd, CB), vf(slots, 2, rpd, CB),
               dma(9, 2, SLOTS), dma(9, 2, SLOTS),
               vm(hd, rows * WINDOW), line, line, dma(2), dma(2), dma(n_pairs, rows), dma(n_pairs, rows),
               vf(n, 8, 128), vf(n - 1, 8, 128), dma(2), dma(13),
               vm(total, width), vm(total, width), vf(total, width), vm(total, width), vm(hd, total), vm(width, total), vm(hd, width), vm(hd, total), line, line, vf(*cos_t.shape), vf(*cos_t.shape), vf(16, width)]
    mid = pl.pallas_call(
        functools.partial(bwd_kernel, n, head_dim, (rows, toks, width, hd, ff)), out_shape=[dx_t, f(slots, 2, rpd, CB)],
        in_specs=vmem_spec(2) + any_spec(22), out_specs=any_spec(2), scratch_shapes=scratch,
        compiler_params=pltpu.CompilerParams(collective_id=1, has_side_effects=True, vmem_limit_bytes=VMEM_LIMIT),
        name="backward")(ga, gm, x, dout, q, kt, k, v, hat, ot, xm, hm, hmt, qr, lse, cos_t, sin_t, wq, wk, wv, wo, wg, wu, wd)
    outs = [f(heads, rpd, head_dim)] * 3 + [f(rpd, width), f(rpd, ff), f(rpd, ff), f(ff // n, width)]
    return pl.pallas_call(
        functools.partial(spread_kernel, (head_dim, n, width, ff)), out_shape=[dx_t, f(1, rpd), f(1, rpd)] + outs,
        in_specs=any_spec(2), out_specs=any_spec(1) + vmem_spec(2) + any_spec(7),
        scratch_shapes=[vm(total, width), vf(slots, 2, rpd, CB), *[vf(*o.shape) for o in outs], dma(10)],
        name="spread")(*mid)


def solution(mesh):
    n = mesh.shape["seq"]

    def device_step(hidden, positions, g_attn, g_mlp, w_query, w_key, w_value, w_out, w_gate, w_up, w_down, d_out):
        rows, toks, width = hidden.shape
        layers, _, heads, head_dim = w_query.shape
        hd = heads * head_dim
        half = head_dim // 2
        inv_freq = 1.0 / (10000.0 ** (jnp.arange(half, dtype=F32) * (2.0 / head_dim)))
        turn = lambda w: w[0].transpose(1, 2, 0).reshape(hd, width)
        wq, wk, wv = turn(w_query), turn(w_key), turn(w_value)
        fwd = run_fwd(n, hidden, positions, inv_freq[:, None], g_attn, g_mlp, wq, wk, wv, w_out[0], head_dim)
        out = run_bwd(n, head_dim, g_attn, g_mlp, hidden.reshape(rows * toks, width), d_out.reshape(rows * toks, width), *fwd,
                      wq, wk, wv, w_out[0], w_gate[0], w_up[0], w_down[0], rows)
        dx, dga, dgm, dq, dk, dv, do, dg, du, dd = out
        back = lambda w: w.transpose(1, 0, 2)[None]
        return (dx.reshape(rows, toks, width), dga, dgm, back(dq), back(dk), back(dv), do[None], dg[None], du[None], dd[None])

    tok_spec = P("data", "seq", None)
    vec_spec = P(None, ("data", "seq"))
    mat_spec = P(None, ("data", "seq"), None)
    head_spec = P(None, ("data", "seq"), None, None)
    in_specs = (tok_spec, P("data", "seq")) + (P(),) * 9 + (tok_spec,)
    out_specs = (tok_spec, vec_spec, vec_spec, head_spec, head_spec, head_spec, mat_spec, mat_spec, mat_spec, mat_spec)
    return jax.shard_map(device_step, mesh=mesh, in_specs=in_specs, out_specs=out_specs, check_vma=False)
```

```python
import functools, math
import numpy as np
import jax, jax.numpy as jnp
from jax import lax
from jax.experimental import pallas as pl
from jax.experimental.pallas import tpu as pltpu
from jax.sharding import PartitionSpec as P

WINDOW = 256
NORM_EPS = 1e-5
QB = 128
BF, F32 = jnp.bfloat16, jnp.float32
NN, NT, TN = ((1,), (0,)), ((1,), (1,)), ((0,), (0,))
MESH = pl.DeviceIdType.MESH
NEG = -1e30
VMEM_LIMIT = 67043328


def dot(a, b, dims=NN):
    return lax.dot_general(a, b, (dims, ((), ())), preferred_element_type=F32)


def cdiv_loop(n, body):
    lax.fori_loop(0, n, lambda i, c: body(i) or c, 0)


def mod(a, b):
    return a % b if isinstance(a, int) else lax.rem(a, b)


def aligned(a, b):
    return a if isinstance(a, int) else pl.multiple_of(a, b)


def rope(blk, cos_b, sin_b, sign, head_dim):
    half = head_dim // 2
    parts = []
    for h in range(blk.shape[0] // head_dim):
        first = blk[h * head_dim:h * head_dim + half]
        second = blk[h * head_dim + half:(h + 1) * head_dim]
        if sign > 0:
            parts += [first * cos_b - second * sin_b, second * cos_b + first * sin_b]
        else:
            parts += [first * cos_b + second * sin_b, second * cos_b - first * sin_b]
    return jnp.concatenate(parts, axis=0)


def normed(x, gain):
    xf = x.astype(F32)
    inv = lax.rsqrt(jnp.mean(xf * xf, axis=-1, keepdims=True) + NORM_EPS)
    return (xf * inv * gain).astype(BF)


def stack_pair(pair_t):
    half = pair_t.shape[0] // 2
    zero = jnp.zeros((half, pair_t.shape[1]), pair_t.dtype)
    return jnp.concatenate(
        [jnp.concatenate([pair_t[:half], zero], axis=0), jnp.concatenate([zero, pair_t[half:]], axis=0)], axis=1)


def unstack_pair(both):
    half, cols = both.shape[0] // 2, both.shape[1] // 2
    return jnp.concatenate([both[:half, :cols], both[half:, cols:]], axis=0)


def col_sum(x):
    return jnp.sum(x, axis=0, keepdims=True)


def merged(scores, upper, bias0, bias1):
    return jnp.where(upper, scores[:QB] + bias0, scores[2 * QB:]), scores[QB:2 * QB] + bias1


def banded(p02, p1, upper):
    return jnp.concatenate(
        [jnp.where(upper, p02, 0.0).astype(BF), p1.astype(BF), jnp.where(upper, 0.0, p02).astype(BF)], axis=0)


def upper_mask():
    key_ids = lax.broadcasted_iota(jnp.int32, (QB, 2 * QB), 0)
    query_ids = lax.broadcasted_iota(jnp.int32, (QB, 2 * QB), 1) % QB
    return key_ids > query_ids


def start_bias(first, blk):
    bias = jnp.where(first, NEG, 0.0).astype(F32)
    return (bias if blk < 2 else 0.0), (bias if blk < 1 else 0.0)


def fwd_kernel(n, head_dim, x_h, pos, invf, ga, gm, wq_h, wk_h, wv_h, wo_h,
               q_h, kt_h, k_h, v_h, hat_h, ot_h, xm_h, hm_h, hmt_h, qr_h, lse_h, cos_t, sin_t,
               xv, halo, qr, lse, pos_halo, wq, wk, wv, wo, q, kt, k, v, vt, hat, ot, xm, hm, hmt, hb, hh, acc, acc2, ak, av, cos_h, sin_h,
               sc0, sc1, sc2, pb0, pb1, pb2, ldx, ld, st, snd, rcv, qsnd, qrcv):
    sc, pb = (sc0, sc1, sc2), (pb0, pb1, pb2)
    rows, toks, width = xv.shape
    ext, total, pw = toks + WINDOW, rows * toks, 2 * head_dim
    n_pairs = wq.shape[0] // pw
    tb, n_steps = toks // QB, n_pairs * rows
    me = lax.axis_index("seq")
    right, left = lax.rem(me + 1, n), lax.rem(me + n - 1, n)
    load_x = [pltpu.make_async_copy(x_h.at[b], xv.at[b], ldx.at[b]) for b in range(rows)]
    load_w = [pltpu.make_async_copy(s, d, ld.at[i]) for i, (s, d) in enumerate(((wq_h, wq), (wk_h, wk), (wv_h, wv), (wo_h, wo)))]
    for c in load_x:
        c.start()
    barrier = pltpu.get_barrier_semaphore()
    for other in (left, right):
        pl.semaphore_signal(barrier, inc=1, device_id={"seq": other}, device_id_type=MESH)

    def push(i, s, d):
        return pltpu.make_async_remote_copy(src_ref=s, dst_ref=d, send_sem=snd.at[i], recv_sem=rcv.at[i], device_id={"seq": right}, device_id_type=MESH)

    def push_rows(b):
        return push(b, x_h.at[b, toks - WINDOW:, :], halo.at[b])

    send_pos = push(rows, pos, pos_halo)

    def angles(cos_ref, sin_ref, positions):
        count = positions.shape[1]
        for b in range(rows):
            ang = invf[:] * positions[b:b + 1, :].astype(F32)
            cos_ref[:, b * count:(b + 1) * count] = jnp.cos(ang)
            sin_ref[:, b * count:(b + 1) * count] = jnp.sin(ang)

    angles(cos_t, sin_t, pos[:])

    def norm_rows(b):
        for i in range(tb):
            h = normed(xv[b, i * QB:(i + 1) * QB, :], ga[:])
            hb[pl.ds(pl.multiple_of((b * tb + i) * QB, QB), QB), :] = h

    with jax.named_scope("f_norm"):
        for c in load_x:
            c.wait()
        for c in load_w:
            c.start()
        cdiv_loop(rows, norm_rows)
    pl.semaphore_wait(barrier, 2)
    send_pos.start()
    for b in range(rows):
        push_rows(b).start()
    keep_hat = pltpu.make_async_copy(hat, hat_h, st.at[0])
    tables = cos_t[:], sin_t[:]

    def put_q(src):
        for p in range(n_pairs):
            r = slice(p * pw, (p + 1) * pw)
            q[r, :] = (rope(src[r, :], *tables, 1, head_dim) * (head_dim ** -0.5)).astype(BF)

    def put_own(src, dst_t, dst):
        for p in range(n_pairs):
            r = slice(p * pw, (p + 1) * pw)
            both = (rope(src[r, :], *tables, 1, head_dim) if dst is k else src[r, :]).astype(BF)
            for b in range(rows):
                blk = both[:, b * toks:(b + 1) * toks]
                own = slice(b * ext + WINDOW, (b + 1) * ext)
                dst_t[r, own] = blk
                dst[own, r] = blk.T

    with jax.named_scope("f_mm"):
        load_w[0].wait()
        load_w[1].wait()
        load_w[2].wait()
        acc[:] = dot(wq[:], hb[:], NT)
        acc2[:] = dot(wk[:], hb[:], NT)
        put_q(acc)
        acc[:] = dot(wv[:], hb[:], NT)
        put_own(acc2, kt, k)
        for i in range(total // QB):
            r = slice(i * QB, (i + 1) * QB)
            hat[:, r] = hb[r, :].T
        put_own(acc, vt, v)
    keep_hat.start()
    keep_q = pltpu.make_async_copy(q, q_h, st.at[1])
    keep_q.start()

    def push_q(b):
        return pltpu.make_async_remote_copy(src_ref=q.at[:, b * toks:b * toks + WINDOW], dst_ref=qr.at[:, b * WINDOW:(b + 1) * WINDOW],
                                            send_sem=qsnd.at[b], recv_sem=qrcv.at[b], device_id={"seq": left}, device_id_type=MESH)

    for b in range(rows):
        push_q(b).start()
    send_pos.wait()
    angles(cos_h, sin_h, pos_halo[:, toks - WINDOW:])

    def keeps(b):
        wide, cols = pl.ds(pl.multiple_of(b * ext, QB), ext), pl.ds(pl.multiple_of(b * toks, QB), toks)
        ends = ((kt.at[:, wide], kt_h.at[:, wide]), (k.at[wide, :], k_h.at[wide, :]), (v.at[wide, :], v_h.at[wide, :]),
                (ot.at[:, cols], ot_h.at[:, cols]), (hm.at[cols, :], hm_h.at[cols, :]), (hmt.at[:, cols], hmt_h.at[:, cols]),
                (xm.at[cols, :], xm_h.at[cols, :]))
        return [pltpu.make_async_copy(s, d, st.at[2 + b * len(ends) + i]) for i, (s, d) in enumerate(ends)]

    def halo_in(b):
        with jax.named_scope("f_halo_wait"):
            push_rows(b).wait()
        with jax.named_scope("f_halo"):
            for i in range(WINDOW // QB):
                r = slice(i * QB, (i + 1) * QB)
                hh[r, :] = normed(halo[b, r, :], ga[:])
            ak[:] = dot(wk[:], hh[:], NT)
            av[:] = dot(wv[:], hh[:], NT)
            cols = pl.ds(pl.multiple_of(b * WINDOW, QB), WINDOW)
            wide = pl.ds(pl.multiple_of(b * ext, QB), WINDOW)
            near = cos_h[:, cols], sin_h[:, cols]
            for src, dst_t, dst in ((ak, kt, k), (av, vt, v)):
                for p in range(n_pairs):
                    r = slice(p * pw, (p + 1) * pw)
                    blk = (rope(src[r, :], *near, 1, head_dim) if dst is k else src[r, :]).astype(BF)
                    dst_t[r, wide] = blk
                    dst[wide, r] = blk.T
        for c in keeps(b)[:3]:
            c.start()

    upper = upper_mask()
    first = me == 0

    def spots(it, blk):
        b, p = it // n_pairs, mod(it, n_pairs)
        pr = pl.ds(aligned(p * pw, pw), pw)
        return pr, pl.ds(aligned(b * toks + blk * QB, QB), QB), pl.ds(aligned(b * ext + blk * QB, QB), 3 * QB)

    def score(it):
        for blk in range(tb):
            pr, cols, keys = spots(it, blk)
            sc[blk][:] = dot(k[keys, pr], stack_pair(q[pr, cols]))

    def soften(it, blk):
        s02, s1 = merged(sc[blk][:], upper, *start_bias(first, blk))
        top = jnp.max(jnp.maximum(s02, s1), axis=0, keepdims=True)
        e02, e1 = jnp.exp(s02 - top), jnp.exp(s1 - top)
        mass = col_sum(e02 + e1)
        inv = 1.0 / mass
        lse[it, blk:blk + 1, :] = top + jnp.log(mass)
        pb[blk][:] = banded(e02 * inv, e1 * inv, upper)

    def mix(it):
        for blk in range(tb):
            pr, cols, keys = spots(it, blk)
            ot[pr, cols] = unstack_pair(dot(vt[pr, keys], pb[blk][:])).astype(BF)

    def project(b):
        cols = pl.ds(pl.multiple_of(b * toks, QB), toks)
        with jax.named_scope("f_proj"):
            mid = (xv[b].astype(F32) + dot(ot[:, cols], wo[:], TN)).astype(BF)
            xm[cols, :] = mid
            h = normed(mid, gm[:])
            hm[cols, :] = h
            hmt[:, cols] = h.T
        for c in keeps(b)[3:]:
            c.start()

    keep_qr, keep_lse = (pltpu.make_async_copy(*ends, ld.at[i]) for i, ends in enumerate(((qr, qr_h), (lse, lse_h))))
    load_w[3].wait()
    for blk in range(tb):
        pb[blk][:] = jnp.zeros(pb[blk].shape, BF)

    def walk(i):
        it = i - 1

        @pl.when((lax.rem(i, n_pairs) == 0) & (i < n_steps))
        def _():
            halo_in(i // n_pairs)

        @pl.when(i == 0)
        def _():
            score(0)

        @pl.when((i > 0) & (i <= n_steps))
        def _():
            with jax.named_scope("f_attn"):
                mix(jnp.maximum(it - 1, 0))
                for blk in range(tb):
                    soften(it, blk)
                score(jnp.minimum(i, n_steps - 1))

        @pl.when(i == n_steps)
        def _():
            for b in range(rows):
                push_q(b).wait()
            keep_qr.start()

        @pl.when(i > n_steps)
        def _():
            mix(n_steps - 1)

        @pl.when((lax.rem(it, n_pairs) == 0) & (it > 0))
        def _():
            project(it // n_pairs - 1)

    cdiv_loop(n_steps + 2, walk)
    with jax.named_scope("f_store_wait"):
        keep_lse.start()
        keep_hat.wait()
        keep_q.wait()
        keep_qr.wait()
        keep_lse.wait()
        for b in range(rows):
            for c in keeps(b):
                c.wait()


def any_spec(k):
    return [pl.BlockSpec(memory_space=pl.ANY)] * k


def vmem_spec(k):
    return [pl.BlockSpec(memory_space=pltpu.VMEM)] * k


def run_fwd(n, x, pos, invf, ga, gm, wq, wk, wv, wo, head_dim):
    rows, toks, width = x.shape
    hd = wq.shape[0]
    ext, total, n_halo = toks + WINDOW, rows * toks, rows * WINDOW
    half = head_dim // 2
    sds = lambda *s: jax.ShapeDtypeStruct(s, BF)
    dma = lambda *s: pltpu.SemaphoreType.DMA(s)
    outs = [sds(hd, total), sds(hd, rows * ext), sds(rows * ext, hd), sds(rows * ext, hd), sds(width, total), sds(hd, total), sds(total, width), sds(total, width), sds(width, total)]
    outs += [sds(hd, n_halo), jax.ShapeDtypeStruct((rows * hd // (2 * head_dim), 8, 2 * QB), F32)] + [jax.ShapeDtypeStruct((half, total), F32)] * 2
    vm = lambda *s: pltpu.VMEM(s, BF)
    vf = lambda *s: pltpu.VMEM(s, F32)
    scratch = [vm(rows, toks, width), vm(rows, WINDOW, width), vm(hd, n_halo), vf(rows * hd // (2 * head_dim), 8, 2 * QB), pltpu.VMEM((rows, toks), jnp.int32), vm(hd, width), vm(hd, width), vm(hd, width), vm(hd, width),
               vm(hd, total), vm(hd, rows * ext), vm(rows * ext, hd), vm(rows * ext, hd), vm(hd, rows * ext), vm(width, total), vm(hd, total), vm(total, width), vm(total, width), vm(width, total), vm(total, width), vm(WINDOW, width),
               vf(hd, total), vf(hd, total), vf(hd, WINDOW), vf(hd, WINDOW), vf(half, n_halo), vf(half, n_halo),
               *[vf(3 * QB, 2 * QB)] * 3, *[vm(3 * QB, 2 * QB)] * 3,
               dma(rows), dma(4), dma(2 + 7 * rows), dma(rows + 1), dma(rows + 1), dma(rows), dma(rows)]
    return pl.pallas_call(
        functools.partial(fwd_kernel, n, head_dim), out_shape=outs,
        in_specs=any_spec(1) + vmem_spec(4) + any_spec(4), out_specs=any_spec(11) + vmem_spec(2), scratch_shapes=scratch,
        compiler_params=pltpu.CompilerParams(collective_id=0, has_side_effects=True, vmem_limit_bytes=VMEM_LIMIT),
        name="forward")(x, pos, invf, ga, gm, wq, wk, wv, wo)


LAG = 2
SLOTS = 2 * LAG
RING = 8
CB = 256


def at(ref, *idx):
    return ref.at[idx]


class Torus:
    def __init__(self, n, head, last, turn, parts, recv0, recv1, recv2, recv3, recv4, recv5, acc, acc2, fin, snd, rcv):
        assert math.isqrt(n // 2) == 4
        me = lax.axis_index("seq")
        self.core = lax.rem(me, 2)
        chip = me // 2
        self.x, self.y = lax.rem(chip, 4), chip // 4
        self.head, self.last, self.turn = head, last, turn
        self.parts, self.recv0, self.recv1, self.recv2, self.recv3, self.recv4, self.recv5 = parts, recv0, recv1, recv2, recv3, recv4, recv5
        self.acc, self.acc2, self.fin, self.snd, self.rcv = acc, acc2, fin, snd, rcv
        self.partner = me + 1 - 2 * self.core
        self.rows, self.columns = [lax.rem(self.y + d, 4) * 4 for d in range(4)], [lax.rem(self.x + d, 4) for d in range(4)]
        self.hops = [[self.device(0, d) for d in range(4)], [self.device(d, 0) for d in range(4)]]

    def device(self, dy, dx):
        return (self.rows[dy] + self.columns[dx]) * 2 + self.core

    def copy(self, lane, kind, slot, src, dst, target):
        return pltpu.make_async_remote_copy(
            src_ref=src, dst_ref=dst, send_sem=self.snd.at[lane, kind, slot], recv_sem=self.rcv.at[lane, kind, slot],
            device_id={"seq": target}, device_id_type=MESH)

    def late(self, pair, yes, no):
        first, end = self.turn
        return jnp.where((pair >= first) & (pair < end), yes, no)

    def swap(self, ring, slot):
        return self.copy(0, 0, slot, self.parts.at[ring, :, :, 1 - self.core], self.recv0.at[slot], self.partner)

    def copies(self, stage, kind, pair, held, slot):
        axis = kind if stage < 3 else 1 - kind
        plus, minus = self.hops[axis][1], self.hops[axis][-1]
        half = CB // 2
        if stage == 1:
            if axis == 0:
                minus = self.late(pair, plus, minus)
            ends = [(self.acc.at[kind, held, 2, :2], self.recv1), (self.acc.at[kind, held, 2, 2:], self.recv1)]
        elif stage == 2:
            ends = [(self.acc.at[kind, held, 1], self.recv2), (self.acc.at[kind, held, 3], self.recv2)]
        elif stage == 3:
            ends = [(self.acc2.at[kind, held, 2, :, :half], self.recv3), (self.acc2.at[kind, held, 2, :, half:], self.recv3)]
        else:
            ends = [(self.acc2.at[kind, held, 1], self.recv4), (self.acc2.at[kind, held, 3], self.recv4)]
        lane = 2 * stage - 1
        return [self.copy(lane + i, kind, slot, src, buf.at[kind, slot, i], (plus, minus)[i]) for i, (src, buf) in enumerate(ends)]

    def add(self, stage, kind, pair, held, slot, ring):
        acc, acc2 = self.acc, self.acc2
        if stage == 1:
            for r1 in range(4):
                for r2 in range(4):
                    ry, rx = (r2, r1) if kind == 0 else (r1, r2)
                    chip = self.rows[ry] + self.columns[rx]
                    acc[kind, held, r1, r2] = self.parts[ring, kind, chip, self.core] + self.recv0[slot, kind, chip]
        elif stage == 2:
            back = self.late(pair, 1, 3) if kind == 0 else 3
            acc[kind, held, 1, :2] += self.recv1[kind, slot, 0]
            acc[kind, held, back, 2:] += self.recv1[kind, slot, 1]
        elif stage == 3:
            acc2[kind, held] = acc[kind, held, 0] + (self.recv2[kind, slot, 0] + self.recv2[kind, slot, 1])
        elif stage == 4:
            half = CB // 2
            acc2[kind, held, 1, :, :half] += self.recv3[kind, slot, 0]
            acc2[kind, held, 3, :, half:] += self.recv3[kind, slot, 1]
        else:
            self.fin[pair, kind] = acc2[kind, held, 0] + (self.recv4[kind, slot, 0] + self.recv4[kind, slot, 1])

    def direct(self, kind, held, slot):
        return [self.copy(8 + d, kind, slot, self.acc2.at[kind, held, d], self.recv5.at[kind, slot, d - 1], self.hops[1 - kind][d]) for d in range(1, 4)]

    def early(self, pair):
        return (pair >= 0) & (pair <= self.head)

    def final(self, pair):
        return (pair == self.last) | ((pair > self.head) & (pair < self.last) & (mod(abs(pair - self.head), 2) == 0))

    def tick(self, t, tail=False):
        now, land, before = mod(t, SLOTS), mod(t + SLOTS - LAG, SLOTS), mod(t + SLOTS - 1, SLOTS)
        ring_now, ring_land = mod(t, RING), mod(t + RING - 1, RING)
        for stage in range(5, -1, -1):
            pair = t - LAG * stage + min(stage, 1)
            held = before if stage % 2 else mod(t + 1, SLOTS)

            def move(last_hops, stage=stage, pair=pair, held=held):
                if stage == 0:
                    self.swap(ring_now, now).start()
                    return
                if stage == 1:
                    with jax.named_scope("t_wait1"):
                        self.swap(ring_land, before).wait()
                for kind in range(2):
                    if last_hops and stage == 4:
                        with jax.named_scope("t_wait6"):
                            for c in self.direct(kind, held, land):
                                c.wait()
                        got = self.recv5[kind, land]
                        self.fin[pair, kind] = self.acc2[kind, held, 0] + (got[0] + got[1] + got[2])
                        continue
                    if stage > 1:
                        with jax.named_scope(f"t_wait{stage}"):
                            for c in self.copies(stage - 1, kind, pair, held, land):
                                c.wait()
                    self.add(stage, kind, pair, held, land if stage > 1 else before, ring_land)
                    if stage < 5:
                        for c in self.direct(kind, held, now) if last_hops and stage == 3 else self.copies(stage, kind, pair, held, now):
                            c.start()

            def when(which, fn):
                if isinstance(which, bool):
                    fn() if which else None
                else:
                    pl.when(which)(fn)

            if stage < 3:
                when(self.early(pair) | self.final(pair), functools.partial(move, False))
            else:
                when(self.early(pair), functools.partial(move, False))
                if tail and stage < 5:
                    when(self.final(pair), functools.partial(move, True))


def pick(i, table):
    out = 0
    for key, value in table.items():
        out = jnp.where(i == key, value, out)
    return out


def norm_back(x, gain, grad, res):
    xf = x.astype(F32)
    inv = lax.rsqrt(jnp.mean(xf * xf, axis=-1, keepdims=True) + NORM_EPS)
    unit = xf * inv
    gu = grad * gain
    out = inv * (gu - unit * jnp.mean(gu * unit, axis=-1, keepdims=True)) + res.astype(F32)
    gu = grad * unit
    return out.astype(BF), jnp.sum(gu.reshape(-1, 8, gu.shape[-1]), axis=0)


def plan(n_mlp, n_down, nc):
    order = [("o", g) for g in range(nc)] + [(name, g) for g in range(nc) for name in "qkv"]
    base, head = n_mlp + n_down, n_mlp + n_down + nc - 1
    last = 2 * (base - 1 - head + len(order) // 2) + head - 1
    spot = lambda pair: min(max(pair, 2 * pair - head), last)
    return head, {name: (spot(base + i // 2), i % 2) for i, name in enumerate(order)}, last


def bwd_kernel(n, head_dim, dims, ga, gm, x_h, dout_h, q_h, kt_h, k_h, v_h, hat_h, ot_h, xm_h, hm_h, hmt_h, qr_h, lse_h, cos_h, sin_h,
               wq_h, wk_h, wv_h, wo_h, wg_h, wu_h, wd_h,
               dx_h, fin_h,
               parts, recv0, recv1, recv2, recv3, recv4, recv5, acc, acc2, fin, snd, rcv,
               dor, lser, deltar, hsnd, hrcv, osnd, orcv, gsend, grecv, gsem, ld,
               xbuf, mbuf, gnm, gmid, ot, hat, wo, dot_, lse, delta, cos_i, sin_i, dgain):
    rows, toks, width, hd, ff = dims
    ext, total = toks + WINDOW, rows * toks
    pw = 2 * head_dim
    n_pairs = hd // pw
    tb, n_steps = toks // QB, n_pairs * rows
    nb, nc, sub = ff // CB, width // CB, ff // width
    rpd = width // n
    per, half_sub = CB // pw, sub // 2
    head, place, end = plan(nb, nc * half_sub, nc)
    comm = Torus(n, head, end, (nb, nb + n_pairs + 1), parts, recv0, recv1, recv2, recv3, recv4, recv5, acc, acc2, fin, snd, rcv)
    me = lax.axis_index("seq")
    left = lax.rem(me + n - 1, n)
    barrier = pltpu.get_barrier_semaphore()

    def greet(i):
        pl.semaphore_signal(barrier, inc=1, device_id={"seq": lax.rem(me + i + 1, n)}, device_id_type=MESH)

    def load(i, s, d):
        c = pltpu.make_async_copy(s, d, ld.at[i])
        c.start()
        return c

    def late(i):
        s, d = ((xm_h, mbuf), (ot_h, ot), (hat_h, hat), (wo_h, wo), (lse_h, lse), (cos_h, cos_i), (sin_h, sin_i))[i]
        return pltpu.make_async_copy(s, d, ld.at[1 + i])

    def to_left(src, dst, send_sem, recv_sem):
        return pltpu.make_async_remote_copy(src_ref=src, dst_ref=dst, send_sem=send_sem, recv_sem=recv_sem,
                                            device_id={"seq": left}, device_id_type=MESH)

    n_late = 7

    def push_rows(i):
        return to_left(*((lse_h, lser), (delta, deltar))[i], hsnd.at[i], hrcv.at[i])

    def push_out(p):
        pr = pl.ds(aligned(p * pw, pw), pw)
        return [to_left(dot_.at[pr, pl.ds(b * toks, WINDOW)], dor.at[pr, pl.ds(b * WINDOW, WINDOW)], osnd.at[p, b], orcv.at[p, b])
                for b in range(rows)]

    def give_out(p):
        for c in push_out(p):
            c.start()

    def put(spot, value):
        pair, kind = spot
        parts[mod(pair, RING), kind] = value.reshape(n // 2, 2, rpd, CB)

    def spot_of(name, g):
        known = {i: place[name, i] for i in range(nc)}
        return pick(g, {i: s[0] for i, s in known.items()}), pick(g, {i: s[1] for i, s in known.items()})

    def spots(it, blk):
        p, b = it // rows, mod(it, rows)
        pr = pl.ds(aligned(p * pw, pw), pw)
        return pr, pl.ds(aligned(b * toks + blk * QB, QB), QB), pl.ds(aligned(b * ext + blk * QB, QB), 3 * QB)

    def row_of(it):
        return mod(it, rows) * n_pairs + it // rows

    def mlp(hm, hmt, actt, wgu, wd, dgu, wld):
        def weights(j, slot):
            c = aligned(j * CB, CB)
            return [pltpu.make_async_copy(wg_h.at[:, pl.ds(c, CB)], wgu.at[slot, :, :CB], wld.at[slot, 0]),
                    pltpu.make_async_copy(wu_h.at[:, pl.ds(c, CB)], wgu.at[slot, :, CB:], wld.at[slot, 1]),
                    pltpu.make_async_copy(wd_h.at[pl.ds(c, CB), :], wd.at[slot], wld.at[slot, 2])]

        for c in weights(0, 0):
            c.start()
        ld_hm, ld_x, ld_hmt = load(8, hm_h, hm), load(0, dout_h, xbuf), load(9, hmt_h, hmt)
        cdiv_loop(n - 1, greet)
        gnm[:] = jnp.zeros_like(gnm)
        gsend[:] = jnp.zeros_like(gsend)
        dgain[:] = jnp.zeros_like(dgain)
        ld_hm.wait()
        ld_x.wait()
        ld_hmt.wait()
        for i in range(n_late):
            late(i).start()

        def block(j):
            slot = lax.rem(j, 2)
            for c in weights(j, slot):
                c.wait()

            @pl.when(j + 1 < nb)
            def _():
                for c in weights(j + 1, 1 - slot):
                    c.start()

            c0 = pl.multiple_of(j * CB, CB)
            with jax.named_scope("b_mlp"):
                for b in range(rows):
                    r = slice(b * toks, (b + 1) * toks)
                    gu = dot(hm[r, :], wgu[slot])
                    gact = dot(xbuf[r, :], wd[slot], NT).astype(BF).astype(F32)
                    gate, up = gu[:, :CB], gu[:, CB:]
                    sig = 1.0 / (1.0 + jnp.exp(-gate))
                    swish = gate * sig
                    actt[pl.ds(c0, CB), r] = (swish * up).astype(BF).T
                    dgu[r, :CB] = (gact * up * (sig + swish * (1.0 - sig))).astype(BF)
                    dgu[r, CB:] = (gact * swish).astype(BF)
                both = dot(hmt[:], dgu[:])
                ring = lax.rem(j, RING)
                parts[ring, 0] = both[:, :CB].reshape(n // 2, 2, rpd, CB)
                parts[ring, 1] = both[:, CB:].reshape(n // 2, 2, rpd, CB)
                for b in range(rows):
                    r = slice(b * toks, (b + 1) * toks)
                    gnm[r, :] += dot(dgu[r, :], wgu[slot], NT)

            @pl.when(j == 0)
            def _():
                pl.semaphore_wait(barrier, n - 1)
                push_rows(0).start()

            comm.tick(j)

        cdiv_loop(nb, block)

        def down(c):
            share = n // 2 // sub
            c0 = pl.multiple_of(c * CB, CB)
            for m in range(sub):
                res = dot(actt[m * width:(m + 1) * width, :], xbuf[:, pl.ds(c0, CB)]).reshape(share, 2, sub, rpd, CB)
                for i in range(sub):
                    pair = nb + c * half_sub + i // 2
                    parts[lax.rem(pair, RING), i % 2, m * share:(m + 1) * share] = res[:, :, i]

        for i in range(n_late):
            late(i).wait()

        def mid(b):
            for i in range(tb):
                r = pl.ds(pl.multiple_of((b * tb + i) * QB, QB), QB)
                out, dg = norm_back(mbuf[r, :], gm[:], gnm[r, :], xbuf[r, :])
                gmid[r, :] = out
                dgain[8:, :] += dg

        def deltas(p):
            for it in range(rows):
                for blk in range(tb):
                    pr, cols, _ = spots(p * rows + it, blk)
                    both = dot_[pr, cols].astype(F32) * ot[pr, cols].astype(F32)
                    delta[row_of(p * rows + it), blk:blk + 1, :] = jnp.concatenate(
                        [col_sum(both[:head_dim]), col_sum(both[head_dim:])], axis=1)

        def column(c):
            with jax.named_scope("b_down"):
                down(c)
            comm.tick(nb + c + jnp.minimum(c, 1))

            @pl.when(c == 1)
            def _():
                give_out(c)

            @pl.when(c == 0)
            def _():
                with jax.named_scope("b_mid"):
                    cdiv_loop(rows, mid)
                with jax.named_scope("b_dot"):
                    dot_[:] = dot(wo[:], gmid[:], NT).astype(BF)
                    cdiv_loop(n_pairs, deltas)
                comm.tick(nb + 1)
                push_rows(1).start()
                give_out(0)

        cdiv_loop(nc, column)

    vm = lambda *s: pltpu.VMEM(s, BF)
    vf = lambda *s: pltpu.VMEM(s, F32)
    pl.run_scoped(mlp, vm(total, width), vm(width, total), vm(ff, total), vm(2, width, 2 * CB), vm(2, CB, width), vm(total, 2 * CB),
                  pltpu.SemaphoreType.DMA((2, 3)))
    def attention(q, kt, k, v, qr, dv, sc0, sc1, sc2, sr, dp0, dp1, dp2, dr, pb0, pb1, pb2, pr_, ds0, ds1, ds2, dsr):
        dqt, dkt = ot, q
        wq, wk, wv = k.at[:hd], kt.at[:, :width], v.at[:hd]
        sc, dp, pb, ds = (sc0, sc1, sc2), (dp0, dp1, dp2), (pb0, pb1, pb2), (ds0, ds1, ds2)
        lds = [load(8 + i, s, d) for i, (s, d) in enumerate(((q_h, q), (k_h, k), (v_h, v), (qr_h, qr), (kt_h, kt)))]

        def out_grad(g):
            put(spot_of("o", g), dot(ot[:], gmid[:, pl.ds(pl.multiple_of(g * CB, CB), CB)]))

        with jax.named_scope("b_dwo"):
            cdiv_loop(nc, out_grad)
        first_tick = nb + nc + 1
        comm.tick(first_tick)
        give_out(2)
        upper = upper_mask()
        first, last = me == 0, me == n - 1
        halves = slice(0, WINDOW), slice(WINDOW, 3 * QB)

        def right(it, i):
            p, b = it // rows, mod(it, rows)
            return pl.ds(aligned(p * pw, pw), pw), pl.ds(aligned(b * WINDOW + i * QB, QB), QB), pl.ds(aligned(b * ext + toks + i * QB, QB), WINDOW - i * QB)

        def score(it):
            for blk in range(tb):
                pr, cols, keys = spots(it, blk)
                sc[blk][:] = dot(k[keys, pr], stack_pair(q[pr, cols]))
                dp[blk][:] = dot(v[keys, pr], stack_pair(dot_[pr, cols]))
            for i, rs in enumerate(halves):
                pr, cols, keys = right(it, i)
                sr[rs, :] = dot(k[keys, pr], stack_pair(qr[pr, cols]))
                dr[rs, :] = dot(v[keys, pr], stack_pair(dor[pr, cols]))

        def soften(it):
            row = row_of(it)
            for blk in range(tb):
                s02, s1 = merged(sc[blk][:], upper, *start_bias(first, blk))
                norm, mean = lse[row, blk:blk + 1, :], delta[row, blk:blk + 1, :]
                p02, p1 = jnp.exp(s02 - norm), jnp.exp(s1 - norm)
                g02, g1 = jnp.where(upper, dp[blk][:QB], dp[blk][2 * QB:]), dp[blk][QB:2 * QB]
                pb[blk][:] = banded(p02, p1, upper)
                ds[blk][:] = banded(p02 * (g02 - mean), p1 * (g1 - mean), upper)
            for blk in range(tb):
                i = blk // 2
                rs = slice(blk * QB, (blk + 1) * QB)
                p = jnp.exp(sr[rs, :] - jnp.where(last, -NEG, lser[row, i:i + 1, :]))
                g = p * (dr[rs, :] - deltar[row, i:i + 1, :])
                pr_[rs, :] = (p if blk == 1 else jnp.where(upper, p, 0.0)).astype(BF)
                dsr[rs, :] = (g if blk == 1 else jnp.where(upper, g, 0.0)).astype(BF)

        def grads(it):
            ks, vs = [], []
            for blk in range(tb):
                pr, cols, keys = spots(it, blk)
                own = slice(max(0, 2 - blk) * QB, 3 * QB)
                vs.append(dot(pb[blk][own, :], stack_pair(dot_[pr, cols]), NT))
                ks.append(dot(ds[blk][own, :], stack_pair(q[pr, cols]), NT))
                dq = unstack_pair(dot(kt[pr, keys], ds[blk][:])) * (head_dim ** -0.5)
                dqt[pr, cols] = rope(dq, cos_i[:, cols], sin_i[:, cols], -1, head_dim).astype(BF)
            for i, rs in enumerate(halves):
                pr, cols, _ = right(it, i)
                vs.append(dot(pr_[rs, :], stack_pair(dor[pr, cols]), NT))
                ks.append(dot(dsr[rs, :], stack_pair(qr[pr, cols]), NT))
            for j in range(tb):
                pr, cols, _ = spots(it, j)
                gv, gk = (sum(x[i][(j - max(0, i - 2)) * QB:(j - max(0, i - 2) + 1) * QB] for i in range(j, j + 3)) for x in (vs, ks))
                dv[cols, pr] = gv.astype(BF)
                dkt[pr, cols] = rope(gk.T, cos_i[:, cols], sin_i[:, cols], -1, head_dim).astype(BF)

        def close_group(g):
            cols = pl.ds(pl.multiple_of(g * CB, CB), CB)
            with jax.named_scope("b_dwqkv"):
                put(spot_of("q", g), dot(hat[:], dqt[cols, :], NT))
                put(spot_of("k", g), dot(hat[:], dkt[cols, :], NT))
                put(spot_of("v", g), dot(hat[:], dv[:, cols]))

        def weights():
            return [pltpu.make_async_copy(s, d, ld.at[8 + i]) for i, (s, d) in enumerate(((wq_h, wq), (wk_h, wk), (wv_h, wv), (x_h, xbuf)))]

        def arrived(p):
            with jax.named_scope("b_hwait"):
                for c in push_out(p):
                    c.wait()

        def walk(it):
            ahead = it + 1

            @pl.when((lax.rem(ahead, rows) == 0) & (ahead < n_steps))
            def _():
                arrived(ahead // rows)

            @pl.when(it < n_steps)
            def _():
                with jax.named_scope("b_attn"):
                    grads(it - 1)
                    soften(it)
                    score(jnp.minimum(ahead, n_steps - 1))

            @pl.when(it == n_steps)
            def _():
                grads(n_steps - 1)
                for c in weights():
                    c.start()

            p, step = it // rows - 1, lax.rem(it, rows)

            @pl.when((step == 0) & (lax.rem(p, per) == per - 1))
            def _():
                close_group(p // per)

            now = first_tick + 1 + p + step // (rows - 1)
            twice = now - head

            @pl.when((step == 0) | ((step == rows - 1) & (twice > 0)))
            def _():
                comm.tick(now + jnp.maximum(twice - step // (rows - 1), 0))

            @pl.when((step == 0) & (p + 3 < n_pairs))
            def _():
                give_out(p + 3)

        for c in lds[:-1]:
            c.wait()
        for i in range(2):
            push_rows(i).wait()
        arrived(0)
        score(0)
        soften(0)
        score(1)
        lds[-1].wait()
        cdiv_loop(n_steps, lambda i: walk(i + 1))
        comm.tick(end)
        for c in weights():
            c.wait()

        def into(b):
            r = pl.ds(pl.multiple_of(b * toks, QB), toks)
            with jax.named_scope("b_into"):
                gnm[r, :] = dot(dqt[:, r], wq[:], TN) + dot(dkt[:, r], wk[:], TN) + dot(dv[r, :], wv[:])

            with jax.named_scope("b_final"):
                for i in range(tb):
                    r = pl.ds(pl.multiple_of((b * tb + i) * QB, QB), QB)
                    out, dg = norm_back(xbuf[r, :], ga[:], gnm[r, :], gmid[r, :])
                    mbuf[r, :] = out
                    dgain[:8, :] += dg
            comm.tick(end + 1 + b, True)

        cdiv_loop(rows, into)

    score_bufs = [vf(3 * QB, 2 * QB)] * 8 + [vm(3 * QB, 2 * QB)] * 8
    pl.run_scoped(attention, vm(hd, total), vm(hd, rows * ext), vm(rows * ext, hd), vm(rows * ext, hd), vm(hd, rows * WINDOW), vm(total, hd), *score_bufs)
    out_copy = load(1, mbuf, dx_h)
    gains = jnp.concatenate([col_sum(dgain[:8, :]), col_sum(dgain[8:, :]), jnp.zeros((6, width), F32)], axis=0)
    for p in range(n):
        gsend[p, :, :rpd] = gains[:, p * rpd:(p + 1) * rpd]

    def spread(i):
        to = lax.rem(me + i + 1, n)
        pltpu.make_async_remote_copy(src_ref=gsend.at[to], dst_ref=grecv.at[i], send_sem=gsem.at[0], recv_sem=gsem.at[1],
                                     device_id={"seq": to}, device_id_type=MESH).start()

    cdiv_loop(n - 1, spread)
    stop = end + 4 * LAG
    run = lambda lo, hi: lax.fori_loop(lo, hi, lambda t, c: comm.tick(t, True) or c, 0)
    run(end + 1 + rows, stop - LAG)
    most, rest = pl.ds(0, end - 1), pl.ds(end - 1, LAG + 1)
    keep_most = load(0, fin.at[most], fin_h.at[most])
    to_left(gsend.at[pl.ds(0, n - 1)], grecv, gsem.at[0], gsem.at[1]).wait()
    sums = gsend[me]
    for i in range(n - 1):
        sums = sums + grecv[i]
    fin[end + 1, 0, :8, :128] = sums
    out_copy.wait()
    run(stop - LAG, stop)
    with jax.named_scope("b_end"):
        keep_rest = load(1, fin.at[rest], fin_h.at[rest])
        keep_most.wait()
        keep_rest.wait()


def spread_kernel(dims, dx_i, fin_i, dx_o, dga_o, dgm_o, *refs):
    head_dim, n, width, ff = dims
    outs, (buf, fin), stage, sem = refs[:7], refs[7:9], refs[9:16], refs[16]
    dq, dk, dv, do, dg, du, dd = stage
    nb, nc, sub = ff // CB, width // CB, ff // width
    rpd = width // n
    head, place, end = plan(nb, nc * sub // 2, nc)
    get, get_fin, out = (pltpu.make_async_copy(*ends, sem.at[len(outs) + i]) for i, ends in enumerate(((dx_i, buf), (fin_i, fin), (buf, dx_o))))
    get_fin.start()
    get.start()
    get_fin.wait()
    gains = fin[end + 1, 0]
    dga_o[:] = gains[:1, :rpd]
    dgm_o[:] = gains[1:2, :rpd]
    for j in range(nb):
        dg[:, j * CB:(j + 1) * CB] = fin[j, 0]
        du[:, j * CB:(j + 1) * CB] = fin[j, 1]
    for c in range(nc):
        for i in range(sub):
            pair = nb + (c * sub + i) // 2
            dd[i * rpd:(i + 1) * rpd, c * CB:(c + 1) * CB] = fin[pair, i % 2]
    for g in range(nc):
        do[:, g * CB:(g + 1) * CB] = fin[place["o", g]]
        for name, ref in (("q", dq), ("k", dk), ("v", dv)):
            val = fin[place[name, g]]
            for h in range(CB // head_dim):
                ref[g * (CB // head_dim) + h] = val[:, h * head_dim:(h + 1) * head_dim]
    keeps = [pltpu.make_async_copy(s, d, sem.at[i]) for i, (s, d) in enumerate(zip(stage, outs))]
    for c in keeps:
        c.start()
    get.wait()
    out.start()
    for c in keeps:
        c.wait()
    out.wait()


def run_bwd(n, head_dim, ga, gm, x, dout, q, kt, k, v, hat, ot, xm, hm, hmt, qr, lse, cos_t, sin_t, wq, wk, wv, wo, wg, wu, wd, rows):
    total, width = x.shape
    hd, ff = wq.shape[0], wg.shape[1]
    toks = total // rows
    rpd, heads = width // n, hd // head_dim
    nb, nc, sub = ff // CB, width // CB, ff // width
    slots = plan(nb, nc * sub // 2, nc)[2] + 2
    n_pairs = hd // (2 * head_dim)
    f = lambda *s: jax.ShapeDtypeStruct(s, F32)
    dx_t = jax.ShapeDtypeStruct((total, width), BF)
    vm = lambda *s: pltpu.VMEM(s, BF)
    vf = lambda *s: pltpu.VMEM(s, F32)
    dma = lambda *s: pltpu.SemaphoreType.DMA(s)
    line, duo = vf(rows * n_pairs, 8, 2 * QB), (2, SLOTS)
    scratch = [vf(RING, 2, n // 2, 2, rpd, CB), vf(SLOTS, 2, n // 2, rpd, CB), vf(*duo, 2, 2, rpd, CB), vf(*duo, 2, 4, rpd, CB),
               vf(*duo, 2, rpd, CB // 2), vf(*duo, 2, rpd, CB), vf(*duo, 3, rpd, CB), vf(*duo, 4, 4, rpd, CB), vf(*duo, 4, rpd, CB), vf(slots, 2, rpd, CB),
               dma(12, *duo), dma(12, *duo),
               vm(hd, rows * WINDOW), line, line, dma(2), dma(2), dma(n_pairs, rows), dma(n_pairs, rows),
               vf(n, 8, 128), vf(n - 1, 8, 128), dma(2), dma(13),
               vm(total, width), vm(total, width), vf(total, width), vm(total, width), vm(hd, total), vm(width, total), vm(hd, width), vm(hd, total), line, line, vf(*cos_t.shape), vf(*cos_t.shape), vf(16, width)]
    mid = pl.pallas_call(
        functools.partial(bwd_kernel, n, head_dim, (rows, toks, width, hd, ff)), out_shape=[dx_t, f(slots, 2, rpd, CB)],
        in_specs=vmem_spec(2) + any_spec(22), out_specs=any_spec(2), scratch_shapes=scratch,
        compiler_params=pltpu.CompilerParams(collective_id=1, has_side_effects=True, vmem_limit_bytes=VMEM_LIMIT),
        name="backward")(ga, gm, x, dout, q, kt, k, v, hat, ot, xm, hm, hmt, qr, lse, cos_t, sin_t, wq, wk, wv, wo, wg, wu, wd)
    outs = [f(heads, rpd, head_dim)] * 3 + [f(rpd, width), f(rpd, ff), f(rpd, ff), f(ff // n, width)]
    return pl.pallas_call(
        functools.partial(spread_kernel, (head_dim, n, width, ff)), out_shape=[dx_t, f(1, rpd), f(1, rpd)] + outs,
        in_specs=any_spec(2), out_specs=any_spec(1) + vmem_spec(2) + any_spec(7),
        scratch_shapes=[vm(total, width), vf(slots, 2, rpd, CB), *[vf(*o.shape) for o in outs], dma(10)],
        name="spread")(*mid)


def solution(mesh):
    n = mesh.shape["seq"]

    def device_step(hidden, positions, g_attn, g_mlp, w_query, w_key, w_value, w_out, w_gate, w_up, w_down, d_out):
        rows, toks, width = hidden.shape
        layers, _, heads, head_dim = w_query.shape
        hd = heads * head_dim
        half = head_dim // 2
        inv_freq = 1.0 / (10000.0 ** (jnp.arange(half, dtype=F32) * (2.0 / head_dim)))
        turn = lambda w: w[0].transpose(1, 2, 0).reshape(hd, width)
        wq, wk, wv = turn(w_query), turn(w_key), turn(w_value)
        fwd = run_fwd(n, hidden, positions, inv_freq[:, None], g_attn, g_mlp, wq, wk, wv, w_out[0], head_dim)
        out = run_bwd(n, head_dim, g_attn, g_mlp, hidden.reshape(rows * toks, width), d_out.reshape(rows * toks, width), *fwd,
                      wq, wk, wv, w_out[0], w_gate[0], w_up[0], w_down[0], rows)
        dx, dga, dgm, dq, dk, dv, do, dg, du, dd = out
        back = lambda w: w.transpose(1, 0, 2)[None]
        return (dx.reshape(rows, toks, width), dga, dgm, back(dq), back(dk), back(dv), do[None], dg[None], du[None], dd[None])

    tok_spec, grad_spec = P("data", "seq"), P(None, ("data", "seq"))
    in_specs = (tok_spec, tok_spec) + (P(),) * 9 + (tok_spec,)
    out_specs = (tok_spec,) + (grad_spec,) * 9
    return jax.shard_map(device_step, mesh=mesh, in_specs=in_specs, out_specs=out_specs, check_vma=False)
```

```python
import functools, math
import numpy as np
import jax, jax.numpy as jnp
from jax import lax
from jax.experimental import pallas as pl
from jax.experimental.pallas import tpu as pltpu
from jax.sharding import PartitionSpec as P

WINDOW = 256
NORM_EPS = 1e-5
QB = 128
BF, F32 = jnp.bfloat16, jnp.float32
NN, NT, TN = ((1,), (0,)), ((1,), (1,)), ((0,), (0,))
MESH = pl.DeviceIdType.MESH
NEG = -1e30
VMEM_LIMIT = 67043328


def dot(a, b, dims=NN):
    return lax.dot_general(a, b, (dims, ((), ())), preferred_element_type=F32)


def cdiv_loop(n, body):
    lax.fori_loop(0, n, lambda i, c: body(i) or c, 0)


def mod(a, b):
    return a % b if isinstance(a, int) else lax.rem(a, b)


def aligned(a, b):
    return a if isinstance(a, int) else pl.multiple_of(a, b)


def rope(blk, cos_b, sin_b, sign, head_dim):
    half = head_dim // 2
    parts = []
    for h in range(blk.shape[0] // head_dim):
        first = blk[h * head_dim:h * head_dim + half]
        second = blk[h * head_dim + half:(h + 1) * head_dim]
        if sign > 0:
            parts += [first * cos_b - second * sin_b, second * cos_b + first * sin_b]
        else:
            parts += [first * cos_b + second * sin_b, second * cos_b - first * sin_b]
    return jnp.concatenate(parts, axis=0)


def normed(x, gain):
    xf = x.astype(F32)
    inv = lax.rsqrt(jnp.mean(xf * xf, axis=-1, keepdims=True) + NORM_EPS)
    return (xf * inv * gain).astype(BF)


def stack_pair(pair_t):
    half = pair_t.shape[0] // 2
    zero = jnp.zeros((half, pair_t.shape[1]), pair_t.dtype)
    return jnp.concatenate(
        [jnp.concatenate([pair_t[:half], zero], axis=0), jnp.concatenate([zero, pair_t[half:]], axis=0)], axis=1)


def unstack_pair(both):
    half, cols = both.shape[0] // 2, both.shape[1] // 2
    return jnp.concatenate([both[:half, :cols], both[half:, cols:]], axis=0)


def col_sum(x):
    return jnp.sum(x, axis=0, keepdims=True)


def merged(scores, upper, bias0, bias1):
    return jnp.where(upper, scores[:QB] + bias0, scores[2 * QB:]), scores[QB:2 * QB] + bias1


def banded(p02, p1, upper):
    return jnp.concatenate(
        [jnp.where(upper, p02, 0.0).astype(BF), p1.astype(BF), jnp.where(upper, 0.0, p02).astype(BF)], axis=0)


def upper_mask():
    key_ids = lax.broadcasted_iota(jnp.int32, (QB, 2 * QB), 0)
    query_ids = lax.broadcasted_iota(jnp.int32, (QB, 2 * QB), 1) % QB
    return key_ids > query_ids


def start_bias(first, blk):
    bias = jnp.where(first, NEG, 0.0).astype(F32)
    return (bias if blk < 2 else 0.0), (bias if blk < 1 else 0.0)


def fwd_kernel(n, head_dim, x_h, pos, invf, ga, gm, wq_h, wk_h, wv_h, wo_h,
               q_h, kt_h, k_h, v_h, hat_h, ot_h, xm_h, hm_h, hmt_h, qr_h, lse_h, cos_t, sin_t,
               xv, halo, qr, lse, pos_halo, wq, wk, wv, wo, q, kt, k, v, vt, hat, ot, xm, hm, hmt, hb, hh, acc, acc2, ak, av, cos_h, sin_h,
               sc0, sc1, sc2, pb0, pb1, pb2, ldx, ld, st, snd, rcv, qsnd, qrcv):
    sc, pb = (sc0, sc1, sc2), (pb0, pb1, pb2)
    rows, toks, width = xv.shape
    ext, total, pw = toks + WINDOW, rows * toks, 2 * head_dim
    n_pairs = wq.shape[0] // pw
    tb, n_steps = toks // QB, n_pairs * rows
    me = lax.axis_index("seq")
    right, left = lax.rem(me + 1, n), lax.rem(me + n - 1, n)
    load_x = [pltpu.make_async_copy(x_h.at[b], xv.at[b], ldx.at[b]) for b in range(rows)]
    load_w = [pltpu.make_async_copy(s, d, ld.at[i]) for i, (s, d) in enumerate(((wq_h, wq), (wk_h, wk), (wv_h, wv), (wo_h, wo)))]
    for c in load_x:
        c.start()
    barrier = pltpu.get_barrier_semaphore()
    for other in (left, right):
        pl.semaphore_signal(barrier, inc=1, device_id={"seq": other}, device_id_type=MESH)

    def push(i, s, d):
        return pltpu.make_async_remote_copy(src_ref=s, dst_ref=d, send_sem=snd.at[i], recv_sem=rcv.at[i], device_id={"seq": right}, device_id_type=MESH)

    def push_rows(b):
        return push(b, x_h.at[b, toks - WINDOW:, :], halo.at[b])

    send_pos = push(rows, pos, pos_halo)

    def angles(cos_ref, sin_ref, positions):
        count = positions.shape[1]
        for b in range(rows):
            ang = invf[:] * positions[b:b + 1, :].astype(F32)
            cos_ref[:, b * count:(b + 1) * count] = jnp.cos(ang)
            sin_ref[:, b * count:(b + 1) * count] = jnp.sin(ang)

    angles(cos_t, sin_t, pos[:])

    def norm_rows(b):
        for i in range(tb):
            h = normed(xv[b, i * QB:(i + 1) * QB, :], ga[:])
            hb[pl.ds(pl.multiple_of((b * tb + i) * QB, QB), QB), :] = h

    with jax.named_scope("f_norm"):
        for c in load_x:
            c.wait()
        for c in load_w:
            c.start()
        cdiv_loop(rows, norm_rows)
    pl.semaphore_wait(barrier, 2)
    send_pos.start()
    for b in range(rows):
        push_rows(b).start()
    keep_hat = pltpu.make_async_copy(hat, hat_h, st.at[0])
    tables = cos_t[:], sin_t[:]

    def put_q(src):
        for p in range(n_pairs):
            r = slice(p * pw, (p + 1) * pw)
            q[r, :] = (rope(src[r, :], *tables, 1, head_dim) * (head_dim ** -0.5)).astype(BF)

    def put_own(src, dst_t, dst):
        for p in range(n_pairs):
            r = slice(p * pw, (p + 1) * pw)
            both = (rope(src[r, :], *tables, 1, head_dim) if dst is k else src[r, :]).astype(BF)
            for b in range(rows):
                blk = both[:, b * toks:(b + 1) * toks]
                own = slice(b * ext + WINDOW, (b + 1) * ext)
                dst_t[r, own] = blk
                dst[own, r] = blk.T

    with jax.named_scope("f_mm"):
        load_w[0].wait()
        load_w[1].wait()
        load_w[2].wait()
        acc[:] = dot(wq[:], hb[:], NT)
        acc2[:] = dot(wk[:], hb[:], NT)
        put_q(acc)
        acc[:] = dot(wv[:], hb[:], NT)
        put_own(acc2, kt, k)
        for i in range(total // QB):
            r = slice(i * QB, (i + 1) * QB)
            hat[:, r] = hb[r, :].T
        put_own(acc, vt, v)
    keep_hat.start()
    keep_q = pltpu.make_async_copy(q, q_h, st.at[1])
    keep_q.start()

    def push_q(b):
        return pltpu.make_async_remote_copy(src_ref=q.at[:, b * toks:b * toks + WINDOW], dst_ref=qr.at[:, b * WINDOW:(b + 1) * WINDOW],
                                            send_sem=qsnd.at[b], recv_sem=qrcv.at[b], device_id={"seq": left}, device_id_type=MESH)

    for b in range(rows):
        push_q(b).start()
    send_pos.wait()
    angles(cos_h, sin_h, pos_halo[:, toks - WINDOW:])

    def keeps(b):
        wide, cols = pl.ds(pl.multiple_of(b * ext, QB), ext), pl.ds(pl.multiple_of(b * toks, QB), toks)
        ends = ((kt.at[:, wide], kt_h.at[:, wide]), (k.at[wide, :], k_h.at[wide, :]), (v.at[wide, :], v_h.at[wide, :]),
                (ot.at[:, cols], ot_h.at[:, cols]), (hm.at[cols, :], hm_h.at[cols, :]), (hmt.at[:, cols], hmt_h.at[:, cols]),
                (xm.at[cols, :], xm_h.at[cols, :]))
        return [pltpu.make_async_copy(s, d, st.at[2 + b * len(ends) + i]) for i, (s, d) in enumerate(ends)]

    def halo_in(b):
        with jax.named_scope("f_halo_wait"):
            push_rows(b).wait()
        with jax.named_scope("f_halo"):
            for i in range(WINDOW // QB):
                r = slice(i * QB, (i + 1) * QB)
                hh[r, :] = normed(halo[b, r, :], ga[:])
            ak[:] = dot(wk[:], hh[:], NT)
            av[:] = dot(wv[:], hh[:], NT)
            cols = pl.ds(pl.multiple_of(b * WINDOW, QB), WINDOW)
            wide = pl.ds(pl.multiple_of(b * ext, QB), WINDOW)
            near = cos_h[:, cols], sin_h[:, cols]
            for src, dst_t, dst in ((ak, kt, k), (av, vt, v)):
                for p in range(n_pairs):
                    r = slice(p * pw, (p + 1) * pw)
                    blk = (rope(src[r, :], *near, 1, head_dim) if dst is k else src[r, :]).astype(BF)
                    dst_t[r, wide] = blk
                    dst[wide, r] = blk.T
        for c in keeps(b)[:3]:
            c.start()

    upper = upper_mask()
    first = me == 0

    def spots(it, blk):
        b, p = it // n_pairs, mod(it, n_pairs)
        pr = pl.ds(aligned(p * pw, pw), pw)
        return pr, pl.ds(aligned(b * toks + blk * QB, QB), QB), pl.ds(aligned(b * ext + blk * QB, QB), 3 * QB)

    def score(it):
        for blk in range(tb):
            pr, cols, keys = spots(it, blk)
            sc[blk][:] = dot(k[keys, pr], stack_pair(q[pr, cols]))

    def soften(it, blk):
        s02, s1 = merged(sc[blk][:], upper, *start_bias(first, blk))
        top = jnp.max(jnp.maximum(s02, s1), axis=0, keepdims=True)
        e02, e1 = jnp.exp(s02 - top), jnp.exp(s1 - top)
        mass = col_sum(e02 + e1)
        inv = 1.0 / mass
        lse[it, blk:blk + 1, :] = top + jnp.log(mass)
        pb[blk][:] = banded(e02 * inv, e1 * inv, upper)

    def mix(it):
        for blk in range(tb):
            pr, cols, keys = spots(it, blk)
            ot[pr, cols] = unstack_pair(dot(vt[pr, keys], pb[blk][:])).astype(BF)

    def project(b):
        cols = pl.ds(pl.multiple_of(b * toks, QB), toks)
        with jax.named_scope("f_proj"):
            mid = (xv[b].astype(F32) + dot(ot[:, cols], wo[:], TN)).astype(BF)
            xm[cols, :] = mid
            h = normed(mid, gm[:])
            hm[cols, :] = h
            hmt[:, cols] = h.T
        for c in keeps(b)[3:]:
            c.start()

    keep_qr, keep_lse = (pltpu.make_async_copy(*ends, ld.at[i]) for i, ends in enumerate(((qr, qr_h), (lse, lse_h))))
    load_w[3].wait()
    for blk in range(tb):
        pb[blk][:] = jnp.zeros(pb[blk].shape, BF)

    def walk(i):
        it = i - 1

        @pl.when((lax.rem(i, n_pairs) == 0) & (i < n_steps))
        def _():
            halo_in(i // n_pairs)

        @pl.when(i == 0)
        def _():
            score(0)

        @pl.when((i > 0) & (i <= n_steps))
        def _():
            with jax.named_scope("f_attn"):
                mix(jnp.maximum(it - 1, 0))
                for blk in range(tb):
                    soften(it, blk)
                score(jnp.minimum(i, n_steps - 1))

        @pl.when(i == n_steps)
        def _():
            for b in range(rows):
                push_q(b).wait()
            keep_qr.start()

        @pl.when(i > n_steps)
        def _():
            mix(n_steps - 1)

        @pl.when((lax.rem(it, n_pairs) == 0) & (it > 0))
        def _():
            project(it // n_pairs - 1)

    cdiv_loop(n_steps + 2, walk)
    with jax.named_scope("f_store_wait"):
        keep_lse.start()
        keep_hat.wait()
        keep_q.wait()
        keep_qr.wait()
        keep_lse.wait()
        for b in range(rows):
            for c in keeps(b):
                c.wait()


def any_spec(k):
    return [pl.BlockSpec(memory_space=pl.ANY)] * k


def vmem_spec(k):
    return [pl.BlockSpec(memory_space=pltpu.VMEM)] * k


def run_fwd(n, x, pos, invf, ga, gm, wq, wk, wv, wo, head_dim):
    rows, toks, width = x.shape
    hd = wq.shape[0]
    ext, total, n_halo = toks + WINDOW, rows * toks, rows * WINDOW
    half = head_dim // 2
    sds = lambda *s: jax.ShapeDtypeStruct(s, BF)
    dma = lambda *s: pltpu.SemaphoreType.DMA(s)
    outs = [sds(hd, total), sds(hd, rows * ext), sds(rows * ext, hd), sds(rows * ext, hd), sds(width, total), sds(hd, total), sds(total, width), sds(total, width), sds(width, total)]
    outs += [sds(hd, n_halo), jax.ShapeDtypeStruct((rows * hd // (2 * head_dim), 8, 2 * QB), F32)] + [jax.ShapeDtypeStruct((half, total), F32)] * 2
    vm = lambda *s: pltpu.VMEM(s, BF)
    vf = lambda *s: pltpu.VMEM(s, F32)
    scratch = [vm(rows, toks, width), vm(rows, WINDOW, width), vm(hd, n_halo), vf(rows * hd // (2 * head_dim), 8, 2 * QB), pltpu.VMEM((rows, toks), jnp.int32), vm(hd, width), vm(hd, width), vm(hd, width), vm(hd, width),
               vm(hd, total), vm(hd, rows * ext), vm(rows * ext, hd), vm(rows * ext, hd), vm(hd, rows * ext), vm(width, total), vm(hd, total), vm(total, width), vm(total, width), vm(width, total), vm(total, width), vm(WINDOW, width),
               vf(hd, total), vf(hd, total), vf(hd, WINDOW), vf(hd, WINDOW), vf(half, n_halo), vf(half, n_halo),
               *[vf(3 * QB, 2 * QB)] * 3, *[vm(3 * QB, 2 * QB)] * 3,
               dma(rows), dma(4), dma(2 + 7 * rows), dma(rows + 1), dma(rows + 1), dma(rows), dma(rows)]
    return pl.pallas_call(
        functools.partial(fwd_kernel, n, head_dim), out_shape=outs,
        in_specs=any_spec(1) + vmem_spec(4) + any_spec(4), out_specs=any_spec(11) + vmem_spec(2), scratch_shapes=scratch,
        compiler_params=pltpu.CompilerParams(collective_id=0, has_side_effects=True, vmem_limit_bytes=VMEM_LIMIT),
        name="forward")(x, pos, invf, ga, gm, wq, wk, wv, wo)


LAG = 2
SLOTS = 2 * LAG
RING = 8
CB = 256


def at(ref, *idx):
    return ref.at[idx]


class Torus:
    def __init__(self, n, head, last, turn, parts, recv0, recv1, recv2, recv3, recv4, recv5, acc, acc2, fin, snd, rcv):
        assert math.isqrt(n // 2) == 4
        me = lax.axis_index("seq")
        self.core = lax.rem(me, 2)
        chip = me // 2
        self.x, self.y = lax.rem(chip, 4), chip // 4
        self.head, self.last, self.turn = head, last, turn
        self.parts, self.recv0, self.recv1, self.recv2, self.recv3, self.recv4, self.recv5 = parts, recv0, recv1, recv2, recv3, recv4, recv5
        self.acc, self.acc2, self.fin, self.snd, self.rcv = acc, acc2, fin, snd, rcv
        self.partner = me + 1 - 2 * self.core
        self.rows, self.columns = [lax.rem(self.y + d, 4) * 4 for d in range(4)], [lax.rem(self.x + d, 4) for d in range(4)]
        self.hops = [[self.device(0, d) for d in range(4)], [self.device(d, 0) for d in range(4)]]

    def device(self, dy, dx):
        return (self.rows[dy] + self.columns[dx]) * 2 + self.core

    def copy(self, lane, kind, slot, src, dst, target):
        return pltpu.make_async_remote_copy(
            src_ref=src, dst_ref=dst, send_sem=self.snd.at[lane, kind, slot], recv_sem=self.rcv.at[lane, kind, slot],
            device_id={"seq": target}, device_id_type=MESH)

    def late(self, pair, yes, no):
        first, end = self.turn
        return jnp.where((pair >= first) & (pair < end), yes, no)

    def swap(self, ring, slot):
        return self.copy(0, 0, slot, self.parts.at[ring, :, :, 1 - self.core], self.recv0.at[slot], self.partner)

    def landing(self, stage):
        return (self.recv0, self.recv1, self.recv2, self.recv3, self.recv4, self.recv5)[stage]

    def arrived(self, stage, kind, slot):
        whole = self.landing(stage).at[kind, slot]
        self.copy(stage, kind, slot, whole, whole, self.partner).wait()

    def send(self, stage, kind, pair, held, slot):
        axis = kind if stage < 3 else 1 - kind
        plus, minus = self.hops[axis][1], self.hops[axis][-1]
        half = CB // 2
        if stage == 1:
            if axis == 0:
                minus = self.late(pair, plus, minus)
            ends = self.acc.at[kind, held, 2, :2], self.acc.at[kind, held, 2, 2:]
        elif stage == 2:
            ends = self.acc.at[kind, held, 1], self.acc.at[kind, held, 3]
        elif stage == 3:
            ends = self.acc2.at[kind, held, 2, :, :half], self.acc2.at[kind, held, 2, :, half:]
        else:
            ends = self.acc2.at[kind, held, 1], self.acc2.at[kind, held, 3]
        for i, src in enumerate(ends):
            self.copy(stage, kind, slot, src, self.landing(stage).at[kind, slot, i], (plus, minus)[i]).start()

    def add(self, stage, kind, pair, held, slot, ring):
        acc, acc2 = self.acc, self.acc2
        if stage == 1:
            for r1 in range(4):
                for r2 in range(4):
                    ry, rx = (r2, r1) if kind == 0 else (r1, r2)
                    chip = self.rows[ry] + self.columns[rx]
                    acc[kind, held, r1, r2] = self.parts[ring, kind, chip, self.core] + self.recv0[slot, kind, chip]
        elif stage == 2:
            back = self.late(pair, 1, 3) if kind == 0 else 3
            acc[kind, held, 1, :2] += self.recv1[kind, slot, 0]
            acc[kind, held, back, 2:] += self.recv1[kind, slot, 1]
        elif stage == 3:
            acc2[kind, held] = acc[kind, held, 0] + (self.recv2[kind, slot, 0] + self.recv2[kind, slot, 1])
        elif stage == 4:
            half = CB // 2
            acc2[kind, held, 1, :, :half] += self.recv3[kind, slot, 0]
            acc2[kind, held, 3, :, half:] += self.recv3[kind, slot, 1]
        else:
            self.fin[pair, kind] = acc2[kind, held, 0] + (self.recv4[kind, slot, 0] + self.recv4[kind, slot, 1])

    def direct(self, kind, held, slot):
        for d in range(1, 4):
            self.copy(5, kind, slot, self.acc2.at[kind, held, d], self.recv5.at[kind, slot, d - 1], self.hops[1 - kind][d]).start()

    def early(self, pair):
        return (pair >= 0) & (pair <= self.head)

    def final(self, pair):
        return (pair == self.last) | ((pair > self.head) & (pair < self.last) & (mod(abs(pair - self.head), 2) == 0))

    def when(self, which, fn):
        if isinstance(which, bool):
            fn() if which else None
        else:
            pl.when(which)(fn)

    def offer(self, t):
        self.when(self.early(t) | self.final(t), lambda: self.swap(mod(t, RING), mod(t, SLOTS)).start())

    def tick(self, t):
        self.offer(t)
        self.advance(t)

    def advance(self, t, tail=False):
        now, land, before = mod(t, SLOTS), mod(t + SLOTS - LAG, SLOTS), mod(t + SLOTS - 1, SLOTS)
        ring_land = mod(t + RING - 1, RING)
        for stage in range(5, 0, -1):
            pair = t - LAG * stage + 1
            held = before if stage % 2 else mod(t + 1, SLOTS)

            def move(last_hops, stage=stage, pair=pair, held=held):
                if stage == 1:
                    with jax.named_scope("t_wait1"):
                        self.swap(ring_land, before).wait()
                for kind in range(2):
                    if last_hops and stage == 4:
                        with jax.named_scope("t_wait6"):
                            self.arrived(5, kind, land)
                        got = self.recv5[kind, land]
                        self.fin[pair, kind] = self.acc2[kind, held, 0] + (got[0] + got[1] + got[2])
                        continue
                    if stage > 1:
                        with jax.named_scope(f"t_wait{stage}"):
                            self.arrived(stage - 1, kind, land)
                    self.add(stage, kind, pair, held, land if stage > 1 else before, ring_land)
                    if last_hops and stage == 3:
                        self.direct(kind, held, now)
                    elif stage < 5:
                        self.send(stage, kind, pair, held, now)

            if stage < 3:
                self.when(self.early(pair) | self.final(pair), functools.partial(move, False))
            else:
                self.when(self.early(pair), functools.partial(move, False))
                if tail and stage < 5:
                    self.when(self.final(pair), functools.partial(move, True))


def pick(i, table):
    out = 0
    for key, value in table.items():
        out = jnp.where(i == key, value, out)
    return out


def norm_back(x, gain, grad, res):
    xf = x.astype(F32)
    inv = lax.rsqrt(jnp.mean(xf * xf, axis=-1, keepdims=True) + NORM_EPS)
    unit = xf * inv
    gu = grad * gain
    out = inv * (gu - unit * jnp.mean(gu * unit, axis=-1, keepdims=True)) + res.astype(F32)
    gu = grad * unit
    return out.astype(BF), jnp.sum(gu.reshape(-1, 8, gu.shape[-1]), axis=0)


def plan(n_mlp, n_down, nc):
    order = [("o", g) for g in range(nc)] + [(name, g) for g in range(nc) for name in "qkv"]
    base, head = n_mlp + n_down, n_mlp + n_down + nc - 1
    last = 2 * (base - 1 - head + len(order) // 2) + head - 1
    spot = lambda pair: min(max(pair, 2 * pair - head), last)
    return head, {name: (spot(base + i // 2), i % 2) for i, name in enumerate(order)}, last


def bwd_kernel(n, head_dim, dims, ga, gm, x_h, dout_h, q_h, kt_h, k_h, v_h, hat_h, ot_h, xm_h, hm_h, hmt_h, qr_h, lse_h, cos_h, sin_h,
               wq_h, wk_h, wv_h, wo_h, wg_h, wu_h, wd_h,
               dx_h, fin_h,
               parts, recv0, recv1, recv2, recv3, recv4, recv5, acc, acc2, fin, snd, rcv,
               dor, lser, deltar, hsnd, hrcv, osnd, orcv, gsend, grecv, gsem, ld,
               xbuf, mbuf, gnm, gmid, ot, hat, wo, dot_, lse, delta, cos_i, sin_i, dgain):
    rows, toks, width, hd, ff = dims
    ext, total = toks + WINDOW, rows * toks
    pw = 2 * head_dim
    n_pairs = hd // pw
    tb, n_steps = toks // QB, n_pairs * rows
    nb, nc, sub = ff // CB, width // CB, ff // width
    rpd = width // n
    per, half_sub = CB // pw, sub // 2
    head, place, end = plan(nb, nc * half_sub, nc)
    comm = Torus(n, head, end, (nb, nb + n_pairs + 1), parts, recv0, recv1, recv2, recv3, recv4, recv5, acc, acc2, fin, snd, rcv)
    me = lax.axis_index("seq")
    left = lax.rem(me + n - 1, n)
    barrier = pltpu.get_barrier_semaphore()

    def greet(i):
        pl.semaphore_signal(barrier, inc=1, device_id={"seq": lax.rem(me + i + 1, n)}, device_id_type=MESH)

    def load(i, s, d):
        c = pltpu.make_async_copy(s, d, ld.at[i])
        c.start()
        return c

    def late(i):
        s, d = ((xm_h, mbuf), (ot_h, ot), (hat_h, hat), (wo_h, wo), (lse_h, lse), (cos_h, cos_i), (sin_h, sin_i))[i]
        return pltpu.make_async_copy(s, d, ld.at[1 + i])

    def to_left(src, dst, send_sem, recv_sem):
        return pltpu.make_async_remote_copy(src_ref=src, dst_ref=dst, send_sem=send_sem, recv_sem=recv_sem,
                                            device_id={"seq": left}, device_id_type=MESH)

    n_late = 7

    def push_rows(i):
        return to_left(*((lse_h, lser), (delta, deltar))[i], hsnd.at[i], hrcv.at[i])

    def push_out(p):
        pr = pl.ds(aligned(p * pw, pw), pw)
        return [to_left(dot_.at[pr, pl.ds(b * toks, WINDOW)], dor.at[pr, pl.ds(b * WINDOW, WINDOW)], osnd.at[p], orcv.at[p])
                for b in range(rows)]

    def give_out(p):
        for c in push_out(p):
            c.start()

    def put(spot, value):
        pair, kind = spot
        parts[mod(pair, RING), kind] = value.reshape(n // 2, 2, rpd, CB)

    def spot_of(name, g):
        known = {i: place[name, i] for i in range(nc)}
        return pick(g, {i: s[0] for i, s in known.items()}), pick(g, {i: s[1] for i, s in known.items()})

    def spots(it, blk):
        p, b = it // rows, mod(it, rows)
        pr = pl.ds(aligned(p * pw, pw), pw)
        return pr, pl.ds(aligned(b * toks + blk * QB, QB), QB), pl.ds(aligned(b * ext + blk * QB, QB), 3 * QB)

    def row_of(it):
        return mod(it, rows) * n_pairs + it // rows

    def mlp(hm, hmt, actt, wgu, wd, dgu, wld):
        def weights(j, slot):
            c = aligned(j * CB, CB)
            return [pltpu.make_async_copy(wg_h.at[:, pl.ds(c, CB)], wgu.at[slot, :, :CB], wld.at[slot, 0]),
                    pltpu.make_async_copy(wu_h.at[:, pl.ds(c, CB)], wgu.at[slot, :, CB:], wld.at[slot, 1]),
                    pltpu.make_async_copy(wd_h.at[pl.ds(c, CB), :], wd.at[slot], wld.at[slot, 2])]

        for c in weights(0, 0):
            c.start()
        ld_hm, ld_x, ld_hmt = load(8, hm_h, hm), load(0, dout_h, xbuf), load(9, hmt_h, hmt)
        cdiv_loop(n - 1, greet)
        gnm[:] = jnp.zeros_like(gnm)
        gsend[:] = jnp.zeros_like(gsend)
        dgain[:] = jnp.zeros_like(dgain)
        ld_hm.wait()
        ld_x.wait()
        ld_hmt.wait()
        for i in range(n_late):
            late(i).start()

        def block(j):
            slot = lax.rem(j, 2)
            for c in weights(j, slot):
                c.wait()

            @pl.when(j + 1 < nb)
            def _():
                for c in weights(j + 1, 1 - slot):
                    c.start()

            c0 = pl.multiple_of(j * CB, CB)
            with jax.named_scope("b_mlp"):
                for b in range(rows):
                    r = slice(b * toks, (b + 1) * toks)
                    gu = dot(hm[r, :], wgu[slot])
                    gact = dot(xbuf[r, :], wd[slot], NT).astype(BF).astype(F32)
                    gate, up = gu[:, :CB], gu[:, CB:]
                    sig = 1.0 / (1.0 + jnp.exp(-gate))
                    swish = gate * sig
                    actt[pl.ds(c0, CB), r] = (swish * up).astype(BF).T
                    dgu[r, :CB] = (gact * up * (sig + swish * (1.0 - sig))).astype(BF)
                    dgu[r, CB:] = (gact * swish).astype(BF)
                both = dot(hmt[:], dgu[:])
                ring = lax.rem(j, RING)
                parts[ring, 0] = both[:, :CB].reshape(n // 2, 2, rpd, CB)
                parts[ring, 1] = both[:, CB:].reshape(n // 2, 2, rpd, CB)
                for b in range(rows):
                    r = slice(b * toks, (b + 1) * toks)
                    gnm[r, :] += dot(dgu[r, :], wgu[slot], NT)

            @pl.when(j == 0)
            def _():
                pl.semaphore_wait(barrier, n - 1)
                push_rows(0).start()

            comm.tick(j)

        cdiv_loop(nb, block)

        def down(c):
            share = n // 2 // sub
            c0 = pl.multiple_of(c * CB, CB)
            for m in range(sub):
                res = dot(actt[m * width:(m + 1) * width, :], xbuf[:, pl.ds(c0, CB)]).reshape(share, 2, sub, rpd, CB)
                for i in range(sub):
                    pair = nb + c * half_sub + i // 2
                    parts[lax.rem(pair, RING), i % 2, m * share:(m + 1) * share] = res[:, :, i]

        for i in range(n_late):
            late(i).wait()

        def mid(b):
            for i in range(tb):
                r = pl.ds(pl.multiple_of((b * tb + i) * QB, QB), QB)
                out, dg = norm_back(mbuf[r, :], gm[:], gnm[r, :], xbuf[r, :])
                gmid[r, :] = out
                dgain[8:, :] += dg

        def deltas(p):
            for it in range(rows):
                for blk in range(tb):
                    pr, cols, _ = spots(p * rows + it, blk)
                    both = dot_[pr, cols].astype(F32) * ot[pr, cols].astype(F32)
                    delta[row_of(p * rows + it), blk:blk + 1, :] = jnp.concatenate(
                        [col_sum(both[:head_dim]), col_sum(both[head_dim:])], axis=1)

        def column(c):
            with jax.named_scope("b_down"):
                down(c)
            comm.tick(nb + c + jnp.minimum(c, 1))

            @pl.when(c == 1)
            def _():
                give_out(c)

            @pl.when(c == 0)
            def _():
                with jax.named_scope("b_mid"):
                    cdiv_loop(rows, mid)
                with jax.named_scope("b_dot"):
                    dot_[:] = dot(wo[:], gmid[:], NT).astype(BF)
                    cdiv_loop(n_pairs, deltas)
                comm.tick(nb + 1)
                push_rows(1).start()
                give_out(0)

        cdiv_loop(nc, column)

    vm = lambda *s: pltpu.VMEM(s, BF)
    vf = lambda *s: pltpu.VMEM(s, F32)
    pl.run_scoped(mlp, vm(total, width), vm(width, total), vm(ff, total), vm(2, width, 2 * CB), vm(2, CB, width), vm(total, 2 * CB),
                  pltpu.SemaphoreType.DMA((2, 3)))
    def attention(q, kt, k, v, qr, dv, sc0, sc1, sc2, sr, dp0, dp1, dp2, dr, pb0, pb1, pb2, pr_, ds0, ds1, ds2, dsr):
        dqt, dkt = ot, q
        wq, wk, wv = k.at[:hd], kt.at[:, :width], v.at[:hd]
        sc, dp, pb, ds = (sc0, sc1, sc2), (dp0, dp1, dp2), (pb0, pb1, pb2), (ds0, ds1, ds2)
        lds = [load(8 + i, s, d) for i, (s, d) in enumerate(((q_h, q), (k_h, k), (v_h, v), (qr_h, qr), (kt_h, kt)))]

        def out_grad(g):
            put(spot_of("o", g), dot(ot[:], gmid[:, pl.ds(pl.multiple_of(g * CB, CB), CB)]))

        with jax.named_scope("b_dwo"):
            cdiv_loop(nc, out_grad)
        first_tick = nb + nc + 1
        comm.tick(first_tick)
        give_out(2)
        upper = upper_mask()
        first, last = me == 0, me == n - 1
        halves = slice(0, WINDOW), slice(WINDOW, 3 * QB)

        def right(it, i):
            p, b = it // rows, mod(it, rows)
            return pl.ds(aligned(p * pw, pw), pw), pl.ds(aligned(b * WINDOW + i * QB, QB), QB), pl.ds(aligned(b * ext + toks + i * QB, QB), WINDOW - i * QB)

        def score(it):
            for blk in range(tb):
                pr, cols, keys = spots(it, blk)
                sc[blk][:] = dot(k[keys, pr], stack_pair(q[pr, cols]))
                dp[blk][:] = dot(v[keys, pr], stack_pair(dot_[pr, cols]))
            for i, rs in enumerate(halves):
                pr, cols, keys = right(it, i)
                sr[rs, :] = dot(k[keys, pr], stack_pair(qr[pr, cols]))
                dr[rs, :] = dot(v[keys, pr], stack_pair(dor[pr, cols]))

        def soften(it):
            row = row_of(it)
            for blk in range(tb):
                s02, s1 = merged(sc[blk][:], upper, *start_bias(first, blk))
                norm, mean = lse[row, blk:blk + 1, :], delta[row, blk:blk + 1, :]
                p02, p1 = jnp.exp(s02 - norm), jnp.exp(s1 - norm)
                g02, g1 = jnp.where(upper, dp[blk][:QB], dp[blk][2 * QB:]), dp[blk][QB:2 * QB]
                pb[blk][:] = banded(p02, p1, upper)
                ds[blk][:] = banded(p02 * (g02 - mean), p1 * (g1 - mean), upper)
            for blk in range(tb):
                i = blk // 2
                rs = slice(blk * QB, (blk + 1) * QB)
                p = jnp.exp(sr[rs, :] - jnp.where(last, -NEG, lser[row, i:i + 1, :]))
                g = p * (dr[rs, :] - deltar[row, i:i + 1, :])
                pr_[rs, :] = (p if blk == 1 else jnp.where(upper, p, 0.0)).astype(BF)
                dsr[rs, :] = (g if blk == 1 else jnp.where(upper, g, 0.0)).astype(BF)

        def grads(it):
            ks, vs = [], []
            for blk in range(tb):
                pr, cols, keys = spots(it, blk)
                own = slice(max(0, 2 - blk) * QB, 3 * QB)
                vs.append(dot(pb[blk][own, :], stack_pair(dot_[pr, cols]), NT))
                ks.append(dot(ds[blk][own, :], stack_pair(q[pr, cols]), NT))
                dq = unstack_pair(dot(kt[pr, keys], ds[blk][:])) * (head_dim ** -0.5)
                dqt[pr, cols] = rope(dq, cos_i[:, cols], sin_i[:, cols], -1, head_dim).astype(BF)
            for i, rs in enumerate(halves):
                pr, cols, _ = right(it, i)
                vs.append(dot(pr_[rs, :], stack_pair(dor[pr, cols]), NT))
                ks.append(dot(dsr[rs, :], stack_pair(qr[pr, cols]), NT))
            for j in range(tb):
                pr, cols, _ = spots(it, j)
                gv, gk = (sum(x[i][(j - max(0, i - 2)) * QB:(j - max(0, i - 2) + 1) * QB] for i in range(j, j + 3)) for x in (vs, ks))
                dv[cols, pr] = gv.astype(BF)
                dkt[pr, cols] = rope(gk.T, cos_i[:, cols], sin_i[:, cols], -1, head_dim).astype(BF)

        def close_group(g):
            cols = pl.ds(pl.multiple_of(g * CB, CB), CB)
            with jax.named_scope("b_dwqkv"):
                put(spot_of("q", g), dot(hat[:], dqt[cols, :], NT))
                put(spot_of("k", g), dot(hat[:], dkt[cols, :], NT))
                put(spot_of("v", g), dot(hat[:], dv[:, cols]))

        def weights():
            return [pltpu.make_async_copy(s, d, ld.at[8 + i]) for i, (s, d) in enumerate(((wq_h, wq), (wk_h, wk), (wv_h, wv), (x_h, xbuf)))]

        def arrived(p):
            whole = dor.at[pl.ds(aligned(p * pw, pw), pw), :]
            with jax.named_scope("b_hwait"):
                to_left(whole, whole, osnd.at[p], orcv.at[p]).wait()

        def walk(it):
            ahead = it + 1

            @pl.when((lax.rem(ahead, rows) == 0) & (ahead < n_steps))
            def _():
                arrived(ahead // rows)

            @pl.when(it < n_steps)
            def _():
                with jax.named_scope("b_attn"):
                    grads(it - 1)
                    soften(it)
                    score(jnp.minimum(ahead, n_steps - 1))

            @pl.when(it == n_steps)
            def _():
                grads(n_steps - 1)
                for c in weights():
                    c.start()

            p, step = it // rows - 1, lax.rem(it, rows)

            @pl.when((step == 0) & (lax.rem(p, per) == per - 1))
            def _():
                close_group(p // per)

            now = first_tick + 1 + p + step // (rows - 1)
            twice = now - head

            @pl.when(it == n_steps)
            def _():
                comm.offer(end)

            @pl.when((step == 0) | ((step == rows - 1) & (twice > 0)))
            def _():
                comm.tick(now + jnp.maximum(twice - step // (rows - 1), 0))

            @pl.when((step == 0) & (p + 3 < n_pairs))
            def _():
                give_out(p + 3)

        for c in lds[:-1]:
            c.wait()
        for i in range(2):
            push_rows(i).wait()
        arrived(0)
        score(0)
        soften(0)
        score(1)
        lds[-1].wait()
        cdiv_loop(n_steps, lambda i: walk(i + 1))
        for c in weights():
            c.wait()

        def into(b):
            r = pl.ds(pl.multiple_of(b * toks, QB), toks)
            with jax.named_scope("b_into"):
                gnm[r, :] = dot(dqt[:, r], wq[:], TN) + dot(dkt[:, r], wk[:], TN) + dot(dv[r, :], wv[:])

            with jax.named_scope("b_final"):
                for i in range(tb):
                    r = pl.ds(pl.multiple_of((b * tb + i) * QB, QB), QB)
                    out, dg = norm_back(xbuf[r, :], ga[:], gnm[r, :], gmid[r, :])
                    mbuf[r, :] = out
                    dgain[:8, :] += dg

            @pl.when(b == 0)
            def _():
                comm.advance(end)

            comm.advance(end + 1 + b, True)

        cdiv_loop(rows, into)

    score_bufs = [vf(3 * QB, 2 * QB)] * 8 + [vm(3 * QB, 2 * QB)] * 8
    pl.run_scoped(attention, vm(hd, total), vm(hd, rows * ext), vm(rows * ext, hd), vm(rows * ext, hd), vm(hd, rows * WINDOW), vm(total, hd), *score_bufs)
    out_copy = load(1, mbuf, dx_h)
    gains = jnp.concatenate([col_sum(dgain[:8, :]), col_sum(dgain[8:, :]), jnp.zeros((6, width), F32)], axis=0)
    for p in range(n):
        gsend[p, :, :rpd] = gains[:, p * rpd:(p + 1) * rpd]

    def spread(i):
        to = lax.rem(me + i + 1, n)
        pltpu.make_async_remote_copy(src_ref=gsend.at[to], dst_ref=grecv.at[i], send_sem=gsem.at[0], recv_sem=gsem.at[1],
                                     device_id={"seq": to}, device_id_type=MESH).start()

    cdiv_loop(n - 1, spread)
    stop = end + 4 * LAG
    run = lambda lo, hi: lax.fori_loop(lo, hi, lambda t, c: comm.advance(t, True) or c, 0)
    run(end + 1 + rows, stop - 1)
    most, rest = pl.ds(0, end), pl.ds(end, 2)
    keep_most = load(0, fin.at[most], fin_h.at[most])
    to_left(gsend.at[pl.ds(0, n - 1)], grecv, gsem.at[0], gsem.at[1]).wait()
    sums = gsend[me]
    for i in range(n - 1):
        sums = sums + grecv[i]
    fin[end + 1, 0, :8, :128] = sums
    out_copy.wait()
    run(stop - 1, stop)
    with jax.named_scope("b_end"):
        keep_rest = load(1, fin.at[rest], fin_h.at[rest])
        keep_most.wait()
        keep_rest.wait()


def spread_kernel(dims, dx_i, fin_i, dx_o, dga_o, dgm_o, *refs):
    head_dim, n, width, ff = dims
    outs, (buf, fin), stage, sem = refs[:7], refs[7:9], refs[9:16], refs[16]
    dq, dk, dv, do, dg, du, dd = stage
    nb, nc, sub = ff // CB, width // CB, ff // width
    rpd = width // n
    head, place, end = plan(nb, nc * sub // 2, nc)
    get, get_fin, out = (pltpu.make_async_copy(*ends, sem.at[len(outs) + i]) for i, ends in enumerate(((dx_i, buf), (fin_i, fin), (buf, dx_o))))
    get_fin.start()
    get.start()
    get_fin.wait()
    gains = fin[end + 1, 0]
    dga_o[:] = gains[:1, :rpd]
    dgm_o[:] = gains[1:2, :rpd]
    for j in range(nb):
        dg[:, j * CB:(j + 1) * CB] = fin[j, 0]
        du[:, j * CB:(j + 1) * CB] = fin[j, 1]
    for c in range(nc):
        for i in range(sub):
            pair = nb + (c * sub + i) // 2
            dd[i * rpd:(i + 1) * rpd, c * CB:(c + 1) * CB] = fin[pair, i % 2]
    for g in range(nc):
        do[:, g * CB:(g + 1) * CB] = fin[place["o", g]]
        for name, ref in (("q", dq), ("k", dk), ("v", dv)):
            val = fin[place[name, g]]
            for h in range(CB // head_dim):
                ref[g * (CB // head_dim) + h] = val[:, h * head_dim:(h + 1) * head_dim]
    keeps = [pltpu.make_async_copy(s, d, sem.at[i]) for i, (s, d) in enumerate(zip(stage, outs))]
    for c in keeps:
        c.start()
    get.wait()
    out.start()
    for c in keeps:
        c.wait()
    out.wait()


def run_bwd(n, head_dim, ga, gm, x, dout, q, kt, k, v, hat, ot, xm, hm, hmt, qr, lse, cos_t, sin_t, wq, wk, wv, wo, wg, wu, wd, rows):
    total, width = x.shape
    hd, ff = wq.shape[0], wg.shape[1]
    toks = total // rows
    rpd, heads = width // n, hd // head_dim
    nb, nc, sub = ff // CB, width // CB, ff // width
    slots = plan(nb, nc * sub // 2, nc)[2] + 2
    n_pairs = hd // (2 * head_dim)
    f = lambda *s: jax.ShapeDtypeStruct(s, F32)
    dx_t = jax.ShapeDtypeStruct((total, width), BF)
    vm = lambda *s: pltpu.VMEM(s, BF)
    vf = lambda *s: pltpu.VMEM(s, F32)
    dma = lambda *s: pltpu.SemaphoreType.DMA(s)
    line, duo = vf(rows * n_pairs, 8, 2 * QB), (2, SLOTS)
    scratch = [vf(RING, 2, n // 2, 2, rpd, CB), vf(SLOTS, 2, n // 2, rpd, CB), vf(*duo, 2, 2, rpd, CB), vf(*duo, 2, 4, rpd, CB),
               vf(*duo, 2, rpd, CB // 2), vf(*duo, 2, rpd, CB), vf(*duo, 3, rpd, CB), vf(*duo, 4, 4, rpd, CB), vf(*duo, 4, rpd, CB), vf(slots, 2, rpd, CB),
               dma(6, *duo), dma(6, *duo),
               vm(hd, rows * WINDOW), line, line, dma(2), dma(2), dma(n_pairs), dma(n_pairs),
               vf(n, 8, 128), vf(n - 1, 8, 128), dma(2), dma(13),
               vm(total, width), vm(total, width), vf(total, width), vm(total, width), vm(hd, total), vm(width, total), vm(hd, width), vm(hd, total), line, line, vf(*cos_t.shape), vf(*cos_t.shape), vf(16, width)]
    mid = pl.pallas_call(
        functools.partial(bwd_kernel, n, head_dim, (rows, toks, width, hd, ff)), out_shape=[dx_t, f(slots, 2, rpd, CB)],
        in_specs=vmem_spec(2) + any_spec(22), out_specs=any_spec(2), scratch_shapes=scratch,
        compiler_params=pltpu.CompilerParams(collective_id=1, has_side_effects=True, vmem_limit_bytes=VMEM_LIMIT),
        name="backward")(ga, gm, x, dout, q, kt, k, v, hat, ot, xm, hm, hmt, qr, lse, cos_t, sin_t, wq, wk, wv, wo, wg, wu, wd)
    outs = [f(heads, rpd, head_dim)] * 3 + [f(rpd, width), f(rpd, ff), f(rpd, ff), f(ff // n, width)]
    return pl.pallas_call(
        functools.partial(spread_kernel, (head_dim, n, width, ff)), out_shape=[dx_t, f(1, rpd), f(1, rpd)] + outs,
        in_specs=any_spec(2), out_specs=any_spec(1) + vmem_spec(2) + any_spec(7),
        scratch_shapes=[vm(total, width), vf(slots, 2, rpd, CB), *[vf(*o.shape) for o in outs], dma(10)],
        name="spread")(*mid)


def solution(mesh):
    n = mesh.shape["seq"]

    def device_step(hidden, positions, g_attn, g_mlp, w_query, w_key, w_value, w_out, w_gate, w_up, w_down, d_out):
        rows, toks, width = hidden.shape
        layers, _, heads, head_dim = w_query.shape
        hd = heads * head_dim
        half = head_dim // 2
        inv_freq = 1.0 / (10000.0 ** (jnp.arange(half, dtype=F32) * (2.0 / head_dim)))
        turn = lambda w: w[0].transpose(1, 2, 0).reshape(hd, width)
        wq, wk, wv = turn(w_query), turn(w_key), turn(w_value)
        fwd = run_fwd(n, hidden, positions, inv_freq[:, None], g_attn, g_mlp, wq, wk, wv, w_out[0], head_dim)
        out = run_bwd(n, head_dim, g_attn, g_mlp, hidden.reshape(rows * toks, width), d_out.reshape(rows * toks, width), *fwd,
                      wq, wk, wv, w_out[0], w_gate[0], w_up[0], w_down[0], rows)
        dx, dga, dgm, dq, dk, dv, do, dg, du, dd = out
        back = lambda w: w.transpose(1, 0, 2)[None]
        return (dx.reshape(rows, toks, width), dga, dgm, back(dq), back(dk), back(dv), do[None], dg[None], du[None], dd[None])

    tok_spec, grad_spec = P("data", "seq"), P(None, ("data", "seq"))
    in_specs = (tok_spec, tok_spec) + (P(),) * 9 + (tok_spec,)
    out_specs = (tok_spec,) + (grad_spec,) * 9
    return jax.shard_map(device_step, mesh=mesh, in_specs=in_specs, out_specs=out_specs, check_vma=False)
```

```python
import functools, math
import numpy as np
import jax, jax.numpy as jnp
from jax import lax
from jax.experimental import pallas as pl
from jax.experimental.pallas import tpu as pltpu
from jax.sharding import PartitionSpec as P

WINDOW = 256
NORM_EPS = 1e-5
QB = 128
BF, F32 = jnp.bfloat16, jnp.float32
NN, NT, TN = ((1,), (0,)), ((1,), (1,)), ((0,), (0,))
MESH = pl.DeviceIdType.MESH
NEG = -1e30
VMEM_LIMIT = 67043328


def dot(a, b, dims=NN):
    return lax.dot_general(a, b, (dims, ((), ())), preferred_element_type=F32)


def cdiv_loop(n, body):
    lax.fori_loop(0, n, lambda i, c: body(i) or c, 0)


def mod(a, b):
    return a % b if isinstance(a, int) else lax.rem(a, b)


def aligned(a, b):
    return a if isinstance(a, int) else pl.multiple_of(a, b)


def rope(blk, cos_b, sin_b, sign, head_dim):
    half = head_dim // 2
    parts = []
    for h in range(blk.shape[0] // head_dim):
        first = blk[h * head_dim:h * head_dim + half]
        second = blk[h * head_dim + half:(h + 1) * head_dim]
        if sign > 0:
            parts += [first * cos_b - second * sin_b, second * cos_b + first * sin_b]
        else:
            parts += [first * cos_b + second * sin_b, second * cos_b - first * sin_b]
    return jnp.concatenate(parts, axis=0)


def normed(x, gain):
    xf = x.astype(F32)
    inv = lax.rsqrt(jnp.mean(xf * xf, axis=-1, keepdims=True) + NORM_EPS)
    return (xf * inv * gain).astype(BF)


def stack_pair(pair_t):
    half = pair_t.shape[0] // 2
    zero = jnp.zeros((half, pair_t.shape[1]), pair_t.dtype)
    return jnp.concatenate(
        [jnp.concatenate([pair_t[:half], zero], axis=0), jnp.concatenate([zero, pair_t[half:]], axis=0)], axis=1)


def unstack_pair(both):
    half, cols = both.shape[0] // 2, both.shape[1] // 2
    return jnp.concatenate([both[:half, :cols], both[half:, cols:]], axis=0)


def col_sum(x):
    return jnp.sum(x, axis=0, keepdims=True)


def merged(scores, upper, bias0, bias1):
    return jnp.where(upper, scores[:QB] + bias0, scores[2 * QB:]), scores[QB:2 * QB] + bias1


def banded(p02, p1, upper):
    return jnp.concatenate(
        [jnp.where(upper, p02, 0.0).astype(BF), p1.astype(BF), jnp.where(upper, 0.0, p02).astype(BF)], axis=0)


def upper_mask():
    key_ids = lax.broadcasted_iota(jnp.int32, (QB, 2 * QB), 0)
    query_ids = lax.broadcasted_iota(jnp.int32, (QB, 2 * QB), 1) % QB
    return key_ids > query_ids


def start_bias(first, blk):
    bias = jnp.where(first, NEG, 0.0).astype(F32)
    return (bias if blk < 2 else 0.0), (bias if blk < 1 else 0.0)


def fwd_kernel(n, head_dim, x_h, pos_h, invf_h, ga_h, gm_h, wq_h, wk_h, wv_h, wo_h,
               q_h, kt_h, k_h, v_h, hat_h, ot_h, xm_h, hm_h, hmt_h, qr_h, lse_h, cos_t, sin_t,
               pos, invf, ga, gm, xv, halo, qr, lse, pos_halo, wq, wk, wv, wo, q, kt, k, v, vt, hat, ot, xm, hm, hmt, hb, hh, acc, acc2, ak, av, cos_h, sin_h,
               sc0, sc1, sc2, pb0, pb1, pb2, ldx, ld, st, snd, rcv, qsnd, qrcv):
    sc, pb = (sc0, sc1, sc2), (pb0, pb1, pb2)
    rows, toks, width = xv.shape
    ext, total, pw = toks + WINDOW, rows * toks, 2 * head_dim
    n_pairs = wq.shape[0] // pw
    tb, n_steps = toks // QB, n_pairs * rows
    me = lax.axis_index("seq")
    right, left = lax.rem(me + 1, n), lax.rem(me + n - 1, n)
    load_x = [pltpu.make_async_copy(x_h.at[b], xv.at[b], ldx.at[b]) for b in range(rows)]
    load_w = [pltpu.make_async_copy(s, d, ld.at[i]) for i, (s, d) in enumerate(((wq_h, wq), (wk_h, wk), (wv_h, wv), (wo_h, wo)))]
    load_s = [pltpu.make_async_copy(s, d, ldx.at[rows + i]) for i, (s, d) in enumerate(((pos_h, pos), (invf_h, invf), (ga_h, ga), (gm_h, gm)))]
    for c in load_s + load_x:
        c.start()
    barrier = pltpu.get_barrier_semaphore()
    for other in (left, right):
        pl.semaphore_signal(barrier, inc=1, device_id={"seq": other}, device_id_type=MESH)

    def push(i, s, d):
        return pltpu.make_async_remote_copy(src_ref=s, dst_ref=d, send_sem=snd.at[i], recv_sem=rcv.at[i], device_id={"seq": right}, device_id_type=MESH)

    def push_rows(b):
        return push(b, x_h.at[b, toks - WINDOW:, :], halo.at[b])

    send_pos = push(rows, pos, pos_halo)

    def angles(cos_ref, sin_ref, positions):
        count = positions.shape[1]
        for b in range(rows):
            ang = invf[:] * positions[b:b + 1, :].astype(F32)
            cos_ref[:, b * count:(b + 1) * count] = jnp.cos(ang)
            sin_ref[:, b * count:(b + 1) * count] = jnp.sin(ang)

    for c in load_s:
        c.wait()
    angles(cos_t, sin_t, pos[:])

    def norm_rows(b):
        for i in range(tb):
            h = normed(xv[b, i * QB:(i + 1) * QB, :], ga[:])
            hb[pl.ds(pl.multiple_of((b * tb + i) * QB, QB), QB), :] = h

    with jax.named_scope("f_norm"):
        for c in load_x:
            c.wait()
        for c in load_w:
            c.start()
        cdiv_loop(rows, norm_rows)
    pl.semaphore_wait(barrier, 2)
    send_pos.start()
    for b in range(rows):
        push_rows(b).start()
    keep_hat = pltpu.make_async_copy(hat, hat_h, st.at[0])
    tables = cos_t[:], sin_t[:]

    def put_q(src):
        for p in range(n_pairs):
            r = slice(p * pw, (p + 1) * pw)
            q[r, :] = (rope(src[r, :], *tables, 1, head_dim) * (head_dim ** -0.5)).astype(BF)

    def put_own(src, dst_t, dst):
        for p in range(n_pairs):
            r = slice(p * pw, (p + 1) * pw)
            both = (rope(src[r, :], *tables, 1, head_dim) if dst is k else src[r, :]).astype(BF)
            for b in range(rows):
                blk = both[:, b * toks:(b + 1) * toks]
                own = slice(b * ext + WINDOW, (b + 1) * ext)
                dst_t[r, own] = blk
                dst[own, r] = blk.T

    with jax.named_scope("f_mm"):
        load_w[0].wait()
        load_w[1].wait()
        load_w[2].wait()
        acc[:] = dot(wq[:], hb[:], NT)
        acc2[:] = dot(wk[:], hb[:], NT)
        put_q(acc)
        acc[:] = dot(wv[:], hb[:], NT)
        put_own(acc2, kt, k)
        for i in range(total // QB):
            r = slice(i * QB, (i + 1) * QB)
            hat[:, r] = hb[r, :].T
        put_own(acc, vt, v)
    keep_hat.start()
    keep_q = pltpu.make_async_copy(q, q_h, st.at[1])
    keep_q.start()

    def push_q(b):
        return pltpu.make_async_remote_copy(src_ref=q.at[:, b * toks:b * toks + WINDOW], dst_ref=qr.at[:, b * WINDOW:(b + 1) * WINDOW],
                                            send_sem=qsnd.at[b], recv_sem=qrcv.at[b], device_id={"seq": left}, device_id_type=MESH)

    for b in range(rows):
        push_q(b).start()
    send_pos.wait()
    angles(cos_h, sin_h, pos_halo[:, toks - WINDOW:])

    def keeps(b):
        wide, cols = pl.ds(pl.multiple_of(b * ext, QB), ext), pl.ds(pl.multiple_of(b * toks, QB), toks)
        ends = ((kt.at[:, wide], kt_h.at[:, wide]), (k.at[wide, :], k_h.at[wide, :]), (v.at[wide, :], v_h.at[wide, :]),
                (ot.at[:, cols], ot_h.at[:, cols]), (hm.at[cols, :], hm_h.at[cols, :]), (hmt.at[:, cols], hmt_h.at[:, cols]),
                (xm.at[cols, :], xm_h.at[cols, :]))
        return [pltpu.make_async_copy(s, d, st.at[2 + b * len(ends) + i]) for i, (s, d) in enumerate(ends)]

    def halo_in(b):
        with jax.named_scope("f_halo_wait"):
            push_rows(b).wait()
        with jax.named_scope("f_halo"):
            for i in range(WINDOW // QB):
                r = slice(i * QB, (i + 1) * QB)
                hh[r, :] = normed(halo[b, r, :], ga[:])
            ak[:] = dot(wk[:], hh[:], NT)
            av[:] = dot(wv[:], hh[:], NT)
            cols = pl.ds(pl.multiple_of(b * WINDOW, QB), WINDOW)
            wide = pl.ds(pl.multiple_of(b * ext, QB), WINDOW)
            near = cos_h[:, cols], sin_h[:, cols]
            for src, dst_t, dst in ((ak, kt, k), (av, vt, v)):
                for p in range(n_pairs):
                    r = slice(p * pw, (p + 1) * pw)
                    blk = (rope(src[r, :], *near, 1, head_dim) if dst is k else src[r, :]).astype(BF)
                    dst_t[r, wide] = blk
                    dst[wide, r] = blk.T
        for c in keeps(b)[:3]:
            c.start()

    upper = upper_mask()
    first = me == 0

    def spots(it, blk):
        b, p = it // n_pairs, mod(it, n_pairs)
        pr = pl.ds(aligned(p * pw, pw), pw)
        return pr, pl.ds(aligned(b * toks + blk * QB, QB), QB), pl.ds(aligned(b * ext + blk * QB, QB), 3 * QB)

    def score(it):
        for blk in range(tb):
            pr, cols, keys = spots(it, blk)
            sc[blk][:] = dot(k[keys, pr], stack_pair(q[pr, cols]))

    def soften(it, blk):
        s02, s1 = merged(sc[blk][:], upper, *start_bias(first, blk))
        top = jnp.max(jnp.maximum(s02, s1), axis=0, keepdims=True)
        e02, e1 = jnp.exp(s02 - top), jnp.exp(s1 - top)
        mass = col_sum(e02 + e1)
        inv = 1.0 / mass
        lse[it, blk:blk + 1, :] = top + jnp.log(mass)
        pb[blk][:] = banded(e02 * inv, e1 * inv, upper)

    def mix(it):
        for blk in range(tb):
            pr, cols, keys = spots(it, blk)
            ot[pr, cols] = unstack_pair(dot(vt[pr, keys], pb[blk][:])).astype(BF)

    def project(b):
        cols = pl.ds(pl.multiple_of(b * toks, QB), toks)
        with jax.named_scope("f_proj"):
            mid = (xv[b].astype(F32) + dot(ot[:, cols], wo[:], TN)).astype(BF)
            xm[cols, :] = mid
            h = normed(mid, gm[:])
            hm[cols, :] = h
            hmt[:, cols] = h.T
        for c in keeps(b)[3:]:
            c.start()

    keep_qr, keep_lse = (pltpu.make_async_copy(*ends, ld.at[i]) for i, ends in enumerate(((qr, qr_h), (lse, lse_h))))
    load_w[3].wait()
    for blk in range(tb):
        pb[blk][:] = jnp.zeros(pb[blk].shape, BF)

    def walk(i):
        it = i - 1

        @pl.when((lax.rem(i, n_pairs) == 0) & (i < n_steps))
        def _():
            halo_in(i // n_pairs)

        @pl.when(i == 0)
        def _():
            score(0)

        @pl.when((i > 0) & (i <= n_steps))
        def _():
            with jax.named_scope("f_attn"):
                mix(jnp.maximum(it - 1, 0))
                for blk in range(tb):
                    soften(it, blk)
                score(jnp.minimum(i, n_steps - 1))

        @pl.when(i == n_steps)
        def _():
            for b in range(rows):
                push_q(b).wait()
            keep_qr.start()

        @pl.when(i > n_steps)
        def _():
            mix(n_steps - 1)

        @pl.when((lax.rem(it, n_pairs) == 0) & (it > 0))
        def _():
            project(it // n_pairs - 1)

    cdiv_loop(n_steps + 2, walk)
    with jax.named_scope("f_store_wait"):
        keep_lse.start()
        keep_hat.wait()
        keep_q.wait()
        keep_qr.wait()
        keep_lse.wait()
        for b in range(rows):
            for c in keeps(b):
                c.wait()


def any_spec(k):
    return [pl.BlockSpec(memory_space=pl.ANY)] * k


def vmem_spec(k):
    return [pl.BlockSpec(memory_space=pltpu.VMEM)] * k


def run_fwd(n, x, pos, invf, ga, gm, wq, wk, wv, wo, head_dim):
    rows, toks, width = x.shape
    hd = wq.shape[0]
    ext, total, n_halo = toks + WINDOW, rows * toks, rows * WINDOW
    half = head_dim // 2
    sds = lambda *s: jax.ShapeDtypeStruct(s, BF)
    dma = lambda *s: pltpu.SemaphoreType.DMA(s)
    outs = [sds(hd, total), sds(hd, rows * ext), sds(rows * ext, hd), sds(rows * ext, hd), sds(width, total), sds(hd, total), sds(total, width), sds(total, width), sds(width, total)]
    outs += [sds(hd, n_halo), jax.ShapeDtypeStruct((rows * hd // (2 * head_dim), 8, 2 * QB), F32)] + [jax.ShapeDtypeStruct((half, total), F32)] * 2
    vm = lambda *s: pltpu.VMEM(s, BF)
    vf = lambda *s: pltpu.VMEM(s, F32)
    scratch = [pltpu.VMEM((rows, toks), jnp.int32), vf(*invf.shape), vf(*ga.shape), vf(*ga.shape), vm(rows, toks, width), vm(rows, WINDOW, width), vm(hd, n_halo), vf(rows * hd // (2 * head_dim), 8, 2 * QB), pltpu.VMEM((rows, toks), jnp.int32), vm(hd, width), vm(hd, width), vm(hd, width), vm(hd, width),
               vm(hd, total), vm(hd, rows * ext), vm(rows * ext, hd), vm(rows * ext, hd), vm(hd, rows * ext), vm(width, total), vm(hd, total), vm(total, width), vm(total, width), vm(width, total), vm(total, width), vm(WINDOW, width),
               vf(hd, total), vf(hd, total), vf(hd, WINDOW), vf(hd, WINDOW), vf(half, n_halo), vf(half, n_halo),
               *[f(3 * QB, 2 * QB) for f in (vf, vm) for _ in range(3)],
               dma(rows + 4), dma(4), dma(2 + 7 * rows), dma(rows + 1), dma(rows + 1), dma(rows), dma(rows)]
    return pl.pallas_call(
        functools.partial(fwd_kernel, n, head_dim), out_shape=outs,
        in_specs=any_spec(9), out_specs=any_spec(11) + vmem_spec(2), scratch_shapes=scratch,
        compiler_params=pltpu.CompilerParams(collective_id=0, has_side_effects=True, vmem_limit_bytes=VMEM_LIMIT),
        name="forward")(x, pos, invf, ga, gm, wq, wk, wv, wo)


LAG = 2
SLOTS = 2 * LAG
RING = 8
CB = 256


def at(ref, *idx):
    return ref.at[idx]


class Torus:
    def __init__(self, n, head, last, turn, parts, recv0, recv1, recv2, recv3, recv4, recv5, acc, acc2, fin, snd, rcv):
        assert math.isqrt(n // 2) == 4
        me = lax.axis_index("seq")
        self.core = lax.rem(me, 2)
        chip = me // 2
        self.x, self.y = lax.rem(chip, 4), chip // 4
        self.head, self.last, self.turn = head, last, turn
        self.parts, self.recv0, self.recv1, self.recv2, self.recv3, self.recv4, self.recv5 = parts, recv0, recv1, recv2, recv3, recv4, recv5
        self.acc, self.acc2, self.fin, self.snd, self.rcv = acc, acc2, fin, snd, rcv
        self.partner = me + 1 - 2 * self.core
        self.rows, self.columns = [lax.rem(self.y + d, 4) * 4 for d in range(4)], [lax.rem(self.x + d, 4) for d in range(4)]
        self.hops = [[self.device(0, d) for d in range(4)], [self.device(d, 0) for d in range(4)]]

    def device(self, dy, dx):
        return (self.rows[dy] + self.columns[dx]) * 2 + self.core

    def copy(self, lane, kind, slot, src, dst, target):
        return pltpu.make_async_remote_copy(
            src_ref=src, dst_ref=dst, send_sem=self.snd.at[lane, kind, slot], recv_sem=self.rcv.at[lane, kind, slot],
            device_id={"seq": target}, device_id_type=MESH)

    def late(self, pair, yes, no):
        first, end = self.turn
        return jnp.where((pair >= first) & (pair < end), yes, no)

    def swap(self, ring, slot):
        return self.copy(0, 0, slot, self.parts.at[ring, :, :, 1 - self.core], self.recv0.at[slot], self.partner)

    def landing(self, stage):
        return (self.recv0, self.recv1, self.recv2, self.recv3, self.recv4, self.recv5)[stage]

    def arrived(self, stage, kind, slot):
        whole = self.landing(stage).at[kind, slot]
        self.copy(stage, kind, slot, whole, whole, self.partner).wait()

    def send(self, stage, kind, pair, held, slot):
        axis = kind if stage < 3 else 1 - kind
        plus, minus = self.hops[axis][1], self.hops[axis][-1]
        half = CB // 2
        if stage == 1:
            if axis == 0:
                minus = self.late(pair, plus, minus)
            ends = self.acc.at[kind, held, 2, :2], self.acc.at[kind, held, 2, 2:]
        elif stage == 2:
            ends = self.acc.at[kind, held, 1], self.acc.at[kind, held, 3]
        elif stage == 3:
            ends = self.acc2.at[kind, held, 2, :, :half], self.acc2.at[kind, held, 2, :, half:]
        else:
            ends = self.acc2.at[kind, held, 1], self.acc2.at[kind, held, 3]
        for i, src in enumerate(ends):
            self.copy(stage, kind, slot, src, self.landing(stage).at[kind, slot, i], (plus, minus)[i]).start()

    def add(self, stage, kind, pair, held, slot, ring):
        acc, acc2 = self.acc, self.acc2
        if stage == 1:
            for r1 in range(4):
                for r2 in range(4):
                    ry, rx = (r2, r1) if kind == 0 else (r1, r2)
                    chip = self.rows[ry] + self.columns[rx]
                    acc[kind, held, r1, r2] = self.parts[ring, kind, chip, self.core] + self.recv0[slot, kind, chip]
        elif stage == 2:
            back = self.late(pair, 1, 3) if kind == 0 else 3
            acc[kind, held, 1, :2] += self.recv1[kind, slot, 0]
            acc[kind, held, back, 2:] += self.recv1[kind, slot, 1]
        elif stage == 3:
            acc2[kind, held] = acc[kind, held, 0] + (self.recv2[kind, slot, 0] + self.recv2[kind, slot, 1])
        elif stage == 4:
            half = CB // 2
            acc2[kind, held, 1, :, :half] += self.recv3[kind, slot, 0]
            acc2[kind, held, 3, :, half:] += self.recv3[kind, slot, 1]
        else:
            self.fin[pair, kind] = acc2[kind, held, 0] + (self.recv4[kind, slot, 0] + self.recv4[kind, slot, 1])

    def direct(self, kind, held, slot):
        for d in range(1, 4):
            self.copy(5, kind, slot, self.acc2.at[kind, held, d], self.recv5.at[kind, slot, d - 1], self.hops[1 - kind][d]).start()

    def early(self, pair):
        return (pair >= 0) & (pair <= self.head)

    def final(self, pair):
        return (pair == self.last) | ((pair > self.head) & (pair < self.last) & (mod(abs(pair - self.head), 2) == 0))

    def when(self, which, fn):
        if isinstance(which, bool):
            fn() if which else None
        else:
            pl.when(which)(fn)

    def offer(self, t):
        self.when(self.early(t) | self.final(t), lambda: self.swap(mod(t, RING), mod(t, SLOTS)).start())

    def tick(self, t):
        self.offer(t)
        self.advance(t)

    def advance(self, t, tail=False):
        now, land, before = mod(t, SLOTS), mod(t + SLOTS - LAG, SLOTS), mod(t + SLOTS - 1, SLOTS)
        ring_land = mod(t + RING - 1, RING)
        for stage in range(5, 0, -1):
            pair = t - LAG * stage + 1
            held = before if stage % 2 else mod(t + 1, SLOTS)

            def move(last_hops, stage=stage, pair=pair, held=held):
                if stage == 1:
                    with jax.named_scope("t_wait1"):
                        self.swap(ring_land, before).wait()
                for kind in range(2):
                    if last_hops and stage == 4:
                        with jax.named_scope("t_wait6"):
                            self.arrived(5, kind, land)
                        got = self.recv5[kind, land]
                        self.fin[pair, kind] = self.acc2[kind, held, 0] + (got[0] + got[1] + got[2])
                        continue
                    if stage > 1:
                        with jax.named_scope(f"t_wait{stage}"):
                            self.arrived(stage - 1, kind, land)
                    self.add(stage, kind, pair, held, land if stage > 1 else before, ring_land)
                    if last_hops and stage == 3:
                        self.direct(kind, held, now)
                    elif stage < 5:
                        self.send(stage, kind, pair, held, now)

            if stage < 3:
                self.when(self.early(pair) | self.final(pair), functools.partial(move, False))
            else:
                self.when(self.early(pair), functools.partial(move, False))
                if tail and stage < 5:
                    self.when(self.final(pair), functools.partial(move, True))


def pick(i, table):
    out = 0
    for key, value in table.items():
        out = jnp.where(i == key, value, out)
    return out


def norm_back(x, gain, grad, res):
    xf = x.astype(F32)
    inv = lax.rsqrt(jnp.mean(xf * xf, axis=-1, keepdims=True) + NORM_EPS)
    unit = xf * inv
    gu = grad * gain
    out = inv * (gu - unit * jnp.mean(gu * unit, axis=-1, keepdims=True)) + res.astype(F32)
    gu = grad * unit
    return out.astype(BF), jnp.sum(gu.reshape(-1, 8, gu.shape[-1]), axis=0)


def plan(n_mlp, n_down, nc):
    order = [("o", g) for g in range(nc)] + [(name, g) for g in range(nc) for name in "qkv"]
    base, head = n_mlp + n_down, n_mlp + n_down + nc - 1
    last = 2 * (base - 1 - head + len(order) // 2) + head - 1
    spot = lambda pair: min(max(pair, 2 * pair - head), last)
    return head, {name: (spot(base + i // 2), i % 2) for i, name in enumerate(order)}, last


def bwd_kernel(n, head_dim, dims, ga_h, gm_h, x_h, dout_h, q_h, kt_h, k_h, v_h, hat_h, ot_h, xm_h, hm_h, hmt_h, qr_h, lse_h, cos_h, sin_h,
               wq_h, wk_h, wv_h, wo_h, wg_h, wu_h, wd_h,
               dx_h, fin_h,
               parts, recv0, recv1, recv2, recv3, recv4, recv5, acc, acc2, fin, snd, rcv,
               dor, lser, deltar, hsnd, hrcv, osnd, orcv, gsend, grecv, gsem, ld,
               xbuf, mbuf, gnm, gmid, ot, hat, wo, dot_, lse, delta, cos_i, sin_i, ga, gm, dgain):
    rows, toks, width, hd, ff = dims
    ext, total = toks + WINDOW, rows * toks
    pw = 2 * head_dim
    n_pairs = hd // pw
    tb, n_steps = toks // QB, n_pairs * rows
    nb, nc, sub = ff // CB, width // CB, ff // width
    rpd = width // n
    per, half_sub = CB // pw, sub // 2
    head, place, end = plan(nb, nc * half_sub, nc)
    comm = Torus(n, head, end, (nb, nb + n_pairs + 1), parts, recv0, recv1, recv2, recv3, recv4, recv5, acc, acc2, fin, snd, rcv)
    me = lax.axis_index("seq")
    left = lax.rem(me + n - 1, n)
    barrier = pltpu.get_barrier_semaphore()

    def greet(i):
        pl.semaphore_signal(barrier, inc=1, device_id={"seq": lax.rem(me + i + 1, n)}, device_id_type=MESH)

    def load(i, s, d):
        c = pltpu.make_async_copy(s, d, ld.at[i])
        c.start()
        return c

    def late(i):
        s, d = ((xm_h, mbuf), (ot_h, ot), (hat_h, hat), (wo_h, wo), (lse_h, lse), (cos_h, cos_i), (sin_h, sin_i), (ga_h, ga), (gm_h, gm))[i]
        return pltpu.make_async_copy(s, d, ld.at[1 + i])

    def to_left(src, dst, send_sem, recv_sem):
        return pltpu.make_async_remote_copy(src_ref=src, dst_ref=dst, send_sem=send_sem, recv_sem=recv_sem,
                                            device_id={"seq": left}, device_id_type=MESH)

    n_late = 9

    def push_rows(i):
        return to_left(*((lse_h, lser), (delta, deltar))[i], hsnd.at[i], hrcv.at[i])

    def push_out(p):
        pr = pl.ds(aligned(p * pw, pw), pw)
        return [to_left(dot_.at[pr, pl.ds(b * toks, WINDOW)], dor.at[pr, pl.ds(b * WINDOW, WINDOW)], osnd.at[p], orcv.at[p])
                for b in range(rows)]

    def give_out(p):
        for c in push_out(p):
            c.start()

    def put(spot, value):
        pair, kind = spot
        parts[mod(pair, RING), kind] = value.reshape(n // 2, 2, rpd, CB)

    def spot_of(name, g):
        known = {i: place[name, i] for i in range(nc)}
        return pick(g, {i: s[0] for i, s in known.items()}), pick(g, {i: s[1] for i, s in known.items()})

    def spots(it, blk):
        p, b = it // rows, mod(it, rows)
        pr = pl.ds(aligned(p * pw, pw), pw)
        return pr, pl.ds(aligned(b * toks + blk * QB, QB), QB), pl.ds(aligned(b * ext + blk * QB, QB), 3 * QB)

    def row_of(it):
        return mod(it, rows) * n_pairs + it // rows

    def mlp(hm, hmt, actt, wgu, wd, dgu, wld):
        def weights(j, slot):
            c = aligned(j * CB, CB)
            return [pltpu.make_async_copy(wg_h.at[:, pl.ds(c, CB)], wgu.at[slot, :, :CB], wld.at[slot, 0]),
                    pltpu.make_async_copy(wu_h.at[:, pl.ds(c, CB)], wgu.at[slot, :, CB:], wld.at[slot, 1]),
                    pltpu.make_async_copy(wd_h.at[pl.ds(c, CB), :], wd.at[slot], wld.at[slot, 2])]

        for c in weights(0, 0):
            c.start()
        ld_hm, ld_x, ld_hmt = load(10, hm_h, hm), load(0, dout_h, xbuf), load(11, hmt_h, hmt)
        cdiv_loop(n - 1, greet)
        gnm[:] = jnp.zeros_like(gnm)
        gsend[:] = jnp.zeros_like(gsend)
        dgain[:] = jnp.zeros_like(dgain)
        ld_hm.wait()
        ld_x.wait()
        ld_hmt.wait()
        for i in range(n_late):
            late(i).start()

        def block(j):
            slot = lax.rem(j, 2)
            for c in weights(j, slot):
                c.wait()

            @pl.when(j + 1 < nb)
            def _():
                for c in weights(j + 1, 1 - slot):
                    c.start()

            c0 = pl.multiple_of(j * CB, CB)
            with jax.named_scope("b_mlp"):
                for b in range(rows):
                    r = slice(b * toks, (b + 1) * toks)
                    gu = dot(hm[r, :], wgu[slot])
                    gact = dot(xbuf[r, :], wd[slot], NT).astype(BF).astype(F32)
                    gate, up = gu[:, :CB], gu[:, CB:]
                    sig = 1.0 / (1.0 + jnp.exp(-gate))
                    swish = gate * sig
                    actt[pl.ds(c0, CB), r] = (swish * up).astype(BF).T
                    dgu[r, :CB] = (gact * up * (sig + swish * (1.0 - sig))).astype(BF)
                    dgu[r, CB:] = (gact * swish).astype(BF)
                both = dot(hmt[:], dgu[:])
                ring = lax.rem(j, RING)
                parts[ring, 0] = both[:, :CB].reshape(n // 2, 2, rpd, CB)
                parts[ring, 1] = both[:, CB:].reshape(n // 2, 2, rpd, CB)
                for b in range(rows):
                    r = slice(b * toks, (b + 1) * toks)
                    gnm[r, :] += dot(dgu[r, :], wgu[slot], NT)

            @pl.when(j == 0)
            def _():
                pl.semaphore_wait(barrier, n - 1)
                push_rows(0).start()

            comm.tick(j)

        cdiv_loop(nb, block)

        def down(c):
            share = n // 2 // sub
            c0 = pl.multiple_of(c * CB, CB)
            for m in range(sub):
                res = dot(actt[m * width:(m + 1) * width, :], xbuf[:, pl.ds(c0, CB)]).reshape(share, 2, sub, rpd, CB)
                for i in range(sub):
                    pair = nb + c * half_sub + i // 2
                    parts[lax.rem(pair, RING), i % 2, m * share:(m + 1) * share] = res[:, :, i]

        for i in range(n_late):
            late(i).wait()

        def mid(b):
            for i in range(tb):
                r = pl.ds(pl.multiple_of((b * tb + i) * QB, QB), QB)
                out, dg = norm_back(mbuf[r, :], gm[:], gnm[r, :], xbuf[r, :])
                gmid[r, :] = out
                dgain[8:, :] += dg

        def deltas(p):
            for it in range(rows):
                for blk in range(tb):
                    pr, cols, _ = spots(p * rows + it, blk)
                    both = dot_[pr, cols].astype(F32) * ot[pr, cols].astype(F32)
                    delta[row_of(p * rows + it), blk:blk + 1, :] = jnp.concatenate(
                        [col_sum(both[:head_dim]), col_sum(both[head_dim:])], axis=1)

        def column(c):
            with jax.named_scope("b_down"):
                down(c)
            comm.tick(nb + c + jnp.minimum(c, 1))

            @pl.when(c > 0)
            def _():
                give_out(c)

            @pl.when(c == 0)
            def _():
                with jax.named_scope("b_mid"):
                    cdiv_loop(rows, mid)
                with jax.named_scope("b_dot"):
                    dot_[:] = dot(wo[:], gmid[:], NT).astype(BF)
                    cdiv_loop(n_pairs, deltas)
                comm.tick(nb + 1)
                push_rows(1).start()
                give_out(0)

        cdiv_loop(nc, column)

    vm = lambda *s: pltpu.VMEM(s, BF)
    vf = lambda *s: pltpu.VMEM(s, F32)
    pl.run_scoped(mlp, vm(total, width), vm(width, total), vm(ff, total), vm(2, width, 2 * CB), vm(2, CB, width), vm(total, 2 * CB),
                  pltpu.SemaphoreType.DMA((2, 3)))
    def attention(q, kt, k, v, qr, dv, sc0, sc1, sc2, sr, dp0, dp1, dp2, dr, pb0, pb1, pb2, pr_, ds0, ds1, ds2, dsr):
        dqt, dkt = ot, q
        wq, wk, wv = k.at[:hd], kt.at[:, :width], v.at[:hd]
        sc, dp, pb, ds = (sc0, sc1, sc2), (dp0, dp1, dp2), (pb0, pb1, pb2), (ds0, ds1, ds2)
        lds = [load(10 + i, s, d) for i, (s, d) in enumerate(((q_h, q), (k_h, k), (v_h, v), (qr_h, qr), (kt_h, kt)))]

        def out_grad(g):
            put(spot_of("o", g), dot(ot[:], gmid[:, pl.ds(pl.multiple_of(g * CB, CB), CB)]))

        with jax.named_scope("b_dwo"):
            cdiv_loop(nc, out_grad)
        first_tick = nb + nc + 1
        upper = upper_mask()
        first, last = me == 0, me == n - 1
        halves = slice(0, WINDOW), slice(WINDOW, 3 * QB)

        def right(it, i):
            p, b = it // rows, mod(it, rows)
            return pl.ds(aligned(p * pw, pw), pw), pl.ds(aligned(b * WINDOW + i * QB, QB), QB), pl.ds(aligned(b * ext + toks + i * QB, QB), WINDOW - i * QB)

        def score(it):
            for blk in range(tb):
                pr, cols, keys = spots(it, blk)
                sc[blk][:] = dot(k[keys, pr], stack_pair(q[pr, cols]))
                dp[blk][:] = dot(v[keys, pr], stack_pair(dot_[pr, cols]))
            for i, rs in enumerate(halves):
                pr, cols, keys = right(it, i)
                sr[rs, :] = dot(k[keys, pr], stack_pair(qr[pr, cols]))
                dr[rs, :] = dot(v[keys, pr], stack_pair(dor[pr, cols]))

        def soften(it):
            row = row_of(it)
            for blk in range(tb):
                s02, s1 = merged(sc[blk][:], upper, *start_bias(first, blk))
                norm, mean = lse[row, blk:blk + 1, :], delta[row, blk:blk + 1, :]
                p02, p1 = jnp.exp(s02 - norm), jnp.exp(s1 - norm)
                g02, g1 = jnp.where(upper, dp[blk][:QB], dp[blk][2 * QB:]), dp[blk][QB:2 * QB]
                pb[blk][:] = banded(p02, p1, upper)
                ds[blk][:] = banded(p02 * (g02 - mean), p1 * (g1 - mean), upper)
            for blk in range(tb):
                i = blk // 2
                rs = slice(blk * QB, (blk + 1) * QB)
                p = jnp.exp(sr[rs, :] - jnp.where(last, -NEG, lser[row, i:i + 1, :]))
                g = p * (dr[rs, :] - deltar[row, i:i + 1, :])
                pr_[rs, :] = (p if blk == 1 else jnp.where(upper, p, 0.0)).astype(BF)
                dsr[rs, :] = (g if blk == 1 else jnp.where(upper, g, 0.0)).astype(BF)

        def grads(it):
            ks, vs = [], []
            for blk in range(tb):
                pr, cols, keys = spots(it, blk)
                own = slice(max(0, 2 - blk) * QB, 3 * QB)
                vs.append(dot(pb[blk][own, :], stack_pair(dot_[pr, cols]), NT))
                ks.append(dot(ds[blk][own, :], stack_pair(q[pr, cols]), NT))
                dq = unstack_pair(dot(kt[pr, keys], ds[blk][:])) * (head_dim ** -0.5)
                dqt[pr, cols] = rope(dq, cos_i[:, cols], sin_i[:, cols], -1, head_dim).astype(BF)
            for i, rs in enumerate(halves):
                pr, cols, _ = right(it, i)
                vs.append(dot(pr_[rs, :], stack_pair(dor[pr, cols]), NT))
                ks.append(dot(dsr[rs, :], stack_pair(qr[pr, cols]), NT))
            for j in range(tb):
                pr, cols, _ = spots(it, j)
                gv, gk = (sum(x[i][(j - max(0, i - 2)) * QB:(j - max(0, i - 2) + 1) * QB] for i in range(j, j + 3)) for x in (vs, ks))
                dv[cols, pr] = gv.astype(BF)
                dkt[pr, cols] = rope(gk.T, cos_i[:, cols], sin_i[:, cols], -1, head_dim).astype(BF)

        def close_group(g):
            cols = pl.ds(pl.multiple_of(g * CB, CB), CB)
            with jax.named_scope("b_dwqkv"):
                put(spot_of("q", g), dot(hat[:], dqt[cols, :], NT))
                put(spot_of("k", g), dot(hat[:], dkt[cols, :], NT))
                put(spot_of("v", g), dot(hat[:], dv[:, cols]))

        def weights():
            return [pltpu.make_async_copy(s, d, ld.at[10 + i]) for i, (s, d) in enumerate(((wq_h, wq), (wk_h, wk), (wv_h, wv), (x_h, xbuf)))]

        def arrived(p):
            whole = dor.at[pl.ds(aligned(p * pw, pw), pw), :]
            with jax.named_scope("b_hwait"):
                to_left(whole, whole, osnd.at[p], orcv.at[p]).wait()

        def walk(it):
            ahead = it + 1

            @pl.when((lax.rem(ahead, rows) == 0) & (ahead < n_steps))
            def _():
                arrived(ahead // rows)

            @pl.when(it < n_steps)
            def _():
                with jax.named_scope("b_attn"):
                    grads(it - 1)
                    soften(it)
                    score(jnp.minimum(ahead, n_steps - 1))

            @pl.when(it == n_steps)
            def _():
                grads(n_steps - 1)
                for c in weights():
                    c.start()

            p, step = it // rows - 1, lax.rem(it, rows)

            @pl.when((step == 0) & (lax.rem(p, per) == per - 1))
            def _():
                close_group(p // per)

            now = first_tick + 1 + p + step // (rows - 1)
            twice = now - head

            @pl.when(it == n_steps)
            def _():
                comm.offer(end)

            @pl.when((step == 0) | ((step == rows - 1) & ((twice > 0) | (p < 0))))
            def _():
                comm.tick(now + jnp.maximum(twice - step // (rows - 1), 0) + jnp.minimum(p, 0))

            @pl.when((step == 0) & (p + 3 < n_pairs))
            def _():
                give_out(p + 3)

        for c in lds[:-1]:
            c.wait()
        for i in range(2):
            push_rows(i).wait()
        arrived(0)
        score(0)
        soften(0)
        score(1)
        lds[-1].wait()
        cdiv_loop(n_steps, lambda i: walk(i + 1))
        for c in weights():
            c.wait()

        def into(b):
            r = pl.ds(aligned(b * toks, QB), toks)
            with jax.named_scope("b_into"):
                gnm[r, :] = dot(dqt[:, r], wq[:], TN) + dot(dkt[:, r], wk[:], TN) + dot(dv[r, :], wv[:])

            with jax.named_scope("b_final"):
                for i in range(tb):
                    r = pl.ds(aligned((b * tb + i) * QB, QB), QB)
                    out, dg = norm_back(xbuf[r, :], ga[:], gnm[r, :], gmid[r, :])
                    mbuf[r, :] = out
                    dgain[:8, :] += dg

        def share_gains():
            out_copy.start()
            gains = jnp.concatenate([col_sum(dgain[:8, :]), col_sum(dgain[8:, :]), jnp.zeros((6, width), F32)], axis=0)
            for p in range(n):
                gsend[p, :, :rpd] = gains[:, p * rpd:(p + 1) * rpd]

            def spread(i):
                to = lax.rem(me + i + 1, n)
                pltpu.make_async_remote_copy(src_ref=gsend.at[to], dst_ref=grecv.at[i], send_sem=gsem.at[0], recv_sem=gsem.at[1],
                                             device_id={"seq": to}, device_id_type=MESH).start()

            cdiv_loop(n - 1, spread)

        def finish(i):
            comm.advance(end + i, True)

            @pl.when(i == 1)
            def _():
                cdiv_loop(rows - 1, into)

            @pl.when(i == LAG + 1)
            def _():
                into(rows - 1)
                share_gains()

        cdiv_loop(4 * LAG - 1, finish)

    score_bufs = [f(3 * QB, 2 * QB) for f in (vf, vm) for _ in range(8)]
    out_copy = pltpu.make_async_copy(mbuf, dx_h, ld.at[0])
    pl.run_scoped(attention, vm(hd, total), vm(hd, rows * ext), vm(rows * ext, hd), vm(rows * ext, hd), vm(hd, rows * WINDOW), vm(total, hd), *score_bufs)
    most, rest = pl.ds(0, end), pl.ds(end, 2)
    keep_most = load(1, fin.at[most], fin_h.at[most])
    to_left(gsend.at[pl.ds(0, n - 1)], grecv, gsem.at[0], gsem.at[1]).wait()
    sums = gsend[me]
    for i in range(n - 1):
        sums = sums + grecv[i]
    fin[end + 1, 0, :8, :128] = sums
    out_copy.wait()
    comm.advance(end + 4 * LAG - 1, True)
    with jax.named_scope("b_end"):
        keep_rest = load(0, fin.at[rest], fin_h.at[rest])
        keep_most.wait()
        keep_rest.wait()


def spread_kernel(dims, dx_i, fin_i, dx_o, dga_o, dgm_o, *refs):
    head_dim, n, width, ff = dims
    outs, (buf, fin), stage, sem = refs[:7], refs[7:9], refs[9:16], refs[16]
    dq, dk, dv, do, dg, du, dd = stage
    nb, nc, sub = ff // CB, width // CB, ff // width
    rpd = width // n
    head, place, end = plan(nb, nc * sub // 2, nc)
    get_fin = pltpu.make_async_copy(fin_i, fin, sem.at[len(outs)])
    get_fin.start()
    cut = buf.shape[0] // nc
    gets, puts = ([pltpu.make_async_copy(s.at[pl.ds(i * cut, cut)], d.at[pl.ds(i * cut, cut)], sem.at[len(outs) + k + i]) for i in range(nc)]
                  for k, s, d in ((1, dx_i, buf), (nc + 1, buf, dx_o)))
    for c in gets:
        c.start()
    get_fin.wait()
    gains = fin[end + 1, 0]
    dga_o[:] = gains[:1, :rpd]
    dgm_o[:] = gains[1:2, :rpd]
    for j in range(nb):
        dg[:, j * CB:(j + 1) * CB] = fin[j, 0]
        du[:, j * CB:(j + 1) * CB] = fin[j, 1]
    for c in range(nc):
        for i in range(sub):
            pair = nb + (c * sub + i) // 2
            dd[i * rpd:(i + 1) * rpd, c * CB:(c + 1) * CB] = fin[pair, i % 2]
    for g in range(nc):
        do[:, g * CB:(g + 1) * CB] = fin[place["o", g]]
        for name, ref in (("q", dq), ("k", dk), ("v", dv)):
            val = fin[place[name, g]]
            for h in range(CB // head_dim):
                ref[g * (CB // head_dim) + h] = val[:, h * head_dim:(h + 1) * head_dim]
    keeps = [pltpu.make_async_copy(s, d, sem.at[i]) for i, (s, d) in enumerate(zip(stage, outs))]
    for c in keeps:
        c.start()
    for get, out in zip(gets, puts):
        get.wait()
        out.start()
    for c in keeps + puts:
        c.wait()


def run_bwd(n, head_dim, ga, gm, x, dout, q, kt, k, v, hat, ot, xm, hm, hmt, qr, lse, cos_t, sin_t, wq, wk, wv, wo, wg, wu, wd, rows):
    total, width = x.shape
    hd, ff = wq.shape[0], wg.shape[1]
    toks = total // rows
    rpd, heads = width // n, hd // head_dim
    nb, nc, sub = ff // CB, width // CB, ff // width
    slots = plan(nb, nc * sub // 2, nc)[2] + 2
    n_pairs = hd // (2 * head_dim)
    f = lambda *s: jax.ShapeDtypeStruct(s, F32)
    dx_t = jax.ShapeDtypeStruct((total, width), BF)
    vm = lambda *s: pltpu.VMEM(s, BF)
    vf = lambda *s: pltpu.VMEM(s, F32)
    dma = lambda *s: pltpu.SemaphoreType.DMA(s)
    line, duo = vf(rows * n_pairs, 8, 2 * QB), (2, SLOTS)
    scratch = [vf(RING, 2, n // 2, 2, rpd, CB), vf(SLOTS, 2, n // 2, rpd, CB), vf(*duo, 2, 2, rpd, CB), vf(*duo, 2, 4, rpd, CB),
               vf(*duo, 2, rpd, CB // 2), vf(*duo, 2, rpd, CB), vf(*duo, 3, rpd, CB), vf(*duo, 4, 4, rpd, CB), vf(*duo, 4, rpd, CB), vf(slots, 2, rpd, CB),
               dma(6, *duo), dma(6, *duo),
               vm(hd, rows * WINDOW), line, line, dma(2), dma(2), dma(n_pairs), dma(n_pairs),
               vf(n, 8, 128), vf(n - 1, 8, 128), dma(2), dma(15),
               vm(total, width), vm(total, width), vf(total, width), vm(total, width), vm(hd, total), vm(width, total), vm(hd, width), vm(hd, total), line, line, vf(*cos_t.shape), vf(*cos_t.shape), vf(*ga.shape), vf(*ga.shape), vf(16, width)]
    mid = pl.pallas_call(
        functools.partial(bwd_kernel, n, head_dim, (rows, toks, width, hd, ff)), out_shape=[dx_t, f(slots, 2, rpd, CB)],
        in_specs=any_spec(24), out_specs=any_spec(2), scratch_shapes=scratch,
        compiler_params=pltpu.CompilerParams(collective_id=1, has_side_effects=True, vmem_limit_bytes=VMEM_LIMIT),
        name="backward")(ga, gm, x, dout, q, kt, k, v, hat, ot, xm, hm, hmt, qr, lse, cos_t, sin_t, wq, wk, wv, wo, wg, wu, wd)
    outs = [f(heads, rpd, head_dim)] * 3 + [f(rpd, width), f(rpd, ff), f(rpd, ff), f(ff // n, width)]
    return pl.pallas_call(
        functools.partial(spread_kernel, (head_dim, n, width, ff)), out_shape=[dx_t, f(1, rpd), f(1, rpd)] + outs,
        in_specs=any_spec(2), out_specs=any_spec(1) + vmem_spec(2) + any_spec(7),
        scratch_shapes=[vm(total, width), vf(slots, 2, rpd, CB), *[vf(*o.shape) for o in outs], dma(8 + 2 * nc)],
        name="spread")(*mid)


def solution(mesh):
    n = mesh.shape["seq"]

    def device_step(hidden, positions, g_attn, g_mlp, w_query, w_key, w_value, w_out, w_gate, w_up, w_down, d_out):
        rows, toks, width = hidden.shape
        layers, _, heads, head_dim = w_query.shape
        hd = heads * head_dim
        half = head_dim // 2
        inv_freq = 1.0 / (10000.0 ** (jnp.arange(half, dtype=F32) * (2.0 / head_dim)))
        turn = lambda w: w[0].transpose(1, 2, 0).reshape(hd, width)
        wq, wk, wv = turn(w_query), turn(w_key), turn(w_value)
        fwd = run_fwd(n, hidden, positions, inv_freq[:, None], g_attn, g_mlp, wq, wk, wv, w_out[0], head_dim)
        out = run_bwd(n, head_dim, g_attn, g_mlp, hidden.reshape(rows * toks, width), d_out.reshape(rows * toks, width), *fwd,
                      wq, wk, wv, w_out[0], w_gate[0], w_up[0], w_down[0], rows)
        dx, dga, dgm, dq, dk, dv, do, dg, du, dd = out
        back = lambda w: w.transpose(1, 0, 2)[None]
        return (dx.reshape(rows, toks, width), dga, dgm, back(dq), back(dk), back(dv), do[None], dg[None], du[None], dd[None])

    tok_spec, grad_spec = P("data", "seq"), P(None, ("data", "seq"))
    in_specs = (tok_spec, tok_spec) + (P(),) * 9 + (tok_spec,)
    out_specs = (tok_spec,) + (grad_spec,) * 9
    return jax.shard_map(device_step, mesh=mesh, in_specs=in_specs, out_specs=out_specs, check_vma=False)
```

```python
import functools, math
import numpy as np
import jax, jax.numpy as jnp
from jax import lax
from jax.experimental import pallas as pl
from jax.experimental.pallas import tpu as pltpu
from jax.sharding import PartitionSpec as P

WINDOW = 256
NORM_EPS = 1e-5
QB = 128
BF, F32 = jnp.bfloat16, jnp.float32
NN, NT, TN = ((1,), (0,)), ((1,), (1,)), ((0,), (0,))
MESH = pl.DeviceIdType.MESH
NEG = -1e30
VMEM_LIMIT = 67043328


def dot(a, b, dims=NN):
    return lax.dot_general(a, b, (dims, ((), ())), preferred_element_type=F32)


def cdiv_loop(n, body):
    lax.fori_loop(0, n, lambda i, c: body(i) or c, 0)


def mod(a, b):
    return a % b if isinstance(a, int) else lax.rem(a, b)


def aligned(a, b):
    return a if isinstance(a, int) else pl.multiple_of(a, b)


def rope(blk, cos_b, sin_b, sign, head_dim):
    half = head_dim // 2
    parts = []
    for h in range(blk.shape[0] // head_dim):
        first = blk[h * head_dim:h * head_dim + half]
        second = blk[h * head_dim + half:(h + 1) * head_dim]
        if sign > 0:
            parts += [first * cos_b - second * sin_b, second * cos_b + first * sin_b]
        else:
            parts += [first * cos_b + second * sin_b, second * cos_b - first * sin_b]
    return jnp.concatenate(parts, axis=0)


def normed(x, gain):
    xf = x.astype(F32)
    inv = lax.rsqrt(jnp.mean(xf * xf, axis=-1, keepdims=True) + NORM_EPS)
    return (xf * inv * gain).astype(BF)


def stack_pair(pair_t):
    half = pair_t.shape[0] // 2
    zero = jnp.zeros((half, pair_t.shape[1]), pair_t.dtype)
    return jnp.concatenate(
        [jnp.concatenate([pair_t[:half], zero], axis=0), jnp.concatenate([zero, pair_t[half:]], axis=0)], axis=1)


def unstack_pair(both):
    half, cols = both.shape[0] // 2, both.shape[1] // 2
    return jnp.concatenate([both[:half, :cols], both[half:, cols:]], axis=0)


def col_sum(x):
    return jnp.sum(x, axis=0, keepdims=True)


def merged(scores, upper, bias0, bias1):
    return jnp.where(upper, scores[:QB] + bias0, scores[2 * QB:]), scores[QB:2 * QB] + bias1


def banded(p02, p1, upper):
    return jnp.concatenate(
        [jnp.where(upper, p02, 0.0).astype(BF), p1.astype(BF), jnp.where(upper, 0.0, p02).astype(BF)], axis=0)


def upper_mask():
    key_ids = lax.broadcasted_iota(jnp.int32, (QB, 2 * QB), 0)
    query_ids = lax.broadcasted_iota(jnp.int32, (QB, 2 * QB), 1) % QB
    return key_ids > query_ids


def start_bias(first, blk):
    bias = jnp.where(first, NEG, 0.0).astype(F32)
    return (bias if blk < 2 else 0.0), (bias if blk < 1 else 0.0)


def fwd_kernel(n, head_dim, x_h, pos_h, invf_h, ga_h, gm_h, wq_h, wk_h, wv_h, wo_h,
               q_h, kt_h, k_h, v_h, hat_h, ot_h, xm_h, hm_h, hmt_h, qr_h, lse_h, cos_t, sin_t,
               pos, invf, ga, gm, xv, halo, qr, lse, pos_halo, wq, wk, wv, wo, q, kt, k, v, vt, hat, ot, xm, hm, hmt, hb, hh, acc, acc2, ak, av, cos_h, sin_h,
               sc0, sc1, sc2, pb0, pb1, pb2, ldx, ld, st, snd, rcv, qsnd, qrcv):
    sc, pb = (sc0, sc1, sc2), (pb0, pb1, pb2)
    rows, toks, width = xv.shape
    ext, total, pw = toks + WINDOW, rows * toks, 2 * head_dim
    n_pairs = wq.shape[0] // pw
    tb, n_steps = toks // QB, n_pairs * rows
    me = lax.axis_index("seq")
    right, left = lax.rem(me + 1, n), lax.rem(me + n - 1, n)
    load_x = [pltpu.make_async_copy(x_h.at[b], xv.at[b], ldx.at[b]) for b in range(rows)]
    load_w = [pltpu.make_async_copy(s, d, ld.at[i]) for i, (s, d) in enumerate(((wq_h, wq), (wk_h, wk), (wv_h, wv), (wo_h, wo)))]
    load_s = [pltpu.make_async_copy(s, d, ldx.at[rows + i]) for i, (s, d) in enumerate(((pos_h, pos), (invf_h, invf), (ga_h, ga), (gm_h, gm)))]
    for c in load_s + load_x:
        c.start()
    barrier = pltpu.get_barrier_semaphore()
    for other in (left, right):
        pl.semaphore_signal(barrier, inc=1, device_id={"seq": other}, device_id_type=MESH)

    def push(i, s, d):
        return pltpu.make_async_remote_copy(src_ref=s, dst_ref=d, send_sem=snd.at[i], recv_sem=rcv.at[i], device_id={"seq": right}, device_id_type=MESH)

    def push_rows(b):
        return push(b, x_h.at[b, toks - WINDOW:, :], halo.at[b])

    send_pos = push(rows, pos, pos_halo)

    def angles(cos_ref, sin_ref, positions):
        count = positions.shape[1]
        for b in range(rows):
            ang = invf[:] * positions[b:b + 1, :].astype(F32)
            cos_ref[:, b * count:(b + 1) * count] = jnp.cos(ang)
            sin_ref[:, b * count:(b + 1) * count] = jnp.sin(ang)

    for c in load_s:
        c.wait()
    angles(cos_t, sin_t, pos[:])

    def norm_rows(b):
        for i in range(tb):
            h = normed(xv[b, i * QB:(i + 1) * QB, :], ga[:])
            hb[pl.ds(pl.multiple_of((b * tb + i) * QB, QB), QB), :] = h

    with jax.named_scope("f_norm"):
        for c in load_x:
            c.wait()
        for c in load_w:
            c.start()
        cdiv_loop(rows, norm_rows)
    pl.semaphore_wait(barrier, 2)
    send_pos.start()
    for b in range(rows):
        push_rows(b).start()
    keep_hat = pltpu.make_async_copy(hat, hat_h, st.at[0])
    tables = cos_t[:], sin_t[:]

    def put_q(src):
        for p in range(n_pairs):
            r = slice(p * pw, (p + 1) * pw)
            q[r, :] = (rope(src[r, :], *tables, 1, head_dim) * (head_dim ** -0.5)).astype(BF)

    def put_own(src, dst_t, dst):
        for p in range(n_pairs):
            r = slice(p * pw, (p + 1) * pw)
            both = (rope(src[r, :], *tables, 1, head_dim) if dst is k else src[r, :]).astype(BF)
            for b in range(rows):
                blk = both[:, b * toks:(b + 1) * toks]
                own = slice(b * ext + WINDOW, (b + 1) * ext)
                dst_t[r, own] = blk
                dst[own, r] = blk.T

    with jax.named_scope("f_mm"):
        load_w[0].wait()
        load_w[1].wait()
        load_w[2].wait()
        acc[:] = dot(wq[:], hb[:], NT)
        acc2[:] = dot(wk[:], hb[:], NT)
        put_q(acc)
        acc[:] = dot(wv[:], hb[:], NT)
        put_own(acc2, kt, k)
        for i in range(total // QB):
            r = slice(i * QB, (i + 1) * QB)
            hat[:, r] = hb[r, :].T
        put_own(acc, vt, v)
    keep_hat.start()
    keep_q = pltpu.make_async_copy(q, q_h, st.at[1])
    keep_q.start()

    def push_q(b):
        return pltpu.make_async_remote_copy(src_ref=q.at[:, b * toks:b * toks + WINDOW], dst_ref=qr.at[:, b * WINDOW:(b + 1) * WINDOW],
                                            send_sem=qsnd.at[b], recv_sem=qrcv.at[b], device_id={"seq": left}, device_id_type=MESH)

    for b in range(rows):
        push_q(b).start()
    send_pos.wait()
    angles(cos_h, sin_h, pos_halo[:, toks - WINDOW:])

    def keeps(b):
        wide, cols = pl.ds(pl.multiple_of(b * ext, QB), ext), pl.ds(pl.multiple_of(b * toks, QB), toks)
        ends = ((kt.at[:, wide], kt_h.at[:, wide]), (k.at[wide, :], k_h.at[wide, :]), (v.at[wide, :], v_h.at[wide, :]),
                (ot.at[:, cols], ot_h.at[:, cols]), (hm.at[cols, :], hm_h.at[cols, :]), (hmt.at[:, cols], hmt_h.at[:, cols]),
                (xm.at[cols, :], xm_h.at[cols, :]))
        return [pltpu.make_async_copy(s, d, st.at[2 + b * len(ends) + i]) for i, (s, d) in enumerate(ends)]

    def halo_in(b):
        with jax.named_scope("f_halo_wait"):
            push_rows(b).wait()
        with jax.named_scope("f_halo"):
            for i in range(WINDOW // QB):
                r = slice(i * QB, (i + 1) * QB)
                hh[r, :] = normed(halo[b, r, :], ga[:])
            ak[:] = dot(wk[:], hh[:], NT)
            av[:] = dot(wv[:], hh[:], NT)
            cols = pl.ds(pl.multiple_of(b * WINDOW, QB), WINDOW)
            wide = pl.ds(pl.multiple_of(b * ext, QB), WINDOW)
            near = cos_h[:, cols], sin_h[:, cols]
            for src, dst_t, dst in ((ak, kt, k), (av, vt, v)):
                for p in range(n_pairs):
                    r = slice(p * pw, (p + 1) * pw)
                    blk = (rope(src[r, :], *near, 1, head_dim) if dst is k else src[r, :]).astype(BF)
                    dst_t[r, wide] = blk
                    dst[wide, r] = blk.T
        for c in keeps(b)[:3]:
            c.start()

    upper = upper_mask()
    first = me == 0

    def spots(it, blk):
        b, p = it // n_pairs, mod(it, n_pairs)
        pr = pl.ds(aligned(p * pw, pw), pw)
        return pr, pl.ds(aligned(b * toks + blk * QB, QB), QB), pl.ds(aligned(b * ext + blk * QB, QB), 3 * QB)

    def score(it):
        for blk in range(tb):
            pr, cols, keys = spots(it, blk)
            sc[blk][:] = dot(k[keys, pr], stack_pair(q[pr, cols]))

    def soften(it, blk):
        s02, s1 = merged(sc[blk][:], upper, *start_bias(first, blk))
        top = jnp.max(jnp.maximum(s02, s1), axis=0, keepdims=True)
        e02, e1 = jnp.exp(s02 - top), jnp.exp(s1 - top)
        mass = col_sum(e02 + e1)
        inv = 1.0 / mass
        lse[it, blk:blk + 1, :] = top + jnp.log(mass)
        pb[blk][:] = banded(e02 * inv, e1 * inv, upper)

    def mix(it):
        for blk in range(tb):
            pr, cols, keys = spots(it, blk)
            ot[pr, cols] = unstack_pair(dot(vt[pr, keys], pb[blk][:])).astype(BF)

    def project(b):
        cols = pl.ds(pl.multiple_of(b * toks, QB), toks)
        with jax.named_scope("f_proj"):
            mid = (xv[b].astype(F32) + dot(ot[:, cols], wo[:], TN)).astype(BF)
            xm[cols, :] = mid
            h = normed(mid, gm[:])
            hm[cols, :] = h
            hmt[:, cols] = h.T
        for c in keeps(b)[3:]:
            c.start()

    keep_qr, keep_lse = (pltpu.make_async_copy(*ends, ld.at[i]) for i, ends in enumerate(((qr, qr_h), (lse, lse_h))))
    load_w[3].wait()
    for blk in range(tb):
        pb[blk][:] = jnp.zeros(pb[blk].shape, BF)

    def walk(i):
        it = i - 1

        @pl.when((lax.rem(i, n_pairs) == 0) & (i < n_steps))
        def _():
            halo_in(i // n_pairs)

        @pl.when(i == 0)
        def _():
            score(0)

        @pl.when((i > 0) & (i <= n_steps))
        def _():
            with jax.named_scope("f_attn"):
                mix(jnp.maximum(it - 1, 0))
                for blk in range(tb):
                    soften(it, blk)
                score(jnp.minimum(i, n_steps - 1))

        @pl.when(i == n_steps)
        def _():
            for b in range(rows):
                push_q(b).wait()
            keep_qr.start()

        @pl.when(i > n_steps)
        def _():
            mix(n_steps - 1)

        @pl.when((lax.rem(it, n_pairs) == 0) & (it > 0))
        def _():
            project(it // n_pairs - 1)

    cdiv_loop(n_steps + 2, walk)
    with jax.named_scope("f_store_wait"):
        keep_lse.start()
        keep_hat.wait()
        keep_q.wait()
        keep_qr.wait()
        keep_lse.wait()
        for b in range(rows):
            for c in keeps(b):
                c.wait()


def any_spec(k):
    return [pl.BlockSpec(memory_space=pl.ANY)] * k


def vmem_spec(k):
    return [pl.BlockSpec(memory_space=pltpu.VMEM)] * k


def run_fwd(n, x, pos, invf, ga, gm, wq, wk, wv, wo, head_dim):
    rows, toks, width = x.shape
    hd = wq.shape[0]
    ext, total, n_halo = toks + WINDOW, rows * toks, rows * WINDOW
    half = head_dim // 2
    sds = lambda *s: jax.ShapeDtypeStruct(s, BF)
    dma = lambda *s: pltpu.SemaphoreType.DMA(s)
    outs = [sds(hd, total), sds(hd, rows * ext), sds(rows * ext, hd), sds(rows * ext, hd), sds(width, total), sds(hd, total), sds(total, width), sds(total, width), sds(width, total)]
    outs += [sds(hd, n_halo), jax.ShapeDtypeStruct((rows * hd // (2 * head_dim), 8, 2 * QB), F32)] + [jax.ShapeDtypeStruct((half, total), F32)] * 2
    vm = lambda *s: pltpu.VMEM(s, BF)
    vf = lambda *s: pltpu.VMEM(s, F32)
    scratch = [pltpu.VMEM((rows, toks), jnp.int32), vf(*invf.shape), vf(*ga.shape), vf(*ga.shape), vm(rows, toks, width), vm(rows, WINDOW, width), vm(hd, n_halo), vf(rows * hd // (2 * head_dim), 8, 2 * QB), pltpu.VMEM((rows, toks), jnp.int32), vm(hd, width), vm(hd, width), vm(hd, width), vm(hd, width),
               vm(hd, total), vm(hd, rows * ext), vm(rows * ext, hd), vm(rows * ext, hd), vm(hd, rows * ext), vm(width, total), vm(hd, total), vm(total, width), vm(total, width), vm(width, total), vm(total, width), vm(WINDOW, width),
               vf(hd, total), vf(hd, total), vf(hd, WINDOW), vf(hd, WINDOW), vf(half, n_halo), vf(half, n_halo),
               *[f(3 * QB, 2 * QB) for f in (vf, vm) for _ in range(3)],
               dma(rows + 4), dma(4), dma(2 + 7 * rows), dma(rows + 1), dma(rows + 1), dma(rows), dma(rows)]
    return pl.pallas_call(
        functools.partial(fwd_kernel, n, head_dim), out_shape=outs,
        in_specs=any_spec(9), out_specs=any_spec(11) + vmem_spec(2), scratch_shapes=scratch,
        compiler_params=pltpu.CompilerParams(collective_id=0, has_side_effects=True, vmem_limit_bytes=VMEM_LIMIT),
        name="forward")(x, pos, invf, ga, gm, wq, wk, wv, wo)


LAG = 2
SLOTS = 2 * LAG
RING = 8
CB = 256


def at(ref, *idx):
    return ref.at[idx]


class Torus:
    def __init__(self, n, head, last, turn, parts, recv0, recv1, recv2, recv3, recv4, recv5, acc, acc2, fin, snd, rcv):
        assert math.isqrt(n // 2) == 4
        me = lax.axis_index("seq")
        self.core = lax.rem(me, 2)
        chip = me // 2
        self.x, self.y = lax.rem(chip, 4), chip // 4
        self.head, self.last, self.turn = head, last, turn
        self.parts, self.recv0, self.recv1, self.recv2, self.recv3, self.recv4, self.recv5 = parts, recv0, recv1, recv2, recv3, recv4, recv5
        self.acc, self.acc2, self.fin, self.snd, self.rcv = acc, acc2, fin, snd, rcv
        self.partner = me + 1 - 2 * self.core
        self.rows, self.columns = [lax.rem(self.y + d, 4) * 4 for d in range(4)], [lax.rem(self.x + d, 4) for d in range(4)]
        self.hops = [[self.device(0, d) for d in range(4)], [self.device(d, 0) for d in range(4)]]

    def device(self, dy, dx):
        return (self.rows[dy] + self.columns[dx]) * 2 + self.core

    def copy(self, lane, kind, slot, src, dst, target):
        return pltpu.make_async_remote_copy(
            src_ref=src, dst_ref=dst, send_sem=self.snd.at[lane, kind, slot], recv_sem=self.rcv.at[lane, kind, slot],
            device_id={"seq": target}, device_id_type=MESH)

    def late(self, axis, pair, yes, no):
        first, end = self.turn
        busy = (pair >= first) & (pair < end)
        return jnp.where(busy & (self.x == 3) if axis else busy, yes, no)

    def swap(self, ring, slot):
        return self.copy(0, 0, slot, self.parts.at[ring, :, :, 1 - self.core], self.recv0.at[slot], self.partner)

    def landing(self, stage):
        return (self.recv0, self.recv1, self.recv2, self.recv3, self.recv4, self.recv5)[stage]

    def arrived(self, stage, kind, slot):
        whole = self.landing(stage).at[kind, slot]
        self.copy(stage, kind, slot, whole, whole, self.partner).wait()

    def send(self, stage, kind, pair, held, slot):
        axis = kind if stage < 3 else 1 - kind
        plus, minus = self.hops[axis][1], self.hops[axis][-1]
        half = CB // 2
        if stage == 1:
            minus = self.late(axis, pair, plus, minus)
            ends = self.acc.at[kind, held, 2, :2], self.acc.at[kind, held, 2, 2:]
        elif stage == 2:
            ends = self.acc.at[kind, held, 1], self.acc.at[kind, held, 3]
        elif stage == 3:
            ends = self.acc2.at[kind, held, 2, :, :half], self.acc2.at[kind, held, 2, :, half:]
        else:
            ends = self.acc2.at[kind, held, 1], self.acc2.at[kind, held, 3]
        for i, src in enumerate(ends):
            self.copy(stage, kind, slot, src, self.landing(stage).at[kind, slot, i], (plus, minus)[i]).start()

    def add(self, stage, kind, pair, held, slot, ring):
        acc, acc2 = self.acc, self.acc2
        if stage == 1:
            for r1 in range(4):
                for r2 in range(4):
                    ry, rx = (r2, r1) if kind == 0 else (r1, r2)
                    chip = self.rows[ry] + self.columns[rx]
                    acc[kind, held, r1, r2] = self.parts[ring, kind, chip, self.core] + self.recv0[slot, kind, chip]
        elif stage == 2:
            back = self.late(kind, pair, 1, 3)
            acc[kind, held, 1, :2] += self.recv1[kind, slot, 0]
            acc[kind, held, back, 2:] += self.recv1[kind, slot, 1]
        elif stage == 3:
            acc2[kind, held] = acc[kind, held, 0] + (self.recv2[kind, slot, 0] + self.recv2[kind, slot, 1])
        elif stage == 4:
            half = CB // 2
            acc2[kind, held, 1, :, :half] += self.recv3[kind, slot, 0]
            acc2[kind, held, 3, :, half:] += self.recv3[kind, slot, 1]
        else:
            self.fin[pair, kind] = acc2[kind, held, 0] + (self.recv4[kind, slot, 0] + self.recv4[kind, slot, 1])

    def direct(self, kind, held, slot):
        for d in range(1, 4):
            self.copy(5, kind, slot, self.acc2.at[kind, held, d], self.recv5.at[kind, slot, d - 1], self.hops[1 - kind][d]).start()

    def early(self, pair):
        return (pair >= 0) & (pair <= self.head)

    def final(self, pair):
        return (pair == self.last) | ((pair > self.head) & (pair < self.last) & (mod(abs(pair - self.head), 2) == 0))

    def when(self, which, fn):
        if isinstance(which, bool):
            fn() if which else None
        else:
            pl.when(which)(fn)

    def offer(self, t):
        self.when(self.early(t) | self.final(t), lambda: self.swap(mod(t, RING), mod(t, SLOTS)).start())

    def tick(self, t):
        self.offer(t)
        self.advance(t)

    def advance(self, t, tail=False):
        now, land, before = mod(t, SLOTS), mod(t + SLOTS - LAG, SLOTS), mod(t + SLOTS - 1, SLOTS)
        ring_land = mod(t + RING - 1, RING)
        for stage in range(5, 0, -1):
            pair = t - LAG * stage + 1
            held = before if stage % 2 else mod(t + 1, SLOTS)

            def move(last_hops, stage=stage, pair=pair, held=held):
                if stage == 1:
                    with jax.named_scope("t_wait1"):
                        self.swap(ring_land, before).wait()
                for kind in range(2):
                    if last_hops and stage == 4:
                        with jax.named_scope("t_wait6"):
                            self.arrived(5, kind, land)
                        got = self.recv5[kind, land]
                        self.fin[pair, kind] = self.acc2[kind, held, 0] + (got[0] + got[1] + got[2])
                        continue
                    if stage > 1:
                        with jax.named_scope(f"t_wait{stage}"):
                            self.arrived(stage - 1, kind, land)
                    self.add(stage, kind, pair, held, land if stage > 1 else before, ring_land)
                    if last_hops and stage == 3:
                        self.direct(kind, held, now)
                    elif stage < 5:
                        self.send(stage, kind, pair, held, now)

            if stage < 3:
                self.when(self.early(pair) | self.final(pair), functools.partial(move, False))
            else:
                self.when(self.early(pair), functools.partial(move, False))
                if tail and stage < 5:
                    self.when(self.final(pair), functools.partial(move, True))


def pick(i, table):
    out = 0
    for key, value in table.items():
        out = jnp.where(i == key, value, out)
    return out


def norm_back(x, gain, grad, res):
    xf = x.astype(F32)
    inv = lax.rsqrt(jnp.mean(xf * xf, axis=-1, keepdims=True) + NORM_EPS)
    unit = xf * inv
    gu = grad * gain
    out = inv * (gu - unit * jnp.mean(gu * unit, axis=-1, keepdims=True)) + res.astype(F32)
    gu = grad * unit
    return out.astype(BF), jnp.sum(gu.reshape(-1, 8, gu.shape[-1]), axis=0)


def plan(n_mlp, n_down, nc):
    order = [("o", g) for g in range(nc)] + [(name, g) for g in range(nc) for name in "qkv"]
    base, head = n_mlp + n_down, n_mlp + n_down + nc - 1
    last = 2 * (base - 1 - head + len(order) // 2) + head - 1
    spot = lambda pair: min(max(pair, 2 * pair - head), last)
    return head, {name: (spot(base + i // 2), i % 2) for i, name in enumerate(order)}, last


def bwd_kernel(n, head_dim, dims, ga_h, gm_h, x_h, dout_h, q_h, kt_h, k_h, v_h, hat_h, ot_h, xm_h, hm_h, hmt_h, qr_h, lse_h, cos_h, sin_h,
               wq_h, wk_h, wv_h, wo_h, wg_h, wu_h, wd_h,
               dx_h, fin_h,
               parts, recv0, recv1, recv2, recv3, recv4, recv5, acc, acc2, fin, snd, rcv,
               dor, lser, deltar, hsnd, hrcv, osnd, orcv, gsend, grecv, gsem, ld,
               xbuf, mbuf, gnm, gmid, ot, hat, wo, dot_, lse, delta, cos_i, sin_i, ga, gm, dgain):
    rows, toks, width, hd, ff = dims
    ext, total = toks + WINDOW, rows * toks
    pw = 2 * head_dim
    n_pairs = hd // pw
    tb, n_steps = toks // QB, n_pairs * rows
    nb, nc, sub = ff // CB, width // CB, ff // width
    rpd = width // n
    per, half_sub = CB // pw, sub // 2
    head, place, end = plan(nb, nc * half_sub, nc)
    comm = Torus(n, head, end, (nb, nb + n_pairs + 1), parts, recv0, recv1, recv2, recv3, recv4, recv5, acc, acc2, fin, snd, rcv)
    me = lax.axis_index("seq")
    left = lax.rem(me + n - 1, n)
    barrier = pltpu.get_barrier_semaphore()

    def greet(i):
        pl.semaphore_signal(barrier, inc=1, device_id={"seq": lax.rem(me + i + 1, n)}, device_id_type=MESH)

    def load(i, s, d):
        c = pltpu.make_async_copy(s, d, ld.at[i])
        c.start()
        return c

    def late(i):
        s, d = ((xm_h, mbuf), (ot_h, ot), (hat_h, hat), (wo_h, wo), (lse_h, lse), (cos_h, cos_i), (sin_h, sin_i), (ga_h, ga), (gm_h, gm))[i]
        return pltpu.make_async_copy(s, d, ld.at[1 + i])

    def to_left(src, dst, send_sem, recv_sem):
        return pltpu.make_async_remote_copy(src_ref=src, dst_ref=dst, send_sem=send_sem, recv_sem=recv_sem,
                                            device_id={"seq": left}, device_id_type=MESH)

    n_late = 9

    def push_rows(i):
        return to_left(*((lse_h, lser), (delta, deltar))[i], hsnd.at[i], hrcv.at[i])

    def push_out(p):
        pr = pl.ds(aligned(p * pw, pw), pw)
        return [to_left(dot_.at[pr, pl.ds(b * toks, WINDOW)], dor.at[pr, pl.ds(b * WINDOW, WINDOW)], osnd.at[p], orcv.at[p])
                for b in range(rows)]

    def give_out(p):
        for c in push_out(p):
            c.start()

    def put(spot, value):
        pair, kind = spot
        parts[mod(pair, RING), kind] = value.reshape(n // 2, 2, rpd, CB)

    def spot_of(name, g):
        known = {i: place[name, i] for i in range(nc)}
        return pick(g, {i: s[0] for i, s in known.items()}), pick(g, {i: s[1] for i, s in known.items()})

    def spots(it, blk):
        p, b = it // rows, mod(it, rows)
        pr = pl.ds(aligned(p * pw, pw), pw)
        return pr, pl.ds(aligned(b * toks + blk * QB, QB), QB), pl.ds(aligned(b * ext + blk * QB, QB), 3 * QB)

    def row_of(it):
        return mod(it, rows) * n_pairs + it // rows

    def mlp(hm, hmt, actt, wgu, wd, dgu, wld):
        def weights(j, slot):
            c = aligned(j * CB, CB)
            return [pltpu.make_async_copy(wg_h.at[:, pl.ds(c, CB)], wgu.at[slot, :, :CB], wld.at[slot, 0]),
                    pltpu.make_async_copy(wu_h.at[:, pl.ds(c, CB)], wgu.at[slot, :, CB:], wld.at[slot, 1]),
                    pltpu.make_async_copy(wd_h.at[pl.ds(c, CB), :], wd.at[slot], wld.at[slot, 2])]

        for c in weights(0, 0):
            c.start()
        ld_hm, ld_x, ld_hmt = load(10, hm_h, hm), load(0, dout_h, xbuf), load(11, hmt_h, hmt)
        cdiv_loop(n - 1, greet)
        gnm[:] = jnp.zeros_like(gnm)
        gsend[:] = jnp.zeros_like(gsend)
        dgain[:] = jnp.zeros_like(dgain)
        ld_hm.wait()
        ld_x.wait()
        ld_hmt.wait()
        for i in range(n_late):
            late(i).start()

        def block(j):
            slot = lax.rem(j, 2)
            for c in weights(j, slot):
                c.wait()

            @pl.when(j + 1 < nb)
            def _():
                for c in weights(j + 1, 1 - slot):
                    c.start()

            c0 = pl.multiple_of(j * CB, CB)
            with jax.named_scope("b_mlp"):
                for b in range(rows):
                    r = slice(b * toks, (b + 1) * toks)
                    gu = dot(hm[r, :], wgu[slot])
                    gact = dot(xbuf[r, :], wd[slot], NT).astype(BF).astype(F32)
                    gate, up = gu[:, :CB], gu[:, CB:]
                    sig = 1.0 / (1.0 + jnp.exp(-gate))
                    swish = gate * sig
                    actt[pl.ds(c0, CB), r] = (swish * up).astype(BF).T
                    dgu[r, :CB] = (gact * up * (sig + swish * (1.0 - sig))).astype(BF)
                    dgu[r, CB:] = (gact * swish).astype(BF)
                both = dot(hmt[:], dgu[:])
                ring = lax.rem(j, RING)
                parts[ring, 0] = both[:, :CB].reshape(n // 2, 2, rpd, CB)
                parts[ring, 1] = both[:, CB:].reshape(n // 2, 2, rpd, CB)
                for b in range(rows):
                    r = slice(b * toks, (b + 1) * toks)
                    gnm[r, :] += dot(dgu[r, :], wgu[slot], NT)

            @pl.when(j == 0)
            def _():
                pl.semaphore_wait(barrier, n - 1)
                push_rows(0).start()

            comm.tick(j)

        cdiv_loop(nb, block)

        def down(c):
            share = n // 2 // sub
            c0 = pl.multiple_of(c * CB, CB)
            for m in range(sub):
                res = dot(actt[m * width:(m + 1) * width, :], xbuf[:, pl.ds(c0, CB)]).reshape(share, 2, sub, rpd, CB)
                for i in range(sub):
                    pair = nb + c * half_sub + i // 2
                    parts[lax.rem(pair, RING), i % 2, m * share:(m + 1) * share] = res[:, :, i]

        for i in range(n_late):
            late(i).wait()

        def mid(b):
            for i in range(tb):
                r = pl.ds(pl.multiple_of((b * tb + i) * QB, QB), QB)
                out, dg = norm_back(mbuf[r, :], gm[:], gnm[r, :], xbuf[r, :])
                gmid[r, :] = out
                dgain[8:, :] += dg

        def deltas(p):
            for it in range(rows):
                for blk in range(tb):
                    pr, cols, _ = spots(p * rows + it, blk)
                    both = dot_[pr, cols].astype(F32) * ot[pr, cols].astype(F32)
                    delta[row_of(p * rows + it), blk:blk + 1, :] = jnp.concatenate(
                        [col_sum(both[:head_dim]), col_sum(both[head_dim:])], axis=1)

        def column(c):
            with jax.named_scope("b_down"):
                down(c)
            comm.tick(nb + c + jnp.minimum(c, 1))

            @pl.when(c > 0)
            def _():
                give_out(c)

            @pl.when(c == 0)
            def _():
                with jax.named_scope("b_mid"):
                    cdiv_loop(rows, mid)
                with jax.named_scope("b_dot"):
                    dot_[:] = dot(wo[:], gmid[:], NT).astype(BF)
                    cdiv_loop(n_pairs, deltas)
                comm.tick(nb + 1)
                push_rows(1).start()
                give_out(0)

        cdiv_loop(nc, column)

    vm = lambda *s: pltpu.VMEM(s, BF)
    vf = lambda *s: pltpu.VMEM(s, F32)
    pl.run_scoped(mlp, vm(total, width), vm(width, total), vm(ff, total), vm(2, width, 2 * CB), vm(2, CB, width), vm(total, 2 * CB),
                  pltpu.SemaphoreType.DMA((2, 3)))
    def attention(q, kt, k, v, qr, dv, sc0, sc1, sc2, sr, dp0, dp1, dp2, dr, pb0, pb1, pb2, pr_, ds0, ds1, ds2, dsr):
        dqt, dkt = ot, q
        wq, wk, wv = k.at[:hd], kt.at[:, :width], v.at[:hd]
        sc, dp, pb, ds = (sc0, sc1, sc2), (dp0, dp1, dp2), (pb0, pb1, pb2), (ds0, ds1, ds2)
        lds = [load(10 + i, s, d) for i, (s, d) in enumerate(((q_h, q), (k_h, k), (v_h, v), (qr_h, qr), (kt_h, kt)))]

        def out_grad(g):
            put(spot_of("o", g), dot(ot[:], gmid[:, pl.ds(pl.multiple_of(g * CB, CB), CB)]))

        with jax.named_scope("b_dwo"):
            cdiv_loop(nc, out_grad)
        first_tick = nb + nc + 1
        upper = upper_mask()
        first, last = me == 0, me == n - 1
        halves = slice(0, WINDOW), slice(WINDOW, 3 * QB)

        def right(it, i):
            p, b = it // rows, mod(it, rows)
            return pl.ds(aligned(p * pw, pw), pw), pl.ds(aligned(b * WINDOW + i * QB, QB), QB), pl.ds(aligned(b * ext + toks + i * QB, QB), WINDOW - i * QB)

        def score(it):
            for blk in range(tb):
                pr, cols, keys = spots(it, blk)
                sc[blk][:] = dot(k[keys, pr], stack_pair(q[pr, cols]))
                dp[blk][:] = dot(v[keys, pr], stack_pair(dot_[pr, cols]))
            for i, rs in enumerate(halves):
                pr, cols, keys = right(it, i)
                sr[rs, :] = dot(k[keys, pr], stack_pair(qr[pr, cols]))
                dr[rs, :] = dot(v[keys, pr], stack_pair(dor[pr, cols]))

        def soften(it):
            row = row_of(it)
            for blk in range(tb):
                s02, s1 = merged(sc[blk][:], upper, *start_bias(first, blk))
                norm, mean = lse[row, blk:blk + 1, :], delta[row, blk:blk + 1, :]
                p02, p1 = jnp.exp(s02 - norm), jnp.exp(s1 - norm)
                g02, g1 = jnp.where(upper, dp[blk][:QB], dp[blk][2 * QB:]), dp[blk][QB:2 * QB]
                pb[blk][:] = banded(p02, p1, upper)
                ds[blk][:] = banded(p02 * (g02 - mean), p1 * (g1 - mean), upper)
            for blk in range(tb):
                i = blk // 2
                rs = slice(blk * QB, (blk + 1) * QB)
                p = jnp.exp(sr[rs, :] - jnp.where(last, -NEG, lser[row, i:i + 1, :]))
                g = p * (dr[rs, :] - deltar[row, i:i + 1, :])
                pr_[rs, :] = (p if blk == 1 else jnp.where(upper, p, 0.0)).astype(BF)
                dsr[rs, :] = (g if blk == 1 else jnp.where(upper, g, 0.0)).astype(BF)

        def grads(it):
            ks, vs = [], []
            for blk in range(tb):
                pr, cols, keys = spots(it, blk)
                own = slice(max(0, 2 - blk) * QB, 3 * QB)
                vs.append(dot(pb[blk][own, :], stack_pair(dot_[pr, cols]), NT))
                ks.append(dot(ds[blk][own, :], stack_pair(q[pr, cols]), NT))
                dq = unstack_pair(dot(kt[pr, keys], ds[blk][:])) * (head_dim ** -0.5)
                dqt[pr, cols] = rope(dq, cos_i[:, cols], sin_i[:, cols], -1, head_dim).astype(BF)
            for i, rs in enumerate(halves):
                pr, cols, _ = right(it, i)
                vs.append(dot(pr_[rs, :], stack_pair(dor[pr, cols]), NT))
                ks.append(dot(dsr[rs, :], stack_pair(qr[pr, cols]), NT))
            for j in range(tb):
                pr, cols, _ = spots(it, j)
                gv, gk = (sum(x[i][(j - max(0, i - 2)) * QB:(j - max(0, i - 2) + 1) * QB] for i in range(j, j + 3)) for x in (vs, ks))
                dv[cols, pr] = gv.astype(BF)
                dkt[pr, cols] = rope(gk.T, cos_i[:, cols], sin_i[:, cols], -1, head_dim).astype(BF)

        def close_group(g):
            cols = pl.ds(pl.multiple_of(g * CB, CB), CB)
            with jax.named_scope("b_dwqkv"):
                put(spot_of("q", g), dot(hat[:], dqt[cols, :], NT))
                put(spot_of("k", g), dot(hat[:], dkt[cols, :], NT))
                put(spot_of("v", g), dot(hat[:], dv[:, cols]))

        def weights():
            return [pltpu.make_async_copy(s, d, ld.at[10 + i]) for i, (s, d) in enumerate(((wq_h, wq), (wk_h, wk), (wv_h, wv), (x_h, xbuf)))]

        def arrived(p):
            whole = dor.at[pl.ds(aligned(p * pw, pw), pw), :]
            with jax.named_scope("b_hwait"):
                to_left(whole, whole, osnd.at[p], orcv.at[p]).wait()

        def walk(it):
            ahead = it + 1

            @pl.when((lax.rem(ahead, rows) == 0) & (ahead < n_steps))
            def _():
                arrived(ahead // rows)

            @pl.when(it < n_steps)
            def _():
                with jax.named_scope("b_attn"):
                    grads(it - 1)
                    soften(it)
                    score(jnp.minimum(ahead, n_steps - 1))

            @pl.when(it == n_steps)
            def _():
                grads(n_steps - 1)
                for c in weights():
                    c.start()

            p, step = it // rows - 1, lax.rem(it, rows)

            @pl.when((step == 0) & (lax.rem(p, per) == per - 1))
            def _():
                close_group(p // per)

            now = first_tick + 1 + p + step // (rows - 1)
            twice = now - head

            @pl.when(it == n_steps)
            def _():
                comm.offer(end)

            @pl.when((step == 0) | ((step == rows - 1) & ((twice > 0) | (p < 0))))
            def _():
                comm.tick(now + jnp.maximum(twice - step // (rows - 1), 0) + jnp.minimum(p, 0))

            @pl.when((step == 0) & (p + 3 < n_pairs))
            def _():
                give_out(p + 3)

        for c in lds[:-1]:
            c.wait()
        for i in range(2):
            push_rows(i).wait()
        arrived(0)
        score(0)
        soften(0)
        score(1)
        lds[-1].wait()
        cdiv_loop(n_steps, lambda i: walk(i + 1))
        for c in weights():
            c.wait()

        def into(b):
            r = pl.ds(aligned(b * toks, QB), toks)
            with jax.named_scope("b_into"):
                gnm[r, :] = dot(dqt[:, r], wq[:], TN) + dot(dkt[:, r], wk[:], TN) + dot(dv[r, :], wv[:])

            with jax.named_scope("b_final"):
                for i in range(tb):
                    r = pl.ds(aligned((b * tb + i) * QB, QB), QB)
                    out, dg = norm_back(xbuf[r, :], ga[:], gnm[r, :], gmid[r, :])
                    mbuf[r, :] = out
                    dgain[:8, :] += dg

        def share_gains():
            out_copy.start()
            gains = jnp.concatenate([col_sum(dgain[:8, :]), col_sum(dgain[8:, :]), jnp.zeros((6, width), F32)], axis=0)
            for p in range(n):
                gsend[p, :, :rpd] = gains[:, p * rpd:(p + 1) * rpd]

            def spread(i):
                to = lax.rem(me + i + 1, n)
                pltpu.make_async_remote_copy(src_ref=gsend.at[to], dst_ref=grecv.at[i], send_sem=gsem.at[0], recv_sem=gsem.at[1],
                                             device_id={"seq": to}, device_id_type=MESH).start()

            cdiv_loop(n - 1, spread)

        def finish(i):
            comm.advance(end + i, True)

            @pl.when(i == 1)
            def _():
                cdiv_loop(rows - 1, into)

            @pl.when(i == LAG + 1)
            def _():
                into(rows - 1)
                share_gains()

        cdiv_loop(4 * LAG - 1, finish)

    score_bufs = [f(3 * QB, 2 * QB) for f in (vf, vm) for _ in range(8)]
    out_copy = pltpu.make_async_copy(mbuf, dx_h, ld.at[0])
    pl.run_scoped(attention, vm(hd, total), vm(hd, rows * ext), vm(rows * ext, hd), vm(rows * ext, hd), vm(hd, rows * WINDOW), vm(total, hd), *score_bufs)
    most, rest = pl.ds(0, end), pl.ds(end, 2)
    keep_most = load(1, fin.at[most], fin_h.at[most])
    to_left(gsend.at[pl.ds(0, n - 1)], grecv, gsem.at[0], gsem.at[1]).wait()
    sums = gsend[me]
    for i in range(n - 1):
        sums = sums + grecv[i]
    fin[end + 1, 0, :8, :128] = sums
    out_copy.wait()
    comm.advance(end + 4 * LAG - 1, True)
    with jax.named_scope("b_end"):
        keep_rest = load(0, fin.at[rest], fin_h.at[rest])
        keep_most.wait()
        keep_rest.wait()


def spread_kernel(dims, dx_i, fin_i, dx_o, dga_o, dgm_o, *refs):
    head_dim, n, width, ff = dims
    outs, (buf, fin), stage, sem = refs[:7], refs[7:9], refs[9:16], refs[16]
    dq, dk, dv, do, dg, du, dd = stage
    nb, nc, sub = ff // CB, width // CB, ff // width
    rpd = width // n
    head, place, end = plan(nb, nc * sub // 2, nc)
    get_fin = pltpu.make_async_copy(fin_i, fin, sem.at[len(outs)])
    get_fin.start()
    cut = buf.shape[0] // nc
    gets, puts = ([pltpu.make_async_copy(s.at[pl.ds(i * cut, cut)], d.at[pl.ds(i * cut, cut)], sem.at[len(outs) + k + i]) for i in range(nc)]
                  for k, s, d in ((1, dx_i, buf), (nc + 1, buf, dx_o)))
    for c in gets:
        c.start()
    get_fin.wait()
    gains = fin[end + 1, 0]
    dga_o[:] = gains[:1, :rpd]
    dgm_o[:] = gains[1:2, :rpd]
    for j in range(nb):
        dg[:, j * CB:(j + 1) * CB] = fin[j, 0]
        du[:, j * CB:(j + 1) * CB] = fin[j, 1]
    for c in range(nc):
        for i in range(sub):
            pair = nb + (c * sub + i) // 2
            dd[i * rpd:(i + 1) * rpd, c * CB:(c + 1) * CB] = fin[pair, i % 2]
    for g in range(nc):
        do[:, g * CB:(g + 1) * CB] = fin[place["o", g]]
        for name, ref in (("q", dq), ("k", dk), ("v", dv)):
            val = fin[place[name, g]]
            for h in range(CB // head_dim):
                ref[g * (CB // head_dim) + h] = val[:, h * head_dim:(h + 1) * head_dim]
    keeps = [pltpu.make_async_copy(s, d, sem.at[i]) for i, (s, d) in enumerate(zip(stage, outs))]
    for c in keeps:
        c.start()
    for get, out in zip(gets, puts):
        get.wait()
        out.start()
    for c in keeps + puts:
        c.wait()


def run_bwd(n, head_dim, ga, gm, x, dout, q, kt, k, v, hat, ot, xm, hm, hmt, qr, lse, cos_t, sin_t, wq, wk, wv, wo, wg, wu, wd, rows):
    total, width = x.shape
    hd, ff = wq.shape[0], wg.shape[1]
    toks = total // rows
    rpd, heads = width // n, hd // head_dim
    nb, nc, sub = ff // CB, width // CB, ff // width
    slots = plan(nb, nc * sub // 2, nc)[2] + 2
    n_pairs = hd // (2 * head_dim)
    f = lambda *s: jax.ShapeDtypeStruct(s, F32)
    dx_t = jax.ShapeDtypeStruct((total, width), BF)
    vm = lambda *s: pltpu.VMEM(s, BF)
    vf = lambda *s: pltpu.VMEM(s, F32)
    dma = lambda *s: pltpu.SemaphoreType.DMA(s)
    line, duo = vf(rows * n_pairs, 8, 2 * QB), (2, SLOTS)
    scratch = [vf(RING, 2, n // 2, 2, rpd, CB), vf(SLOTS, 2, n // 2, rpd, CB), vf(*duo, 2, 2, rpd, CB), vf(*duo, 2, 4, rpd, CB),
               vf(*duo, 2, rpd, CB // 2), vf(*duo, 2, rpd, CB), vf(*duo, 3, rpd, CB), vf(*duo, 4, 4, rpd, CB), vf(*duo, 4, rpd, CB), vf(slots, 2, rpd, CB),
               dma(6, *duo), dma(6, *duo),
               vm(hd, rows * WINDOW), line, line, dma(2), dma(2), dma(n_pairs), dma(n_pairs),
               vf(n, 8, 128), vf(n - 1, 8, 128), dma(2), dma(15),
               vm(total, width), vm(total, width), vf(total, width), vm(total, width), vm(hd, total), vm(width, total), vm(hd, width), vm(hd, total), line, line, vf(*cos_t.shape), vf(*cos_t.shape), vf(*ga.shape), vf(*ga.shape), vf(16, width)]
    mid = pl.pallas_call(
        functools.partial(bwd_kernel, n, head_dim, (rows, toks, width, hd, ff)), out_shape=[dx_t, f(slots, 2, rpd, CB)],
        in_specs=any_spec(24), out_specs=any_spec(2), scratch_shapes=scratch,
        compiler_params=pltpu.CompilerParams(collective_id=1, has_side_effects=True, vmem_limit_bytes=VMEM_LIMIT),
        name="backward")(ga, gm, x, dout, q, kt, k, v, hat, ot, xm, hm, hmt, qr, lse, cos_t, sin_t, wq, wk, wv, wo, wg, wu, wd)
    outs = [f(heads, rpd, head_dim)] * 3 + [f(rpd, width), f(rpd, ff), f(rpd, ff), f(ff // n, width)]
    return pl.pallas_call(
        functools.partial(spread_kernel, (head_dim, n, width, ff)), out_shape=[dx_t, f(1, rpd), f(1, rpd)] + outs,
        in_specs=any_spec(2), out_specs=any_spec(1) + vmem_spec(2) + any_spec(7),
        scratch_shapes=[vm(total, width), vf(slots, 2, rpd, CB), *[vf(*o.shape) for o in outs], dma(8 + 2 * nc)],
        name="spread")(*mid)


def solution(mesh):
    n = mesh.shape["seq"]

    def device_step(hidden, positions, g_attn, g_mlp, w_query, w_key, w_value, w_out, w_gate, w_up, w_down, d_out):
        rows, toks, width = hidden.shape
        layers, _, heads, head_dim = w_query.shape
        hd = heads * head_dim
        half = head_dim // 2
        inv_freq = 1.0 / (10000.0 ** (jnp.arange(half, dtype=F32) * (2.0 / head_dim)))
        turn = lambda w: w[0].transpose(1, 2, 0).reshape(hd, width)
        wq, wk, wv = turn(w_query), turn(w_key), turn(w_value)
        fwd = run_fwd(n, hidden, positions, inv_freq[:, None], g_attn, g_mlp, wq, wk, wv, w_out[0], head_dim)
        out = run_bwd(n, head_dim, g_attn, g_mlp, hidden.reshape(rows * toks, width), d_out.reshape(rows * toks, width), *fwd,
                      wq, wk, wv, w_out[0], w_gate[0], w_up[0], w_down[0], rows)
        dx, dga, dgm, dq, dk, dv, do, dg, du, dd = out
        back = lambda w: w.transpose(1, 0, 2)[None]
        return (dx.reshape(rows, toks, width), dga, dgm, back(dq), back(dk), back(dv), do[None], dg[None], du[None], dd[None])

    tok_spec, grad_spec = P("data", "seq"), P(None, ("data", "seq"))
    in_specs = (tok_spec, tok_spec) + (P(),) * 9 + (tok_spec,)
    out_specs = (tok_spec,) + (grad_spec,) * 9
    return jax.shard_map(device_step, mesh=mesh, in_specs=in_specs, out_specs=out_specs, check_vma=False)
```

```python
import functools, math
import numpy as np
import jax, jax.numpy as jnp
from jax import lax
from jax.experimental import pallas as pl
from jax.experimental.pallas import tpu as pltpu
from jax.sharding import PartitionSpec as P

WINDOW = 256
NORM_EPS = 1e-5
QB = 128
BF, F32 = jnp.bfloat16, jnp.float32
NN, NT, TN = ((1,), (0,)), ((1,), (1,)), ((0,), (0,))
MESH = pl.DeviceIdType.MESH
NEG = -1e30
VMEM_LIMIT = 67043328


def dot(a, b, dims=NN):
    return lax.dot_general(a, b, (dims, ((), ())), preferred_element_type=F32)


def cdiv_loop(n, body):
    lax.fori_loop(0, n, lambda i, c: body(i) or c, 0)


def mod(a, b):
    return a % b if isinstance(a, int) else lax.rem(a, b)


def aligned(a, b):
    return a if isinstance(a, int) else pl.multiple_of(a, b)


def rope(blk, cos_b, sin_b, sign, head_dim):
    half = head_dim // 2
    parts = []
    for h in range(blk.shape[0] // head_dim):
        first = blk[h * head_dim:h * head_dim + half]
        second = blk[h * head_dim + half:(h + 1) * head_dim]
        if sign > 0:
            parts += [first * cos_b - second * sin_b, second * cos_b + first * sin_b]
        else:
            parts += [first * cos_b + second * sin_b, second * cos_b - first * sin_b]
    return jnp.concatenate(parts, axis=0)


def normed(x, gain):
    xf = x.astype(F32)
    inv = lax.rsqrt(jnp.mean(xf * xf, axis=-1, keepdims=True) + NORM_EPS)
    return (xf * inv * gain).astype(BF)


def stack_pair(pair_t):
    half = pair_t.shape[0] // 2
    zero = jnp.zeros((half, pair_t.shape[1]), pair_t.dtype)
    return jnp.concatenate(
        [jnp.concatenate([pair_t[:half], zero], axis=0), jnp.concatenate([zero, pair_t[half:]], axis=0)], axis=1)


def unstack_pair(both):
    half, cols = both.shape[0] // 2, both.shape[1] // 2
    return jnp.concatenate([both[:half, :cols], both[half:, cols:]], axis=0)


def col_sum(x):
    return jnp.sum(x, axis=0, keepdims=True)


def merged(scores, upper, bias0, bias1):
    return jnp.where(upper, scores[:QB] + bias0, scores[2 * QB:]), scores[QB:2 * QB] + bias1


def banded(p02, p1, upper):
    return jnp.concatenate(
        [jnp.where(upper, p02, 0.0).astype(BF), p1.astype(BF), jnp.where(upper, 0.0, p02).astype(BF)], axis=0)


def upper_mask():
    key_ids = lax.broadcasted_iota(jnp.int32, (QB, 2 * QB), 0)
    query_ids = lax.broadcasted_iota(jnp.int32, (QB, 2 * QB), 1) % QB
    return key_ids > query_ids


def start_bias(first, blk):
    bias = jnp.where(first, NEG, 0.0).astype(F32)
    return (bias if blk < 2 else 0.0), (bias if blk < 1 else 0.0)


def fwd_kernel(n, head_dim, x_h, pos_h, invf_h, ga_h, gm_h, wq_h, wk_h, wv_h, wo_h,
               q_h, kt_h, k_h, v_h, hat_h, ot_h, xm_h, hm_h, hmt_h, qr_h, lse_h, cos_t, sin_t,
               pos, invf, ga, gm, xv, halo, qr, lse, pos_halo, wq, wk, wv, wo, q, kt, k, v, vt, hat, ot, xm, hm, hmt, hb, hh, acc, acc2, ak, av, cos_h, sin_h,
               sc0, sc1, sc2, pb0, pb1, pb2, ldx, ld, st, snd, rcv, qsnd, qrcv):
    sc, pb = (sc0, sc1, sc2), (pb0, pb1, pb2)
    rows, toks, width = xv.shape
    ext, total, pw = toks + WINDOW, rows * toks, 2 * head_dim
    n_pairs = wq.shape[0] // pw
    tb, n_steps = toks // QB, n_pairs * rows
    me = lax.axis_index("seq")
    right, left = lax.rem(me + 1, n), lax.rem(me + n - 1, n)
    load_x = [pltpu.make_async_copy(x_h.at[b], xv.at[b], ldx.at[b]) for b in range(rows)]
    load_w = [pltpu.make_async_copy(s, d, ld.at[i]) for i, (s, d) in enumerate(((wq_h, wq), (wk_h, wk), (wv_h, wv), (wo_h, wo)))]
    load_s = [pltpu.make_async_copy(s, d, ldx.at[rows + i]) for i, (s, d) in enumerate(((pos_h, pos), (invf_h, invf), (ga_h, ga), (gm_h, gm)))]
    for c in load_s + load_x:
        c.start()
    barrier = pltpu.get_barrier_semaphore()
    for other in (left, right):
        pl.semaphore_signal(barrier, inc=1, device_id={"seq": other}, device_id_type=MESH)

    def push(i, s, d):
        return pltpu.make_async_remote_copy(src_ref=s, dst_ref=d, send_sem=snd.at[i], recv_sem=rcv.at[i], device_id={"seq": right}, device_id_type=MESH)

    def push_rows(b):
        return push(b, x_h.at[b, toks - WINDOW:, :], halo.at[b])

    send_pos = push(rows, pos, pos_halo)

    def angles(cos_ref, sin_ref, positions):
        count = positions.shape[1]
        for b in range(rows):
            ang = invf[:] * positions[b:b + 1, :].astype(F32)
            cos_ref[:, b * count:(b + 1) * count] = jnp.cos(ang)
            sin_ref[:, b * count:(b + 1) * count] = jnp.sin(ang)

    for c in load_s:
        c.wait()
    angles(cos_t, sin_t, pos[:])

    def norm_rows(b):
        for i in range(tb):
            h = normed(xv[b, i * QB:(i + 1) * QB, :], ga[:])
            hb[pl.ds(pl.multiple_of((b * tb + i) * QB, QB), QB), :] = h

    with jax.named_scope("f_norm"):
        for c in load_x:
            c.wait()
        for c in load_w:
            c.start()
        cdiv_loop(rows, norm_rows)
    pl.semaphore_wait(barrier, 2)
    send_pos.start()
    for b in range(rows):
        push_rows(b).start()
    keep_hat = pltpu.make_async_copy(hat, hat_h, st.at[0])
    tables = cos_t[:], sin_t[:]

    def put_q(src):
        for p in range(n_pairs):
            r = slice(p * pw, (p + 1) * pw)
            q[r, :] = (rope(src[r, :], *tables, 1, head_dim) * (head_dim ** -0.5)).astype(BF)

    def put_own(src, dst_t, dst):
        for p in range(n_pairs):
            r = slice(p * pw, (p + 1) * pw)
            both = (rope(src[r, :], *tables, 1, head_dim) if dst is k else src[r, :]).astype(BF)
            for b in range(rows):
                blk = both[:, b * toks:(b + 1) * toks]
                own = slice(b * ext + WINDOW, (b + 1) * ext)
                dst_t[r, own] = blk
                dst[own, r] = blk.T

    with jax.named_scope("f_mm"):
        load_w[0].wait()
        load_w[1].wait()
        load_w[2].wait()
        acc[:] = dot(wq[:], hb[:], NT)
        acc2[:] = dot(wk[:], hb[:], NT)
        put_q(acc)
        acc[:] = dot(wv[:], hb[:], NT)
        put_own(acc2, kt, k)
        for i in range(total // QB):
            r = slice(i * QB, (i + 1) * QB)
            hat[:, r] = hb[r, :].T
        put_own(acc, vt, v)
    keep_hat.start()
    keep_q = pltpu.make_async_copy(q, q_h, st.at[1])
    keep_q.start()

    def push_q(b):
        return pltpu.make_async_remote_copy(src_ref=q.at[:, b * toks:b * toks + WINDOW], dst_ref=qr.at[:, b * WINDOW:(b + 1) * WINDOW],
                                            send_sem=qsnd.at[b], recv_sem=qrcv.at[b], device_id={"seq": left}, device_id_type=MESH)

    for b in range(rows):
        push_q(b).start()
    send_pos.wait()
    angles(cos_h, sin_h, pos_halo[:, toks - WINDOW:])

    def keeps(b):
        wide, cols = pl.ds(pl.multiple_of(b * ext, QB), ext), pl.ds(pl.multiple_of(b * toks, QB), toks)
        ends = ((kt.at[:, wide], kt_h.at[:, wide]), (k.at[wide, :], k_h.at[wide, :]), (v.at[wide, :], v_h.at[wide, :]),
                (ot.at[:, cols], ot_h.at[:, cols]), (hm.at[cols, :], hm_h.at[cols, :]), (hmt.at[:, cols], hmt_h.at[:, cols]),
                (xm.at[cols, :], xm_h.at[cols, :]))
        return [pltpu.make_async_copy(s, d, st.at[2 + b * len(ends) + i]) for i, (s, d) in enumerate(ends)]

    def halo_in(b):
        with jax.named_scope("f_halo_wait"):
            push_rows(b).wait()
        with jax.named_scope("f_halo"):
            for i in range(WINDOW // QB):
                r = slice(i * QB, (i + 1) * QB)
                hh[r, :] = normed(halo[b, r, :], ga[:])
            ak[:] = dot(wk[:], hh[:], NT)
            av[:] = dot(wv[:], hh[:], NT)
            cols = pl.ds(pl.multiple_of(b * WINDOW, QB), WINDOW)
            wide = pl.ds(pl.multiple_of(b * ext, QB), WINDOW)
            near = cos_h[:, cols], sin_h[:, cols]
            for src, dst_t, dst in ((ak, kt, k), (av, vt, v)):
                for p in range(n_pairs):
                    r = slice(p * pw, (p + 1) * pw)
                    blk = (rope(src[r, :], *near, 1, head_dim) if dst is k else src[r, :]).astype(BF)
                    dst_t[r, wide] = blk
                    dst[wide, r] = blk.T
        for c in keeps(b)[:3]:
            c.start()

    upper = upper_mask()
    first = me == 0

    def spots(it, blk):
        b, p = it // n_pairs, mod(it, n_pairs)
        pr = pl.ds(aligned(p * pw, pw), pw)
        return pr, pl.ds(aligned(b * toks + blk * QB, QB), QB), pl.ds(aligned(b * ext + blk * QB, QB), 3 * QB)

    def score(it):
        for blk in range(tb):
            pr, cols, keys = spots(it, blk)
            sc[blk][:] = dot(k[keys, pr], stack_pair(q[pr, cols]))

    def soften(it, blk):
        s02, s1 = merged(sc[blk][:], upper, *start_bias(first, blk))
        top = jnp.max(jnp.maximum(s02, s1), axis=0, keepdims=True)
        e02, e1 = jnp.exp(s02 - top), jnp.exp(s1 - top)
        mass = col_sum(e02 + e1)
        inv = 1.0 / mass
        lse[it, blk:blk + 1, :] = top + jnp.log(mass)
        pb[blk][:] = banded(e02 * inv, e1 * inv, upper)

    def mix(it):
        for blk in range(tb):
            pr, cols, keys = spots(it, blk)
            ot[pr, cols] = unstack_pair(dot(vt[pr, keys], pb[blk][:])).astype(BF)

    def project(b):
        cols = pl.ds(pl.multiple_of(b * toks, QB), toks)
        with jax.named_scope("f_proj"):
            mid = (xv[b].astype(F32) + dot(ot[:, cols], wo[:], TN)).astype(BF)
            xm[cols, :] = mid
            h = normed(mid, gm[:])
            hm[cols, :] = h
            hmt[:, cols] = h.T
        for c in keeps(b)[3:]:
            c.start()

    keep_qr, keep_lse = (pltpu.make_async_copy(*ends, ld.at[i]) for i, ends in enumerate(((qr, qr_h), (lse, lse_h))))
    load_w[3].wait()
    for blk in range(tb):
        pb[blk][:] = jnp.zeros(pb[blk].shape, BF)

    def walk(i):
        it = i - 1

        @pl.when((lax.rem(i, n_pairs) == 0) & (i < n_steps))
        def _():
            halo_in(i // n_pairs)

        @pl.when(i == 0)
        def _():
            score(0)

        @pl.when((i > 0) & (i <= n_steps))
        def _():
            with jax.named_scope("f_attn"):
                mix(jnp.maximum(it - 1, 0))
                for blk in range(tb):
                    soften(it, blk)
                score(jnp.minimum(i, n_steps - 1))

        @pl.when(i == n_steps)
        def _():
            for b in range(rows):
                push_q(b).wait()
            keep_qr.start()

        @pl.when(i > n_steps)
        def _():
            mix(n_steps - 1)

        @pl.when((lax.rem(it, n_pairs) == 0) & (it > 0))
        def _():
            project(it // n_pairs - 1)

    cdiv_loop(n_steps + 2, walk)
    with jax.named_scope("f_store_wait"):
        keep_lse.start()
        keep_hat.wait()
        keep_q.wait()
        keep_qr.wait()
        keep_lse.wait()
        for b in range(rows):
            for c in keeps(b):
                c.wait()


def any_spec(k):
    return [pl.BlockSpec(memory_space=pl.ANY)] * k


def vmem_spec(k):
    return [pl.BlockSpec(memory_space=pltpu.VMEM)] * k


def run_fwd(n, x, pos, invf, ga, gm, wq, wk, wv, wo, head_dim):
    rows, toks, width = x.shape
    hd = wq.shape[0]
    ext, total, n_halo = toks + WINDOW, rows * toks, rows * WINDOW
    half = head_dim // 2
    sds = lambda *s: jax.ShapeDtypeStruct(s, BF)
    dma = lambda *s: pltpu.SemaphoreType.DMA(s)
    outs = [sds(hd, total), sds(hd, rows * ext), sds(rows * ext, hd), sds(rows * ext, hd), sds(width, total), sds(hd, total), sds(total, width), sds(total, width), sds(width, total)]
    outs += [sds(hd, n_halo), jax.ShapeDtypeStruct((rows * hd // (2 * head_dim), 8, 2 * QB), F32)] + [jax.ShapeDtypeStruct((half, total), F32)] * 2
    vm = lambda *s: pltpu.VMEM(s, BF)
    vf = lambda *s: pltpu.VMEM(s, F32)
    scratch = [pltpu.VMEM((rows, toks), jnp.int32), vf(*invf.shape), vf(*ga.shape), vf(*ga.shape), vm(rows, toks, width), vm(rows, WINDOW, width), vm(hd, n_halo), vf(rows * hd // (2 * head_dim), 8, 2 * QB), pltpu.VMEM((rows, toks), jnp.int32), vm(hd, width), vm(hd, width), vm(hd, width), vm(hd, width),
               vm(hd, total), vm(hd, rows * ext), vm(rows * ext, hd), vm(rows * ext, hd), vm(hd, rows * ext), vm(width, total), vm(hd, total), vm(total, width), vm(total, width), vm(width, total), vm(total, width), vm(WINDOW, width),
               vf(hd, total), vf(hd, total), vf(hd, WINDOW), vf(hd, WINDOW), vf(half, n_halo), vf(half, n_halo),
               *[f(3 * QB, 2 * QB) for f in (vf, vm) for _ in range(3)],
               dma(rows + 4), dma(4), dma(2 + 7 * rows), dma(rows + 1), dma(rows + 1), dma(rows), dma(rows)]
    return pl.pallas_call(
        functools.partial(fwd_kernel, n, head_dim), out_shape=outs,
        in_specs=any_spec(9), out_specs=any_spec(11) + vmem_spec(2), scratch_shapes=scratch,
        compiler_params=pltpu.CompilerParams(collective_id=0, has_side_effects=True, vmem_limit_bytes=VMEM_LIMIT),
        name="forward")(x, pos, invf, ga, gm, wq, wk, wv, wo)


LAG = 2
SLOTS = 2 * LAG
RING = 8
CB = 256


def at(ref, *idx):
    return ref.at[idx]


class Torus:
    def __init__(self, n, head, last, turn, parts, recv0, recv1, recv2, recv3, recv4, recv5, acc, acc2, fin, snd, rcv):
        assert math.isqrt(n // 2) == 4
        me = lax.axis_index("seq")
        self.core = lax.rem(me, 2)
        chip = me // 2
        self.x, self.y = lax.rem(chip, 4), chip // 4
        self.head, self.last, self.turn = head, last, turn
        self.parts, self.recv0, self.recv1, self.recv2, self.recv3, self.recv4, self.recv5 = parts, recv0, recv1, recv2, recv3, recv4, recv5
        self.acc, self.acc2, self.fin, self.snd, self.rcv = acc, acc2, fin, snd, rcv
        self.partner = me + 1 - 2 * self.core
        self.rows, self.columns = [lax.rem(self.y + d, 4) * 4 for d in range(4)], [lax.rem(self.x + d, 4) for d in range(4)]
        self.hops = [[self.device(0, d) for d in range(4)], [self.device(d, 0) for d in range(4)]]

    def device(self, dy, dx):
        return (self.rows[dy] + self.columns[dx]) * 2 + self.core

    def copy(self, lane, kind, slot, src, dst, target):
        return pltpu.make_async_remote_copy(
            src_ref=src, dst_ref=dst, send_sem=self.snd.at[lane, kind, slot], recv_sem=self.rcv.at[lane, kind, slot],
            device_id={"seq": target}, device_id_type=MESH)

    def late(self, axis, pair, yes, no):
        first, end = self.turn
        busy = (pair >= first) & (pair < end)
        return jnp.where(busy & (self.x == 3) if axis else busy, yes, no)

    def swap(self, ring, slot):
        return self.copy(0, 0, slot, self.parts.at[ring, :, :, 1 - self.core], self.recv0.at[slot], self.partner)

    def landing(self, stage):
        return (self.recv0, self.recv1, self.recv2, self.recv3, self.recv4, self.recv5)[stage]

    def arrived(self, stage, kind, slot):
        whole = self.landing(stage).at[kind, slot]
        self.copy(stage, kind, slot, whole, whole, self.partner).wait()

    def send(self, stage, kind, pair, held, slot):
        axis = kind if stage < 3 else 1 - kind
        plus, minus = self.hops[axis][1], self.hops[axis][-1]
        half = CB // 2
        if stage == 1:
            minus = self.late(axis, pair, plus, minus)
            ends = self.acc.at[kind, held, 2, :2], self.acc.at[kind, held, 2, 2:]
        elif stage == 2:
            ends = self.acc.at[kind, held, 1], self.acc.at[kind, held, 3]
        elif stage == 3:
            ends = self.acc2.at[kind, held, 2, :, :half], self.acc2.at[kind, held, 2, :, half:]
        else:
            ends = self.acc2.at[kind, held, 1], self.acc2.at[kind, held, 3]
        for i, src in enumerate(ends):
            self.copy(stage, kind, slot, src, self.landing(stage).at[kind, slot, i], (plus, minus)[i]).start()

    def add(self, stage, kind, pair, held, slot, ring):
        acc, acc2 = self.acc, self.acc2
        if stage == 1:
            for r1 in range(4):
                for r2 in range(4):
                    ry, rx = (r2, r1) if kind == 0 else (r1, r2)
                    chip = self.rows[ry] + self.columns[rx]
                    acc[kind, held, r1, r2] = self.parts[ring, kind, chip, self.core] + self.recv0[slot, kind, chip]
        elif stage == 2:
            back = self.late(kind, pair, 1, 3)
            acc[kind, held, 1, :2] += self.recv1[kind, slot, 0]
            acc[kind, held, back, 2:] += self.recv1[kind, slot, 1]
        elif stage == 3:
            acc2[kind, held] = acc[kind, held, 0] + (self.recv2[kind, slot, 0] + self.recv2[kind, slot, 1])
        elif stage == 4:
            half = CB // 2
            acc2[kind, held, 1, :, :half] += self.recv3[kind, slot, 0]
            acc2[kind, held, 3, :, half:] += self.recv3[kind, slot, 1]
        else:
            self.fin[pair, kind] = acc2[kind, held, 0] + (self.recv4[kind, slot, 0] + self.recv4[kind, slot, 1])

    def direct(self, kind, held, slot):
        for d in range(1, 4):
            self.copy(5, kind, slot, self.acc2.at[kind, held, d], self.recv5.at[kind, slot, d - 1], self.hops[1 - kind][d]).start()

    def early(self, pair):
        return (pair >= 0) & (pair <= self.head)

    def final(self, pair):
        return (pair == self.last) | ((pair > self.head) & (pair < self.last) & (mod(abs(pair - self.head), 2) == 0))

    def when(self, which, fn):
        if isinstance(which, bool):
            fn() if which else None
        else:
            pl.when(which)(fn)

    def offer(self, t):
        self.when(self.early(t) | self.final(t), lambda: self.swap(mod(t, RING), mod(t, SLOTS)).start())

    def tick(self, t):
        self.offer(t)
        self.advance(t)

    def advance(self, t, tail=False):
        now, land, before = mod(t, SLOTS), mod(t + SLOTS - LAG, SLOTS), mod(t + SLOTS - 1, SLOTS)
        ring_land = mod(t + RING - 1, RING)
        for stage in range(5, 0, -1):
            pair = t - LAG * stage + 1
            held = before if stage % 2 else mod(t + 1, SLOTS)

            def move(last_hops, stage=stage, pair=pair, held=held):
                if stage == 1:
                    with jax.named_scope("t_wait1"):
                        self.swap(ring_land, before).wait()
                for kind in range(2):
                    if last_hops and stage == 4:
                        with jax.named_scope("t_wait6"):
                            self.arrived(5, kind, land)
                        got = self.recv5[kind, land]
                        self.fin[pair, kind] = self.acc2[kind, held, 0] + (got[0] + got[1] + got[2])
                        continue
                    if stage > 1:
                        with jax.named_scope(f"t_wait{stage}"):
                            self.arrived(stage - 1, kind, land)
                    self.add(stage, kind, pair, held, land if stage > 1 else before, ring_land)
                    if last_hops and stage == 3:
                        self.direct(kind, held, now)
                    elif stage < 5:
                        self.send(stage, kind, pair, held, now)

            if stage < 3:
                self.when(self.early(pair) | self.final(pair), functools.partial(move, False))
            else:
                self.when(self.early(pair), functools.partial(move, False))
                if tail and stage < 5:
                    self.when(self.final(pair), functools.partial(move, True))


def pick(i, table):
    out = 0
    for key, value in table.items():
        out = jnp.where(i == key, value, out)
    return out


def norm_back(x, gain, grad, res):
    xf = x.astype(F32)
    inv = lax.rsqrt(jnp.mean(xf * xf, axis=-1, keepdims=True) + NORM_EPS)
    unit = xf * inv
    gu = grad * gain
    out = inv * (gu - unit * jnp.mean(gu * unit, axis=-1, keepdims=True)) + res.astype(F32)
    gu = grad * unit
    return out.astype(BF), jnp.sum(gu.reshape(-1, 8, gu.shape[-1]), axis=0)


def plan(n_mlp, n_down, nc):
    order = [("o", g) for g in range(nc)] + [(name, g) for g in range(nc) for name in "qkv"]
    base, head = n_mlp + n_down, n_mlp + n_down + nc - 1
    last = 2 * (base - 1 - head + len(order) // 2) + head - 1
    spot = lambda pair: min(max(pair, 2 * pair - head), last)
    return head, {name: (spot(base + i // 2), i % 2) for i, name in enumerate(order)}, last


def bwd_kernel(n, head_dim, dims, ga_h, gm_h, x_h, dout_h, q_h, kt_h, k_h, v_h, hat_h, ot_h, xm_h, hm_h, hmt_h, qr_h, lse_h, cos_h, sin_h,
               wq_h, wk_h, wv_h, wo_h, wg_h, wu_h, wd_h,
               dx_h, fin_h,
               parts, recv0, recv1, recv2, recv3, recv4, recv5, acc, acc2, fin, snd, rcv,
               dor, lser, deltar, hsnd, hrcv, osnd, orcv, gsend, grecv, gsem, ld,
               xbuf, mbuf, gnm, gmid, ot, hat, wo, dot_, lse, delta, cos_i, sin_i, ga, gm, dgain):
    rows, toks, width, hd, ff = dims
    ext, total = toks + WINDOW, rows * toks
    pw = 2 * head_dim
    n_pairs = hd // pw
    tb, n_steps = toks // QB, n_pairs * rows
    nb, nc, sub = ff // CB, width // CB, ff // width
    rpd = width // n
    per, half_sub = CB // pw, sub // 2
    head, place, end = plan(nb, nc * half_sub, nc)
    comm = Torus(n, head, end, (nb, nb + n_pairs + 1), parts, recv0, recv1, recv2, recv3, recv4, recv5, acc, acc2, fin, snd, rcv)
    me = lax.axis_index("seq")
    left = lax.rem(me + n - 1, n)
    barrier = pltpu.get_barrier_semaphore()

    def greet(i):
        pl.semaphore_signal(barrier, inc=1, device_id={"seq": lax.rem(me + i + 1, n)}, device_id_type=MESH)

    def load(i, s, d):
        c = pltpu.make_async_copy(s, d, ld.at[i])
        c.start()
        return c

    def late(i):
        s, d = ((xm_h, mbuf), (ot_h, ot), (hat_h, hat), (wo_h, wo), (lse_h, lse), (cos_h, cos_i), (sin_h, sin_i), (ga_h, ga), (gm_h, gm))[i]
        return pltpu.make_async_copy(s, d, ld.at[1 + i])

    def to_left(src, dst, send_sem, recv_sem):
        return pltpu.make_async_remote_copy(src_ref=src, dst_ref=dst, send_sem=send_sem, recv_sem=recv_sem,
                                            device_id={"seq": left}, device_id_type=MESH)

    n_late = 9

    def push_rows(i):
        return to_left(*((lse_h, lser), (delta, deltar))[i], hsnd.at[i], hrcv.at[i])

    def push_out(p):
        pr = pl.ds(aligned(p * pw, pw), pw)
        return [to_left(dot_.at[pr, pl.ds(b * toks, WINDOW)], dor.at[pr, pl.ds(b * WINDOW, WINDOW)], osnd.at[p], orcv.at[p])
                for b in range(rows)]

    def give_out(p):
        for c in push_out(p):
            c.start()

    def put(spot, value):
        pair, kind = spot
        parts[mod(pair, RING), kind] = value.reshape(n // 2, 2, rpd, CB)

    def spot_of(name, g):
        known = {i: place[name, i] for i in range(nc)}
        return pick(g, {i: s[0] for i, s in known.items()}), pick(g, {i: s[1] for i, s in known.items()})

    def spots(it, blk):
        p, b = it // rows, mod(it, rows)
        pr = pl.ds(aligned(p * pw, pw), pw)
        return pr, pl.ds(aligned(b * toks + blk * QB, QB), QB), pl.ds(aligned(b * ext + blk * QB, QB), 3 * QB)

    def row_of(it):
        return mod(it, rows) * n_pairs + it // rows

    def mlp(hm, hmt, actt, wgu, wd, dgu, wld):
        def weights(j, slot):
            c = aligned(j * CB, CB)
            return [pltpu.make_async_copy(wg_h.at[:, pl.ds(c, CB)], wgu.at[slot, :, :CB], wld.at[slot, 0]),
                    pltpu.make_async_copy(wu_h.at[:, pl.ds(c, CB)], wgu.at[slot, :, CB:], wld.at[slot, 1]),
                    pltpu.make_async_copy(wd_h.at[pl.ds(c, CB), :], wd.at[slot], wld.at[slot, 2])]

        for c in weights(0, 0):
            c.start()
        ld_hm, ld_x, ld_hmt = load(10, hm_h, hm), load(0, dout_h, xbuf), load(11, hmt_h, hmt)
        cdiv_loop(n - 1, greet)
        gnm[:] = jnp.zeros_like(gnm)
        gsend[:] = jnp.zeros_like(gsend)
        dgain[:] = jnp.zeros_like(dgain)
        ld_hm.wait()
        ld_x.wait()
        ld_hmt.wait()
        for i in range(n_late):
            late(i).start()

        def block(j):
            slot = lax.rem(j, 2)
            for c in weights(j, slot):
                c.wait()

            @pl.when(j + 1 < nb)
            def _():
                for c in weights(j + 1, 1 - slot):
                    c.start()

            c0 = pl.multiple_of(j * CB, CB)
            with jax.named_scope("b_mlp"):
                for b in range(rows):
                    r = slice(b * toks, (b + 1) * toks)
                    gu = dot(hm[r, :], wgu[slot])
                    gact = dot(xbuf[r, :], wd[slot], NT).astype(BF).astype(F32)
                    gate, up = gu[:, :CB], gu[:, CB:]
                    sig = 1.0 / (1.0 + jnp.exp(-gate))
                    swish = gate * sig
                    actt[pl.ds(c0, CB), r] = (swish * up).astype(BF).T
                    dgu[r, :CB] = (gact * up * (sig + swish * (1.0 - sig))).astype(BF)
                    dgu[r, CB:] = (gact * swish).astype(BF)
                both = dot(hmt[:], dgu[:])
                ring = lax.rem(j, RING)
                parts[ring, 0] = both[:, :CB].reshape(n // 2, 2, rpd, CB)
                parts[ring, 1] = both[:, CB:].reshape(n // 2, 2, rpd, CB)
                for b in range(rows):
                    r = slice(b * toks, (b + 1) * toks)
                    gnm[r, :] += dot(dgu[r, :], wgu[slot], NT)

            @pl.when(j == 0)
            def _():
                pl.semaphore_wait(barrier, n - 1)
                push_rows(0).start()

            comm.tick(j)

        cdiv_loop(nb, block)

        def down(c):
            share = n // 2 // sub
            c0 = pl.multiple_of(c * CB, CB)
            for m in range(sub):
                res = dot(actt[m * width:(m + 1) * width, :], xbuf[:, pl.ds(c0, CB)]).reshape(share, 2, sub, rpd, CB)
                for i in range(sub):
                    pair = nb + c * half_sub + i // 2
                    parts[lax.rem(pair, RING), i % 2, m * share:(m + 1) * share] = res[:, :, i]

        for i in range(n_late):
            late(i).wait()

        def mid(b):
            for i in range(tb):
                r = pl.ds(pl.multiple_of((b * tb + i) * QB, QB), QB)
                out, dg = norm_back(mbuf[r, :], gm[:], gnm[r, :], xbuf[r, :])
                gmid[r, :] = out
                dgain[8:, :] += dg

        def deltas(p):
            for it in range(rows):
                for blk in range(tb):
                    pr, cols, _ = spots(p * rows + it, blk)
                    both = dot_[pr, cols].astype(F32) * ot[pr, cols].astype(F32)
                    delta[row_of(p * rows + it), blk:blk + 1, :] = jnp.concatenate(
                        [col_sum(both[:head_dim]), col_sum(both[head_dim:])], axis=1)

        def column(c):
            with jax.named_scope("b_down"):
                down(c)

            @pl.when(c < nc - 1)
            def _():
                comm.tick(nb + c + jnp.minimum(c, 1))

            @pl.when(c > 0)
            def _():
                give_out(c)

            @pl.when(c == 0)
            def _():
                with jax.named_scope("b_mid"):
                    cdiv_loop(rows, mid)
                with jax.named_scope("b_dot"):
                    dot_[:] = dot(wo[:], gmid[:], NT).astype(BF)
                    cdiv_loop(n_pairs, deltas)
                comm.tick(nb + 1)
                push_rows(1).start()
                give_out(0)

        cdiv_loop(nc, column)

    vm = lambda *s: pltpu.VMEM(s, BF)
    vf = lambda *s: pltpu.VMEM(s, F32)
    pl.run_scoped(mlp, vm(total, width), vm(width, total), vm(ff, total), vm(2, width, 2 * CB), vm(2, CB, width), vm(total, 2 * CB),
                  pltpu.SemaphoreType.DMA((2, 3)))
    def attention(q, kt, k, v, qr, dv, sc0, sc1, sc2, sr, dp0, dp1, dp2, dr, pb0, pb1, pb2, pr_, ds0, ds1, ds2, dsr):
        dqt, dkt = ot, q
        wq, wk, wv = k.at[:hd], kt.at[:, :width], v.at[:hd]
        sc, dp, pb, ds = (sc0, sc1, sc2), (dp0, dp1, dp2), (pb0, pb1, pb2), (ds0, ds1, ds2)
        lds = [load(10 + i, s, d) for i, (s, d) in enumerate(((q_h, q), (k_h, k), (v_h, v), (qr_h, qr), (kt_h, kt)))]

        def out_grad(g):
            put(spot_of("o", g), dot(ot[:], gmid[:, pl.ds(pl.multiple_of(g * CB, CB), CB)]))

        with jax.named_scope("b_dwo"):
            cdiv_loop(nc, out_grad)
        first_tick = nb + nc + 1
        comm.tick(first_tick - 1)
        upper = upper_mask()
        first, last = me == 0, me == n - 1
        halves = slice(0, WINDOW), slice(WINDOW, 3 * QB)

        def right(it, i):
            p, b = it // rows, mod(it, rows)
            return pl.ds(aligned(p * pw, pw), pw), pl.ds(aligned(b * WINDOW + i * QB, QB), QB), pl.ds(aligned(b * ext + toks + i * QB, QB), WINDOW - i * QB)

        def score(it):
            for blk in range(tb):
                pr, cols, keys = spots(it, blk)
                sc[blk][:] = dot(k[keys, pr], stack_pair(q[pr, cols]))
                dp[blk][:] = dot(v[keys, pr], stack_pair(dot_[pr, cols]))
            for i, rs in enumerate(halves):
                pr, cols, keys = right(it, i)
                sr[rs, :] = dot(k[keys, pr], stack_pair(qr[pr, cols]))
                dr[rs, :] = dot(v[keys, pr], stack_pair(dor[pr, cols]))

        def soften(it):
            row = row_of(it)
            for blk in range(tb):
                s02, s1 = merged(sc[blk][:], upper, *start_bias(first, blk))
                norm, mean = lse[row, blk:blk + 1, :], delta[row, blk:blk + 1, :]
                p02, p1 = jnp.exp(s02 - norm), jnp.exp(s1 - norm)
                g02, g1 = jnp.where(upper, dp[blk][:QB], dp[blk][2 * QB:]), dp[blk][QB:2 * QB]
                pb[blk][:] = banded(p02, p1, upper)
                ds[blk][:] = banded(p02 * (g02 - mean), p1 * (g1 - mean), upper)
            for blk in range(tb):
                i = blk // 2
                rs = slice(blk * QB, (blk + 1) * QB)
                p = jnp.exp(sr[rs, :] - jnp.where(last, -NEG, lser[row, i:i + 1, :]))
                g = p * (dr[rs, :] - deltar[row, i:i + 1, :])
                pr_[rs, :] = (p if blk == 1 else jnp.where(upper, p, 0.0)).astype(BF)
                dsr[rs, :] = (g if blk == 1 else jnp.where(upper, g, 0.0)).astype(BF)

        def grads(it):
            ks, vs = [], []
            for blk in range(tb):
                pr, cols, keys = spots(it, blk)
                own = slice(max(0, 2 - blk) * QB, 3 * QB)
                vs.append(dot(pb[blk][own, :], stack_pair(dot_[pr, cols]), NT))
                ks.append(dot(ds[blk][own, :], stack_pair(q[pr, cols]), NT))
                dq = unstack_pair(dot(kt[pr, keys], ds[blk][:])) * (head_dim ** -0.5)
                dqt[pr, cols] = rope(dq, cos_i[:, cols], sin_i[:, cols], -1, head_dim).astype(BF)
            for i, rs in enumerate(halves):
                pr, cols, _ = right(it, i)
                vs.append(dot(pr_[rs, :], stack_pair(dor[pr, cols]), NT))
                ks.append(dot(dsr[rs, :], stack_pair(qr[pr, cols]), NT))
            for j in range(tb):
                pr, cols, _ = spots(it, j)
                gv, gk = (sum(x[i][(j - max(0, i - 2)) * QB:(j - max(0, i - 2) + 1) * QB] for i in range(j, j + 3)) for x in (vs, ks))
                dv[cols, pr] = gv.astype(BF)
                dkt[pr, cols] = rope(gk.T, cos_i[:, cols], sin_i[:, cols], -1, head_dim).astype(BF)

        def close_group(g):
            cols = pl.ds(pl.multiple_of(g * CB, CB), CB)
            with jax.named_scope("b_dwqkv"):
                put(spot_of("q", g), dot(hat[:], dqt[cols, :], NT))
                put(spot_of("k", g), dot(hat[:], dkt[cols, :], NT))
                put(spot_of("v", g), dot(hat[:], dv[:, cols]))

        def weights():
            return [pltpu.make_async_copy(s, d, ld.at[10 + i]) for i, (s, d) in enumerate(((wq_h, wq), (wk_h, wk), (wv_h, wv), (x_h, xbuf)))]

        def arrived(p):
            whole = dor.at[pl.ds(aligned(p * pw, pw), pw), :]
            with jax.named_scope("b_hwait"):
                to_left(whole, whole, osnd.at[p], orcv.at[p]).wait()

        def walk(it):
            ahead = it + 1

            @pl.when((lax.rem(ahead, rows) == 0) & (ahead < n_steps))
            def _():
                arrived(ahead // rows)

            @pl.when(it < n_steps)
            def _():
                with jax.named_scope("b_attn"):
                    grads(it - 1)
                    soften(it)
                    score(jnp.minimum(ahead, n_steps - 1))

            @pl.when(it == n_steps)
            def _():
                grads(n_steps - 1)
                for c in weights():
                    c.start()

            p, step = it // rows - 1, lax.rem(it, rows)

            @pl.when((step == 0) & (lax.rem(p, per) == per - 1))
            def _():
                close_group(p // per)

            now = first_tick + 1 + p + step // (rows - 1)
            twice = now - head

            @pl.when(it == n_steps)
            def _():
                comm.offer(end)

            @pl.when((step == 0) | ((step == rows - 1) & (twice > 0)) | (it == 1))
            def _():
                comm.tick(now + jnp.maximum(twice - step // (rows - 1), 0))

            @pl.when((step == 0) & (p + 3 < n_pairs))
            def _():
                give_out(p + 3)

        for c in lds[:-1]:
            c.wait()
        for i in range(2):
            push_rows(i).wait()
        arrived(0)
        score(0)
        soften(0)
        score(1)
        lds[-1].wait()
        cdiv_loop(n_steps, lambda i: walk(i + 1))
        for c in weights():
            c.wait()

        def into(b):
            r = pl.ds(aligned(b * toks, QB), toks)
            with jax.named_scope("b_into"):
                gnm[r, :] = dot(dqt[:, r], wq[:], TN) + dot(dkt[:, r], wk[:], TN) + dot(dv[r, :], wv[:])

            with jax.named_scope("b_final"):
                for i in range(tb):
                    r = pl.ds(aligned((b * tb + i) * QB, QB), QB)
                    out, dg = norm_back(xbuf[r, :], ga[:], gnm[r, :], gmid[r, :])
                    mbuf[r, :] = out
                    dgain[:8, :] += dg

        def share_gains():
            out_copy.start()
            gains = jnp.concatenate([col_sum(dgain[:8, :]), col_sum(dgain[8:, :]), jnp.zeros((6, width), F32)], axis=0)
            for p in range(n):
                gsend[p, :, :rpd] = gains[:, p * rpd:(p + 1) * rpd]

            def spread(i):
                to = lax.rem(me + i + 1, n)
                pltpu.make_async_remote_copy(src_ref=gsend.at[to], dst_ref=grecv.at[i], send_sem=gsem.at[0], recv_sem=gsem.at[1],
                                             device_id={"seq": to}, device_id_type=MESH).start()

            cdiv_loop(n - 1, spread)

        def finish(i):
            comm.advance(end + i, True)

            @pl.when(i == 1)
            def _():
                into(0)

            @pl.when(i == LAG + 1)
            def _():
                cdiv_loop(rows - 1, lambda b: into(b + 1))
                share_gains()

        cdiv_loop(4 * LAG - 1, finish)

    score_bufs = [f(3 * QB, 2 * QB) for f in (vf, vm) for _ in range(8)]
    out_copy = pltpu.make_async_copy(mbuf, dx_h, ld.at[0])
    pl.run_scoped(attention, vm(hd, total), vm(hd, rows * ext), vm(rows * ext, hd), vm(rows * ext, hd), vm(hd, rows * WINDOW), vm(total, hd), *score_bufs)
    most, rest = pl.ds(0, end), pl.ds(end, 2)
    keep_most = load(1, fin.at[most], fin_h.at[most])
    to_left(gsend.at[pl.ds(0, n - 1)], grecv, gsem.at[0], gsem.at[1]).wait()
    sums = gsend[me]
    for i in range(n - 1):
        sums = sums + grecv[i]
    fin[end + 1, 0, :8, :128] = sums
    out_copy.wait()
    comm.advance(end + 4 * LAG - 1, True)
    with jax.named_scope("b_end"):
        keep_rest = load(0, fin.at[rest], fin_h.at[rest])
        keep_most.wait()
        keep_rest.wait()


def spread_kernel(dims, dx_i, fin_i, dx_o, dga_o, dgm_o, *refs):
    head_dim, n, width, ff = dims
    outs, (buf, fin), stage, sem = refs[:7], refs[7:9], refs[9:16], refs[16]
    dq, dk, dv, do, dg, du, dd = stage
    nb, nc, sub = ff // CB, width // CB, ff // width
    rpd = width // n
    head, place, end = plan(nb, nc * sub // 2, nc)
    get_fin = pltpu.make_async_copy(fin_i, fin, sem.at[len(outs)])
    get_fin.start()
    cut = buf.shape[0] // nc
    gets, puts = ([pltpu.make_async_copy(s.at[pl.ds(i * cut, cut)], d.at[pl.ds(i * cut, cut)], sem.at[len(outs) + k + i]) for i in range(nc)]
                  for k, s, d in ((1, dx_i, buf), (nc + 1, buf, dx_o)))
    for c in gets:
        c.start()
    get_fin.wait()
    gains = fin[end + 1, 0]
    dga_o[:] = gains[:1, :rpd]
    dgm_o[:] = gains[1:2, :rpd]
    for j in range(nb):
        dg[:, j * CB:(j + 1) * CB] = fin[j, 0]
        du[:, j * CB:(j + 1) * CB] = fin[j, 1]
    for c in range(nc):
        for i in range(sub):
            pair = nb + (c * sub + i) // 2
            dd[i * rpd:(i + 1) * rpd, c * CB:(c + 1) * CB] = fin[pair, i % 2]
    for g in range(nc):
        do[:, g * CB:(g + 1) * CB] = fin[place["o", g]]
        for name, ref in (("q", dq), ("k", dk), ("v", dv)):
            val = fin[place[name, g]]
            for h in range(CB // head_dim):
                ref[g * (CB // head_dim) + h] = val[:, h * head_dim:(h + 1) * head_dim]
    keeps = [pltpu.make_async_copy(s, d, sem.at[i]) for i, (s, d) in enumerate(zip(stage, outs))]
    for c in keeps:
        c.start()
    for get, out in zip(gets, puts):
        get.wait()
        out.start()
    for c in keeps + puts:
        c.wait()


def run_bwd(n, head_dim, ga, gm, x, dout, q, kt, k, v, hat, ot, xm, hm, hmt, qr, lse, cos_t, sin_t, wq, wk, wv, wo, wg, wu, wd, rows):
    total, width = x.shape
    hd, ff = wq.shape[0], wg.shape[1]
    toks = total // rows
    rpd, heads = width // n, hd // head_dim
    nb, nc, sub = ff // CB, width // CB, ff // width
    slots = plan(nb, nc * sub // 2, nc)[2] + 2
    n_pairs = hd // (2 * head_dim)
    f = lambda *s: jax.ShapeDtypeStruct(s, F32)
    dx_t = jax.ShapeDtypeStruct((total, width), BF)
    vm = lambda *s: pltpu.VMEM(s, BF)
    vf = lambda *s: pltpu.VMEM(s, F32)
    dma = lambda *s: pltpu.SemaphoreType.DMA(s)
    line, duo = vf(rows * n_pairs, 8, 2 * QB), (2, SLOTS)
    scratch = [vf(RING, 2, n // 2, 2, rpd, CB), vf(SLOTS, 2, n // 2, rpd, CB), vf(*duo, 2, 2, rpd, CB), vf(*duo, 2, 4, rpd, CB),
               vf(*duo, 2, rpd, CB // 2), vf(*duo, 2, rpd, CB), vf(*duo, 3, rpd, CB), vf(*duo, 4, 4, rpd, CB), vf(*duo, 4, rpd, CB), vf(slots, 2, rpd, CB),
               dma(6, *duo), dma(6, *duo),
               vm(hd, rows * WINDOW), line, line, dma(2), dma(2), dma(n_pairs), dma(n_pairs),
               vf(n, 8, 128), vf(n - 1, 8, 128), dma(2), dma(15),
               vm(total, width), vm(total, width), vf(total, width), vm(total, width), vm(hd, total), vm(width, total), vm(hd, width), vm(hd, total), line, line, vf(*cos_t.shape), vf(*cos_t.shape), vf(*ga.shape), vf(*ga.shape), vf(16, width)]
    mid = pl.pallas_call(
        functools.partial(bwd_kernel, n, head_dim, (rows, toks, width, hd, ff)), out_shape=[dx_t, f(slots, 2, rpd, CB)],
        in_specs=any_spec(24), out_specs=any_spec(2), scratch_shapes=scratch,
        compiler_params=pltpu.CompilerParams(collective_id=1, has_side_effects=True, vmem_limit_bytes=VMEM_LIMIT),
        name="backward")(ga, gm, x, dout, q, kt, k, v, hat, ot, xm, hm, hmt, qr, lse, cos_t, sin_t, wq, wk, wv, wo, wg, wu, wd)
    outs = [f(heads, rpd, head_dim)] * 3 + [f(rpd, width), f(rpd, ff), f(rpd, ff), f(ff // n, width)]
    return pl.pallas_call(
        functools.partial(spread_kernel, (head_dim, n, width, ff)), out_shape=[dx_t, f(1, rpd), f(1, rpd)] + outs,
        in_specs=any_spec(2), out_specs=any_spec(1) + vmem_spec(2) + any_spec(7),
        scratch_shapes=[vm(total, width), vf(slots, 2, rpd, CB), *[vf(*o.shape) for o in outs], dma(8 + 2 * nc)],
        name="spread")(*mid)


def solution(mesh):
    n = mesh.shape["seq"]

    def device_step(hidden, positions, g_attn, g_mlp, w_query, w_key, w_value, w_out, w_gate, w_up, w_down, d_out):
        rows, toks, width = hidden.shape
        layers, _, heads, head_dim = w_query.shape
        hd = heads * head_dim
        half = head_dim // 2
        inv_freq = 1.0 / (10000.0 ** (jnp.arange(half, dtype=F32) * (2.0 / head_dim)))
        turn = lambda w: w[0].transpose(1, 2, 0).reshape(hd, width)
        wq, wk, wv = turn(w_query), turn(w_key), turn(w_value)
        fwd = run_fwd(n, hidden, positions, inv_freq[:, None], g_attn, g_mlp, wq, wk, wv, w_out[0], head_dim)
        out = run_bwd(n, head_dim, g_attn, g_mlp, hidden.reshape(rows * toks, width), d_out.reshape(rows * toks, width), *fwd,
                      wq, wk, wv, w_out[0], w_gate[0], w_up[0], w_down[0], rows)
        dx, dga, dgm, dq, dk, dv, do, dg, du, dd = out
        back = lambda w: w.transpose(1, 0, 2)[None]
        return (dx.reshape(rows, toks, width), dga, dgm, back(dq), back(dk), back(dv), do[None], dg[None], du[None], dd[None])

    tok_spec, grad_spec = P("data", "seq"), P(None, ("data", "seq"))
    in_specs = (tok_spec, tok_spec) + (P(),) * 9 + (tok_spec,)
    out_specs = (tok_spec,) + (grad_spec,) * 9
    return jax.shard_map(device_step, mesh=mesh, in_specs=in_specs, out_specs=out_specs, check_vma=False)
```

```python
import functools, math
import numpy as np
import jax, jax.numpy as jnp
from jax import lax
from jax.experimental import pallas as pl
from jax.experimental.pallas import tpu as pltpu
from jax.sharding import PartitionSpec as P

WINDOW = 256
NORM_EPS = 1e-5
QB = 128
BF, F32 = jnp.bfloat16, jnp.float32
NN, NT, TN = ((1,), (0,)), ((1,), (1,)), ((0,), (0,))
MESH = pl.DeviceIdType.MESH
NEG = -1e30
VMEM_LIMIT = 67043328


def dot(a, b, dims=NN):
    return lax.dot_general(a, b, (dims, ((), ())), preferred_element_type=F32)


def cdiv_loop(n, body):
    lax.fori_loop(0, n, lambda i, c: body(i) or c, 0)


def mod(a, b):
    return a % b if isinstance(a, int) else lax.rem(a, b)


def aligned(a, b):
    return a if isinstance(a, int) else pl.multiple_of(a, b)


def rope(blk, cos_b, sin_b, sign, head_dim):
    half = head_dim // 2
    parts = []
    for h in range(blk.shape[0] // head_dim):
        first = blk[h * head_dim:h * head_dim + half]
        second = blk[h * head_dim + half:(h + 1) * head_dim]
        if sign > 0:
            parts += [first * cos_b - second * sin_b, second * cos_b + first * sin_b]
        else:
            parts += [first * cos_b + second * sin_b, second * cos_b - first * sin_b]
    return jnp.concatenate(parts, axis=0)


def normed(x, gain):
    xf = x.astype(F32)
    inv = lax.rsqrt(jnp.mean(xf * xf, axis=-1, keepdims=True) + NORM_EPS)
    return (xf * inv * gain).astype(BF)


def stack_pair(pair_t):
    half = pair_t.shape[0] // 2
    zero = jnp.zeros((half, pair_t.shape[1]), pair_t.dtype)
    return jnp.concatenate(
        [jnp.concatenate([pair_t[:half], zero], axis=0), jnp.concatenate([zero, pair_t[half:]], axis=0)], axis=1)


def unstack_pair(both):
    half, cols = both.shape[0] // 2, both.shape[1] // 2
    return jnp.concatenate([both[:half, :cols], both[half:, cols:]], axis=0)


def col_sum(x):
    return jnp.sum(x, axis=0, keepdims=True)


def merged(scores, upper, bias0, bias1):
    return jnp.where(upper, scores[:QB] + bias0, scores[2 * QB:]), scores[QB:2 * QB] + bias1


def banded(p02, p1, upper):
    return jnp.concatenate(
        [jnp.where(upper, p02, 0.0).astype(BF), p1.astype(BF), jnp.where(upper, 0.0, p02).astype(BF)], axis=0)


def upper_mask():
    key_ids = lax.broadcasted_iota(jnp.int32, (QB, 2 * QB), 0)
    query_ids = lax.broadcasted_iota(jnp.int32, (QB, 2 * QB), 1) % QB
    return key_ids > query_ids


def start_bias(first, blk):
    bias = jnp.where(first, NEG, 0.0).astype(F32)
    return (bias if blk < 2 else 0.0), (bias if blk < 1 else 0.0)


def fwd_kernel(n, head_dim, x_h, pos_h, invf_h, ga_h, gm_h, wq_h, wk_h, wv_h, wo_h,
               q_h, kt_h, k_h, v_h, hat_h, ot_h, xm_h, hm_h, hmt_h, qr_h, lse_h, cos_t, sin_t,
               pos, invf, ga, gm, xv, halo, qr, lse, pos_halo, wq, wk, wv, wo, q, kt, k, v, vt, hat, ot, xm, hm, hmt, hb, hh, acc, acc2, ak, av, cos_h, sin_h,
               sc0, sc1, sc2, pb0, pb1, pb2, ldx, ld, st, snd, rcv, qsnd, qrcv):
    sc, pb = (sc0, sc1, sc2), (pb0, pb1, pb2)
    rows, toks, width = xv.shape
    ext, total, pw = toks + WINDOW, rows * toks, 2 * head_dim
    n_pairs = wq.shape[0] // pw
    tb, n_steps = toks // QB, n_pairs * rows
    me = lax.axis_index("seq")
    right, left = lax.rem(me + 1, n), lax.rem(me + n - 1, n)
    load_x = [pltpu.make_async_copy(x_h.at[b], xv.at[b], ldx.at[b]) for b in range(rows)]
    load_w = [pltpu.make_async_copy(s, d, ld.at[i]) for i, (s, d) in enumerate(((wq_h, wq), (wk_h, wk), (wv_h, wv), (wo_h, wo)))]
    load_s = [pltpu.make_async_copy(s, d, ldx.at[rows + i]) for i, (s, d) in enumerate(((pos_h, pos), (invf_h, invf), (ga_h, ga), (gm_h, gm)))]
    for c in load_s + load_x:
        c.start()
    barrier = pltpu.get_barrier_semaphore()
    for other in (left, right):
        pl.semaphore_signal(barrier, inc=1, device_id={"seq": other}, device_id_type=MESH)

    def push(i, s, d):
        return pltpu.make_async_remote_copy(src_ref=s, dst_ref=d, send_sem=snd.at[i], recv_sem=rcv.at[i], device_id={"seq": right}, device_id_type=MESH)

    def push_rows(b):
        return push(b, x_h.at[b, toks - WINDOW:, :], halo.at[b])

    send_pos = push(rows, pos, pos_halo)

    def angles(cos_ref, sin_ref, positions):
        count = positions.shape[1]
        for b in range(rows):
            ang = invf[:] * positions[b:b + 1, :].astype(F32)
            cos_ref[:, b * count:(b + 1) * count] = jnp.cos(ang)
            sin_ref[:, b * count:(b + 1) * count] = jnp.sin(ang)

    for c in load_s:
        c.wait()
    angles(cos_t, sin_t, pos[:])

    def norm_rows(b):
        for i in range(tb):
            h = normed(xv[b, i * QB:(i + 1) * QB, :], ga[:])
            hb[pl.ds(pl.multiple_of((b * tb + i) * QB, QB), QB), :] = h

    with jax.named_scope("f_norm"):
        for c in load_x:
            c.wait()
        for c in load_w:
            c.start()
        cdiv_loop(rows, norm_rows)
    pl.semaphore_wait(barrier, 2)
    send_pos.start()
    for b in range(rows):
        push_rows(b).start()
    keep_hat = pltpu.make_async_copy(hat, hat_h, st.at[0])
    tables = cos_t[:], sin_t[:]

    def put_q(src):
        for p in range(n_pairs):
            r = slice(p * pw, (p + 1) * pw)
            q[r, :] = (rope(src[r, :], *tables, 1, head_dim) * (head_dim ** -0.5)).astype(BF)

    def put_own(src, dst_t, dst):
        for p in range(n_pairs):
            r = slice(p * pw, (p + 1) * pw)
            both = (rope(src[r, :], *tables, 1, head_dim) if dst is k else src[r, :]).astype(BF)
            for b in range(rows):
                blk = both[:, b * toks:(b + 1) * toks]
                own = slice(b * ext + WINDOW, (b + 1) * ext)
                dst_t[r, own] = blk
                dst[own, r] = blk.T

    with jax.named_scope("f_mm"):
        load_w[0].wait()
        load_w[1].wait()
        load_w[2].wait()
        acc[:] = dot(wq[:], hb[:], NT)
        acc2[:] = dot(wk[:], hb[:], NT)
        put_q(acc)
        acc[:] = dot(wv[:], hb[:], NT)
        put_own(acc2, kt, k)
        for i in range(total // QB):
            r = slice(i * QB, (i + 1) * QB)
            hat[:, r] = hb[r, :].T
        put_own(acc, vt, v)
    keep_hat.start()
    keep_q = pltpu.make_async_copy(q, q_h, st.at[1])
    keep_q.start()

    def push_q(b):
        return pltpu.make_async_remote_copy(src_ref=q.at[:, b * toks:b * toks + WINDOW], dst_ref=qr.at[:, b * WINDOW:(b + 1) * WINDOW],
                                            send_sem=qsnd.at[b], recv_sem=qrcv.at[b], device_id={"seq": left}, device_id_type=MESH)

    for b in range(rows):
        push_q(b).start()
    send_pos.wait()
    angles(cos_h, sin_h, pos_halo[:, toks - WINDOW:])

    def keeps(b):
        wide, cols = pl.ds(pl.multiple_of(b * ext, QB), ext), pl.ds(pl.multiple_of(b * toks, QB), toks)
        ends = ((kt.at[:, wide], kt_h.at[:, wide]), (k.at[wide, :], k_h.at[wide, :]), (v.at[wide, :], v_h.at[wide, :]),
                (ot.at[:, cols], ot_h.at[:, cols]), (hm.at[cols, :], hm_h.at[cols, :]), (hmt.at[:, cols], hmt_h.at[:, cols]),
                (xm.at[cols, :], xm_h.at[cols, :]))
        return [pltpu.make_async_copy(s, d, st.at[2 + b * len(ends) + i]) for i, (s, d) in enumerate(ends)]

    def halo_in(b):
        with jax.named_scope("f_halo_wait"):
            push_rows(b).wait()
        with jax.named_scope("f_halo"):
            for i in range(WINDOW // QB):
                r = slice(i * QB, (i + 1) * QB)
                hh[r, :] = normed(halo[b, r, :], ga[:])
            ak[:] = dot(wk[:], hh[:], NT)
            av[:] = dot(wv[:], hh[:], NT)
            cols = pl.ds(pl.multiple_of(b * WINDOW, QB), WINDOW)
            wide = pl.ds(pl.multiple_of(b * ext, QB), WINDOW)
            near = cos_h[:, cols], sin_h[:, cols]
            for src, dst_t, dst in ((ak, kt, k), (av, vt, v)):
                for p in range(n_pairs):
                    r = slice(p * pw, (p + 1) * pw)
                    blk = (rope(src[r, :], *near, 1, head_dim) if dst is k else src[r, :]).astype(BF)
                    dst_t[r, wide] = blk
                    dst[wide, r] = blk.T
        for c in keeps(b)[:3]:
            c.start()

    upper = upper_mask()
    first = me == 0

    def spots(it, blk):
        b, p = it // n_pairs, mod(it, n_pairs)
        pr = pl.ds(aligned(p * pw, pw), pw)
        return pr, pl.ds(aligned(b * toks + blk * QB, QB), QB), pl.ds(aligned(b * ext + blk * QB, QB), 3 * QB)

    def score(it):
        for blk in range(tb):
            pr, cols, keys = spots(it, blk)
            sc[blk][:] = dot(k[keys, pr], stack_pair(q[pr, cols]))

    def soften(it, blk):
        s02, s1 = merged(sc[blk][:], upper, *start_bias(first, blk))
        top = jnp.max(jnp.maximum(s02, s1), axis=0, keepdims=True)
        e02, e1 = jnp.exp(s02 - top), jnp.exp(s1 - top)
        mass = col_sum(e02 + e1)
        inv = 1.0 / mass
        lse[it, blk:blk + 1, :] = top + jnp.log(mass)
        pb[blk][:] = banded(e02 * inv, e1 * inv, upper)

    def mix(it):
        for blk in range(tb):
            pr, cols, keys = spots(it, blk)
            ot[pr, cols] = unstack_pair(dot(vt[pr, keys], pb[blk][:])).astype(BF)

    def project(b):
        cols = pl.ds(pl.multiple_of(b * toks, QB), toks)
        with jax.named_scope("f_proj"):
            mid = (xv[b].astype(F32) + dot(ot[:, cols], wo[:], TN)).astype(BF)
            xm[cols, :] = mid
            h = normed(mid, gm[:])
            hm[cols, :] = h
            hmt[:, cols] = h.T
        for c in keeps(b)[3:]:
            c.start()

    keep_qr, keep_lse = (pltpu.make_async_copy(*ends, ld.at[i]) for i, ends in enumerate(((qr, qr_h), (lse, lse_h))))
    load_w[3].wait()
    for blk in range(tb):
        pb[blk][:] = jnp.zeros(pb[blk].shape, BF)

    def walk(i):
        it = i - 1

        @pl.when((lax.rem(i, n_pairs) == 0) & (i < n_steps))
        def _():
            halo_in(i // n_pairs)

        @pl.when(i == 0)
        def _():
            score(0)

        @pl.when((i > 0) & (i <= n_steps))
        def _():
            with jax.named_scope("f_attn"):
                mix(jnp.maximum(it - 1, 0))
                for blk in range(tb):
                    soften(it, blk)
                score(jnp.minimum(i, n_steps - 1))

        @pl.when(i == n_steps)
        def _():
            for b in range(rows):
                push_q(b).wait()
            keep_qr.start()

        @pl.when(i > n_steps)
        def _():
            mix(n_steps - 1)

        @pl.when((lax.rem(it, n_pairs) == 0) & (it > 0))
        def _():
            project(it // n_pairs - 1)

    cdiv_loop(n_steps + 2, walk)
    with jax.named_scope("f_store_wait"):
        keep_lse.start()
        keep_hat.wait()
        keep_q.wait()
        keep_qr.wait()
        keep_lse.wait()
        for b in range(rows):
            for c in keeps(b):
                c.wait()


def any_spec(k):
    return [pl.BlockSpec(memory_space=pl.ANY)] * k


def vmem_spec(k):
    return [pl.BlockSpec(memory_space=pltpu.VMEM)] * k


def run_fwd(n, x, pos, invf, ga, gm, wq, wk, wv, wo, head_dim):
    rows, toks, width = x.shape
    hd = wq.shape[0]
    ext, total, n_halo = toks + WINDOW, rows * toks, rows * WINDOW
    half = head_dim // 2
    sds = lambda *s: jax.ShapeDtypeStruct(s, BF)
    dma = lambda *s: pltpu.SemaphoreType.DMA(s)
    outs = [sds(hd, total), sds(hd, rows * ext), sds(rows * ext, hd), sds(rows * ext, hd), sds(width, total), sds(hd, total), sds(total, width), sds(total, width), sds(width, total)]
    outs += [sds(hd, n_halo), jax.ShapeDtypeStruct((rows * hd // (2 * head_dim), 8, 2 * QB), F32)] + [jax.ShapeDtypeStruct((half, total), F32)] * 2
    vm = lambda *s: pltpu.VMEM(s, BF)
    vf = lambda *s: pltpu.VMEM(s, F32)
    scratch = [pltpu.VMEM((rows, toks), jnp.int32), vf(*invf.shape), vf(*ga.shape), vf(*ga.shape), vm(rows, toks, width), vm(rows, WINDOW, width), vm(hd, n_halo), vf(rows * hd // (2 * head_dim), 8, 2 * QB), pltpu.VMEM((rows, toks), jnp.int32), vm(hd, width), vm(hd, width), vm(hd, width), vm(hd, width),
               vm(hd, total), vm(hd, rows * ext), vm(rows * ext, hd), vm(rows * ext, hd), vm(hd, rows * ext), vm(width, total), vm(hd, total), vm(total, width), vm(total, width), vm(width, total), vm(total, width), vm(WINDOW, width),
               vf(hd, total), vf(hd, total), vf(hd, WINDOW), vf(hd, WINDOW), vf(half, n_halo), vf(half, n_halo),
               *[f(3 * QB, 2 * QB) for f in (vf, vm) for _ in range(3)],
               dma(rows + 4), dma(4), dma(2 + 7 * rows), dma(rows + 1), dma(rows + 1), dma(rows), dma(rows)]
    return pl.pallas_call(
        functools.partial(fwd_kernel, n, head_dim), out_shape=outs,
        in_specs=any_spec(9), out_specs=any_spec(11) + vmem_spec(2), scratch_shapes=scratch,
        compiler_params=pltpu.CompilerParams(collective_id=0, has_side_effects=True, vmem_limit_bytes=VMEM_LIMIT),
        name="forward")(x, pos, invf, ga, gm, wq, wk, wv, wo)


LAG = 2
SLOTS = 2 * LAG
RING = 8
CB = 256


def at(ref, *idx):
    return ref.at[idx]


class Torus:
    def __init__(self, n, head, last, turn, parts, recv0, recv1, recv2, recv3, recv4, recv5, acc, acc2, fin, snd, rcv):
        assert math.isqrt(n // 2) == 4
        me = lax.axis_index("seq")
        self.core = lax.rem(me, 2)
        chip = me // 2
        self.x, self.y = lax.rem(chip, 4), chip // 4
        self.head, self.last, self.turn = head, last, turn
        self.parts, self.recv0, self.recv1, self.recv2, self.recv3, self.recv4, self.recv5 = parts, recv0, recv1, recv2, recv3, recv4, recv5
        self.acc, self.acc2, self.fin, self.snd, self.rcv = acc, acc2, fin, snd, rcv
        self.partner = me + 1 - 2 * self.core
        self.rows, self.columns = [lax.rem(self.y + d, 4) * 4 for d in range(4)], [lax.rem(self.x + d, 4) for d in range(4)]
        self.hops = [[self.device(0, d) for d in range(4)], [self.device(d, 0) for d in range(4)]]

    def device(self, dy, dx):
        return (self.rows[dy] + self.columns[dx]) * 2 + self.core

    def copy(self, lane, kind, slot, src, dst, target):
        return pltpu.make_async_remote_copy(
            src_ref=src, dst_ref=dst, send_sem=self.snd.at[lane, kind, slot], recv_sem=self.rcv.at[lane, kind, slot],
            device_id={"seq": target}, device_id_type=MESH)

    def late(self, axis, pair, yes, no):
        first, end = self.turn
        busy = (pair >= first) & (pair < end)
        return jnp.where(busy & (self.x == 3) if axis else busy, yes, no)

    def swap(self, ring, slot):
        return self.copy(0, 0, slot, self.parts.at[ring, :, :, 1 - self.core], self.recv0.at[slot], self.partner)

    def landing(self, stage):
        return (self.recv0, self.recv1, self.recv2, self.recv3, self.recv4, self.recv5)[stage]

    def arrived(self, stage, kind, slot):
        whole = self.landing(stage).at[kind, slot]
        self.copy(stage, kind, slot, whole, whole, self.partner).wait()

    def send(self, stage, kind, pair, held, slot):
        axis = kind if stage < 3 else 1 - kind
        plus, minus = self.hops[axis][1], self.hops[axis][-1]
        half = CB // 2
        if stage == 1:
            minus = self.late(axis, pair, plus, minus)
            ends = self.acc.at[kind, held, 2, :2], self.acc.at[kind, held, 2, 2:]
        elif stage == 2:
            ends = self.acc.at[kind, held, 1], self.acc.at[kind, held, 3]
        elif stage == 3:
            ends = self.acc2.at[kind, held, 2, :, :half], self.acc2.at[kind, held, 2, :, half:]
        else:
            ends = self.acc2.at[kind, held, 1], self.acc2.at[kind, held, 3]
        for i, src in enumerate(ends):
            self.copy(stage, kind, slot, src, self.landing(stage).at[kind, slot, i], (plus, minus)[i]).start()

    def add(self, stage, kind, pair, held, slot, ring):
        acc, acc2 = self.acc, self.acc2
        if stage == 1:
            for r1 in range(4):
                for r2 in range(4):
                    ry, rx = (r2, r1) if kind == 0 else (r1, r2)
                    chip = self.rows[ry] + self.columns[rx]
                    acc[kind, held, r1, r2] = self.parts[ring, kind, chip, self.core] + self.recv0[slot, kind, chip]
        elif stage == 2:
            back = self.late(kind, pair, 1, 3)
            acc[kind, held, 1, :2] += self.recv1[kind, slot, 0]
            acc[kind, held, back, 2:] += self.recv1[kind, slot, 1]
        elif stage == 3:
            acc2[kind, held] = acc[kind, held, 0] + (self.recv2[kind, slot, 0] + self.recv2[kind, slot, 1])
        elif stage == 4:
            half = CB // 2
            acc2[kind, held, 1, :, :half] += self.recv3[kind, slot, 0]
            acc2[kind, held, 3, :, half:] += self.recv3[kind, slot, 1]
        else:
            self.fin[pair, kind] = acc2[kind, held, 0] + (self.recv4[kind, slot, 0] + self.recv4[kind, slot, 1])

    def direct(self, kind, held, slot):
        for d in range(1, 4):
            self.copy(5, kind, slot, self.acc2.at[kind, held, d], self.recv5.at[kind, slot, d - 1], self.hops[1 - kind][d]).start()

    def early(self, pair):
        return (pair >= 0) & (pair <= self.head)

    def final(self, pair):
        return (pair == self.last) | ((pair > self.head) & (pair < self.last) & (mod(abs(pair - self.head), 2) == 0))

    def when(self, which, fn):
        if isinstance(which, bool):
            fn() if which else None
        else:
            pl.when(which)(fn)

    def offer(self, t):
        self.when(self.early(t) | self.final(t), lambda: self.swap(mod(t, RING), mod(t, SLOTS)).start())

    def tick(self, t):
        self.offer(t)
        self.advance(t)

    def advance(self, t, tail=False):
        now, land, before = mod(t, SLOTS), mod(t + SLOTS - LAG, SLOTS), mod(t + SLOTS - 1, SLOTS)
        ring_land = mod(t + RING - 1, RING)
        for stage in range(5, 0, -1):
            pair = t - LAG * stage + 1
            held = before if stage % 2 else mod(t + 1, SLOTS)

            def move(last_hops, stage=stage, pair=pair, held=held):
                if stage == 1:
                    with jax.named_scope("t_wait1"):
                        self.swap(ring_land, before).wait()
                for kind in range(2):
                    if last_hops and stage == 4:
                        with jax.named_scope("t_wait6"):
                            self.arrived(5, kind, land)
                        got = self.recv5[kind, land]
                        self.fin[pair, kind] = self.acc2[kind, held, 0] + (got[0] + got[1] + got[2])
                        continue
                    if stage > 1:
                        with jax.named_scope(f"t_wait{stage}"):
                            self.arrived(stage - 1, kind, land)
                    self.add(stage, kind, pair, held, land if stage > 1 else before, ring_land)
                    if last_hops and stage == 3:
                        self.direct(kind, held, now)
                    elif stage < 5:
                        self.send(stage, kind, pair, held, now)

            if stage < 3:
                self.when(self.early(pair) | self.final(pair), functools.partial(move, False))
            else:
                self.when(self.early(pair), functools.partial(move, False))
                if tail and stage < 5:
                    self.when(self.final(pair), functools.partial(move, True))


def pick(i, table):
    out = 0
    for key, value in table.items():
        out = jnp.where(i == key, value, out)
    return out


def norm_back(x, gain, grad, res):
    xf = x.astype(F32)
    inv = lax.rsqrt(jnp.mean(xf * xf, axis=-1, keepdims=True) + NORM_EPS)
    unit = xf * inv
    gu = grad * gain
    out = inv * (gu - unit * jnp.mean(gu * unit, axis=-1, keepdims=True)) + res.astype(F32)
    gu = grad * unit
    return out.astype(BF), jnp.sum(gu.reshape(-1, 8, gu.shape[-1]), axis=0)


def plan(n_mlp, n_down, nc):
    order = [("o", g) for g in range(nc)] + [(name, g) for g in range(nc) for name in "qkv"]
    base, head = n_mlp + n_down, n_mlp + n_down + nc - 1
    last = 2 * (base - 1 - head + len(order) // 2) + head - 1
    spot = lambda pair: min(max(pair, 2 * pair - head), last)
    return head, {name: (spot(base + i // 2), i % 2) for i, name in enumerate(order)}, last


def bwd_kernel(n, head_dim, dims, ga_h, gm_h, x_h, dout_h, q_h, kt_h, k_h, v_h, hat_h, ot_h, xm_h, hm_h, hmt_h, qr_h, lse_h, cos_h, sin_h,
               wq_h, wk_h, wv_h, wo_h, wg_h, wu_h, wd_h,
               dx_h, fin_h,
               parts, recv0, recv1, recv2, recv3, recv4, recv5, acc, acc2, fin, snd, rcv,
               dor, lser, deltar, hsnd, hrcv, osnd, orcv, gsend, grecv, gsem, ld,
               xbuf, mbuf, gnm, gmid, ot, hat, wo, dot_, lse, delta, cos_i, sin_i, ga, gm, dgain):
    rows, toks, width, hd, ff = dims
    ext, total = toks + WINDOW, rows * toks
    pw = 2 * head_dim
    n_pairs = hd // pw
    tb, n_steps = toks // QB, n_pairs * rows
    nb, nc, sub = ff // CB, width // CB, ff // width
    rpd = width // n
    per, half_sub = CB // pw, sub // 2
    head, place, end = plan(nb, nc * half_sub, nc)
    comm = Torus(n, head, end, (nb, nb + n_pairs + 1), parts, recv0, recv1, recv2, recv3, recv4, recv5, acc, acc2, fin, snd, rcv)
    me = lax.axis_index("seq")
    left = lax.rem(me + n - 1, n)
    barrier = pltpu.get_barrier_semaphore()

    def greet(i):
        pl.semaphore_signal(barrier, inc=1, device_id={"seq": lax.rem(me + i + 1, n)}, device_id_type=MESH)

    def load(i, s, d):
        c = pltpu.make_async_copy(s, d, ld.at[i])
        c.start()
        return c

    def late(i):
        s, d = ((xm_h, mbuf), (ot_h, ot), (hat_h, hat), (wo_h, wo), (lse_h, lse), (cos_h, cos_i), (sin_h, sin_i), (ga_h, ga), (gm_h, gm))[i]
        return pltpu.make_async_copy(s, d, ld.at[1 + i])

    def to_left(src, dst, send_sem, recv_sem):
        return pltpu.make_async_remote_copy(src_ref=src, dst_ref=dst, send_sem=send_sem, recv_sem=recv_sem,
                                            device_id={"seq": left}, device_id_type=MESH)

    n_late = 9

    def push_rows(i):
        return to_left(*((lse_h, lser), (delta, deltar))[i], hsnd.at[i], hrcv.at[i])

    def push_out(p):
        pr = pl.ds(aligned(p * pw, pw), pw)
        return [to_left(dot_.at[pr, pl.ds(b * toks, WINDOW)], dor.at[pr, pl.ds(b * WINDOW, WINDOW)], osnd.at[p], orcv.at[p])
                for b in range(rows)]

    def give_out(p):
        for c in push_out(p):
            c.start()

    def put(spot, value):
        pair, kind = spot
        parts[mod(pair, RING), kind] = value.reshape(n // 2, 2, rpd, CB)

    def spot_of(name, g):
        known = {i: place[name, i] for i in range(nc)}
        return pick(g, {i: s[0] for i, s in known.items()}), pick(g, {i: s[1] for i, s in known.items()})

    def spots(it, blk):
        p, b = it // rows, mod(it, rows)
        pr = pl.ds(aligned(p * pw, pw), pw)
        return pr, pl.ds(aligned(b * toks + blk * QB, QB), QB), pl.ds(aligned(b * ext + blk * QB, QB), 3 * QB)

    def row_of(it):
        return mod(it, rows) * n_pairs + it // rows

    def mlp(hm, hmt, actt, wgu, wd, dgu, wld):
        def weights(j, slot):
            c = aligned(j * CB, CB)
            return [pltpu.make_async_copy(wg_h.at[:, pl.ds(c, CB)], wgu.at[slot, :, :CB], wld.at[slot, 0]),
                    pltpu.make_async_copy(wu_h.at[:, pl.ds(c, CB)], wgu.at[slot, :, CB:], wld.at[slot, 1]),
                    pltpu.make_async_copy(wd_h.at[pl.ds(c, CB), :], wd.at[slot], wld.at[slot, 2])]

        for c in weights(0, 0):
            c.start()
        ld_hm, ld_x, ld_hmt = load(10, hm_h, hm), load(0, dout_h, xbuf), load(11, hmt_h, hmt)
        cdiv_loop(n - 1, greet)
        gnm[:] = jnp.zeros_like(gnm)
        gsend[:] = jnp.zeros_like(gsend)
        dgain[:] = jnp.zeros_like(dgain)
        ld_hm.wait()
        ld_x.wait()
        ld_hmt.wait()
        for i in range(n_late):
            late(i).start()

        def block(j):
            slot = lax.rem(j, 2)
            for c in weights(j, slot):
                c.wait()

            @pl.when(j + 1 < nb)
            def _():
                for c in weights(j + 1, 1 - slot):
                    c.start()

            c0 = pl.multiple_of(j * CB, CB)
            with jax.named_scope("b_mlp"):
                for b in range(rows):
                    r = slice(b * toks, (b + 1) * toks)
                    gu = dot(hm[r, :], wgu[slot])
                    gact = dot(xbuf[r, :], wd[slot], NT).astype(BF).astype(F32)
                    gate, up = gu[:, :CB], gu[:, CB:]
                    sig = 1.0 / (1.0 + jnp.exp(-gate))
                    swish = gate * sig
                    actt[pl.ds(c0, CB), r] = (swish * up).astype(BF).T
                    dgu[r, :CB] = (gact * up * (sig + swish * (1.0 - sig))).astype(BF)
                    dgu[r, CB:] = (gact * swish).astype(BF)
                both = dot(hmt[:], dgu[:])
                ring = lax.rem(j, RING)
                parts[ring, 0] = both[:, :CB].reshape(n // 2, 2, rpd, CB)
                parts[ring, 1] = both[:, CB:].reshape(n // 2, 2, rpd, CB)
                for b in range(rows):
                    r = slice(b * toks, (b + 1) * toks)
                    gnm[r, :] += dot(dgu[r, :], wgu[slot], NT)

            @pl.when(j == 0)
            def _():
                pl.semaphore_wait(barrier, n - 1)
                push_rows(0).start()

            comm.tick(j)

        cdiv_loop(nb, block)

        def down(c):
            share = n // 2 // sub
            c0 = pl.multiple_of(c * CB, CB)
            for m in range(sub):
                res = dot(actt[m * width:(m + 1) * width, :], xbuf[:, pl.ds(c0, CB)]).reshape(share, 2, sub, rpd, CB)
                for i in range(sub):
                    pair = nb + c * half_sub + i // 2
                    parts[lax.rem(pair, RING), i % 2, m * share:(m + 1) * share] = res[:, :, i]

        for i in range(n_late):
            late(i).wait()

        def mid(b):
            for i in range(tb):
                r = pl.ds(pl.multiple_of((b * tb + i) * QB, QB), QB)
                out, dg = norm_back(mbuf[r, :], gm[:], gnm[r, :], xbuf[r, :])
                gmid[r, :] = out
                dgain[8:, :] += dg

        def deltas(p):
            for it in range(rows):
                for blk in range(tb):
                    pr, cols, _ = spots(p * rows + it, blk)
                    both = dot_[pr, cols].astype(F32) * ot[pr, cols].astype(F32)
                    delta[row_of(p * rows + it), blk:blk + 1, :] = jnp.concatenate(
                        [col_sum(both[:head_dim]), col_sum(both[head_dim:])], axis=1)

        def column(c):
            with jax.named_scope("b_down"):
                down(c)

            @pl.when(c < nc - 1)
            def _():
                comm.tick(nb + c + jnp.minimum(c, 1))

            @pl.when(c > 0)
            def _():
                give_out(c)

            @pl.when(c == 0)
            def _():
                with jax.named_scope("b_mid"):
                    cdiv_loop(rows, mid)
                with jax.named_scope("b_dot"):
                    dot_[:] = dot(wo[:], gmid[:], NT).astype(BF)
                    cdiv_loop(n_pairs, deltas)
                comm.tick(nb + 1)
                push_rows(1).start()
                give_out(0)

        cdiv_loop(nc, column)

    vm = lambda *s: pltpu.VMEM(s, BF)
    vf = lambda *s: pltpu.VMEM(s, F32)
    pl.run_scoped(mlp, vm(total, width), vm(width, total), vm(ff, total), vm(2, width, 2 * CB), vm(2, CB, width), vm(total, 2 * CB),
                  pltpu.SemaphoreType.DMA((2, 3)))
    def attention(q, kt, k, v, qr, dv, sc0, sc1, sc2, sr, dp0, dp1, dp2, dr, pb0, pb1, pb2, pr_, ds0, ds1, ds2, dsr):
        dqt, dkt = ot, q
        wq, wk, wv = k.at[:hd], kt.at[:, :width], v.at[:hd]
        sc, dp, pb, ds = (sc0, sc1, sc2), (dp0, dp1, dp2), (pb0, pb1, pb2), (ds0, ds1, ds2)
        lds = [load(10 + i, s, d) for i, (s, d) in enumerate(((q_h, q), (k_h, k), (v_h, v), (qr_h, qr), (kt_h, kt)))]

        def out_grad(g):
            put(spot_of("o", g), dot(ot[:], gmid[:, pl.ds(pl.multiple_of(g * CB, CB), CB)]))

        with jax.named_scope("b_dwo"):
            cdiv_loop(nc, out_grad)
        first_tick = nb + nc + 1
        comm.tick(first_tick - 1)
        ends = [rows * p for p in range(1, n_pairs + 1)]
        steps = sorted([1, ends[1] - 1, ends[-2] - 1, ends[-1] - 1, *ends[1:]])
        tick_after = {s: first_tick + i for i, s in enumerate(steps)}
        assert first_tick + len(steps) == end
        upper = upper_mask()
        first, last = me == 0, me == n - 1
        halves = slice(0, WINDOW), slice(WINDOW, 3 * QB)

        def right(it, i):
            p, b = it // rows, mod(it, rows)
            return pl.ds(aligned(p * pw, pw), pw), pl.ds(aligned(b * WINDOW + i * QB, QB), QB), pl.ds(aligned(b * ext + toks + i * QB, QB), WINDOW - i * QB)

        def score(it):
            for blk in range(tb):
                pr, cols, keys = spots(it, blk)
                sc[blk][:] = dot(k[keys, pr], stack_pair(q[pr, cols]))
                dp[blk][:] = dot(v[keys, pr], stack_pair(dot_[pr, cols]))
            for i, rs in enumerate(halves):
                pr, cols, keys = right(it, i)
                sr[rs, :] = dot(k[keys, pr], stack_pair(qr[pr, cols]))
                dr[rs, :] = dot(v[keys, pr], stack_pair(dor[pr, cols]))

        def soften(it):
            row = row_of(it)
            for blk in range(tb):
                s02, s1 = merged(sc[blk][:], upper, *start_bias(first, blk))
                norm, mean = lse[row, blk:blk + 1, :], delta[row, blk:blk + 1, :]
                p02, p1 = jnp.exp(s02 - norm), jnp.exp(s1 - norm)
                g02, g1 = jnp.where(upper, dp[blk][:QB], dp[blk][2 * QB:]), dp[blk][QB:2 * QB]
                pb[blk][:] = banded(p02, p1, upper)
                ds[blk][:] = banded(p02 * (g02 - mean), p1 * (g1 - mean), upper)
            for blk in range(tb):
                i = blk // 2
                rs = slice(blk * QB, (blk + 1) * QB)
                p = jnp.exp(sr[rs, :] - jnp.where(last, -NEG, lser[row, i:i + 1, :]))
                g = p * (dr[rs, :] - deltar[row, i:i + 1, :])
                pr_[rs, :] = (p if blk == 1 else jnp.where(upper, p, 0.0)).astype(BF)
                dsr[rs, :] = (g if blk == 1 else jnp.where(upper, g, 0.0)).astype(BF)

        def grads(it):
            ks, vs = [], []
            for blk in range(tb):
                pr, cols, keys = spots(it, blk)
                own = slice(max(0, 2 - blk) * QB, 3 * QB)
                vs.append(dot(pb[blk][own, :], stack_pair(dot_[pr, cols]), NT))
                ks.append(dot(ds[blk][own, :], stack_pair(q[pr, cols]), NT))
                dq = unstack_pair(dot(kt[pr, keys], ds[blk][:])) * (head_dim ** -0.5)
                dqt[pr, cols] = rope(dq, cos_i[:, cols], sin_i[:, cols], -1, head_dim).astype(BF)
            for i, rs in enumerate(halves):
                pr, cols, _ = right(it, i)
                vs.append(dot(pr_[rs, :], stack_pair(dor[pr, cols]), NT))
                ks.append(dot(dsr[rs, :], stack_pair(qr[pr, cols]), NT))
            for j in range(tb):
                pr, cols, _ = spots(it, j)
                gv, gk = (sum(x[i][(j - max(0, i - 2)) * QB:(j - max(0, i - 2) + 1) * QB] for i in range(j, j + 3)) for x in (vs, ks))
                dv[cols, pr] = gv.astype(BF)
                dkt[pr, cols] = rope(gk.T, cos_i[:, cols], sin_i[:, cols], -1, head_dim).astype(BF)

        def close_group(g):
            cols = pl.ds(pl.multiple_of(g * CB, CB), CB)
            with jax.named_scope("b_dwqkv"):
                put(spot_of("q", g), dot(hat[:], dqt[cols, :], NT))
                put(spot_of("k", g), dot(hat[:], dkt[cols, :], NT))
                put(spot_of("v", g), dot(hat[:], dv[:, cols]))

        def weights():
            return [pltpu.make_async_copy(s, d, ld.at[10 + i]) for i, (s, d) in enumerate(((wq_h, wq), (wk_h, wk), (wv_h, wv), (x_h, xbuf)))]

        def arrived(p):
            whole = dor.at[pl.ds(aligned(p * pw, pw), pw), :]
            with jax.named_scope("b_hwait"):
                to_left(whole, whole, osnd.at[p], orcv.at[p]).wait()

        def walk(it):
            ahead = it + 1

            @pl.when((lax.rem(ahead, rows) == 0) & (ahead < n_steps))
            def _():
                arrived(ahead // rows)

            @pl.when(it < n_steps)
            def _():
                with jax.named_scope("b_attn"):
                    grads(it - 1)
                    soften(it)
                    score(jnp.minimum(ahead, n_steps - 1))

            @pl.when(it == n_steps)
            def _():
                grads(n_steps - 1)
                for c in weights():
                    c.start()

            p, step = it // rows - 1, lax.rem(it, rows)

            @pl.when((step == 0) & (lax.rem(p, per) == per - 1))
            def _():
                close_group(p // per)

            @pl.when(it == n_steps)
            def _():
                comm.offer(end)

            t = pick(it, tick_after)

            @pl.when(t > 0)
            def _():
                comm.tick(t)

            @pl.when((step == 0) & (p + 3 < n_pairs))
            def _():
                give_out(p + 3)

        for c in lds[:-1]:
            c.wait()
        for i in range(2):
            push_rows(i).wait()
        arrived(0)
        score(0)
        soften(0)
        score(1)
        lds[-1].wait()
        cdiv_loop(n_steps, lambda i: walk(i + 1))
        for c in weights():
            c.wait()

        def into(b):
            r = pl.ds(aligned(b * toks, QB), toks)
            with jax.named_scope("b_into"):
                gnm[r, :] = dot(dqt[:, r], wq[:], TN) + dot(dkt[:, r], wk[:], TN) + dot(dv[r, :], wv[:])

            with jax.named_scope("b_final"):
                for i in range(tb):
                    r = pl.ds(aligned((b * tb + i) * QB, QB), QB)
                    out, dg = norm_back(xbuf[r, :], ga[:], gnm[r, :], gmid[r, :])
                    mbuf[r, :] = out
                    dgain[:8, :] += dg

        def share_gains():
            out_copy.start()
            gains = jnp.concatenate([col_sum(dgain[:8, :]), col_sum(dgain[8:, :]), jnp.zeros((6, width), F32)], axis=0)
            for p in range(n):
                gsend[p, :, :rpd] = gains[:, p * rpd:(p + 1) * rpd]

            def spread(i):
                to = lax.rem(me + i + 1, n)
                pltpu.make_async_remote_copy(src_ref=gsend.at[to], dst_ref=grecv.at[i], send_sem=gsem.at[0], recv_sem=gsem.at[1],
                                             device_id={"seq": to}, device_id_type=MESH).start()

            cdiv_loop(n - 1, spread)

        def finish(i):
            comm.advance(end + i, True)

            @pl.when(i == 1)
            def _():
                cdiv_loop(rows - 2, lambda b: into(b + 1))

            @pl.when(i == LAG + 1)
            def _():
                into(rows - 1)
                share_gains()

        into(0)
        cdiv_loop(4 * LAG - 1, finish)

    score_bufs = [f(3 * QB, 2 * QB) for f in (vf, vm) for _ in range(8)]
    out_copy = pltpu.make_async_copy(mbuf, dx_h, ld.at[0])
    pl.run_scoped(attention, vm(hd, total), vm(hd, rows * ext), vm(rows * ext, hd), vm(rows * ext, hd), vm(hd, rows * WINDOW), vm(total, hd), *score_bufs)
    most, rest = pl.ds(0, end), pl.ds(end, 2)
    keep_most = load(1, fin.at[most], fin_h.at[most])
    to_left(gsend.at[pl.ds(0, n - 1)], grecv, gsem.at[0], gsem.at[1]).wait()
    sums = gsend[me]
    for i in range(n - 1):
        sums = sums + grecv[i]
    fin[end + 1, 0, :8, :128] = sums
    out_copy.wait()
    comm.advance(end + 4 * LAG - 1, True)
    with jax.named_scope("b_end"):
        keep_rest = load(0, fin.at[rest], fin_h.at[rest])
        keep_most.wait()
        keep_rest.wait()


def spread_kernel(dims, dx_i, fin_i, dx_o, dga_o, dgm_o, *refs):
    head_dim, n, width, ff = dims
    outs, (buf, fin), stage, sem = refs[:7], refs[7:9], refs[9:16], refs[16]
    dq, dk, dv, do, dg, du, dd = stage
    nb, nc, sub = ff // CB, width // CB, ff // width
    rpd = width // n
    head, place, end = plan(nb, nc * sub // 2, nc)
    get_fin = pltpu.make_async_copy(fin_i, fin, sem.at[len(outs)])
    get_fin.start()
    cut = buf.shape[0] // nc
    gets, puts = ([pltpu.make_async_copy(s.at[pl.ds(i * cut, cut)], d.at[pl.ds(i * cut, cut)], sem.at[len(outs) + k + i]) for i in range(nc)]
                  for k, s, d in ((1, dx_i, buf), (nc + 1, buf, dx_o)))
    for c in gets:
        c.start()
    get_fin.wait()
    gains = fin[end + 1, 0]
    dga_o[:] = gains[:1, :rpd]
    dgm_o[:] = gains[1:2, :rpd]
    for j in range(nb):
        dg[:, j * CB:(j + 1) * CB] = fin[j, 0]
        du[:, j * CB:(j + 1) * CB] = fin[j, 1]
    for c in range(nc):
        for i in range(sub):
            pair = nb + (c * sub + i) // 2
            dd[i * rpd:(i + 1) * rpd, c * CB:(c + 1) * CB] = fin[pair, i % 2]
    for g in range(nc):
        do[:, g * CB:(g + 1) * CB] = fin[place["o", g]]
        for name, ref in (("q", dq), ("k", dk), ("v", dv)):
            val = fin[place[name, g]]
            for h in range(CB // head_dim):
                ref[g * (CB // head_dim) + h] = val[:, h * head_dim:(h + 1) * head_dim]
    keeps = [pltpu.make_async_copy(s, d, sem.at[i]) for i, (s, d) in enumerate(zip(stage, outs))]
    for c in keeps:
        c.start()
    for get, out in zip(gets, puts):
        get.wait()
        out.start()
    for c in keeps + puts:
        c.wait()


def run_bwd(n, head_dim, ga, gm, x, dout, q, kt, k, v, hat, ot, xm, hm, hmt, qr, lse, cos_t, sin_t, wq, wk, wv, wo, wg, wu, wd, rows):
    total, width = x.shape
    hd, ff = wq.shape[0], wg.shape[1]
    toks = total // rows
    rpd, heads = width // n, hd // head_dim
    nb, nc, sub = ff // CB, width // CB, ff // width
    slots = plan(nb, nc * sub // 2, nc)[2] + 2
    n_pairs = hd // (2 * head_dim)
    f = lambda *s: jax.ShapeDtypeStruct(s, F32)
    dx_t = jax.ShapeDtypeStruct((total, width), BF)
    vm = lambda *s: pltpu.VMEM(s, BF)
    vf = lambda *s: pltpu.VMEM(s, F32)
    dma = lambda *s: pltpu.SemaphoreType.DMA(s)
    line, duo = vf(rows * n_pairs, 8, 2 * QB), (2, SLOTS)
    scratch = [vf(RING, 2, n // 2, 2, rpd, CB), vf(SLOTS, 2, n // 2, rpd, CB), vf(*duo, 2, 2, rpd, CB), vf(*duo, 2, 4, rpd, CB),
               vf(*duo, 2, rpd, CB // 2), vf(*duo, 2, rpd, CB), vf(*duo, 3, rpd, CB), vf(*duo, 4, 4, rpd, CB), vf(*duo, 4, rpd, CB), vf(slots, 2, rpd, CB),
               dma(6, *duo), dma(6, *duo),
               vm(hd, rows * WINDOW), line, line, dma(2), dma(2), dma(n_pairs), dma(n_pairs),
               vf(n, 8, 128), vf(n - 1, 8, 128), dma(2), dma(15),
               vm(total, width), vm(total, width), vf(total, width), vm(total, width), vm(hd, total), vm(width, total), vm(hd, width), vm(hd, total), line, line, vf(*cos_t.shape), vf(*cos_t.shape), vf(*ga.shape), vf(*ga.shape), vf(16, width)]
    mid = pl.pallas_call(
        functools.partial(bwd_kernel, n, head_dim, (rows, toks, width, hd, ff)), out_shape=[dx_t, f(slots, 2, rpd, CB)],
        in_specs=any_spec(24), out_specs=any_spec(2), scratch_shapes=scratch,
        compiler_params=pltpu.CompilerParams(collective_id=1, has_side_effects=True, vmem_limit_bytes=VMEM_LIMIT),
        name="backward")(ga, gm, x, dout, q, kt, k, v, hat, ot, xm, hm, hmt, qr, lse, cos_t, sin_t, wq, wk, wv, wo, wg, wu, wd)
    outs = [f(heads, rpd, head_dim)] * 3 + [f(rpd, width), f(rpd, ff), f(rpd, ff), f(ff // n, width)]
    return pl.pallas_call(
        functools.partial(spread_kernel, (head_dim, n, width, ff)), out_shape=[dx_t, f(1, rpd), f(1, rpd)] + outs,
        in_specs=any_spec(2), out_specs=any_spec(1) + vmem_spec(2) + any_spec(7),
        scratch_shapes=[vm(total, width), vf(slots, 2, rpd, CB), *[vf(*o.shape) for o in outs], dma(8 + 2 * nc)],
        name="spread")(*mid)


def solution(mesh):
    n = mesh.shape["seq"]

    def device_step(hidden, positions, g_attn, g_mlp, w_query, w_key, w_value, w_out, w_gate, w_up, w_down, d_out):
        rows, toks, width = hidden.shape
        layers, _, heads, head_dim = w_query.shape
        hd = heads * head_dim
        half = head_dim // 2
        inv_freq = 1.0 / (10000.0 ** (jnp.arange(half, dtype=F32) * (2.0 / head_dim)))
        turn = lambda w: w[0].transpose(1, 2, 0).reshape(hd, width)
        wq, wk, wv = turn(w_query), turn(w_key), turn(w_value)
        fwd = run_fwd(n, hidden, positions, inv_freq[:, None], g_attn, g_mlp, wq, wk, wv, w_out[0], head_dim)
        out = run_bwd(n, head_dim, g_attn, g_mlp, hidden.reshape(rows * toks, width), d_out.reshape(rows * toks, width), *fwd,
                      wq, wk, wv, w_out[0], w_gate[0], w_up[0], w_down[0], rows)
        dx, dga, dgm, dq, dk, dv, do, dg, du, dd = out
        back = lambda w: w.transpose(1, 0, 2)[None]
        return (dx.reshape(rows, toks, width), dga, dgm, back(dq), back(dk), back(dv), do[None], dg[None], du[None], dd[None])

    tok_spec, grad_spec = P("data", "seq"), P(None, ("data", "seq"))
    in_specs = (tok_spec, tok_spec) + (P(),) * 9 + (tok_spec,)
    out_specs = (tok_spec,) + (grad_spec,) * 9
    return jax.shard_map(device_step, mesh=mesh, in_specs=in_specs, out_specs=out_specs, check_vma=False)
```

```python
import functools, math
import numpy as np
import jax, jax.numpy as jnp
from jax import lax
from jax.experimental import pallas as pl
from jax.experimental.pallas import tpu as pltpu
from jax.sharding import PartitionSpec as P

WINDOW = 256
NORM_EPS = 1e-5
QB = 128
BF, F32 = jnp.bfloat16, jnp.float32
NN, NT, TN = ((1,), (0,)), ((1,), (1,)), ((0,), (0,))
MESH = pl.DeviceIdType.MESH
NEG = -1e30
VMEM_LIMIT = 67043328


def dot(a, b, dims=NN):
    return lax.dot_general(a, b, (dims, ((), ())), preferred_element_type=F32)


def cdiv_loop(n, body):
    lax.fori_loop(0, n, lambda i, c: body(i) or c, 0)


def mod(a, b):
    return a % b if isinstance(a, int) else lax.rem(a, b)


def aligned(a, b):
    return a if isinstance(a, int) else pl.multiple_of(a, b)


def rope(blk, cos_b, sin_b, sign, head_dim):
    half = head_dim // 2
    parts = []
    for h in range(blk.shape[0] // head_dim):
        first = blk[h * head_dim:h * head_dim + half]
        second = blk[h * head_dim + half:(h + 1) * head_dim]
        if sign > 0:
            parts += [first * cos_b - second * sin_b, second * cos_b + first * sin_b]
        else:
            parts += [first * cos_b + second * sin_b, second * cos_b - first * sin_b]
    return jnp.concatenate(parts, axis=0)


def normed(x, gain):
    xf = x.astype(F32)
    inv = lax.rsqrt(jnp.mean(xf * xf, axis=-1, keepdims=True) + NORM_EPS)
    return (xf * inv * gain).astype(BF)


def stack_pair(pair_t):
    half = pair_t.shape[0] // 2
    zero = jnp.zeros((half, pair_t.shape[1]), pair_t.dtype)
    return jnp.concatenate(
        [jnp.concatenate([pair_t[:half], zero], axis=0), jnp.concatenate([zero, pair_t[half:]], axis=0)], axis=1)


def unstack_pair(both):
    half, cols = both.shape[0] // 2, both.shape[1] // 2
    return jnp.concatenate([both[:half, :cols], both[half:, cols:]], axis=0)


def col_sum(x):
    return jnp.sum(x, axis=0, keepdims=True)


def merged(scores, upper, bias0, bias1):
    return jnp.where(upper, scores[:QB] + bias0, scores[2 * QB:]), scores[QB:2 * QB] + bias1


def banded(p02, p1, upper):
    return jnp.concatenate(
        [jnp.where(upper, p02, 0.0).astype(BF), p1.astype(BF), jnp.where(upper, 0.0, p02).astype(BF)], axis=0)


def upper_mask():
    key_ids = lax.broadcasted_iota(jnp.int32, (QB, 2 * QB), 0)
    query_ids = lax.broadcasted_iota(jnp.int32, (QB, 2 * QB), 1) % QB
    return key_ids > query_ids


def start_bias(first, blk):
    bias = jnp.where(first, NEG, 0.0).astype(F32)
    return (bias if blk < 2 else 0.0), (bias if blk < 1 else 0.0)


def fwd_kernel(n, head_dim, x_h, pos_h, invf_h, ga_h, gm_h, wq_h, wk_h, wv_h, wo_h,
               q_h, kt_h, k_h, v_h, ha_h, ot_h, xm_h, hm_h, hmt_h, qr_h, lse_h, cos_t, sin_t,
               pos, invf, ga, gm, xv, halo, qr, lse, pos_halo, wq, wk, wv, wo, q, kt, k, v, vt, ot, xm, hm, hmt, hb, hh, acc, acc2, ak, av, cos_h, sin_h,
               sc0, sc1, sc2, pb0, pb1, pb2, ldx, ld, st, snd, rcv, qsnd, qrcv):
    sc, pb = (sc0, sc1, sc2), (pb0, pb1, pb2)
    rows, toks, width = xv.shape
    ext, total, pw = toks + WINDOW, rows * toks, 2 * head_dim
    n_pairs = wq.shape[0] // pw
    tb, n_steps = toks // QB, n_pairs * rows
    me = lax.axis_index("seq")
    right, left = lax.rem(me + 1, n), lax.rem(me + n - 1, n)
    load_x = [pltpu.make_async_copy(x_h.at[b], xv.at[b], ldx.at[b]) for b in range(rows)]
    load_w = [pltpu.make_async_copy(s, d, ld.at[i]) for i, (s, d) in enumerate(((wq_h, wq), (wk_h, wk), (wv_h, wv), (wo_h, wo)))]
    load_s = [pltpu.make_async_copy(s, d, ldx.at[rows + i]) for i, (s, d) in enumerate(((pos_h, pos), (invf_h, invf), (ga_h, ga), (gm_h, gm)))]
    for c in load_s + load_x:
        c.start()
    barrier = pltpu.get_barrier_semaphore()
    for other in (left, right):
        pl.semaphore_signal(barrier, inc=1, device_id={"seq": other}, device_id_type=MESH)

    def push(i, s, d):
        return pltpu.make_async_remote_copy(src_ref=s, dst_ref=d, send_sem=snd.at[i], recv_sem=rcv.at[i], device_id={"seq": right}, device_id_type=MESH)

    def push_rows(b):
        return push(b, x_h.at[b, toks - WINDOW:, :], halo.at[b])

    send_pos = push(rows, pos, pos_halo)

    def angles(cos_ref, sin_ref, positions):
        count = positions.shape[1]
        for b in range(rows):
            ang = invf[:] * positions[b:b + 1, :].astype(F32)
            cos_ref[:, b * count:(b + 1) * count] = jnp.cos(ang)
            sin_ref[:, b * count:(b + 1) * count] = jnp.sin(ang)

    for c in load_s:
        c.wait()
    angles(cos_t, sin_t, pos[:])

    def norm_rows(b):
        for i in range(tb):
            h = normed(xv[b, i * QB:(i + 1) * QB, :], ga[:])
            hb[pl.ds(pl.multiple_of((b * tb + i) * QB, QB), QB), :] = h

    with jax.named_scope("f_norm"):
        for c in load_x:
            c.wait()
        for c in load_w:
            c.start()
        cdiv_loop(rows, norm_rows)
    pl.semaphore_wait(barrier, 2)
    send_pos.start()
    for b in range(rows):
        push_rows(b).start()
    keep_ha = pltpu.make_async_copy(hb, ha_h, st.at[0])
    keep_ha.start()
    tables = cos_t[:], sin_t[:]

    def put_q(src):
        for p in range(n_pairs):
            r = slice(p * pw, (p + 1) * pw)
            q[r, :] = (rope(src[r, :], *tables, 1, head_dim) * (head_dim ** -0.5)).astype(BF)

    def put_own(src, dst_t, dst):
        for p in range(n_pairs):
            r = slice(p * pw, (p + 1) * pw)
            both = (rope(src[r, :], *tables, 1, head_dim) if dst is k else src[r, :]).astype(BF)
            for b in range(rows):
                blk = both[:, b * toks:(b + 1) * toks]
                own = slice(b * ext + WINDOW, (b + 1) * ext)
                dst_t[r, own] = blk
                dst[own, r] = blk.T

    with jax.named_scope("f_mm"):
        load_w[0].wait()
        load_w[1].wait()
        load_w[2].wait()
        acc[:] = dot(wq[:], hb[:], NT)
        acc2[:] = dot(wk[:], hb[:], NT)
        put_q(acc)
        acc[:] = dot(wv[:], hb[:], NT)
        put_own(acc2, kt, k)
        put_own(acc, vt, v)
    keep_q = pltpu.make_async_copy(q, q_h, st.at[1])
    keep_q.start()

    def push_q(b):
        return pltpu.make_async_remote_copy(src_ref=q.at[:, b * toks:b * toks + WINDOW], dst_ref=qr.at[:, b * WINDOW:(b + 1) * WINDOW],
                                            send_sem=qsnd.at[b], recv_sem=qrcv.at[b], device_id={"seq": left}, device_id_type=MESH)

    for b in range(rows):
        push_q(b).start()
    send_pos.wait()
    angles(cos_h, sin_h, pos_halo[:, toks - WINDOW:])

    def keeps(b):
        wide, cols = pl.ds(pl.multiple_of(b * ext, QB), ext), pl.ds(pl.multiple_of(b * toks, QB), toks)
        ends = ((kt.at[:, wide], kt_h.at[:, wide]), (k.at[wide, :], k_h.at[wide, :]), (v.at[wide, :], v_h.at[wide, :]),
                (ot.at[:, cols], ot_h.at[:, cols]), (hm.at[cols, :], hm_h.at[cols, :]), (hmt.at[:, cols], hmt_h.at[:, cols]),
                (xm.at[cols, :], xm_h.at[cols, :]))
        return [pltpu.make_async_copy(s, d, st.at[2 + b * len(ends) + i]) for i, (s, d) in enumerate(ends)]

    def halo_in(b):
        with jax.named_scope("f_halo_wait"):
            push_rows(b).wait()
        with jax.named_scope("f_halo"):
            for i in range(WINDOW // QB):
                r = slice(i * QB, (i + 1) * QB)
                hh[r, :] = normed(halo[b, r, :], ga[:])
            ak[:] = dot(wk[:], hh[:], NT)
            av[:] = dot(wv[:], hh[:], NT)
            cols = pl.ds(pl.multiple_of(b * WINDOW, QB), WINDOW)
            wide = pl.ds(pl.multiple_of(b * ext, QB), WINDOW)
            near = cos_h[:, cols], sin_h[:, cols]
            for src, dst_t, dst in ((ak, kt, k), (av, vt, v)):
                for p in range(n_pairs):
                    r = slice(p * pw, (p + 1) * pw)
                    blk = (rope(src[r, :], *near, 1, head_dim) if dst is k else src[r, :]).astype(BF)
                    dst_t[r, wide] = blk
                    dst[wide, r] = blk.T
        for c in keeps(b)[:3]:
            c.start()

    upper = upper_mask()
    first = me == 0

    def spots(it, blk):
        b, p = it // n_pairs, mod(it, n_pairs)
        pr = pl.ds(aligned(p * pw, pw), pw)
        return pr, pl.ds(aligned(b * toks + blk * QB, QB), QB), pl.ds(aligned(b * ext + blk * QB, QB), 3 * QB)

    def score(it):
        for blk in range(tb):
            pr, cols, keys = spots(it, blk)
            sc[blk][:] = dot(k[keys, pr], stack_pair(q[pr, cols]))

    def soften(it, blk):
        s02, s1 = merged(sc[blk][:], upper, *start_bias(first, blk))
        top = jnp.max(jnp.maximum(s02, s1), axis=0, keepdims=True)
        e02, e1 = jnp.exp(s02 - top), jnp.exp(s1 - top)
        mass = col_sum(e02 + e1)
        inv = 1.0 / mass
        lse[it, blk:blk + 1, :] = top + jnp.log(mass)
        pb[blk][:] = banded(e02 * inv, e1 * inv, upper)

    def mix(it):
        for blk in range(tb):
            pr, cols, keys = spots(it, blk)
            ot[pr, cols] = unstack_pair(dot(vt[pr, keys], pb[blk][:])).astype(BF)

    def project(b):
        cols = pl.ds(pl.multiple_of(b * toks, QB), toks)
        with jax.named_scope("f_proj"):
            mid = (xv[b].astype(F32) + dot(ot[:, cols], wo[:], TN)).astype(BF)
            xm[cols, :] = mid
            h = normed(mid, gm[:])
            hm[cols, :] = h
            hmt[:, cols] = h.T
        for c in keeps(b)[3:]:
            c.start()

    keep_qr, keep_lse = (pltpu.make_async_copy(*ends, ld.at[i]) for i, ends in enumerate(((qr, qr_h), (lse, lse_h))))
    load_w[3].wait()
    for blk in range(tb):
        pb[blk][:] = jnp.zeros(pb[blk].shape, BF)

    def walk(i):
        it = i - 1

        @pl.when((lax.rem(i, n_pairs) == 0) & (i < n_steps))
        def _():
            halo_in(i // n_pairs)

        @pl.when(i == 0)
        def _():
            score(0)

        @pl.when((i > 0) & (i <= n_steps))
        def _():
            with jax.named_scope("f_attn"):
                mix(jnp.maximum(it - 1, 0))
                for blk in range(tb):
                    soften(it, blk)
                score(jnp.minimum(i, n_steps - 1))

        @pl.when(i == n_steps)
        def _():
            for b in range(rows):
                push_q(b).wait()
            keep_qr.start()

        @pl.when(i > n_steps)
        def _():
            mix(n_steps - 1)

        @pl.when((lax.rem(it, n_pairs) == 0) & (it > 0))
        def _():
            project(it // n_pairs - 1)

    cdiv_loop(n_steps + 2, walk)
    with jax.named_scope("f_store_wait"):
        keep_lse.start()
        keep_ha.wait()
        keep_q.wait()
        keep_qr.wait()
        keep_lse.wait()
        for b in range(rows):
            for c in keeps(b):
                c.wait()


def any_spec(k):
    return [pl.BlockSpec(memory_space=pl.ANY)] * k


def vmem_spec(k):
    return [pl.BlockSpec(memory_space=pltpu.VMEM)] * k


def run_fwd(n, x, pos, invf, ga, gm, wq, wk, wv, wo, head_dim):
    rows, toks, width = x.shape
    hd = wq.shape[0]
    ext, total, n_halo = toks + WINDOW, rows * toks, rows * WINDOW
    half = head_dim // 2
    sds = lambda *s: jax.ShapeDtypeStruct(s, BF)
    dma = lambda *s: pltpu.SemaphoreType.DMA(s)
    outs = [sds(hd, total), sds(hd, rows * ext), sds(rows * ext, hd), sds(rows * ext, hd), sds(total, width), sds(hd, total), sds(total, width), sds(total, width), sds(width, total)]
    outs += [sds(hd, n_halo), jax.ShapeDtypeStruct((rows * hd // (2 * head_dim), 8, 2 * QB), F32)] + [jax.ShapeDtypeStruct((half, total), F32)] * 2
    vm = lambda *s: pltpu.VMEM(s, BF)
    vf = lambda *s: pltpu.VMEM(s, F32)
    scratch = [pltpu.VMEM((rows, toks), jnp.int32), vf(*invf.shape), vf(*ga.shape), vf(*ga.shape), vm(rows, toks, width), vm(rows, WINDOW, width), vm(hd, n_halo), vf(rows * hd // (2 * head_dim), 8, 2 * QB), pltpu.VMEM((rows, toks), jnp.int32), vm(hd, width), vm(hd, width), vm(hd, width), vm(hd, width),
               vm(hd, total), vm(hd, rows * ext), vm(rows * ext, hd), vm(rows * ext, hd), vm(hd, rows * ext), vm(hd, total), vm(total, width), vm(total, width), vm(width, total), vm(total, width), vm(WINDOW, width),
               vf(hd, total), vf(hd, total), vf(hd, WINDOW), vf(hd, WINDOW), vf(half, n_halo), vf(half, n_halo),
               *[f(3 * QB, 2 * QB) for f in (vf, vm) for _ in range(3)],
               dma(rows + 4), dma(4), dma(2 + 7 * rows), dma(rows + 1), dma(rows + 1), dma(rows), dma(rows)]
    return pl.pallas_call(
        functools.partial(fwd_kernel, n, head_dim), out_shape=outs,
        in_specs=any_spec(9), out_specs=any_spec(11) + vmem_spec(2), scratch_shapes=scratch,
        compiler_params=pltpu.CompilerParams(collective_id=0, has_side_effects=True, vmem_limit_bytes=VMEM_LIMIT),
        name="forward")(x, pos, invf, ga, gm, wq, wk, wv, wo)


LAG = 2
SLOTS = 2 * LAG
RING = 8
CB = 256


def at(ref, *idx):
    return ref.at[idx]


class Torus:
    def __init__(self, n, head, last, turn, parts, recv0, recv1, recv2, recv3, recv4, recv5, acc, acc2, fin, snd, rcv):
        assert math.isqrt(n // 2) == 4
        me = lax.axis_index("seq")
        self.core = lax.rem(me, 2)
        chip = me // 2
        self.x, self.y = lax.rem(chip, 4), chip // 4
        self.head, self.last, self.turn = head, last, turn
        self.parts, self.recv0, self.recv1, self.recv2, self.recv3, self.recv4, self.recv5 = parts, recv0, recv1, recv2, recv3, recv4, recv5
        self.acc, self.acc2, self.fin, self.snd, self.rcv = acc, acc2, fin, snd, rcv
        self.partner = me + 1 - 2 * self.core
        self.rows, self.columns = [lax.rem(self.y + d, 4) * 4 for d in range(4)], [lax.rem(self.x + d, 4) for d in range(4)]
        self.hops = [[self.device(0, d) for d in range(4)], [self.device(d, 0) for d in range(4)]]

    def device(self, dy, dx):
        return (self.rows[dy] + self.columns[dx]) * 2 + self.core

    def copy(self, lane, kind, slot, src, dst, target):
        return pltpu.make_async_remote_copy(
            src_ref=src, dst_ref=dst, send_sem=self.snd.at[lane, kind, slot], recv_sem=self.rcv.at[lane, kind, slot],
            device_id={"seq": target}, device_id_type=MESH)

    def late(self, axis, pair, yes, no):
        first, end = self.turn
        busy = (pair >= first) & (pair < end)
        return jnp.where(busy & (self.x == 3) if axis else busy, yes, no)

    def swap(self, ring, slot):
        return self.copy(0, 0, slot, self.parts.at[ring, :, :, 1 - self.core], self.recv0.at[slot], self.partner)

    def landing(self, stage):
        return (self.recv0, self.recv1, self.recv2, self.recv3, self.recv4, self.recv5)[stage]

    def arrived(self, stage, kind, slot):
        whole = self.landing(stage).at[kind, slot]
        self.copy(stage, kind, slot, whole, whole, self.partner).wait()

    def send(self, stage, kind, pair, held, slot):
        axis = kind if stage < 3 else 1 - kind
        plus, minus = self.hops[axis][1], self.hops[axis][-1]
        half = CB // 2
        if stage == 1:
            minus = self.late(axis, pair, plus, minus)
            ends = self.acc.at[kind, held, 2, :2], self.acc.at[kind, held, 2, 2:]
        elif stage == 2:
            ends = self.acc.at[kind, held, 1], self.acc.at[kind, held, 3]
        elif stage == 3:
            ends = self.acc2.at[kind, held, 2, :, :half], self.acc2.at[kind, held, 2, :, half:]
        else:
            ends = self.acc2.at[kind, held, 1], self.acc2.at[kind, held, 3]
        for i, src in enumerate(ends):
            self.copy(stage, kind, slot, src, self.landing(stage).at[kind, slot, i], (plus, minus)[i]).start()

    def add(self, stage, kind, pair, held, slot, ring):
        acc, acc2 = self.acc, self.acc2
        if stage == 1:
            for r1 in range(4):
                for r2 in range(4):
                    ry, rx = (r2, r1) if kind == 0 else (r1, r2)
                    chip = self.rows[ry] + self.columns[rx]
                    acc[kind, held, r1, r2] = self.parts[ring, kind, chip, self.core] + self.recv0[slot, kind, chip]
        elif stage == 2:
            back = self.late(kind, pair, 1, 3)
            acc[kind, held, 1, :2] += self.recv1[kind, slot, 0]
            acc[kind, held, back, 2:] += self.recv1[kind, slot, 1]
        elif stage == 3:
            acc2[kind, held] = acc[kind, held, 0] + (self.recv2[kind, slot, 0] + self.recv2[kind, slot, 1])
        elif stage == 4:
            half = CB // 2
            acc2[kind, held, 1, :, :half] += self.recv3[kind, slot, 0]
            acc2[kind, held, 3, :, half:] += self.recv3[kind, slot, 1]
        else:
            self.fin[pair, kind] = acc2[kind, held, 0] + (self.recv4[kind, slot, 0] + self.recv4[kind, slot, 1])

    def direct(self, kind, held, slot):
        for d in range(1, 4):
            self.copy(5, kind, slot, self.acc2.at[kind, held, d], self.recv5.at[kind, slot, d - 1], self.hops[1 - kind][d]).start()

    def early(self, pair):
        return (pair >= 0) & (pair <= self.head)

    def final(self, pair):
        return (pair == self.last) | ((pair > self.head) & (pair < self.last) & (mod(abs(pair - self.head), 2) == 0))

    def when(self, which, fn):
        if isinstance(which, bool):
            fn() if which else None
        else:
            pl.when(which)(fn)

    def offer(self, t):
        self.when(self.early(t) | self.final(t), lambda: self.swap(mod(t, RING), mod(t, SLOTS)).start())

    def tick(self, t):
        self.offer(t)
        self.advance(t)

    def advance(self, t, tail=False):
        now, land, before = mod(t, SLOTS), mod(t + SLOTS - LAG, SLOTS), mod(t + SLOTS - 1, SLOTS)
        ring_land = mod(t + RING - 1, RING)
        for stage in range(5, 0, -1):
            pair = t - LAG * stage + 1
            held = before if stage % 2 else mod(t + 1, SLOTS)

            def move(last_hops, stage=stage, pair=pair, held=held):
                if stage == 1:
                    with jax.named_scope("t_wait1"):
                        self.swap(ring_land, before).wait()
                for kind in range(2):
                    if last_hops and stage == 4:
                        with jax.named_scope("t_wait6"):
                            self.arrived(5, kind, land)
                        got = self.recv5[kind, land]
                        self.fin[pair, kind] = self.acc2[kind, held, 0] + (got[0] + got[1] + got[2])
                        continue
                    if stage > 1:
                        with jax.named_scope(f"t_wait{stage}"):
                            self.arrived(stage - 1, kind, land)
                    self.add(stage, kind, pair, held, land if stage > 1 else before, ring_land)
                    if last_hops and stage == 3:
                        self.direct(kind, held, now)
                    elif stage < 5:
                        self.send(stage, kind, pair, held, now)

            if stage < 3:
                self.when(self.early(pair) | self.final(pair), functools.partial(move, False))
            else:
                self.when(self.early(pair), functools.partial(move, False))
                if tail and stage < 5:
                    self.when(self.final(pair), functools.partial(move, True))


def pick(i, table):
    out = 0
    for key, value in table.items():
        out = jnp.where(i == key, value, out)
    return out


def norm_back(x, gain, grad, res):
    xf = x.astype(F32)
    inv = lax.rsqrt(jnp.mean(xf * xf, axis=-1, keepdims=True) + NORM_EPS)
    unit = xf * inv
    gu = grad * gain
    out = inv * (gu - unit * jnp.mean(gu * unit, axis=-1, keepdims=True)) + res.astype(F32)
    gu = grad * unit
    return out.astype(BF), jnp.sum(gu.reshape(-1, 8, gu.shape[-1]), axis=0)


def plan(n_mlp, n_down, nc):
    order = [("o", g) for g in range(nc)] + [(name, g) for g in range(nc) for name in "qkv"]
    base, head = n_mlp + n_down, n_mlp + n_down + nc - 1
    last = 2 * (base - 1 - head + len(order) // 2) + head - 1
    spot = lambda pair: min(max(pair, 2 * pair - head), last)
    return head, {name: (spot(base + i // 2), i % 2) for i, name in enumerate(order)}, last


def bwd_kernel(n, head_dim, dims, ga_h, gm_h, x_h, dout_h, q_h, kt_h, k_h, v_h, ha_h, ot_h, xm_h, hm_h, hmt_h, qr_h, lse_h, cos_h, sin_h,
               wq_h, wk_h, wv_h, wo_h, wg_h, wu_h, wd_h,
               dx_h, fin_h,
               parts, recv0, recv1, recv2, recv3, recv4, recv5, acc, acc2, fin, snd, rcv,
               dor, lser, deltar, hsnd, hrcv, osnd, orcv, gsend, grecv, gsem, ld,
               xbuf, mbuf, gnm, gmid, ot, hat, wo, dot_, lse, delta, cos_i, sin_i, ga, gm, dgain):
    rows, toks, width, hd, ff = dims
    ext, total = toks + WINDOW, rows * toks
    pw = 2 * head_dim
    n_pairs = hd // pw
    tb, n_steps = toks // QB, n_pairs * rows
    nb, nc, sub = ff // CB, width // CB, ff // width
    rpd = width // n
    per, half_sub = CB // pw, sub // 2
    head, place, end = plan(nb, nc * half_sub, nc)
    comm = Torus(n, head, end, (nb, nb + n_pairs + 1), parts, recv0, recv1, recv2, recv3, recv4, recv5, acc, acc2, fin, snd, rcv)
    me = lax.axis_index("seq")
    left = lax.rem(me + n - 1, n)
    barrier = pltpu.get_barrier_semaphore()

    def greet(i):
        pl.semaphore_signal(barrier, inc=1, device_id={"seq": lax.rem(me + i + 1, n)}, device_id_type=MESH)

    def load(i, s, d):
        c = pltpu.make_async_copy(s, d, ld.at[i])
        c.start()
        return c

    def late(i):
        s, d = ((xm_h, mbuf), (ot_h, ot), (wo_h, wo), (lse_h, lse), (cos_h, cos_i), (sin_h, sin_i), (ga_h, ga), (gm_h, gm))[i]
        return pltpu.make_async_copy(s, d, ld.at[1 + i])

    def to_left(src, dst, send_sem, recv_sem):
        return pltpu.make_async_remote_copy(src_ref=src, dst_ref=dst, send_sem=send_sem, recv_sem=recv_sem,
                                            device_id={"seq": left}, device_id_type=MESH)

    n_late = 8

    def push_rows(i):
        return to_left(*((lse_h, lser), (delta, deltar))[i], hsnd.at[i], hrcv.at[i])

    def push_out(p):
        pr = pl.ds(aligned(p * pw, pw), pw)
        return [to_left(dot_.at[pr, pl.ds(b * toks, WINDOW)], dor.at[pr, pl.ds(b * WINDOW, WINDOW)], osnd.at[p], orcv.at[p])
                for b in range(rows)]

    def give_out(p):
        for c in push_out(p):
            c.start()

    def put(spot, value):
        pair, kind = spot
        parts[mod(pair, RING), kind] = value.reshape(n // 2, 2, rpd, CB)

    def spot_of(name, g):
        known = {i: place[name, i] for i in range(nc)}
        return pick(g, {i: s[0] for i, s in known.items()}), pick(g, {i: s[1] for i, s in known.items()})

    def spots(it, blk):
        p, b = it // rows, mod(it, rows)
        pr = pl.ds(aligned(p * pw, pw), pw)
        return pr, pl.ds(aligned(b * toks + blk * QB, QB), QB), pl.ds(aligned(b * ext + blk * QB, QB), 3 * QB)

    def row_of(it):
        return mod(it, rows) * n_pairs + it // rows

    def mlp(hm, hmt, ha, actt, wgu, wd, dgu, wld):
        def weights(j, slot):
            c = aligned(j * CB, CB)
            return [pltpu.make_async_copy(wg_h.at[:, pl.ds(c, CB)], wgu.at[slot, :, :CB], wld.at[slot, 0]),
                    pltpu.make_async_copy(wu_h.at[:, pl.ds(c, CB)], wgu.at[slot, :, CB:], wld.at[slot, 1]),
                    pltpu.make_async_copy(wd_h.at[pl.ds(c, CB), :], wd.at[slot], wld.at[slot, 2])]

        for c in weights(0, 0):
            c.start()
        ld_hm, ld_x, ld_hmt = load(10, hm_h, hm), load(0, dout_h, xbuf), load(11, hmt_h, hmt)
        cdiv_loop(n - 1, greet)
        gnm[:] = jnp.zeros_like(gnm)
        gsend[:] = jnp.zeros_like(gsend)
        dgain[:] = jnp.zeros_like(dgain)
        ld_hm.wait()
        ld_x.wait()
        ld_hmt.wait()
        for i in range(n_late):
            late(i).start()
        ld_ha = load(10, ha_h, ha)

        def block(j):
            slot = lax.rem(j, 2)
            for c in weights(j, slot):
                c.wait()

            @pl.when(j + 1 < nb)
            def _():
                for c in weights(j + 1, 1 - slot):
                    c.start()

            c0 = pl.multiple_of(j * CB, CB)
            with jax.named_scope("b_mlp"):
                for b in range(rows):
                    r = slice(b * toks, (b + 1) * toks)
                    gu = dot(hm[r, :], wgu[slot])
                    gact = dot(xbuf[r, :], wd[slot], NT).astype(BF).astype(F32)
                    gate, up = gu[:, :CB], gu[:, CB:]
                    sig = 1.0 / (1.0 + jnp.exp(-gate))
                    swish = gate * sig
                    actt[pl.ds(c0, CB), r] = (swish * up).astype(BF).T
                    dgu[r, :CB] = (gact * up * (sig + swish * (1.0 - sig))).astype(BF)
                    dgu[r, CB:] = (gact * swish).astype(BF)
                both = dot(hmt[:], dgu[:])
                ring = lax.rem(j, RING)
                parts[ring, 0] = both[:, :CB].reshape(n // 2, 2, rpd, CB)
                parts[ring, 1] = both[:, CB:].reshape(n // 2, 2, rpd, CB)
                for b in range(rows):
                    r = slice(b * toks, (b + 1) * toks)
                    gnm[r, :] += dot(dgu[r, :], wgu[slot], NT)

            @pl.when(j == 0)
            def _():
                pl.semaphore_wait(barrier, n - 1)
                push_rows(0).start()

            comm.tick(j)

        cdiv_loop(nb, block)

        def down(c):
            share = n // 2 // sub
            c0 = pl.multiple_of(c * CB, CB)
            for m in range(sub):
                res = dot(actt[m * width:(m + 1) * width, :], xbuf[:, pl.ds(c0, CB)]).reshape(share, 2, sub, rpd, CB)
                for i in range(sub):
                    pair = nb + c * half_sub + i // 2
                    parts[lax.rem(pair, RING), i % 2, m * share:(m + 1) * share] = res[:, :, i]
            for i in range(tb * rows // nc):
                r = pl.ds(pl.multiple_of((c * (tb * rows // nc) + i) * QB, QB), QB)
                hat[:, r] = ha[r, :].T

        for i in range(n_late):
            late(i).wait()
        ld_ha.wait()

        def mid(b):
            for i in range(tb):
                r = pl.ds(pl.multiple_of((b * tb + i) * QB, QB), QB)
                out, dg = norm_back(mbuf[r, :], gm[:], gnm[r, :], xbuf[r, :])
                gmid[r, :] = out
                dgain[8:, :] += dg

        def deltas(p):
            for it in range(rows):
                for blk in range(tb):
                    pr, cols, _ = spots(p * rows + it, blk)
                    both = dot_[pr, cols].astype(F32) * ot[pr, cols].astype(F32)
                    delta[row_of(p * rows + it), blk:blk + 1, :] = jnp.concatenate(
                        [col_sum(both[:head_dim]), col_sum(both[head_dim:])], axis=1)

        def column(c):
            with jax.named_scope("b_down"):
                down(c)

            @pl.when(c < nc - 1)
            def _():
                comm.tick(nb + c + jnp.minimum(c, 1))

            @pl.when(c > 0)
            def _():
                give_out(c)

            @pl.when(c == 0)
            def _():
                with jax.named_scope("b_mid"):
                    cdiv_loop(rows, mid)
                with jax.named_scope("b_dot"):
                    dot_[:] = dot(wo[:], gmid[:], NT).astype(BF)
                    cdiv_loop(n_pairs, deltas)
                comm.tick(nb + 1)
                push_rows(1).start()
                give_out(0)

        cdiv_loop(nc, column)

    vm = lambda *s: pltpu.VMEM(s, BF)
    vf = lambda *s: pltpu.VMEM(s, F32)
    pl.run_scoped(mlp, vm(total, width), vm(width, total), vm(total, width), vm(ff, total), vm(2, width, 2 * CB), vm(2, CB, width), vm(total, 2 * CB),
                  pltpu.SemaphoreType.DMA((2, 3)))
    def attention(q, kt, k, v, qr, dv, sc0, sc1, sc2, sr, dp0, dp1, dp2, dr, pb0, pb1, pb2, pr_, ds0, ds1, ds2, dsr):
        dqt, dkt = ot, q
        wq, wk, wv = k.at[:hd], kt.at[:, :width], v.at[:hd]
        sc, dp, pb, ds = (sc0, sc1, sc2), (dp0, dp1, dp2), (pb0, pb1, pb2), (ds0, ds1, ds2)
        lds = [load(10 + i, s, d) for i, (s, d) in enumerate(((q_h, q), (k_h, k), (v_h, v), (qr_h, qr), (kt_h, kt)))]

        def out_grad(g):
            put(spot_of("o", g), dot(ot[:], gmid[:, pl.ds(pl.multiple_of(g * CB, CB), CB)]))

        with jax.named_scope("b_dwo"):
            cdiv_loop(nc, out_grad)
        first_tick = nb + nc + 1
        comm.tick(first_tick - 1)
        ends = [rows * p for p in range(1, n_pairs + 1)]
        steps = sorted([1, ends[1] - 1, ends[-2] - 1, ends[-1] - 1, *ends[1:]])
        tick_after = {s: first_tick + i for i, s in enumerate(steps)}
        assert first_tick + len(steps) == end
        upper = upper_mask()
        first, last = me == 0, me == n - 1
        halves = slice(0, WINDOW), slice(WINDOW, 3 * QB)

        def right(it, i):
            p, b = it // rows, mod(it, rows)
            return pl.ds(aligned(p * pw, pw), pw), pl.ds(aligned(b * WINDOW + i * QB, QB), QB), pl.ds(aligned(b * ext + toks + i * QB, QB), WINDOW - i * QB)

        def score(it):
            for blk in range(tb):
                pr, cols, keys = spots(it, blk)
                sc[blk][:] = dot(k[keys, pr], stack_pair(q[pr, cols]))
                dp[blk][:] = dot(v[keys, pr], stack_pair(dot_[pr, cols]))
            for i, rs in enumerate(halves):
                pr, cols, keys = right(it, i)
                sr[rs, :] = dot(k[keys, pr], stack_pair(qr[pr, cols]))
                dr[rs, :] = dot(v[keys, pr], stack_pair(dor[pr, cols]))

        def soften(it):
            row = row_of(it)
            for blk in range(tb):
                s02, s1 = merged(sc[blk][:], upper, *start_bias(first, blk))
                norm, mean = lse[row, blk:blk + 1, :], delta[row, blk:blk + 1, :]
                p02, p1 = jnp.exp(s02 - norm), jnp.exp(s1 - norm)
                g02, g1 = jnp.where(upper, dp[blk][:QB], dp[blk][2 * QB:]), dp[blk][QB:2 * QB]
                pb[blk][:] = banded(p02, p1, upper)
                ds[blk][:] = banded(p02 * (g02 - mean), p1 * (g1 - mean), upper)
            for blk in range(tb):
                i = blk // 2
                rs = slice(blk * QB, (blk + 1) * QB)
                p = jnp.exp(sr[rs, :] - jnp.where(last, -NEG, lser[row, i:i + 1, :]))
                g = p * (dr[rs, :] - deltar[row, i:i + 1, :])
                pr_[rs, :] = (p if blk == 1 else jnp.where(upper, p, 0.0)).astype(BF)
                dsr[rs, :] = (g if blk == 1 else jnp.where(upper, g, 0.0)).astype(BF)

        def grads(it):
            ks, vs = [], []
            for blk in range(tb):
                pr, cols, keys = spots(it, blk)
                own = slice(max(0, 2 - blk) * QB, 3 * QB)
                vs.append(dot(pb[blk][own, :], stack_pair(dot_[pr, cols]), NT))
                ks.append(dot(ds[blk][own, :], stack_pair(q[pr, cols]), NT))
                dq = unstack_pair(dot(kt[pr, keys], ds[blk][:])) * (head_dim ** -0.5)
                dqt[pr, cols] = rope(dq, cos_i[:, cols], sin_i[:, cols], -1, head_dim).astype(BF)
            for i, rs in enumerate(halves):
                pr, cols, _ = right(it, i)
                vs.append(dot(pr_[rs, :], stack_pair(dor[pr, cols]), NT))
                ks.append(dot(dsr[rs, :], stack_pair(qr[pr, cols]), NT))
            for j in range(tb):
                pr, cols, _ = spots(it, j)
                gv, gk = (sum(x[i][(j - max(0, i - 2)) * QB:(j - max(0, i - 2) + 1) * QB] for i in range(j, j + 3)) for x in (vs, ks))
                dv[cols, pr] = gv.astype(BF)
                dkt[pr, cols] = rope(gk.T, cos_i[:, cols], sin_i[:, cols], -1, head_dim).astype(BF)

        def close_group(g):
            cols = pl.ds(pl.multiple_of(g * CB, CB), CB)
            with jax.named_scope("b_dwqkv"):
                put(spot_of("q", g), dot(hat[:], dqt[cols, :], NT))
                put(spot_of("k", g), dot(hat[:], dkt[cols, :], NT))
                put(spot_of("v", g), dot(hat[:], dv[:, cols]))

        def weights():
            return [pltpu.make_async_copy(s, d, ld.at[10 + i]) for i, (s, d) in enumerate(((wq_h, wq), (wk_h, wk), (wv_h, wv), (x_h, xbuf)))]

        def arrived(p):
            whole = dor.at[pl.ds(aligned(p * pw, pw), pw), :]
            with jax.named_scope("b_hwait"):
                to_left(whole, whole, osnd.at[p], orcv.at[p]).wait()

        def walk(it):
            ahead = it + 1

            @pl.when((lax.rem(ahead, rows) == 0) & (ahead < n_steps))
            def _():
                arrived(ahead // rows)

            @pl.when(it < n_steps)
            def _():
                with jax.named_scope("b_attn"):
                    grads(it - 1)
                    soften(it)
                    score(jnp.minimum(ahead, n_steps - 1))

            @pl.when(it == n_steps)
            def _():
                grads(n_steps - 1)
                for c in weights():
                    c.start()

            p, step = it // rows - 1, lax.rem(it, rows)

            @pl.when((step == 0) & (lax.rem(p, per) == per - 1))
            def _():
                close_group(p // per)

            @pl.when(it == n_steps)
            def _():
                comm.offer(end)

            t = pick(it, tick_after)

            @pl.when(t > 0)
            def _():
                comm.tick(t)

            @pl.when((step == 0) & (p + 3 < n_pairs))
            def _():
                give_out(p + 3)

        for c in lds[:-1]:
            c.wait()
        for i in range(2):
            push_rows(i).wait()
        arrived(0)
        score(0)
        soften(0)
        score(1)
        lds[-1].wait()
        cdiv_loop(n_steps, lambda i: walk(i + 1))
        for c in weights():
            c.wait()

        def into(b):
            r = pl.ds(aligned(b * toks, QB), toks)
            with jax.named_scope("b_into"):
                gnm[r, :] = dot(dqt[:, r], wq[:], TN) + dot(dkt[:, r], wk[:], TN) + dot(dv[r, :], wv[:])

            with jax.named_scope("b_final"):
                for i in range(tb):
                    r = pl.ds(aligned((b * tb + i) * QB, QB), QB)
                    out, dg = norm_back(xbuf[r, :], ga[:], gnm[r, :], gmid[r, :])
                    mbuf[r, :] = out
                    dgain[:8, :] += dg

        def share_gains():
            out_copy.start()
            gains = jnp.concatenate([col_sum(dgain[:8, :]), col_sum(dgain[8:, :]), jnp.zeros((6, width), F32)], axis=0)
            for p in range(n):
                gsend[p, :, :rpd] = gains[:, p * rpd:(p + 1) * rpd]

            def spread(i):
                to = lax.rem(me + i + 1, n)
                pltpu.make_async_remote_copy(src_ref=gsend.at[to], dst_ref=grecv.at[i], send_sem=gsem.at[0], recv_sem=gsem.at[1],
                                             device_id={"seq": to}, device_id_type=MESH).start()

            cdiv_loop(n - 1, spread)

        def finish(i):
            comm.advance(end + i, True)

            @pl.when(i == 1)
            def _():
                cdiv_loop(rows - 2, lambda b: into(b + 1))

            @pl.when(i == LAG + 1)
            def _():
                into(rows - 1)
                share_gains()

        into(0)
        cdiv_loop(4 * LAG - 1, finish)

    score_bufs = [f(3 * QB, 2 * QB) for f in (vf, vm) for _ in range(8)]
    out_copy = pltpu.make_async_copy(mbuf, dx_h, ld.at[0])
    pl.run_scoped(attention, vm(hd, total), vm(hd, rows * ext), vm(rows * ext, hd), vm(rows * ext, hd), vm(hd, rows * WINDOW), vm(total, hd), *score_bufs)
    most, rest = pl.ds(0, end), pl.ds(end, 2)
    keep_most = load(1, fin.at[most], fin_h.at[most])
    to_left(gsend.at[pl.ds(0, n - 1)], grecv, gsem.at[0], gsem.at[1]).wait()
    sums = gsend[me]
    for i in range(n - 1):
        sums = sums + grecv[i]
    fin[end + 1, 0, :8, :128] = sums
    out_copy.wait()
    comm.advance(end + 4 * LAG - 1, True)
    with jax.named_scope("b_end"):
        keep_rest = load(0, fin.at[rest], fin_h.at[rest])
        keep_most.wait()
        keep_rest.wait()


def spread_kernel(dims, dx_i, fin_i, dx_o, dga_o, dgm_o, *refs):
    head_dim, n, width, ff = dims
    outs, (buf, fin), stage, sem = refs[:7], refs[7:9], refs[9:16], refs[16]
    dq, dk, dv, do, dg, du, dd = stage
    nb, nc, sub = ff // CB, width // CB, ff // width
    rpd = width // n
    head, place, end = plan(nb, nc * sub // 2, nc)
    get_fin = pltpu.make_async_copy(fin_i, fin, sem.at[len(outs)])
    get_fin.start()
    cut = buf.shape[0] // nc
    gets, puts = ([pltpu.make_async_copy(s.at[pl.ds(i * cut, cut)], d.at[pl.ds(i * cut, cut)], sem.at[len(outs) + k + i]) for i in range(nc)]
                  for k, s, d in ((1, dx_i, buf), (nc + 1, buf, dx_o)))
    for c in gets:
        c.start()
    get_fin.wait()
    gains = fin[end + 1, 0]
    dga_o[:] = gains[:1, :rpd]
    dgm_o[:] = gains[1:2, :rpd]
    for j in range(nb):
        dg[:, j * CB:(j + 1) * CB] = fin[j, 0]
        du[:, j * CB:(j + 1) * CB] = fin[j, 1]
    for c in range(nc):
        for i in range(sub):
            pair = nb + (c * sub + i) // 2
            dd[i * rpd:(i + 1) * rpd, c * CB:(c + 1) * CB] = fin[pair, i % 2]
    for g in range(nc):
        do[:, g * CB:(g + 1) * CB] = fin[place["o", g]]
        for name, ref in (("q", dq), ("k", dk), ("v", dv)):
            val = fin[place[name, g]]
            for h in range(CB // head_dim):
                ref[g * (CB // head_dim) + h] = val[:, h * head_dim:(h + 1) * head_dim]
    keeps = [pltpu.make_async_copy(s, d, sem.at[i]) for i, (s, d) in enumerate(zip(stage, outs))]
    for c in keeps:
        c.start()
    for get, out in zip(gets, puts):
        get.wait()
        out.start()
    for c in keeps + puts:
        c.wait()


def run_bwd(n, head_dim, ga, gm, x, dout, q, kt, k, v, ha, ot, xm, hm, hmt, qr, lse, cos_t, sin_t, wq, wk, wv, wo, wg, wu, wd, rows):
    total, width = x.shape
    hd, ff = wq.shape[0], wg.shape[1]
    toks = total // rows
    rpd, heads = width // n, hd // head_dim
    nb, nc, sub = ff // CB, width // CB, ff // width
    slots = plan(nb, nc * sub // 2, nc)[2] + 2
    n_pairs = hd // (2 * head_dim)
    f = lambda *s: jax.ShapeDtypeStruct(s, F32)
    dx_t = jax.ShapeDtypeStruct((total, width), BF)
    vm = lambda *s: pltpu.VMEM(s, BF)
    vf = lambda *s: pltpu.VMEM(s, F32)
    dma = lambda *s: pltpu.SemaphoreType.DMA(s)
    line, duo = vf(rows * n_pairs, 8, 2 * QB), (2, SLOTS)
    scratch = [vf(RING, 2, n // 2, 2, rpd, CB), vf(SLOTS, 2, n // 2, rpd, CB), vf(*duo, 2, 2, rpd, CB), vf(*duo, 2, 4, rpd, CB),
               vf(*duo, 2, rpd, CB // 2), vf(*duo, 2, rpd, CB), vf(*duo, 3, rpd, CB), vf(*duo, 4, 4, rpd, CB), vf(*duo, 4, rpd, CB), vf(slots, 2, rpd, CB),
               dma(6, *duo), dma(6, *duo),
               vm(hd, rows * WINDOW), line, line, dma(2), dma(2), dma(n_pairs), dma(n_pairs),
               vf(n, 8, 128), vf(n - 1, 8, 128), dma(2), dma(15),
               vm(total, width), vm(total, width), vf(total, width), vm(total, width), vm(hd, total), vm(width, total), vm(hd, width), vm(hd, total), line, line, vf(*cos_t.shape), vf(*cos_t.shape), vf(*ga.shape), vf(*ga.shape), vf(16, width)]
    mid = pl.pallas_call(
        functools.partial(bwd_kernel, n, head_dim, (rows, toks, width, hd, ff)), out_shape=[dx_t, f(slots, 2, rpd, CB)],
        in_specs=any_spec(24), out_specs=any_spec(2), scratch_shapes=scratch,
        compiler_params=pltpu.CompilerParams(collective_id=1, has_side_effects=True, vmem_limit_bytes=VMEM_LIMIT),
        name="backward")(ga, gm, x, dout, q, kt, k, v, ha, ot, xm, hm, hmt, qr, lse, cos_t, sin_t, wq, wk, wv, wo, wg, wu, wd)
    outs = [f(heads, rpd, head_dim)] * 3 + [f(rpd, width), f(rpd, ff), f(rpd, ff), f(ff // n, width)]
    return pl.pallas_call(
        functools.partial(spread_kernel, (head_dim, n, width, ff)), out_shape=[dx_t, f(1, rpd), f(1, rpd)] + outs,
        in_specs=any_spec(2), out_specs=any_spec(1) + vmem_spec(2) + any_spec(7),
        scratch_shapes=[vm(total, width), vf(slots, 2, rpd, CB), *[vf(*o.shape) for o in outs], dma(8 + 2 * nc)],
        name="spread")(*mid)


def solution(mesh):
    n = mesh.shape["seq"]

    def device_step(hidden, positions, g_attn, g_mlp, w_query, w_key, w_value, w_out, w_gate, w_up, w_down, d_out):
        rows, toks, width = hidden.shape
        layers, _, heads, head_dim = w_query.shape
        hd = heads * head_dim
        half = head_dim // 2
        inv_freq = 1.0 / (10000.0 ** (jnp.arange(half, dtype=F32) * (2.0 / head_dim)))
        turn = lambda w: w[0].transpose(1, 2, 0).reshape(hd, width)
        wq, wk, wv = turn(w_query), turn(w_key), turn(w_value)
        fwd = run_fwd(n, hidden, positions, inv_freq[:, None], g_attn, g_mlp, wq, wk, wv, w_out[0], head_dim)
        out = run_bwd(n, head_dim, g_attn, g_mlp, hidden.reshape(rows * toks, width), d_out.reshape(rows * toks, width), *fwd,
                      wq, wk, wv, w_out[0], w_gate[0], w_up[0], w_down[0], rows)
        dx, dga, dgm, dq, dk, dv, do, dg, du, dd = out
        back = lambda w: w.transpose(1, 0, 2)[None]
        return (dx.reshape(rows, toks, width), dga, dgm, back(dq), back(dk), back(dv), do[None], dg[None], du[None], dd[None])

    tok_spec, grad_spec = P("data", "seq"), P(None, ("data", "seq"))
    in_specs = (tok_spec, tok_spec) + (P(),) * 9 + (tok_spec,)
    out_specs = (tok_spec,) + (grad_spec,) * 9
    return jax.shard_map(device_step, mesh=mesh, in_specs=in_specs, out_specs=out_specs, check_vma=False)
```

```python
import functools, math
import numpy as np
import jax, jax.numpy as jnp
from jax import lax
from jax.experimental import pallas as pl
from jax.experimental.pallas import tpu as pltpu
from jax.sharding import PartitionSpec as P

WINDOW = 256
NORM_EPS = 1e-5
QB = 128
BF, F32 = jnp.bfloat16, jnp.float32
NN, NT, TN = ((1,), (0,)), ((1,), (1,)), ((0,), (0,))
MESH = pl.DeviceIdType.MESH
NEG = -1e30
VMEM_LIMIT = 67043328


def dot(a, b, dims=NN):
    return lax.dot_general(a, b, (dims, ((), ())), preferred_element_type=F32)


def cdiv_loop(n, body):
    lax.fori_loop(0, n, lambda i, c: body(i) or c, 0)


def mod(a, b):
    return a % b if isinstance(a, int) else lax.rem(a, b)


def aligned(a, b):
    return a if isinstance(a, int) else pl.multiple_of(a, b)


def rope(blk, cos_b, sin_b, sign, head_dim):
    half = head_dim // 2
    parts = []
    for h in range(blk.shape[0] // head_dim):
        first = blk[h * head_dim:h * head_dim + half]
        second = blk[h * head_dim + half:(h + 1) * head_dim]
        if sign > 0:
            parts += [first * cos_b - second * sin_b, second * cos_b + first * sin_b]
        else:
            parts += [first * cos_b + second * sin_b, second * cos_b - first * sin_b]
    return jnp.concatenate(parts, axis=0)


def normed(x, gain):
    xf = x.astype(F32)
    inv = lax.rsqrt(jnp.mean(xf * xf, axis=-1, keepdims=True) + NORM_EPS)
    return (xf * inv * gain).astype(BF)


def stack_pair(pair_t):
    half = pair_t.shape[0] // 2
    zero = jnp.zeros((half, pair_t.shape[1]), pair_t.dtype)
    return jnp.concatenate(
        [jnp.concatenate([pair_t[:half], zero], axis=0), jnp.concatenate([zero, pair_t[half:]], axis=0)], axis=1)


def unstack_pair(both):
    half, cols = both.shape[0] // 2, both.shape[1] // 2
    return jnp.concatenate([both[:half, :cols], both[half:, cols:]], axis=0)


def col_sum(x):
    return jnp.sum(x, axis=0, keepdims=True)


def merged(scores, upper, bias0, bias1):
    return jnp.where(upper, scores[:QB] + bias0, scores[2 * QB:]), scores[QB:2 * QB] + bias1


def banded(p02, p1, upper):
    return jnp.concatenate(
        [jnp.where(upper, p02, 0.0).astype(BF), p1.astype(BF), jnp.where(upper, 0.0, p02).astype(BF)], axis=0)


def upper_mask():
    key_ids = lax.broadcasted_iota(jnp.int32, (QB, 2 * QB), 0)
    query_ids = lax.broadcasted_iota(jnp.int32, (QB, 2 * QB), 1) % QB
    return key_ids > query_ids


def start_bias(first, blk):
    bias = jnp.where(first, NEG, 0.0).astype(F32)
    return (bias if blk < 2 else 0.0), (bias if blk < 1 else 0.0)


def fwd_kernel(n, head_dim, x_h, pos_h, invf_h, ga_h, gm_h, wq_h, wk_h, wv_h, wo_h,
               q_h, kt_h, k_h, v_h, ha_h, ot_h, xm_h, hm_h, hmt_h, qr_h, lse_h, cos_t, sin_t,
               pos, invf, ga, gm, xv, halo, qr, lse, pos_halo, wq, wk, wv, wo, q, kt, k, v, vt, ot, xm, hm, hmt, hb, hh, acc, acc2, ak, av, cos_h, sin_h,
               sc0, sc1, sc2, pb0, pb1, pb2, ldx, ld, st, snd, rcv, qsnd, qrcv):
    sc, pb = (sc0, sc1, sc2), (pb0, pb1, pb2)
    rows, toks, width = xv.shape
    ext, total, pw = toks + WINDOW, rows * toks, 2 * head_dim
    n_pairs = wq.shape[0] // pw
    tb, n_steps = toks // QB, n_pairs * rows
    me = lax.axis_index("seq")
    right, left = lax.rem(me + 1, n), lax.rem(me + n - 1, n)
    load_x = [pltpu.make_async_copy(x_h.at[b], xv.at[b], ldx.at[b]) for b in range(rows)]
    load_w = [pltpu.make_async_copy(s, d, ld.at[i]) for i, (s, d) in enumerate(((wq_h, wq), (wk_h, wk), (wv_h, wv), (wo_h, wo)))]
    load_s = [pltpu.make_async_copy(s, d, ldx.at[rows + i]) for i, (s, d) in enumerate(((pos_h, pos), (invf_h, invf), (ga_h, ga), (gm_h, gm)))]
    for c in load_s + load_x:
        c.start()
    barrier = pltpu.get_barrier_semaphore()
    for other in (left, right):
        pl.semaphore_signal(barrier, inc=1, device_id={"seq": other}, device_id_type=MESH)

    def push(i, s, d):
        return pltpu.make_async_remote_copy(src_ref=s, dst_ref=d, send_sem=snd.at[i], recv_sem=rcv.at[i], device_id={"seq": right}, device_id_type=MESH)

    def push_rows(b):
        return push(b, x_h.at[b, toks - WINDOW:, :], halo.at[b])

    send_pos = push(rows, pos, pos_halo)

    def angles(cos_ref, sin_ref, positions):
        count = positions.shape[1]
        for b in range(rows):
            ang = invf[:] * positions[b:b + 1, :].astype(F32)
            cos_ref[:, b * count:(b + 1) * count] = jnp.cos(ang)
            sin_ref[:, b * count:(b + 1) * count] = jnp.sin(ang)

    for c in load_s:
        c.wait()
    angles(cos_t, sin_t, pos[:])

    def norm_rows(b):
        for i in range(tb):
            h = normed(xv[b, i * QB:(i + 1) * QB, :], ga[:])
            hb[pl.ds(pl.multiple_of((b * tb + i) * QB, QB), QB), :] = h

    with jax.named_scope("f_norm"):
        for c in load_x:
            c.wait()
        for c in load_w:
            c.start()
        cdiv_loop(rows, norm_rows)
    pl.semaphore_wait(barrier, 2)
    send_pos.start()
    for b in range(rows):
        push_rows(b).start()
    keep_ha = pltpu.make_async_copy(hb, ha_h, st.at[0])
    keep_ha.start()
    tables = cos_t[:], sin_t[:]

    def put_q(src):
        for p in range(n_pairs):
            r = slice(p * pw, (p + 1) * pw)
            q[r, :] = (rope(src[r, :], *tables, 1, head_dim) * (head_dim ** -0.5)).astype(BF)

    def put_own(src, dst_t, dst):
        for p in range(n_pairs):
            r = slice(p * pw, (p + 1) * pw)
            both = (rope(src[r, :], *tables, 1, head_dim) if dst is k else src[r, :]).astype(BF)
            for b in range(rows):
                blk = both[:, b * toks:(b + 1) * toks]
                own = slice(b * ext + WINDOW, (b + 1) * ext)
                dst_t[r, own] = blk
                dst[own, r] = blk.T

    with jax.named_scope("f_mm"):
        load_w[0].wait()
        load_w[1].wait()
        load_w[2].wait()
        acc[:] = dot(wq[:], hb[:], NT)
        acc2[:] = dot(wk[:], hb[:], NT)
        put_q(acc)
        send_pos.wait()
        acc[:] = dot(wv[:], hb[:], NT)
        angles(cos_h, sin_h, pos_halo[:, toks - WINDOW:])
        put_own(acc2, kt, k)
        put_own(acc, vt, v)
    keep_q = pltpu.make_async_copy(q, q_h, st.at[1])
    keep_q.start()

    def push_q(b):
        return pltpu.make_async_remote_copy(src_ref=q.at[:, b * toks:b * toks + WINDOW], dst_ref=qr.at[:, b * WINDOW:(b + 1) * WINDOW],
                                            send_sem=qsnd.at[b], recv_sem=qrcv.at[b], device_id={"seq": left}, device_id_type=MESH)

    for b in range(rows):
        push_q(b).start()

    def keeps(b):
        wide, cols = pl.ds(pl.multiple_of(b * ext, QB), ext), pl.ds(pl.multiple_of(b * toks, QB), toks)
        ends = ((kt.at[:, wide], kt_h.at[:, wide]), (k.at[wide, :], k_h.at[wide, :]), (v.at[wide, :], v_h.at[wide, :]),
                (ot.at[:, cols], ot_h.at[:, cols]), (hm.at[cols, :], hm_h.at[cols, :]), (hmt.at[:, cols], hmt_h.at[:, cols]),
                (xm.at[cols, :], xm_h.at[cols, :]))
        return [pltpu.make_async_copy(s, d, st.at[2 + b * len(ends) + i]) for i, (s, d) in enumerate(ends)]

    def halo_in(b):
        with jax.named_scope("f_halo_wait"):
            push_rows(b).wait()
        with jax.named_scope("f_halo"):
            for i in range(WINDOW // QB):
                r = slice(i * QB, (i + 1) * QB)
                hh[r, :] = normed(halo[b, r, :], ga[:])
            ak[:] = dot(wk[:], hh[:], NT)
            av[:] = dot(wv[:], hh[:], NT)
            cols = pl.ds(pl.multiple_of(b * WINDOW, QB), WINDOW)
            wide = pl.ds(pl.multiple_of(b * ext, QB), WINDOW)
            near = cos_h[:, cols], sin_h[:, cols]
            for src, dst_t, dst in ((ak, kt, k), (av, vt, v)):
                for p in range(n_pairs):
                    r = slice(p * pw, (p + 1) * pw)
                    blk = (rope(src[r, :], *near, 1, head_dim) if dst is k else src[r, :]).astype(BF)
                    dst_t[r, wide] = blk
                    dst[wide, r] = blk.T
        for c in keeps(b)[:3]:
            c.start()

    upper = upper_mask()
    first = me == 0

    def spots(it, blk):
        b, p = it // n_pairs, mod(it, n_pairs)
        pr = pl.ds(aligned(p * pw, pw), pw)
        return pr, pl.ds(aligned(b * toks + blk * QB, QB), QB), pl.ds(aligned(b * ext + blk * QB, QB), 3 * QB)

    def score(it):
        for blk in range(tb):
            pr, cols, keys = spots(it, blk)
            sc[blk][:] = dot(k[keys, pr], stack_pair(q[pr, cols]))

    def soften(it, blk):
        s02, s1 = merged(sc[blk][:], upper, *start_bias(first, blk))
        top = jnp.max(jnp.maximum(s02, s1), axis=0, keepdims=True)
        e02, e1 = jnp.exp(s02 - top), jnp.exp(s1 - top)
        mass = col_sum(e02 + e1)
        inv = 1.0 / mass
        lse[it, blk:blk + 1, :] = top + jnp.log(mass)
        pb[blk][:] = banded(e02 * inv, e1 * inv, upper)

    def mix(it):
        for blk in range(tb):
            pr, cols, keys = spots(it, blk)
            ot[pr, cols] = unstack_pair(dot(vt[pr, keys], pb[blk][:])).astype(BF)

    def project(b):
        cols = pl.ds(pl.multiple_of(b * toks, QB), toks)
        with jax.named_scope("f_proj"):
            mid = (xv[b].astype(F32) + dot(ot[:, cols], wo[:], TN)).astype(BF)
            xm[cols, :] = mid
            h = normed(mid, gm[:])
            hm[cols, :] = h
            hmt[:, cols] = h.T
        for c in keeps(b)[3:]:
            c.start()

    keep_qr, keep_lse = (pltpu.make_async_copy(*ends, ld.at[i]) for i, ends in enumerate(((qr, qr_h), (lse, lse_h))))
    load_w[3].wait()
    for blk in range(tb):
        pb[blk][:] = jnp.zeros(pb[blk].shape, BF)

    def walk(i):
        it = i - 1

        @pl.when((lax.rem(i, n_pairs) == 0) & (i < n_steps))
        def _():
            halo_in(i // n_pairs)

        @pl.when(i == 0)
        def _():
            score(0)

        @pl.when((i > 0) & (i <= n_steps))
        def _():
            with jax.named_scope("f_attn"):
                mix(jnp.maximum(it - 1, 0))
                for blk in range(tb):
                    soften(it, blk)
                score(jnp.minimum(i, n_steps - 1))

        @pl.when(i == n_steps)
        def _():
            for b in range(rows):
                push_q(b).wait()
            keep_qr.start()

        @pl.when(i > n_steps)
        def _():
            mix(n_steps - 1)

        @pl.when((lax.rem(it, n_pairs) == 0) & (it > 0))
        def _():
            project(it // n_pairs - 1)

    cdiv_loop(n_steps + 2, walk)
    with jax.named_scope("f_store_wait"):
        keep_lse.start()
        keep_ha.wait()
        keep_q.wait()
        keep_qr.wait()
        keep_lse.wait()
        for b in range(rows):
            for c in keeps(b):
                c.wait()


def any_spec(k):
    return [pl.BlockSpec(memory_space=pl.ANY)] * k


def vmem_spec(k):
    return [pl.BlockSpec(memory_space=pltpu.VMEM)] * k


def run_fwd(n, x, pos, invf, ga, gm, wq, wk, wv, wo, head_dim):
    rows, toks, width = x.shape
    hd = wq.shape[0]
    ext, total, n_halo = toks + WINDOW, rows * toks, rows * WINDOW
    half = head_dim // 2
    sds = lambda *s: jax.ShapeDtypeStruct(s, BF)
    dma = lambda *s: pltpu.SemaphoreType.DMA(s)
    outs = [sds(hd, total), sds(hd, rows * ext), sds(rows * ext, hd), sds(rows * ext, hd), sds(total, width), sds(hd, total), sds(total, width), sds(total, width), sds(width, total)]
    outs += [sds(hd, n_halo), jax.ShapeDtypeStruct((rows * hd // (2 * head_dim), 8, 2 * QB), F32)] + [jax.ShapeDtypeStruct((half, total), F32)] * 2
    vm = lambda *s: pltpu.VMEM(s, BF)
    vf = lambda *s: pltpu.VMEM(s, F32)
    scratch = [pltpu.VMEM((rows, toks), jnp.int32), vf(*invf.shape), vf(*ga.shape), vf(*ga.shape), vm(rows, toks, width), vm(rows, WINDOW, width), vm(hd, n_halo), vf(rows * hd // (2 * head_dim), 8, 2 * QB), pltpu.VMEM((rows, toks), jnp.int32), vm(hd, width), vm(hd, width), vm(hd, width), vm(hd, width),
               vm(hd, total), vm(hd, rows * ext), vm(rows * ext, hd), vm(rows * ext, hd), vm(hd, rows * ext), vm(hd, total), vm(total, width), vm(total, width), vm(width, total), vm(total, width), vm(WINDOW, width),
               vf(hd, total), vf(hd, total), vf(hd, WINDOW), vf(hd, WINDOW), vf(half, n_halo), vf(half, n_halo),
               *[f(3 * QB, 2 * QB) for f in (vf, vm) for _ in range(3)],
               dma(rows + 4), dma(4), dma(2 + 7 * rows), dma(rows + 1), dma(rows + 1), dma(rows), dma(rows)]
    return pl.pallas_call(
        functools.partial(fwd_kernel, n, head_dim), out_shape=outs,
        in_specs=any_spec(9), out_specs=any_spec(11) + vmem_spec(2), scratch_shapes=scratch,
        compiler_params=pltpu.CompilerParams(collective_id=0, has_side_effects=True, vmem_limit_bytes=VMEM_LIMIT),
        name="forward")(x, pos, invf, ga, gm, wq, wk, wv, wo)


LAG = 2
SLOTS = 2 * LAG
RING = 8
CB = 256


def at(ref, *idx):
    return ref.at[idx]


class Torus:
    def __init__(self, n, head, last, turn, parts, recv0, recv1, recv2, recv3, recv4, recv5, acc, acc2, fin, snd, rcv):
        assert math.isqrt(n // 2) == 4
        me = lax.axis_index("seq")
        self.core = lax.rem(me, 2)
        chip = me // 2
        self.x, self.y = lax.rem(chip, 4), chip // 4
        self.head, self.last, self.turn = head, last, turn
        self.parts, self.recv0, self.recv1, self.recv2, self.recv3, self.recv4, self.recv5 = parts, recv0, recv1, recv2, recv3, recv4, recv5
        self.acc, self.acc2, self.fin, self.snd, self.rcv = acc, acc2, fin, snd, rcv
        self.partner = me + 1 - 2 * self.core
        self.rows, self.columns = [lax.rem(self.y + d, 4) * 4 for d in range(4)], [lax.rem(self.x + d, 4) for d in range(4)]
        self.hops = [[self.device(0, d) for d in range(4)], [self.device(d, 0) for d in range(4)]]

    def device(self, dy, dx):
        return (self.rows[dy] + self.columns[dx]) * 2 + self.core

    def copy(self, lane, kind, slot, src, dst, target):
        return pltpu.make_async_remote_copy(
            src_ref=src, dst_ref=dst, send_sem=self.snd.at[lane, kind, slot], recv_sem=self.rcv.at[lane, kind, slot],
            device_id={"seq": target}, device_id_type=MESH)

    def late(self, axis, pair, yes, no):
        first, end = self.turn
        busy = (pair >= first) & (pair < end)
        return jnp.where(busy & (self.x == 3) if axis else busy, yes, no)

    def swap(self, ring, slot):
        return self.copy(0, 0, slot, self.parts.at[ring, :, :, 1 - self.core], self.recv0.at[slot], self.partner)

    def landing(self, stage):
        return (self.recv0, self.recv1, self.recv2, self.recv3, self.recv4, self.recv5)[stage]

    def arrived(self, stage, kind, slot):
        whole = self.landing(stage).at[kind, slot]
        self.copy(stage, kind, slot, whole, whole, self.partner).wait()

    def send(self, stage, kind, pair, held, slot):
        axis = kind if stage < 3 else 1 - kind
        plus, minus = self.hops[axis][1], self.hops[axis][-1]
        half = CB // 2
        if stage == 1:
            minus = self.late(axis, pair, plus, minus)
            ends = self.acc.at[kind, held, 2, :2], self.acc.at[kind, held, 2, 2:]
        elif stage == 2:
            ends = self.acc.at[kind, held, 1], self.acc.at[kind, held, 3]
        elif stage == 3:
            ends = self.acc2.at[kind, held, 2, :, :half], self.acc2.at[kind, held, 2, :, half:]
        else:
            ends = self.acc2.at[kind, held, 1], self.acc2.at[kind, held, 3]
        for i, src in enumerate(ends):
            self.copy(stage, kind, slot, src, self.landing(stage).at[kind, slot, i], (plus, minus)[i]).start()

    def add(self, stage, kind, pair, held, slot, ring):
        acc, acc2 = self.acc, self.acc2
        if stage == 1:
            for r1 in range(4):
                for r2 in range(4):
                    ry, rx = (r2, r1) if kind == 0 else (r1, r2)
                    chip = self.rows[ry] + self.columns[rx]
                    acc[kind, held, r1, r2] = self.parts[ring, kind, chip, self.core] + self.recv0[slot, kind, chip]
        elif stage == 2:
            back = self.late(kind, pair, 1, 3)
            acc[kind, held, 1, :2] += self.recv1[kind, slot, 0]
            acc[kind, held, back, 2:] += self.recv1[kind, slot, 1]
        elif stage == 3:
            acc2[kind, held] = acc[kind, held, 0] + (self.recv2[kind, slot, 0] + self.recv2[kind, slot, 1])
        elif stage == 4:
            half = CB // 2
            acc2[kind, held, 1, :, :half] += self.recv3[kind, slot, 0]
            acc2[kind, held, 3, :, half:] += self.recv3[kind, slot, 1]
        else:
            self.fin[pair, kind] = acc2[kind, held, 0] + (self.recv4[kind, slot, 0] + self.recv4[kind, slot, 1])

    def direct(self, kind, held, slot):
        for d in range(1, 4):
            self.copy(5, kind, slot, self.acc2.at[kind, held, d], self.recv5.at[kind, slot, d - 1], self.hops[1 - kind][d]).start()

    def early(self, pair):
        return (pair >= 0) & (pair <= self.head)

    def final(self, pair):
        return (pair == self.last) | ((pair > self.head) & (pair < self.last) & (mod(abs(pair - self.head), 2) == 0))

    def when(self, which, fn):
        if isinstance(which, bool):
            fn() if which else None
        else:
            pl.when(which)(fn)

    def offer(self, t):
        self.when(self.early(t) | self.final(t), lambda: self.swap(mod(t, RING), mod(t, SLOTS)).start())

    def tick(self, t):
        self.offer(t)
        self.advance(t)

    def advance(self, t, tail=False):
        now, land, before = mod(t, SLOTS), mod(t + SLOTS - LAG, SLOTS), mod(t + SLOTS - 1, SLOTS)
        ring_land = mod(t + RING - 1, RING)
        for stage in range(5, 0, -1):
            pair = t - LAG * stage + 1
            held = before if stage % 2 else mod(t + 1, SLOTS)

            def move(last_hops, stage=stage, pair=pair, held=held):
                if stage == 1:
                    with jax.named_scope("t_wait1"):
                        self.swap(ring_land, before).wait()
                for kind in range(2):
                    if last_hops and stage == 4:
                        with jax.named_scope("t_wait6"):
                            self.arrived(5, kind, land)
                        got = self.recv5[kind, land]
                        self.fin[pair, kind] = self.acc2[kind, held, 0] + (got[0] + got[1] + got[2])
                        continue
                    if stage > 1:
                        with jax.named_scope(f"t_wait{stage}"):
                            self.arrived(stage - 1, kind, land)
                    self.add(stage, kind, pair, held, land if stage > 1 else before, ring_land)
                    if last_hops and stage == 3:
                        self.direct(kind, held, now)
                    elif stage < 5:
                        self.send(stage, kind, pair, held, now)

            if stage < 3:
                self.when(self.early(pair) | self.final(pair), functools.partial(move, False))
            else:
                self.when(self.early(pair), functools.partial(move, False))
                if tail and stage < 5:
                    self.when(self.final(pair), functools.partial(move, True))


def pick(i, table):
    out = 0
    for key, value in table.items():
        out = jnp.where(i == key, value, out)
    return out


def norm_back(x, gain, grad, res):
    xf = x.astype(F32)
    inv = lax.rsqrt(jnp.mean(xf * xf, axis=-1, keepdims=True) + NORM_EPS)
    unit = xf * inv
    gu = grad * gain
    out = inv * (gu - unit * jnp.mean(gu * unit, axis=-1, keepdims=True)) + res.astype(F32)
    gu = grad * unit
    return out.astype(BF), jnp.sum(gu.reshape(-1, 8, gu.shape[-1]), axis=0)


def plan(n_mlp, n_down, nc):
    order = [("o", g) for g in range(nc)] + [(name, g) for g in range(nc) for name in "qkv"]
    base, head = n_mlp + n_down, n_mlp + n_down + nc - 1
    last = 2 * (base - 1 - head + len(order) // 2) + head - 1
    spot = lambda pair: min(max(pair, 2 * pair - head), last)
    return head, {name: (spot(base + i // 2), i % 2) for i, name in enumerate(order)}, last


def bwd_kernel(n, head_dim, dims, ga_h, gm_h, x_h, dout_h, q_h, kt_h, k_h, v_h, ha_h, ot_h, xm_h, hm_h, hmt_h, qr_h, lse_h, cos_h, sin_h,
               wq_h, wk_h, wv_h, wo_h, wg_h, wu_h, wd_h,
               dx_h, fin_h,
               parts, recv0, recv1, recv2, recv3, recv4, recv5, acc, acc2, fin, snd, rcv,
               dor, lser, deltar, hsnd, hrcv, osnd, orcv, gsend, grecv, gsem, ld,
               xbuf, mbuf, gnm, gmid, ot, hat, wo, dot_, lse, delta, cos_i, sin_i, ga, gm, dgain):
    rows, toks, width, hd, ff = dims
    ext, total = toks + WINDOW, rows * toks
    pw = 2 * head_dim
    n_pairs = hd // pw
    tb, n_steps = toks // QB, n_pairs * rows
    nb, nc, sub = ff // CB, width // CB, ff // width
    rpd = width // n
    per, half_sub = CB // pw, sub // 2
    head, place, end = plan(nb, nc * half_sub, nc)
    comm = Torus(n, head, end, (nb, nb + n_pairs + 1), parts, recv0, recv1, recv2, recv3, recv4, recv5, acc, acc2, fin, snd, rcv)
    me = lax.axis_index("seq")
    left = lax.rem(me + n - 1, n)
    barrier = pltpu.get_barrier_semaphore()

    def greet(i):
        pl.semaphore_signal(barrier, inc=1, device_id={"seq": lax.rem(me + i + 1, n)}, device_id_type=MESH)

    def load(i, s, d):
        c = pltpu.make_async_copy(s, d, ld.at[i])
        c.start()
        return c

    def late(i):
        s, d = ((xm_h, mbuf), (ot_h, ot), (wo_h, wo), (lse_h, lse), (cos_h, cos_i), (sin_h, sin_i), (ga_h, ga), (gm_h, gm))[i]
        return pltpu.make_async_copy(s, d, ld.at[1 + i])

    def to_left(src, dst, send_sem, recv_sem):
        return pltpu.make_async_remote_copy(src_ref=src, dst_ref=dst, send_sem=send_sem, recv_sem=recv_sem,
                                            device_id={"seq": left}, device_id_type=MESH)

    n_late = 8

    def push_rows(i):
        return to_left(*((lse_h, lser), (delta, deltar))[i], hsnd.at[i], hrcv.at[i])

    def push_out(p):
        pr = pl.ds(aligned(p * pw, pw), pw)
        return [to_left(dot_.at[pr, pl.ds(b * toks, WINDOW)], dor.at[pr, pl.ds(b * WINDOW, WINDOW)], osnd.at[p], orcv.at[p])
                for b in range(rows)]

    def give_out(p):
        for c in push_out(p):
            c.start()

    def put(spot, value):
        pair, kind = spot
        parts[mod(pair, RING), kind] = value.reshape(n // 2, 2, rpd, CB)

    def spot_of(name, g):
        known = {i: place[name, i] for i in range(nc)}
        return pick(g, {i: s[0] for i, s in known.items()}), pick(g, {i: s[1] for i, s in known.items()})

    def spots(it, blk):
        p, b = it // rows, mod(it, rows)
        pr = pl.ds(aligned(p * pw, pw), pw)
        return pr, pl.ds(aligned(b * toks + blk * QB, QB), QB), pl.ds(aligned(b * ext + blk * QB, QB), 3 * QB)

    def row_of(it):
        return mod(it, rows) * n_pairs + it // rows

    def mlp(hm, hmt, ha, actt, wgu, wd, dgu, wld):
        def weights(j, slot):
            c = aligned(j * CB, CB)
            return [pltpu.make_async_copy(wg_h.at[:, pl.ds(c, CB)], wgu.at[slot, :, :CB], wld.at[slot, 0]),
                    pltpu.make_async_copy(wu_h.at[:, pl.ds(c, CB)], wgu.at[slot, :, CB:], wld.at[slot, 1]),
                    pltpu.make_async_copy(wd_h.at[pl.ds(c, CB), :], wd.at[slot], wld.at[slot, 2])]

        for c in weights(0, 0):
            c.start()
        ld_hm, ld_x, ld_hmt = load(10, hm_h, hm), load(0, dout_h, xbuf), load(11, hmt_h, hmt)
        cdiv_loop(n - 1, greet)
        gnm[:] = jnp.zeros_like(gnm)
        gsend[:] = jnp.zeros_like(gsend)
        dgain[:] = jnp.zeros_like(dgain)
        ld_hm.wait()
        ld_x.wait()
        ld_hmt.wait()
        for i in range(n_late):
            late(i).start()
        ld_ha = load(10, ha_h, ha)

        def block(j):
            slot = lax.rem(j, 2)
            for c in weights(j, slot):
                c.wait()

            @pl.when(j + 1 < nb)
            def _():
                for c in weights(j + 1, 1 - slot):
                    c.start()

            c0 = pl.multiple_of(j * CB, CB)
            with jax.named_scope("b_mlp"):
                for b in range(rows):
                    r = slice(b * toks, (b + 1) * toks)
                    gu = dot(hm[r, :], wgu[slot])
                    gact = dot(xbuf[r, :], wd[slot], NT).astype(BF).astype(F32)
                    gate, up = gu[:, :CB], gu[:, CB:]
                    sig = 1.0 / (1.0 + jnp.exp(-gate))
                    swish = gate * sig
                    actt[pl.ds(c0, CB), r] = (swish * up).astype(BF).T
                    dgu[r, :CB] = (gact * up * (sig + swish * (1.0 - sig))).astype(BF)
                    dgu[r, CB:] = (gact * swish).astype(BF)
                both = dot(hmt[:], dgu[:])
                ring = lax.rem(j, RING)
                parts[ring, 0] = both[:, :CB].reshape(n // 2, 2, rpd, CB)
                parts[ring, 1] = both[:, CB:].reshape(n // 2, 2, rpd, CB)
                for b in range(rows):
                    r = slice(b * toks, (b + 1) * toks)
                    gnm[r, :] += dot(dgu[r, :], wgu[slot], NT)

            @pl.when(j == 0)
            def _():
                pl.semaphore_wait(barrier, n - 1)
                push_rows(0).start()

            comm.tick(j)

        cdiv_loop(nb, block)

        def down(c):
            share = n // 2 // sub
            c0 = pl.multiple_of(c * CB, CB)
            for m in range(sub):
                res = dot(actt[m * width:(m + 1) * width, :], xbuf[:, pl.ds(c0, CB)]).reshape(share, 2, sub, rpd, CB)
                for i in range(sub):
                    pair = nb + c * half_sub + i // 2
                    parts[lax.rem(pair, RING), i % 2, m * share:(m + 1) * share] = res[:, :, i]
            for i in range(tb * rows // nc):
                r = pl.ds(pl.multiple_of((c * (tb * rows // nc) + i) * QB, QB), QB)
                hat[:, r] = ha[r, :].T

        for i in range(n_late):
            late(i).wait()
        ld_ha.wait()

        def mid(b):
            for i in range(tb):
                r = pl.ds(pl.multiple_of((b * tb + i) * QB, QB), QB)
                out, dg = norm_back(mbuf[r, :], gm[:], gnm[r, :], xbuf[r, :])
                gmid[r, :] = out
                dgain[8:, :] += dg

        def deltas(p):
            for it in range(rows):
                for blk in range(tb):
                    pr, cols, _ = spots(p * rows + it, blk)
                    both = dot_[pr, cols].astype(F32) * ot[pr, cols].astype(F32)
                    delta[row_of(p * rows + it), blk:blk + 1, :] = jnp.concatenate(
                        [col_sum(both[:head_dim]), col_sum(both[head_dim:])], axis=1)

        def column(c):
            with jax.named_scope("b_down"):
                down(c)

            @pl.when(c < nc - 1)
            def _():
                comm.tick(nb + c + jnp.minimum(c, 1))

            @pl.when(c > 0)
            def _():
                give_out(c)

            @pl.when(c == 0)
            def _():
                with jax.named_scope("b_mid"):
                    cdiv_loop(rows, mid)
                with jax.named_scope("b_dot"):
                    dot_[:] = dot(wo[:], gmid[:], NT).astype(BF)
                    cdiv_loop(n_pairs, deltas)
                comm.tick(nb + 1)
                push_rows(1).start()
                give_out(0)

        cdiv_loop(nc, column)

    vm = lambda *s: pltpu.VMEM(s, BF)
    vf = lambda *s: pltpu.VMEM(s, F32)
    pl.run_scoped(mlp, vm(total, width), vm(width, total), vm(total, width), vm(ff, total), vm(2, width, 2 * CB), vm(2, CB, width), vm(total, 2 * CB),
                  pltpu.SemaphoreType.DMA((2, 3)))
    def attention(q, kt, k, v, qr, dv, sc0, sc1, sc2, sr, dp0, dp1, dp2, dr, pb0, pb1, pb2, pr_, ds0, ds1, ds2, dsr):
        dqt, dkt = ot, q
        wq, wk, wv = k.at[:hd], kt.at[:, :width], v.at[:hd]
        sc, dp, pb, ds = (sc0, sc1, sc2), (dp0, dp1, dp2), (pb0, pb1, pb2), (ds0, ds1, ds2)
        lds = [load(10 + i, s, d) for i, (s, d) in enumerate(((q_h, q), (k_h, k), (v_h, v), (qr_h, qr), (kt_h, kt)))]

        def out_grad(g):
            put(spot_of("o", g), dot(ot[:], gmid[:, pl.ds(pl.multiple_of(g * CB, CB), CB)]))

        with jax.named_scope("b_dwo"):
            cdiv_loop(nc, out_grad)
        first_tick = nb + nc + 1
        comm.tick(first_tick - 1)
        ends = [rows * p for p in range(1, n_pairs + 1)]
        steps = sorted([1, ends[1] - 1, ends[-2] - 1, ends[-1] - 1, *ends[1:]])
        tick_after = {s: first_tick + i for i, s in enumerate(steps)}
        assert first_tick + len(steps) == end
        upper = upper_mask()
        first, last = me == 0, me == n - 1
        halves = slice(0, WINDOW), slice(WINDOW, 3 * QB)

        def right(it, i):
            p, b = it // rows, mod(it, rows)
            return pl.ds(aligned(p * pw, pw), pw), pl.ds(aligned(b * WINDOW + i * QB, QB), QB), pl.ds(aligned(b * ext + toks + i * QB, QB), WINDOW - i * QB)

        def score(it):
            for blk in range(tb):
                pr, cols, keys = spots(it, blk)
                sc[blk][:] = dot(k[keys, pr], stack_pair(q[pr, cols]))
                dp[blk][:] = dot(v[keys, pr], stack_pair(dot_[pr, cols]))
            for i, rs in enumerate(halves):
                pr, cols, keys = right(it, i)
                sr[rs, :] = dot(k[keys, pr], stack_pair(qr[pr, cols]))
                dr[rs, :] = dot(v[keys, pr], stack_pair(dor[pr, cols]))

        def soften(it):
            row = row_of(it)
            for blk in range(tb):
                s02, s1 = merged(sc[blk][:], upper, *start_bias(first, blk))
                norm, mean = lse[row, blk:blk + 1, :], delta[row, blk:blk + 1, :]
                p02, p1 = jnp.exp(s02 - norm), jnp.exp(s1 - norm)
                g02, g1 = jnp.where(upper, dp[blk][:QB], dp[blk][2 * QB:]), dp[blk][QB:2 * QB]
                pb[blk][:] = banded(p02, p1, upper)
                ds[blk][:] = banded(p02 * (g02 - mean), p1 * (g1 - mean), upper)
            for blk in range(tb):
                i = blk // 2
                rs = slice(blk * QB, (blk + 1) * QB)
                p = jnp.exp(sr[rs, :] - jnp.where(last, -NEG, lser[row, i:i + 1, :]))
                g = p * (dr[rs, :] - deltar[row, i:i + 1, :])
                pr_[rs, :] = (p if blk == 1 else jnp.where(upper, p, 0.0)).astype(BF)
                dsr[rs, :] = (g if blk == 1 else jnp.where(upper, g, 0.0)).astype(BF)

        def grads(it):
            ks, vs = [], []
            for blk in range(tb):
                pr, cols, keys = spots(it, blk)
                own = slice(max(0, 2 - blk) * QB, 3 * QB)
                vs.append(dot(pb[blk][own, :], stack_pair(dot_[pr, cols]), NT))
                ks.append(dot(ds[blk][own, :], stack_pair(q[pr, cols]), NT))
                dq = unstack_pair(dot(kt[pr, keys], ds[blk][:])) * (head_dim ** -0.5)
                dqt[pr, cols] = rope(dq, cos_i[:, cols], sin_i[:, cols], -1, head_dim).astype(BF)
            for i, rs in enumerate(halves):
                pr, cols, _ = right(it, i)
                vs.append(dot(pr_[rs, :], stack_pair(dor[pr, cols]), NT))
                ks.append(dot(dsr[rs, :], stack_pair(qr[pr, cols]), NT))
            for j in range(tb):
                pr, cols, _ = spots(it, j)
                gv, gk = (sum(x[i][(j - max(0, i - 2)) * QB:(j - max(0, i - 2) + 1) * QB] for i in range(j, j + 3)) for x in (vs, ks))
                dv[cols, pr] = gv.astype(BF)
                dkt[pr, cols] = rope(gk.T, cos_i[:, cols], sin_i[:, cols], -1, head_dim).astype(BF)

        def close_group(g):
            cols = pl.ds(pl.multiple_of(g * CB, CB), CB)
            with jax.named_scope("b_dwqkv"):
                put(spot_of("q", g), dot(hat[:], dqt[cols, :], NT))
                put(spot_of("k", g), dot(hat[:], dkt[cols, :], NT))
                put(spot_of("v", g), dot(hat[:], dv[:, cols]))

        def weights():
            return [pltpu.make_async_copy(s, d, ld.at[10 + i]) for i, (s, d) in enumerate(((wq_h, wq), (wk_h, wk), (wv_h, wv), (x_h, xbuf)))]

        def arrived(p):
            whole = dor.at[pl.ds(aligned(p * pw, pw), pw), :]
            with jax.named_scope("b_hwait"):
                to_left(whole, whole, osnd.at[p], orcv.at[p]).wait()

        def walk(it):
            ahead = it + 1

            @pl.when((lax.rem(ahead, rows) == 0) & (ahead < n_steps))
            def _():
                arrived(ahead // rows)

            @pl.when(it < n_steps)
            def _():
                with jax.named_scope("b_attn"):
                    grads(it - 1)
                    soften(it)
                    score(jnp.minimum(ahead, n_steps - 1))

            @pl.when(it == n_steps)
            def _():
                grads(n_steps - 1)
                for c in weights():
                    c.start()

            p, step = it // rows - 1, lax.rem(it, rows)

            @pl.when((step == 0) & (lax.rem(p, per) == per - 1))
            def _():
                close_group(p // per)

            @pl.when(it == n_steps)
            def _():
                comm.offer(end)

            t = pick(it, tick_after)

            @pl.when(t > 0)
            def _():
                comm.tick(t)

            @pl.when((step == 0) & (p + 3 < n_pairs))
            def _():
                give_out(p + 3)

        for c in lds[:-1]:
            c.wait()
        for i in range(2):
            push_rows(i).wait()
        arrived(0)
        score(0)
        soften(0)
        score(1)
        lds[-1].wait()
        cdiv_loop(n_steps, lambda i: walk(i + 1))
        for c in weights():
            c.wait()

        def into(b):
            r = pl.ds(aligned(b * toks, QB), toks)
            with jax.named_scope("b_into"):
                gnm[r, :] = dot(dqt[:, r], wq[:], TN) + dot(dkt[:, r], wk[:], TN) + dot(dv[r, :], wv[:])

            with jax.named_scope("b_final"):
                for i in range(tb):
                    r = pl.ds(aligned((b * tb + i) * QB, QB), QB)
                    out, dg = norm_back(xbuf[r, :], ga[:], gnm[r, :], gmid[r, :])
                    mbuf[r, :] = out
                    dgain[:8, :] += dg

        def share_gains():
            out_copy.start()
            gains = jnp.concatenate([col_sum(dgain[:8, :]), col_sum(dgain[8:, :]), jnp.zeros((6, width), F32)], axis=0)
            for p in range(n):
                gsend[p, :, :rpd] = gains[:, p * rpd:(p + 1) * rpd]

            def spread(i):
                to = lax.rem(me + i + 1, n)
                pltpu.make_async_remote_copy(src_ref=gsend.at[to], dst_ref=grecv.at[i], send_sem=gsem.at[0], recv_sem=gsem.at[1],
                                             device_id={"seq": to}, device_id_type=MESH).start()

            cdiv_loop(n - 1, spread)

        def finish(i):
            comm.advance(end + i, True)

            @pl.when(i == 1)
            def _():
                cdiv_loop(rows - 2, lambda b: into(b + 1))

            @pl.when(i == LAG + 1)
            def _():
                into(rows - 1)
                share_gains()

        into(0)
        cdiv_loop(4 * LAG - 1, finish)

    score_bufs = [f(3 * QB, 2 * QB) for f in (vf, vm) for _ in range(8)]
    out_copy = pltpu.make_async_copy(mbuf, dx_h, ld.at[0])
    pl.run_scoped(attention, vm(hd, total), vm(hd, rows * ext), vm(rows * ext, hd), vm(rows * ext, hd), vm(hd, rows * WINDOW), vm(total, hd), *score_bufs)
    most, rest = pl.ds(0, end), pl.ds(end, 2)
    keep_most = load(1, fin.at[most], fin_h.at[most])
    to_left(gsend.at[pl.ds(0, n - 1)], grecv, gsem.at[0], gsem.at[1]).wait()
    sums = gsend[me]
    for i in range(n - 1):
        sums = sums + grecv[i]
    fin[end + 1, 0, :8, :128] = sums
    out_copy.wait()
    comm.advance(end + 4 * LAG - 1, True)
    with jax.named_scope("b_end"):
        keep_rest = load(0, fin.at[rest], fin_h.at[rest])
        keep_most.wait()
        keep_rest.wait()


def spread_kernel(dims, dx_i, fin_i, dx_o, dga_o, dgm_o, *refs):
    head_dim, n, width, ff = dims
    outs, (buf, fin), stage, sem = refs[:7], refs[7:9], refs[9:16], refs[16]
    dq, dk, dv, do, dg, du, dd = stage
    nb, nc, sub = ff // CB, width // CB, ff // width
    rpd = width // n
    head, place, end = plan(nb, nc * sub // 2, nc)
    get_fin = pltpu.make_async_copy(fin_i, fin, sem.at[len(outs)])
    get_fin.start()
    cut = buf.shape[0] // nc
    gets, puts = ([pltpu.make_async_copy(s.at[pl.ds(i * cut, cut)], d.at[pl.ds(i * cut, cut)], sem.at[len(outs) + k + i]) for i in range(nc)]
                  for k, s, d in ((1, dx_i, buf), (nc + 1, buf, dx_o)))
    for c in gets:
        c.start()
    get_fin.wait()
    gains = fin[end + 1, 0]
    dga_o[:] = gains[:1, :rpd]
    dgm_o[:] = gains[1:2, :rpd]
    for j in range(nb):
        dg[:, j * CB:(j + 1) * CB] = fin[j, 0]
        du[:, j * CB:(j + 1) * CB] = fin[j, 1]
    for c in range(nc):
        for i in range(sub):
            pair = nb + (c * sub + i) // 2
            dd[i * rpd:(i + 1) * rpd, c * CB:(c + 1) * CB] = fin[pair, i % 2]
    for g in range(nc):
        do[:, g * CB:(g + 1) * CB] = fin[place["o", g]]
        for name, ref in (("q", dq), ("k", dk), ("v", dv)):
            val = fin[place[name, g]]
            for h in range(CB // head_dim):
                ref[g * (CB // head_dim) + h] = val[:, h * head_dim:(h + 1) * head_dim]
    keeps = [pltpu.make_async_copy(s, d, sem.at[i]) for i, (s, d) in enumerate(zip(stage, outs))]
    for c in keeps:
        c.start()
    for get, out in zip(gets, puts):
        get.wait()
        out.start()
    for c in keeps + puts:
        c.wait()


def run_bwd(n, head_dim, ga, gm, x, dout, q, kt, k, v, ha, ot, xm, hm, hmt, qr, lse, cos_t, sin_t, wq, wk, wv, wo, wg, wu, wd, rows):
    total, width = x.shape
    hd, ff = wq.shape[0], wg.shape[1]
    toks = total // rows
    rpd, heads = width // n, hd // head_dim
    nb, nc, sub = ff // CB, width // CB, ff // width
    slots = plan(nb, nc * sub // 2, nc)[2] + 2
    n_pairs = hd // (2 * head_dim)
    f = lambda *s: jax.ShapeDtypeStruct(s, F32)
    dx_t = jax.ShapeDtypeStruct((total, width), BF)
    vm = lambda *s: pltpu.VMEM(s, BF)
    vf = lambda *s: pltpu.VMEM(s, F32)
    dma = lambda *s: pltpu.SemaphoreType.DMA(s)
    line, duo = vf(rows * n_pairs, 8, 2 * QB), (2, SLOTS)
    scratch = [vf(RING, 2, n // 2, 2, rpd, CB), vf(SLOTS, 2, n // 2, rpd, CB), vf(*duo, 2, 2, rpd, CB), vf(*duo, 2, 4, rpd, CB),
               vf(*duo, 2, rpd, CB // 2), vf(*duo, 2, rpd, CB), vf(*duo, 3, rpd, CB), vf(*duo, 4, 4, rpd, CB), vf(*duo, 4, rpd, CB), vf(slots, 2, rpd, CB),
               dma(6, *duo), dma(6, *duo),
               vm(hd, rows * WINDOW), line, line, dma(2), dma(2), dma(n_pairs), dma(n_pairs),
               vf(n, 8, 128), vf(n - 1, 8, 128), dma(2), dma(15),
               vm(total, width), vm(total, width), vf(total, width), vm(total, width), vm(hd, total), vm(width, total), vm(hd, width), vm(hd, total), line, line, vf(*cos_t.shape), vf(*cos_t.shape), vf(*ga.shape), vf(*ga.shape), vf(16, width)]
    mid = pl.pallas_call(
        functools.partial(bwd_kernel, n, head_dim, (rows, toks, width, hd, ff)), out_shape=[dx_t, f(slots, 2, rpd, CB)],
        in_specs=any_spec(24), out_specs=any_spec(2), scratch_shapes=scratch,
        compiler_params=pltpu.CompilerParams(collective_id=1, has_side_effects=True, vmem_limit_bytes=VMEM_LIMIT),
        name="backward")(ga, gm, x, dout, q, kt, k, v, ha, ot, xm, hm, hmt, qr, lse, cos_t, sin_t, wq, wk, wv, wo, wg, wu, wd)
    outs = [f(heads, rpd, head_dim)] * 3 + [f(rpd, width), f(rpd, ff), f(rpd, ff), f(ff // n, width)]
    return pl.pallas_call(
        functools.partial(spread_kernel, (head_dim, n, width, ff)), out_shape=[dx_t, f(1, rpd), f(1, rpd)] + outs,
        in_specs=any_spec(2), out_specs=any_spec(1) + vmem_spec(2) + any_spec(7),
        scratch_shapes=[vm(total, width), vf(slots, 2, rpd, CB), *[vf(*o.shape) for o in outs], dma(8 + 2 * nc)],
        name="spread")(*mid)


def solution(mesh):
    n = mesh.shape["seq"]

    def device_step(hidden, positions, g_attn, g_mlp, w_query, w_key, w_value, w_out, w_gate, w_up, w_down, d_out):
        rows, toks, width = hidden.shape
        layers, _, heads, head_dim = w_query.shape
        hd = heads * head_dim
        half = head_dim // 2
        inv_freq = 1.0 / (np.float32(10000.0) ** (np.arange(half, dtype=np.float32) * np.float32(2.0 / head_dim)))
        turn = lambda w: w[0].transpose(1, 2, 0).reshape(hd, width)
        wq, wk, wv = turn(w_query), turn(w_key), turn(w_value)
        fwd = run_fwd(n, hidden, positions, jnp.asarray(inv_freq.astype(np.float32)[:, None]), g_attn, g_mlp, wq, wk, wv, w_out[0], head_dim)
        out = run_bwd(n, head_dim, g_attn, g_mlp, hidden.reshape(rows * toks, width), d_out.reshape(rows * toks, width), *fwd,
                      wq, wk, wv, w_out[0], w_gate[0], w_up[0], w_down[0], rows)
        dx, dga, dgm, dq, dk, dv, do, dg, du, dd = out
        back = lambda w: w.transpose(1, 0, 2)[None]
        return (dx.reshape(rows, toks, width), dga, dgm, back(dq), back(dk), back(dv), do[None], dg[None], du[None], dd[None])

    tok_spec, grad_spec = P("data", "seq"), P(None, ("data", "seq"))
    in_specs = (tok_spec, tok_spec) + (P(),) * 9 + (tok_spec,)
    out_specs = (tok_spec,) + (grad_spec,) * 9
    return jax.shard_map(device_step, mesh=mesh, in_specs=in_specs, out_specs=out_specs, check_vma=False)
```

```python
import functools, math
import numpy as np
import jax, jax.numpy as jnp
from jax import lax
from jax.experimental import pallas as pl
from jax.experimental.pallas import tpu as pltpu
from jax.sharding import PartitionSpec as P

WINDOW = 256
NORM_EPS = 1e-5
QB = 128
BF, F32 = jnp.bfloat16, jnp.float32
NN, NT, TN = ((1,), (0,)), ((1,), (1,)), ((0,), (0,))
MESH = pl.DeviceIdType.MESH
NEG = -1e30
VMEM_LIMIT = 67043328


def dot(a, b, dims=NN):
    return lax.dot_general(a, b, (dims, ((), ())), preferred_element_type=F32)


def cdiv_loop(n, body):
    lax.fori_loop(0, n, lambda i, c: body(i) or c, 0)


def mod(a, b):
    return a % b if isinstance(a, int) else lax.rem(a, b)


def aligned(a, b):
    return a if isinstance(a, int) else pl.multiple_of(a, b)


def rope(blk, cos_b, sin_b, sign, head_dim):
    half = head_dim // 2
    parts = []
    for h in range(blk.shape[0] // head_dim):
        first = blk[h * head_dim:h * head_dim + half]
        second = blk[h * head_dim + half:(h + 1) * head_dim]
        if sign > 0:
            parts += [first * cos_b - second * sin_b, second * cos_b + first * sin_b]
        else:
            parts += [first * cos_b + second * sin_b, second * cos_b - first * sin_b]
    return jnp.concatenate(parts, axis=0)


def normed(x, gain):
    xf = x.astype(F32)
    inv = lax.rsqrt(jnp.mean(xf * xf, axis=-1, keepdims=True) + NORM_EPS)
    return (xf * inv * gain).astype(BF)


def stack_pair(pair_t):
    half = pair_t.shape[0] // 2
    zero = jnp.zeros((half, pair_t.shape[1]), pair_t.dtype)
    return jnp.concatenate(
        [jnp.concatenate([pair_t[:half], zero], axis=0), jnp.concatenate([zero, pair_t[half:]], axis=0)], axis=1)


def unstack_pair(both):
    half, cols = both.shape[0] // 2, both.shape[1] // 2
    return jnp.concatenate([both[:half, :cols], both[half:, cols:]], axis=0)


def col_sum(x):
    return jnp.sum(x, axis=0, keepdims=True)


def merged(scores, upper, bias0, bias1):
    return jnp.where(upper, scores[:QB] + bias0, scores[2 * QB:]), scores[QB:2 * QB] + bias1


def banded(p02, p1, upper):
    return jnp.concatenate(
        [jnp.where(upper, p02, 0.0).astype(BF), p1.astype(BF), jnp.where(upper, 0.0, p02).astype(BF)], axis=0)


def upper_mask():
    key_ids = lax.broadcasted_iota(jnp.int32, (QB, 2 * QB), 0)
    query_ids = lax.broadcasted_iota(jnp.int32, (QB, 2 * QB), 1) % QB
    return key_ids > query_ids


def start_bias(first, blk):
    bias = jnp.where(first, NEG, 0.0).astype(F32)
    return (bias if blk < 2 else 0.0), (bias if blk < 1 else 0.0)


def fwd_kernel(n, head_dim, x_h, pos_h, invf_h, ga_h, gm_h, wq_h, wk_h, wv_h, wo_h,
               q_h, kt_h, k_h, v_h, ha_h, ot_h, xm_h, hm_h, hmt_h, qr_h, lse_h, cos_t, sin_t,
               pos, invf, ga, gm, xv, halo, qr, lse, pos_halo, wq, wk, wv, wo, q, kt, k, v, vt, ot, xm, hm, hmt, hb, hh, acc, acc2, ak, av, cos_h, sin_h,
               sc0, sc1, sc2, pb0, pb1, pb2, ldx, ld, st, snd, rcv, qsnd, qrcv):
    sc, pb = (sc0, sc1, sc2), (pb0, pb1, pb2)
    rows, toks, width = xv.shape
    ext, total, pw = toks + WINDOW, rows * toks, 2 * head_dim
    n_pairs = wq.shape[0] // pw
    tb, n_steps = toks // QB, n_pairs * rows
    me = lax.axis_index("seq")
    right, left = lax.rem(me + 1, n), lax.rem(me + n - 1, n)
    load_x = [pltpu.make_async_copy(x_h.at[b], xv.at[b], ldx.at[b]) for b in range(rows)]
    load_w = [pltpu.make_async_copy(s, d, ld.at[i]) for i, (s, d) in enumerate(((wq_h, wq), (wk_h, wk), (wv_h, wv), (wo_h, wo)))]
    load_s = [pltpu.make_async_copy(s, d, ldx.at[rows + i]) for i, (s, d) in enumerate(((pos_h, pos), (invf_h, invf), (ga_h, ga), (gm_h, gm)))]
    for c in load_s + load_x:
        c.start()
    barrier = pltpu.get_barrier_semaphore()
    for other in (left, right):
        pl.semaphore_signal(barrier, inc=1, device_id={"seq": other}, device_id_type=MESH)

    def push(i, s, d):
        return pltpu.make_async_remote_copy(src_ref=s, dst_ref=d, send_sem=snd.at[i], recv_sem=rcv.at[i], device_id={"seq": right}, device_id_type=MESH)

    def push_rows(b):
        return push(b, x_h.at[b, toks - WINDOW:, :], halo.at[b])

    send_pos = push(rows, pos, pos_halo)

    def angles(cos_ref, sin_ref, positions):
        count = positions.shape[1]
        for b in range(rows):
            ang = invf[:] * positions[b:b + 1, :].astype(F32)
            cos_ref[:, b * count:(b + 1) * count] = jnp.cos(ang)
            sin_ref[:, b * count:(b + 1) * count] = jnp.sin(ang)

    for c in load_s:
        c.wait()
    angles(cos_t, sin_t, pos[:])

    def norm_rows(b):
        for i in range(tb):
            h = normed(xv[b, i * QB:(i + 1) * QB, :], ga[:])
            hb[pl.ds(pl.multiple_of((b * tb + i) * QB, QB), QB), :] = h

    with jax.named_scope("f_norm"):
        for c in load_x:
            c.wait()
        for c in load_w:
            c.start()
        cdiv_loop(rows, norm_rows)
    pl.semaphore_wait(barrier, 2)
    send_pos.start()
    for b in range(rows):
        push_rows(b).start()
    keep_ha = pltpu.make_async_copy(hb, ha_h, st.at[0])
    keep_ha.start()
    tables = cos_t[:], sin_t[:]

    def put_q(src):
        for p in range(n_pairs):
            r = slice(p * pw, (p + 1) * pw)
            q[r, :] = (rope(src[r, :], *tables, 1, head_dim) * (head_dim ** -0.5)).astype(BF)

    def put_own(src, dst_t, dst):
        for p in range(n_pairs):
            r = slice(p * pw, (p + 1) * pw)
            both = (rope(src[r, :], *tables, 1, head_dim) if dst is k else src[r, :]).astype(BF)
            for b in range(rows):
                blk = both[:, b * toks:(b + 1) * toks]
                own = slice(b * ext + WINDOW, (b + 1) * ext)
                dst_t[r, own] = blk
                dst[own, r] = blk.T

    with jax.named_scope("f_mm"):
        load_w[0].wait()
        load_w[1].wait()
        load_w[2].wait()
        acc[:] = dot(wq[:], hb[:], NT)
        acc2[:] = dot(wk[:], hb[:], NT)
        put_q(acc)
        send_pos.wait()
        acc[:] = dot(wv[:], hb[:], NT)
        angles(cos_h, sin_h, pos_halo[:, toks - WINDOW:])
        put_own(acc2, kt, k)
        put_own(acc, vt, v)
    keep_q = pltpu.make_async_copy(q, q_h, st.at[1])
    keep_q.start()

    def push_q(b):
        return pltpu.make_async_remote_copy(src_ref=q.at[:, b * toks:b * toks + WINDOW], dst_ref=qr.at[:, b * WINDOW:(b + 1) * WINDOW],
                                            send_sem=qsnd.at[b], recv_sem=qrcv.at[b], device_id={"seq": left}, device_id_type=MESH)

    for b in range(rows):
        push_q(b).start()

    def keeps(b):
        wide, cols = pl.ds(pl.multiple_of(b * ext, QB), ext), pl.ds(pl.multiple_of(b * toks, QB), toks)
        ends = ((kt.at[:, wide], kt_h.at[:, wide]), (k.at[wide, :], k_h.at[wide, :]), (v.at[wide, :], v_h.at[wide, :]),
                (ot.at[:, cols], ot_h.at[:, cols]), (hm.at[cols, :], hm_h.at[cols, :]), (hmt.at[:, cols], hmt_h.at[:, cols]),
                (xm.at[cols, :], xm_h.at[cols, :]))
        return [pltpu.make_async_copy(s, d, st.at[2 + b * len(ends) + i]) for i, (s, d) in enumerate(ends)]

    def halo_in(b):
        with jax.named_scope("f_halo_wait"):
            push_rows(b).wait()
        with jax.named_scope("f_halo"):
            for i in range(WINDOW // QB):
                r = slice(i * QB, (i + 1) * QB)
                hh[r, :] = normed(halo[b, r, :], ga[:])
            ak[:] = dot(wk[:], hh[:], NT)
            av[:] = dot(wv[:], hh[:], NT)
            cols = pl.ds(pl.multiple_of(b * WINDOW, QB), WINDOW)
            wide = pl.ds(pl.multiple_of(b * ext, QB), WINDOW)
            near = cos_h[:, cols], sin_h[:, cols]
            for src, dst_t, dst in ((ak, kt, k), (av, vt, v)):
                for p in range(n_pairs):
                    r = slice(p * pw, (p + 1) * pw)
                    blk = (rope(src[r, :], *near, 1, head_dim) if dst is k else src[r, :]).astype(BF)
                    dst_t[r, wide] = blk
                    dst[wide, r] = blk.T
        for c in keeps(b)[:3]:
            c.start()

    upper = upper_mask()
    first = me == 0

    def spots(it, blk):
        b, p = it // n_pairs, mod(it, n_pairs)
        pr = pl.ds(aligned(p * pw, pw), pw)
        return pr, pl.ds(aligned(b * toks + blk * QB, QB), QB), pl.ds(aligned(b * ext + blk * QB, QB), 3 * QB)

    def score(it):
        for blk in range(tb):
            pr, cols, keys = spots(it, blk)
            sc[blk][:] = dot(k[keys, pr], stack_pair(q[pr, cols]))

    def soften(it, blk):
        s02, s1 = merged(sc[blk][:], upper, *start_bias(first, blk))
        top = jnp.max(jnp.maximum(s02, s1), axis=0, keepdims=True)
        e02, e1 = jnp.exp(s02 - top), jnp.exp(s1 - top)
        mass = col_sum(e02 + e1)
        inv = 1.0 / mass
        lse[it, blk:blk + 1, :] = top + jnp.log(mass)
        pb[blk][:] = banded(e02 * inv, e1 * inv, upper)

    def mix(it):
        for blk in range(tb):
            pr, cols, keys = spots(it, blk)
            ot[pr, cols] = unstack_pair(dot(vt[pr, keys], pb[blk][:])).astype(BF)

    def project(b):
        cols = pl.ds(pl.multiple_of(b * toks, QB), toks)
        with jax.named_scope("f_proj"):
            mid = (xv[b].astype(F32) + dot(ot[:, cols], wo[:], TN)).astype(BF)
            xm[cols, :] = mid
            h = normed(mid, gm[:])
            hm[cols, :] = h
            hmt[:, cols] = h.T
        for c in keeps(b)[3:]:
            c.start()

    keep_qr, keep_lse = (pltpu.make_async_copy(*ends, ld.at[i]) for i, ends in enumerate(((qr, qr_h), (lse, lse_h))))
    load_w[3].wait()
    for blk in range(tb):
        pb[blk][:] = jnp.zeros(pb[blk].shape, BF)

    def walk(i):
        it = i - 1

        @pl.when((lax.rem(i, n_pairs) == 0) & (i < n_steps))
        def _():
            halo_in(i // n_pairs)

        @pl.when(i == 0)
        def _():
            score(0)

        @pl.when((i > 0) & (i <= n_steps))
        def _():
            with jax.named_scope("f_attn"):
                mix(jnp.maximum(it - 1, 0))
                for blk in range(tb):
                    soften(it, blk)
                score(jnp.minimum(i, n_steps - 1))

        @pl.when(i == n_steps)
        def _():
            for b in range(rows):
                push_q(b).wait()
            keep_qr.start()

        @pl.when(i > n_steps)
        def _():
            mix(n_steps - 1)

        @pl.when((lax.rem(it, n_pairs) == 0) & (it > 0))
        def _():
            project(it // n_pairs - 1)

    cdiv_loop(n_steps + 2, walk)
    with jax.named_scope("f_store_wait"):
        keep_lse.start()
        keep_ha.wait()
        keep_q.wait()
        keep_qr.wait()
        keep_lse.wait()
        for b in range(rows):
            for c in keeps(b):
                c.wait()


def any_spec(k):
    return [pl.BlockSpec(memory_space=pl.ANY)] * k


def vmem_spec(k):
    return [pl.BlockSpec(memory_space=pltpu.VMEM)] * k


def run_fwd(n, x, pos, invf, ga, gm, wq, wk, wv, wo, head_dim):
    rows, toks, width = x.shape
    hd = wq.shape[0]
    ext, total, n_halo = toks + WINDOW, rows * toks, rows * WINDOW
    half = head_dim // 2
    sds = lambda *s: jax.ShapeDtypeStruct(s, BF)
    dma = lambda *s: pltpu.SemaphoreType.DMA(s)
    outs = [sds(hd, total), sds(hd, rows * ext), sds(rows * ext, hd), sds(rows * ext, hd), sds(total, width), sds(hd, total), sds(total, width), sds(total, width), sds(width, total)]
    outs += [sds(hd, n_halo), jax.ShapeDtypeStruct((rows * hd // (2 * head_dim), 8, 2 * QB), F32)] + [jax.ShapeDtypeStruct((half, total), F32)] * 2
    vm = lambda *s: pltpu.VMEM(s, BF)
    vf = lambda *s: pltpu.VMEM(s, F32)
    scratch = [pltpu.VMEM((rows, toks), jnp.int32), vf(*invf.shape), vf(*ga.shape), vf(*ga.shape), vm(rows, toks, width), vm(rows, WINDOW, width), vm(hd, n_halo), vf(rows * hd // (2 * head_dim), 8, 2 * QB), pltpu.VMEM((rows, toks), jnp.int32), vm(hd, width), vm(hd, width), vm(hd, width), vm(hd, width),
               vm(hd, total), vm(hd, rows * ext), vm(rows * ext, hd), vm(rows * ext, hd), vm(hd, rows * ext), vm(hd, total), vm(total, width), vm(total, width), vm(width, total), vm(total, width), vm(WINDOW, width),
               vf(hd, total), vf(hd, total), vf(hd, WINDOW), vf(hd, WINDOW), vf(half, n_halo), vf(half, n_halo),
               *[f(3 * QB, 2 * QB) for f in (vf, vm) for _ in range(3)],
               dma(rows + 4), dma(4), dma(2 + 7 * rows), dma(rows + 1), dma(rows + 1), dma(rows), dma(rows)]
    return pl.pallas_call(
        functools.partial(fwd_kernel, n, head_dim), out_shape=outs,
        in_specs=any_spec(9), out_specs=any_spec(11) + vmem_spec(2), scratch_shapes=scratch,
        compiler_params=pltpu.CompilerParams(collective_id=0, has_side_effects=True, vmem_limit_bytes=VMEM_LIMIT),
        name="forward")(x, pos, invf, ga, gm, wq, wk, wv, wo)


LAG = 2
SLOTS = 2 * LAG
RING = 8
CB = 256


def at(ref, *idx):
    return ref.at[idx]


class Torus:
    def __init__(self, n, head, last, turn, parts, recv0, recv1, recv2, recv3, recv4, recv5, acc, acc2, fin, snd, rcv):
        assert math.isqrt(n // 2) == 4
        me = lax.axis_index("seq")
        self.core = lax.rem(me, 2)
        chip = me // 2
        self.x, self.y = lax.rem(chip, 4), chip // 4
        self.head, self.last, self.turn = head, last, turn
        self.parts, self.recv0, self.recv1, self.recv2, self.recv3, self.recv4, self.recv5 = parts, recv0, recv1, recv2, recv3, recv4, recv5
        self.acc, self.acc2, self.fin, self.snd, self.rcv = acc, acc2, fin, snd, rcv
        self.partner = me + 1 - 2 * self.core
        self.rows, self.columns = [lax.rem(self.y + d, 4) * 4 for d in range(4)], [lax.rem(self.x + d, 4) for d in range(4)]
        self.hops = [[self.device(0, d) for d in range(4)], [self.device(d, 0) for d in range(4)]]

    def device(self, dy, dx):
        return (self.rows[dy] + self.columns[dx]) * 2 + self.core

    def copy(self, lane, kind, slot, src, dst, target):
        return pltpu.make_async_remote_copy(
            src_ref=src, dst_ref=dst, send_sem=self.snd.at[lane, kind, slot], recv_sem=self.rcv.at[lane, kind, slot],
            device_id={"seq": target}, device_id_type=MESH)

    def late(self, axis, pair, yes, no):
        first, end = self.turn
        busy = (pair >= first) & (pair < end)
        return jnp.where(busy & (self.x == 3) if axis else busy, yes, no)

    def swap(self, ring, slot):
        return self.copy(0, 0, slot, self.parts.at[ring, :, :, 1 - self.core], self.recv0.at[slot], self.partner)

    def landing(self, stage):
        return (self.recv0, self.recv1, self.recv2, self.recv3, self.recv4, self.recv5)[stage]

    def arrived(self, stage, kind, slot):
        whole = self.landing(stage).at[kind, slot]
        self.copy(stage, kind, slot, whole, whole, self.partner).wait()

    def send(self, stage, kind, pair, held, slot):
        axis = kind if stage < 3 else 1 - kind
        plus, minus = self.hops[axis][1], self.hops[axis][-1]
        half = CB // 2
        if stage == 1:
            minus = self.late(axis, pair, plus, minus)
            ends = self.acc.at[kind, held, 2, :2], self.acc.at[kind, held, 2, 2:]
        elif stage == 2:
            ends = self.acc.at[kind, held, 1], self.acc.at[kind, held, 3]
        elif stage == 3:
            ends = self.acc2.at[kind, held, 2, :, :half], self.acc2.at[kind, held, 2, :, half:]
        else:
            ends = self.acc2.at[kind, held, 1], self.acc2.at[kind, held, 3]
        for i, src in enumerate(ends):
            self.copy(stage, kind, slot, src, self.landing(stage).at[kind, slot, i], (plus, minus)[i]).start()

    def add(self, stage, kind, pair, held, slot, ring):
        acc, acc2 = self.acc, self.acc2
        if stage == 1:
            for r1 in range(4):
                for r2 in range(4):
                    ry, rx = (r2, r1) if kind == 0 else (r1, r2)
                    chip = self.rows[ry] + self.columns[rx]
                    acc[kind, held, r1, r2] = self.parts[ring, kind, chip, self.core] + self.recv0[slot, kind, chip]
        elif stage == 2:
            back = self.late(kind, pair, 1, 3)
            acc[kind, held, 1, :2] += self.recv1[kind, slot, 0]
            acc[kind, held, back, 2:] += self.recv1[kind, slot, 1]
        elif stage == 3:
            acc2[kind, held] = acc[kind, held, 0] + (self.recv2[kind, slot, 0] + self.recv2[kind, slot, 1])
        elif stage == 4:
            half = CB // 2
            acc2[kind, held, 1, :, :half] += self.recv3[kind, slot, 0]
            acc2[kind, held, 3, :, half:] += self.recv3[kind, slot, 1]
        else:
            self.fin[pair, kind] = acc2[kind, held, 0] + (self.recv4[kind, slot, 0] + self.recv4[kind, slot, 1])

    def direct(self, kind, held, slot):
        for d in range(1, 4):
            self.copy(5, kind, slot, self.acc2.at[kind, held, d], self.recv5.at[kind, slot, d - 1], self.hops[1 - kind][d]).start()

    def early(self, pair):
        return (pair >= 0) & (pair <= self.head)

    def final(self, pair):
        return (pair == self.last) | ((pair > self.head) & (pair < self.last) & (mod(abs(pair - self.head), 2) == 0))

    def when(self, which, fn):
        if isinstance(which, bool):
            fn() if which else None
        else:
            pl.when(which)(fn)

    def offer(self, t):
        self.when(self.early(t) | self.final(t), lambda: self.swap(mod(t, RING), mod(t, SLOTS)).start())

    def tick(self, t):
        self.offer(t)
        self.advance(t)

    def advance(self, t, tail=False):
        now, land, before = mod(t, SLOTS), mod(t + SLOTS - LAG, SLOTS), mod(t + SLOTS - 1, SLOTS)
        ring_land = mod(t + RING - 1, RING)
        for stage in range(5, 0, -1):
            pair = t - LAG * stage + 1
            held = before if stage % 2 else mod(t + 1, SLOTS)

            def move(last_hops, stage=stage, pair=pair, held=held):
                if stage == 1:
                    with jax.named_scope("t_wait1"):
                        self.swap(ring_land, before).wait()
                for kind in range(2):
                    if last_hops and stage == 4:
                        with jax.named_scope("t_wait6"):
                            self.arrived(5, kind, land)
                        got = self.recv5[kind, land]
                        self.fin[pair, kind] = self.acc2[kind, held, 0] + (got[0] + got[1] + got[2])
                        continue
                    if stage > 1:
                        with jax.named_scope(f"t_wait{stage}"):
                            self.arrived(stage - 1, kind, land)
                    self.add(stage, kind, pair, held, land if stage > 1 else before, ring_land)
                    if last_hops and stage == 3:
                        self.direct(kind, held, now)
                    elif stage < 5:
                        self.send(stage, kind, pair, held, now)

            if stage < 3:
                self.when(self.early(pair) | self.final(pair), functools.partial(move, False))
            else:
                self.when(self.early(pair), functools.partial(move, False))
                if tail and stage < 5:
                    self.when(self.final(pair), functools.partial(move, True))


def pick(i, table):
    out = 0
    for key, value in table.items():
        out = jnp.where(i == key, value, out)
    return out


def norm_back(x, gain, grad, res):
    xf = x.astype(F32)
    inv = lax.rsqrt(jnp.mean(xf * xf, axis=-1, keepdims=True) + NORM_EPS)
    unit = xf * inv
    gu = grad * gain
    out = inv * (gu - unit * jnp.mean(gu * unit, axis=-1, keepdims=True)) + res.astype(F32)
    gu = grad * unit
    return out.astype(BF), jnp.sum(gu.reshape(-1, 8, gu.shape[-1]), axis=0)


def plan(n_mlp, n_down, nc):
    order = [("o", g) for g in range(nc)] + [(name, g) for g in range(nc) for name in "qkv"]
    base, head = n_mlp + n_down, n_mlp + n_down + nc - 1
    last = 2 * (base - 1 - head + len(order) // 2) + head - 1
    spot = lambda pair: min(max(pair, 2 * pair - head), last)
    return head, {name: (spot(base + i // 2), i % 2) for i, name in enumerate(order)}, last


def bwd_kernel(n, head_dim, dims, ga_h, gm_h, x_h, dout_h, q_h, kt_h, k_h, v_h, ha_h, ot_h, xm_h, hm_h, hmt_h, qr_h, lse_h, cos_h, sin_h,
               wq_h, wk_h, wv_h, wo_h, wg_h, wu_h, wd_h,
               dx_h, fin_h,
               parts, recv0, recv1, recv2, recv3, recv4, recv5, acc, acc2, fin, snd, rcv,
               dor, lser, deltar, hsnd, hrcv, osnd, orcv, gsend, grecv, gsem, ld,
               xbuf, mbuf, gnm, gmid, ot, hat, wo, dot_, lse, delta, cos_i, sin_i, ga, gm, dgain):
    rows, toks, width, hd, ff = dims
    ext, total = toks + WINDOW, rows * toks
    pw = 2 * head_dim
    n_pairs = hd // pw
    tb, n_steps = toks // QB, n_pairs * rows
    nb, nc, sub = ff // CB, width // CB, ff // width
    rpd = width // n
    per, half_sub = CB // pw, sub // 2
    head, place, end = plan(nb, nc * half_sub, nc)
    comm = Torus(n, head, end, (nb, nb + n_pairs + 1), parts, recv0, recv1, recv2, recv3, recv4, recv5, acc, acc2, fin, snd, rcv)
    me = lax.axis_index("seq")
    left = lax.rem(me + n - 1, n)
    barrier = pltpu.get_barrier_semaphore()

    def greet(i):
        pl.semaphore_signal(barrier, inc=1, device_id={"seq": lax.rem(me + i + 1, n)}, device_id_type=MESH)

    def load(i, s, d):
        c = pltpu.make_async_copy(s, d, ld.at[i])
        c.start()
        return c

    def late(i):
        s, d = ((xm_h, mbuf), (ot_h, ot), (wo_h, wo), (lse_h, lse), (cos_h, cos_i), (sin_h, sin_i), (ga_h, ga), (gm_h, gm))[i]
        return pltpu.make_async_copy(s, d, ld.at[1 + i])

    def to_left(src, dst, send_sem, recv_sem):
        return pltpu.make_async_remote_copy(src_ref=src, dst_ref=dst, send_sem=send_sem, recv_sem=recv_sem,
                                            device_id={"seq": left}, device_id_type=MESH)

    n_late = 8

    def push_rows(i):
        return to_left(*((lse_h, lser), (delta, deltar))[i], hsnd.at[i], hrcv.at[i])

    def push_out(p):
        pr = pl.ds(aligned(p * pw, pw), pw)
        return [to_left(dot_.at[pr, pl.ds(b * toks, WINDOW)], dor.at[pr, pl.ds(b * WINDOW, WINDOW)], osnd.at[p], orcv.at[p])
                for b in range(rows)]

    def give_out(p):
        for c in push_out(p):
            c.start()

    def put(spot, value):
        pair, kind = spot
        parts[mod(pair, RING), kind] = value.reshape(n // 2, 2, rpd, CB)

    def spot_of(name, g):
        known = {i: place[name, i] for i in range(nc)}
        return pick(g, {i: s[0] for i, s in known.items()}), pick(g, {i: s[1] for i, s in known.items()})

    def spots(it, blk):
        p, b = it // rows, mod(it, rows)
        pr = pl.ds(aligned(p * pw, pw), pw)
        return pr, pl.ds(aligned(b * toks + blk * QB, QB), QB), pl.ds(aligned(b * ext + blk * QB, QB), 3 * QB)

    def row_of(it):
        return mod(it, rows) * n_pairs + it // rows

    def mlp(hm, hmt, ha, actt, wgu, wd, dgu, wld):
        def weights(j, slot):
            c = aligned(j * CB, CB)
            return [pltpu.make_async_copy(wg_h.at[:, pl.ds(c, CB)], wgu.at[slot, :, :CB], wld.at[slot, 0]),
                    pltpu.make_async_copy(wu_h.at[:, pl.ds(c, CB)], wgu.at[slot, :, CB:], wld.at[slot, 1]),
                    pltpu.make_async_copy(wd_h.at[pl.ds(c, CB), :], wd.at[slot], wld.at[slot, 2])]

        for c in weights(0, 0):
            c.start()
        ld_hm, ld_x, ld_hmt = load(10, hm_h, hm), load(0, dout_h, xbuf), load(11, hmt_h, hmt)
        cdiv_loop(n - 1, greet)
        gnm[:] = jnp.zeros_like(gnm)
        gsend[:] = jnp.zeros_like(gsend)
        dgain[:] = jnp.zeros_like(dgain)
        ld_hm.wait()
        ld_x.wait()
        ld_hmt.wait()
        for i in range(n_late):
            late(i).start()
        ld_ha = load(10, ha_h, ha)

        def block(j):
            slot = lax.rem(j, 2)
            for c in weights(j, slot):
                c.wait()

            @pl.when(j + 1 < nb)
            def _():
                for c in weights(j + 1, 1 - slot):
                    c.start()

            c0 = pl.multiple_of(j * CB, CB)
            with jax.named_scope("b_mlp"):
                for b in range(rows):
                    r = slice(b * toks, (b + 1) * toks)
                    gu = dot(hm[r, :], wgu[slot])
                    gact = dot(xbuf[r, :], wd[slot], NT).astype(BF).astype(F32)
                    gate, up = gu[:, :CB], gu[:, CB:]
                    sig = 1.0 / (1.0 + jnp.exp(-gate))
                    swish = gate * sig
                    actt[pl.ds(c0, CB), r] = (swish * up).astype(BF).T
                    dgu[r, :CB] = (gact * up * (sig + swish * (1.0 - sig))).astype(BF)
                    dgu[r, CB:] = (gact * swish).astype(BF)
                both = dot(hmt[:], dgu[:])
                ring = lax.rem(j, RING)
                parts[ring, 0] = both[:, :CB].reshape(n // 2, 2, rpd, CB)
                parts[ring, 1] = both[:, CB:].reshape(n // 2, 2, rpd, CB)
                for b in range(rows):
                    r = slice(b * toks, (b + 1) * toks)
                    gnm[r, :] += dot(dgu[r, :], wgu[slot], NT)

            @pl.when(j == 0)
            def _():
                pl.semaphore_wait(barrier, n - 1)
                push_rows(0).start()

            comm.tick(j)

        cdiv_loop(nb, block)

        def down(c):
            share = n // 2 // sub
            c0 = pl.multiple_of(c * CB, CB)
            for m in range(sub):
                res = dot(actt[m * width:(m + 1) * width, :], xbuf[:, pl.ds(c0, CB)]).reshape(share, 2, sub, rpd, CB)
                for i in range(sub):
                    pair = nb + c * half_sub + i // 2
                    parts[lax.rem(pair, RING), i % 2, m * share:(m + 1) * share] = res[:, :, i]
            for i in range(tb * rows // nc):
                r = pl.ds(pl.multiple_of((c * (tb * rows // nc) + i) * QB, QB), QB)
                hat[:, r] = ha[r, :].T

        for i in range(n_late):
            late(i).wait()
        ld_ha.wait()

        def mid(b):
            for i in range(tb):
                r = pl.ds(pl.multiple_of((b * tb + i) * QB, QB), QB)
                out, dg = norm_back(mbuf[r, :], gm[:], gnm[r, :], xbuf[r, :])
                gmid[r, :] = out
                dgain[8:, :] += dg

        def deltas(p):
            for it in range(rows):
                for blk in range(tb):
                    pr, cols, _ = spots(p * rows + it, blk)
                    both = dot_[pr, cols].astype(F32) * ot[pr, cols].astype(F32)
                    delta[row_of(p * rows + it), blk:blk + 1, :] = jnp.concatenate(
                        [col_sum(both[:head_dim]), col_sum(both[head_dim:])], axis=1)

        def column(c):
            with jax.named_scope("b_down"):
                down(c)

            @pl.when(c < nc - 1)
            def _():
                comm.tick(nb + c + jnp.minimum(c, 1))

            @pl.when(c > 0)
            def _():
                give_out(c)

            @pl.when(c == 0)
            def _():
                with jax.named_scope("b_mid"):
                    cdiv_loop(rows, mid)
                with jax.named_scope("b_dot"):
                    dot_[:] = dot(wo[:], gmid[:], NT).astype(BF)
                    cdiv_loop(n_pairs, deltas)
                comm.tick(nb + 1)
                push_rows(1).start()
                give_out(0)

        cdiv_loop(nc, column)

    vm = lambda *s: pltpu.VMEM(s, BF)
    vf = lambda *s: pltpu.VMEM(s, F32)
    pl.run_scoped(mlp, vm(total, width), vm(width, total), vm(total, width), vm(ff, total), vm(2, width, 2 * CB), vm(2, CB, width), vm(total, 2 * CB),
                  pltpu.SemaphoreType.DMA((2, 3)))
    def attention(q, kt, k, v, qr, dv, sc0, sc1, sc2, sr, dp0, dp1, dp2, dr, pb0, pb1, pb2, pr_, ds0, ds1, ds2, dsr):
        dqt, dkt = ot, q
        wq, wk, wv = k.at[:hd], kt.at[:, :width], v.at[:hd]
        sc, dp, pb, ds = (sc0, sc1, sc2), (dp0, dp1, dp2), (pb0, pb1, pb2), (ds0, ds1, ds2)
        lds = [load(10 + i, s, d) for i, (s, d) in enumerate(((q_h, q), (k_h, k), (v_h, v), (qr_h, qr), (kt_h, kt)))]

        def out_grad(g):
            put(spot_of("o", g), dot(ot[:], gmid[:, pl.ds(pl.multiple_of(g * CB, CB), CB)]))

        with jax.named_scope("b_dwo"):
            cdiv_loop(nc, out_grad)
        first_tick = nb + nc + 1
        comm.tick(first_tick - 1)
        steps = [1, 4, 6, 8, 10, 13, 15, 17, 18]
        tick_after = {s: first_tick + i for i, s in enumerate(steps)}
        assert first_tick + len(steps) == end
        upper = upper_mask()
        first, last = me == 0, me == n - 1
        halves = slice(0, WINDOW), slice(WINDOW, 3 * QB)

        def right(it, i):
            p, b = it // rows, mod(it, rows)
            return pl.ds(aligned(p * pw, pw), pw), pl.ds(aligned(b * WINDOW + i * QB, QB), QB), pl.ds(aligned(b * ext + toks + i * QB, QB), WINDOW - i * QB)

        def score(it):
            for blk in range(tb):
                pr, cols, keys = spots(it, blk)
                sc[blk][:] = dot(k[keys, pr], stack_pair(q[pr, cols]))
                dp[blk][:] = dot(v[keys, pr], stack_pair(dot_[pr, cols]))
            for i, rs in enumerate(halves):
                pr, cols, keys = right(it, i)
                sr[rs, :] = dot(k[keys, pr], stack_pair(qr[pr, cols]))
                dr[rs, :] = dot(v[keys, pr], stack_pair(dor[pr, cols]))

        def soften(it):
            row = row_of(it)
            for blk in range(tb):
                s02, s1 = merged(sc[blk][:], upper, *start_bias(first, blk))
                norm, mean = lse[row, blk:blk + 1, :], delta[row, blk:blk + 1, :]
                p02, p1 = jnp.exp(s02 - norm), jnp.exp(s1 - norm)
                g02, g1 = jnp.where(upper, dp[blk][:QB], dp[blk][2 * QB:]), dp[blk][QB:2 * QB]
                pb[blk][:] = banded(p02, p1, upper)
                ds[blk][:] = banded(p02 * (g02 - mean), p1 * (g1 - mean), upper)
            for blk in range(tb):
                i = blk // 2
                rs = slice(blk * QB, (blk + 1) * QB)
                p = jnp.exp(sr[rs, :] - jnp.where(last, -NEG, lser[row, i:i + 1, :]))
                g = p * (dr[rs, :] - deltar[row, i:i + 1, :])
                pr_[rs, :] = (p if blk == 1 else jnp.where(upper, p, 0.0)).astype(BF)
                dsr[rs, :] = (g if blk == 1 else jnp.where(upper, g, 0.0)).astype(BF)

        def grads(it):
            ks, vs = [], []
            for blk in range(tb):
                pr, cols, keys = spots(it, blk)
                own = slice(max(0, 2 - blk) * QB, 3 * QB)
                vs.append(dot(pb[blk][own, :], stack_pair(dot_[pr, cols]), NT))
                ks.append(dot(ds[blk][own, :], stack_pair(q[pr, cols]), NT))
                dq = unstack_pair(dot(kt[pr, keys], ds[blk][:])) * (head_dim ** -0.5)
                dqt[pr, cols] = rope(dq, cos_i[:, cols], sin_i[:, cols], -1, head_dim).astype(BF)
            for i, rs in enumerate(halves):
                pr, cols, _ = right(it, i)
                vs.append(dot(pr_[rs, :], stack_pair(dor[pr, cols]), NT))
                ks.append(dot(dsr[rs, :], stack_pair(qr[pr, cols]), NT))
            for j in range(tb):
                pr, cols, _ = spots(it, j)
                gv, gk = (sum(x[i][(j - max(0, i - 2)) * QB:(j - max(0, i - 2) + 1) * QB] for i in range(j, j + 3)) for x in (vs, ks))
                dv[cols, pr] = gv.astype(BF)
                dkt[pr, cols] = rope(gk.T, cos_i[:, cols], sin_i[:, cols], -1, head_dim).astype(BF)

        def close_group(g):
            cols = pl.ds(pl.multiple_of(g * CB, CB), CB)
            with jax.named_scope("b_dwqkv"):
                put(spot_of("q", g), dot(hat[:], dqt[cols, :], NT))
                put(spot_of("k", g), dot(hat[:], dkt[cols, :], NT))
                put(spot_of("v", g), dot(hat[:], dv[:, cols]))

        def weights():
            return [pltpu.make_async_copy(s, d, ld.at[10 + i]) for i, (s, d) in enumerate(((wq_h, wq), (wk_h, wk), (wv_h, wv), (x_h, xbuf)))]

        def arrived(p):
            whole = dor.at[pl.ds(aligned(p * pw, pw), pw), :]
            with jax.named_scope("b_hwait"):
                to_left(whole, whole, osnd.at[p], orcv.at[p]).wait()

        def walk(it):
            ahead = it + 1

            @pl.when((lax.rem(ahead, rows) == 0) & (ahead < n_steps))
            def _():
                arrived(ahead // rows)

            @pl.when(it < n_steps)
            def _():
                with jax.named_scope("b_attn"):
                    grads(it - 1)
                    soften(it)
                    score(jnp.minimum(ahead, n_steps - 1))

            @pl.when(it == n_steps)
            def _():
                grads(n_steps - 1)
                for c in weights():
                    c.start()

            p, step = it // rows - 1, lax.rem(it, rows)

            @pl.when((step == 0) & (lax.rem(p, per) == per - 1))
            def _():
                close_group(p // per)

            @pl.when(it == n_steps)
            def _():
                comm.offer(end)

            t = pick(it, tick_after)

            @pl.when(t > 0)
            def _():
                comm.tick(t)

            @pl.when((step == 0) & (p + 3 < n_pairs))
            def _():
                give_out(p + 3)

        for c in lds[:-1]:
            c.wait()
        for i in range(2):
            push_rows(i).wait()
        arrived(0)
        score(0)
        soften(0)
        score(1)
        lds[-1].wait()
        cdiv_loop(n_steps, lambda i: walk(i + 1))
        for c in weights():
            c.wait()

        def into(b):
            r = pl.ds(aligned(b * toks, QB), toks)
            with jax.named_scope("b_into"):
                gnm[r, :] = dot(dqt[:, r], wq[:], TN) + dot(dkt[:, r], wk[:], TN) + dot(dv[r, :], wv[:])

            with jax.named_scope("b_final"):
                for i in range(tb):
                    r = pl.ds(aligned((b * tb + i) * QB, QB), QB)
                    out, dg = norm_back(xbuf[r, :], ga[:], gnm[r, :], gmid[r, :])
                    mbuf[r, :] = out
                    dgain[:8, :] += dg

        def share_gains():
            out_copy.start()
            gains = jnp.concatenate([col_sum(dgain[:8, :]), col_sum(dgain[8:, :]), jnp.zeros((6, width), F32)], axis=0)
            for p in range(n):
                gsend[p, :, :rpd] = gains[:, p * rpd:(p + 1) * rpd]

            def spread(i):
                to = lax.rem(me + i + 1, n)
                pltpu.make_async_remote_copy(src_ref=gsend.at[to], dst_ref=grecv.at[i], send_sem=gsem.at[0], recv_sem=gsem.at[1],
                                             device_id={"seq": to}, device_id_type=MESH).start()

            cdiv_loop(n - 1, spread)

        def finish(i):
            comm.advance(end + i, True)

            @pl.when(i == 1)
            def _():
                cdiv_loop(rows - 2, lambda b: into(b + 1))

            @pl.when(i == LAG + 1)
            def _():
                into(rows - 1)
                share_gains()

        into(0)
        cdiv_loop(4 * LAG - 1, finish)

    score_bufs = [f(3 * QB, 2 * QB) for f in (vf, vm) for _ in range(8)]
    out_copy = pltpu.make_async_copy(mbuf, dx_h, ld.at[0])
    pl.run_scoped(attention, vm(hd, total), vm(hd, rows * ext), vm(rows * ext, hd), vm(rows * ext, hd), vm(hd, rows * WINDOW), vm(total, hd), *score_bufs)
    most, rest = pl.ds(0, end), pl.ds(end, 2)
    keep_most = load(1, fin.at[most], fin_h.at[most])
    to_left(gsend.at[pl.ds(0, n - 1)], grecv, gsem.at[0], gsem.at[1]).wait()
    sums = gsend[me]
    for i in range(n - 1):
        sums = sums + grecv[i]
    fin[end + 1, 0, :8, :128] = sums
    out_copy.wait()
    comm.advance(end + 4 * LAG - 1, True)
    with jax.named_scope("b_end"):
        keep_rest = load(0, fin.at[rest], fin_h.at[rest])
        keep_most.wait()
        keep_rest.wait()


def spread_kernel(dims, dx_i, fin_i, dx_o, dga_o, dgm_o, *refs):
    head_dim, n, width, ff = dims
    outs, (buf, fin), stage, sem = refs[:7], refs[7:9], refs[9:16], refs[16]
    dq, dk, dv, do, dg, du, dd = stage
    nb, nc, sub = ff // CB, width // CB, ff // width
    rpd = width // n
    head, place, end = plan(nb, nc * sub // 2, nc)
    get_fin = pltpu.make_async_copy(fin_i, fin, sem.at[len(outs)])
    get_fin.start()
    cut = buf.shape[0] // nc
    gets, puts = ([pltpu.make_async_copy(s.at[pl.ds(i * cut, cut)], d.at[pl.ds(i * cut, cut)], sem.at[len(outs) + k + i]) for i in range(nc)]
                  for k, s, d in ((1, dx_i, buf), (nc + 1, buf, dx_o)))
    for c in gets:
        c.start()
    get_fin.wait()
    gains = fin[end + 1, 0]
    dga_o[:] = gains[:1, :rpd]
    dgm_o[:] = gains[1:2, :rpd]
    for j in range(nb):
        dg[:, j * CB:(j + 1) * CB] = fin[j, 0]
        du[:, j * CB:(j + 1) * CB] = fin[j, 1]
    for c in range(nc):
        for i in range(sub):
            pair = nb + (c * sub + i) // 2
            dd[i * rpd:(i + 1) * rpd, c * CB:(c + 1) * CB] = fin[pair, i % 2]
    for g in range(nc):
        do[:, g * CB:(g + 1) * CB] = fin[place["o", g]]
        for name, ref in (("q", dq), ("k", dk), ("v", dv)):
            val = fin[place[name, g]]
            for h in range(CB // head_dim):
                ref[g * (CB // head_dim) + h] = val[:, h * head_dim:(h + 1) * head_dim]
    keeps = [pltpu.make_async_copy(s, d, sem.at[i]) for i, (s, d) in enumerate(zip(stage, outs))]
    for c in keeps:
        c.start()
    for get, out in zip(gets, puts):
        get.wait()
        out.start()
    for c in keeps + puts:
        c.wait()


def run_bwd(n, head_dim, ga, gm, x, dout, q, kt, k, v, ha, ot, xm, hm, hmt, qr, lse, cos_t, sin_t, wq, wk, wv, wo, wg, wu, wd, rows):
    total, width = x.shape
    hd, ff = wq.shape[0], wg.shape[1]
    toks = total // rows
    rpd, heads = width // n, hd // head_dim
    nb, nc, sub = ff // CB, width // CB, ff // width
    slots = plan(nb, nc * sub // 2, nc)[2] + 2
    n_pairs = hd // (2 * head_dim)
    f = lambda *s: jax.ShapeDtypeStruct(s, F32)
    dx_t = jax.ShapeDtypeStruct((total, width), BF)
    vm = lambda *s: pltpu.VMEM(s, BF)
    vf = lambda *s: pltpu.VMEM(s, F32)
    dma = lambda *s: pltpu.SemaphoreType.DMA(s)
    line, duo = vf(rows * n_pairs, 8, 2 * QB), (2, SLOTS)
    scratch = [vf(RING, 2, n // 2, 2, rpd, CB), vf(SLOTS, 2, n // 2, rpd, CB), vf(*duo, 2, 2, rpd, CB), vf(*duo, 2, 4, rpd, CB),
               vf(*duo, 2, rpd, CB // 2), vf(*duo, 2, rpd, CB), vf(*duo, 3, rpd, CB), vf(*duo, 4, 4, rpd, CB), vf(*duo, 4, rpd, CB), vf(slots, 2, rpd, CB),
               dma(6, *duo), dma(6, *duo),
               vm(hd, rows * WINDOW), line, line, dma(2), dma(2), dma(n_pairs), dma(n_pairs),
               vf(n, 8, 128), vf(n - 1, 8, 128), dma(2), dma(15),
               vm(total, width), vm(total, width), vf(total, width), vm(total, width), vm(hd, total), vm(width, total), vm(hd, width), vm(hd, total), line, line, vf(*cos_t.shape), vf(*cos_t.shape), vf(*ga.shape), vf(*ga.shape), vf(16, width)]
    mid = pl.pallas_call(
        functools.partial(bwd_kernel, n, head_dim, (rows, toks, width, hd, ff)), out_shape=[dx_t, f(slots, 2, rpd, CB)],
        in_specs=any_spec(24), out_specs=any_spec(2), scratch_shapes=scratch,
        compiler_params=pltpu.CompilerParams(collective_id=1, has_side_effects=True, vmem_limit_bytes=VMEM_LIMIT),
        name="backward")(ga, gm, x, dout, q, kt, k, v, ha, ot, xm, hm, hmt, qr, lse, cos_t, sin_t, wq, wk, wv, wo, wg, wu, wd)
    outs = [f(heads, rpd, head_dim)] * 3 + [f(rpd, width), f(rpd, ff), f(rpd, ff), f(ff // n, width)]
    return pl.pallas_call(
        functools.partial(spread_kernel, (head_dim, n, width, ff)), out_shape=[dx_t, f(1, rpd), f(1, rpd)] + outs,
        in_specs=any_spec(2), out_specs=any_spec(1) + vmem_spec(2) + any_spec(7),
        scratch_shapes=[vm(total, width), vf(slots, 2, rpd, CB), *[vf(*o.shape) for o in outs], dma(8 + 2 * nc)],
        name="spread")(*mid)


def solution(mesh):
    n = mesh.shape["seq"]

    def device_step(hidden, positions, g_attn, g_mlp, w_query, w_key, w_value, w_out, w_gate, w_up, w_down, d_out):
        rows, toks, width = hidden.shape
        layers, _, heads, head_dim = w_query.shape
        hd = heads * head_dim
        half = head_dim // 2
        inv_freq = 1.0 / (np.float32(10000.0) ** (np.arange(half, dtype=np.float32) * np.float32(2.0 / head_dim)))
        turn = lambda w: w[0].transpose(1, 2, 0).reshape(hd, width)
        wq, wk, wv = turn(w_query), turn(w_key), turn(w_value)
        fwd = run_fwd(n, hidden, positions, jnp.asarray(inv_freq.astype(np.float32)[:, None]), g_attn, g_mlp, wq, wk, wv, w_out[0], head_dim)
        out = run_bwd(n, head_dim, g_attn, g_mlp, hidden.reshape(rows * toks, width), d_out.reshape(rows * toks, width), *fwd,
                      wq, wk, wv, w_out[0], w_gate[0], w_up[0], w_down[0], rows)
        dx, dga, dgm, dq, dk, dv, do, dg, du, dd = out
        back = lambda w: w.transpose(1, 0, 2)[None]
        return (dx.reshape(rows, toks, width), dga, dgm, back(dq), back(dk), back(dv), do[None], dg[None], du[None], dd[None])

    tok_spec, grad_spec = P("data", "seq"), P(None, ("data", "seq"))
    in_specs = (tok_spec, tok_spec) + (P(),) * 9 + (tok_spec,)
    out_specs = (tok_spec,) + (grad_spec,) * 9
    return jax.shard_map(device_step, mesh=mesh, in_specs=in_specs, out_specs=out_specs, check_vma=False)
```
